16 devices in a mesh: model: 2 (over z), data: 8 (over y, x, core).
Axes of the slice: x: 2, y: 2, z: 2, core: 2. Of those that a mesh axis runs over, the one named last changes fastest.
Arguments:
- x_in: bfloat16 [96, 512, 512], P('data')
- cot_out: bfloat16 [96, 512, 512], P('data')
- step_emb: bfloat16 [4, 512], replicated
- w_q: bfloat16 [512, 512], P(None, 'model')
- w_k: bfloat16 [512, 512], P(None, 'model')
- w_v: bfloat16 [512, 512], P(None, 'model')
- w_o: bfloat16 [512, 512], P('model')
- w_1: bfloat16 [512, 2048], P(None, 'model')
- w_2: bfloat16 [2048, 512], P('model')
Outputs:
- output 1: float32 [512, 512], P(None, 'model')
- output 2: float32 [512, 512], P(None, 'model')
- output 3: float32 [512, 512], P(None, 'model')
- output 4: float32 [512, 512], P('model')
- output 5: float32 [512, 2048], P(None, 'model')
- output 6: float32 [2048, 512], P('model')
- output 7: bfloat16 [96, 512, 512], P('data')
All inputs are finite; a program needn't handle non-finite values.
Results may differ from the reference program's by a relative error of at most 0.0174562.
Values are sent between devices in bfloat16 or wider.
A program may use at most 1 GiB of HBM per device.

```python
import jax
import jax.numpy as jnp
from jax import lax

BATCH = 96
SEQ = 512
D = 512
HEADS = 8
FF = 2048
LAYERS = 4


def normal_weight(key, rows, cols):
    return (jax.random.normal(key, (rows, cols), jnp.float32) * rows ** -0.5).astype(jnp.bfloat16)


def setup_inputs(seed: int = 0) -> dict:
    key_list = jax.random.split(jax.random.key(seed), 9)
    x_in = jax.random.normal(key_list[0], (BATCH, SEQ, D), jnp.float32).astype(jnp.bfloat16)
    cot_out = jax.random.normal(key_list[1], (BATCH, SEQ, D), jnp.float32).astype(jnp.bfloat16)
    step_emb = (0.5 * jax.random.normal(key_list[2], (LAYERS, D), jnp.float32)).astype(jnp.bfloat16)
    return dict(x_in=x_in, cot_out=cot_out, step_emb=step_emb,
                w_q=normal_weight(key_list[3], D, D), w_k=normal_weight(key_list[4], D, D),
                w_v=normal_weight(key_list[5], D, D), w_o=normal_weight(key_list[6], D, D),
                w_1=normal_weight(key_list[7], D, FF), w_2=normal_weight(key_list[8], FF, D))


def rms_norm(values):
    return values * lax.rsqrt(jnp.mean(values * values, axis=-1, keepdims=True) + 1e-6)


def attend_one(qkv_seq):
    q_seq, k_seq, v_seq = qkv_seq
    head_dim = q_seq.shape[-1]
    scores = jnp.einsum('qhe,khe->hqk', q_seq, k_seq) * (head_dim ** -0.5)
    prob_mat = jax.nn.softmax(scores, axis=-1).astype(jnp.bfloat16).astype(jnp.float32)
    return jnp.einsum('hqk,khe->qhe', prob_mat, v_seq).astype(jnp.bfloat16)


def shared_block(x_cur, step_vec, weights32):
    w_q, w_k, w_v, w_o, w_1, w_2 = weights32
    batch_size, seq_len, width_model = x_cur.shape
    head_shape = (batch_size, seq_len, HEADS, width_model // HEADS)
    x_f = x_cur.astype(jnp.float32) + step_vec.astype(jnp.float32)
    u_f = rms_norm(x_f).astype(jnp.bfloat16).astype(jnp.float32)
    q_all = jnp.einsum('bsd,de->bse', u_f, w_q).astype(jnp.bfloat16).astype(jnp.float32).reshape(head_shape)
    k_all = jnp.einsum('bsd,de->bse', u_f, w_k).astype(jnp.bfloat16).astype(jnp.float32).reshape(head_shape)
    v_all = jnp.einsum('bsd,de->bse', u_f, w_v).astype(jnp.bfloat16).astype(jnp.float32).reshape(head_shape)
    context = lax.map(jax.checkpoint(attend_one), (q_all, k_all, v_all))
    context_f = context.reshape(batch_size, seq_len, width_model).astype(jnp.float32)
    h_f = (x_f + jnp.einsum('bse,ed->bsd', context_f, w_o)).astype(jnp.bfloat16).astype(jnp.float32)
    m_f = rms_norm(h_f).astype(jnp.bfloat16).astype(jnp.float32)
    z_b = jnp.einsum('bsd,df->bsf', m_f, w_1).astype(jnp.bfloat16)
    g_f = jax.nn.gelu(z_b.astype(jnp.float32)).astype(jnp.bfloat16).astype(jnp.float32)
    return (h_f + jnp.einsum('bsf,fd->bsd', g_f, w_2)).astype(jnp.bfloat16)


def reference(x_in, cot_out, step_emb, w_q, w_k, w_v, w_o, w_1, w_2):
    weights32 = tuple(weight.astype(jnp.float32) for weight in (w_q, w_k, w_v, w_o, w_1, w_2))

    def forward(x_start, weight_set):
        def scan_body(x_cur, step_vec):
            return jax.checkpoint(shared_block)(x_cur, step_vec, weight_set), None
        x_last, _ = lax.scan(scan_body, x_start, step_emb)
        return x_last

    _, pull_back = jax.vjp(forward, x_in, weights32)
    d_x, d_w = pull_back(cot_out)
    return (d_w[0], d_w[1], d_w[2], d_w[3], d_w[4], d_w[5], d_x)
```

```python
import functools
import jax
import jax.numpy as jnp
from jax import lax
from jax.experimental import pallas as pl
from jax.experimental.pallas import tpu as pltpu
from jax.sharding import PartitionSpec as P

F32, BF16 = jnp.float32, jnp.bfloat16
T, D, FF, H, E, L = 512, 512, 2048, 8, 64, 4
EPS = 1e-6
LOG2E = 1.4426950408889634
SCALE = E ** -0.5
GK0 = 0.7978845608028654
GK1 = 0.044715


def dot_nn(a, b):
    return lax.dot_general(a, b, (((1,), (0,)), ((), ())), preferred_element_type=F32)


def dot_nt(a, b):
    return lax.dot_general(a, b, (((1,), (1,)), ((), ())), preferred_element_type=F32)


def lanes4(e):
    return jnp.concatenate([e] * (T // 128), axis=1)


def rms_scale(v):
    return lax.rsqrt(jnp.mean(v * v, axis=0, keepdims=True) + EPS)


def rms_pull(v, r, dy):
    a = jnp.mean(dy * v, axis=0, keepdims=True)
    return r * dy - v * (r * r * r * a)


def gelu_fwd(z):
    inner = GK0 * (z + GK1 * (z * z * z))
    return 0.5 * z * (1.0 + jnp.tanh(inner))


def gelu_both(z):
    z2 = z * z
    t = jnp.tanh(z * (GK0 + (GK0 * GK1) * z2))
    hp = 0.5 + 0.5 * t
    g = z * hp
    dg = hp + (0.5 * z) * (1.0 - t * t) * (GK0 + (3.0 * GK0 * GK1) * z2)
    return g, dg


def qrow(hd):
    return 768 * (hd // 4) + 64 * (hd % 4)


def pad_head(rows, hh):
    zero = jnp.zeros_like(rows)
    return jnp.concatenate([rows, zero] if hh == 0 else [zero, rows], axis=0)


def kernel(nseq, x_ref, cot_ref, emb_ref, wqkv_h, wo_h, w1_h, w2_h,
           dx_ref, gqkv_h, go_h, g1_h, g2_h,
           wqkv, wo, w1, w2, wqkvt, wot, w1t, w2t, gqkv, go, g1, g2,
           xs, qkv, ctx, hs, zs, lse, u, m, act, dz, dn, dmid, dctx, dqkv, sem):
    step = pl.program_id(0)
    halves = range(2)
    pairs_in = ([(wqkv_h.at[k], wqkv.at[:, pl.ds(768 * k, 768)]) for k in halves] + [(wo_h, wo)]
                + [(w1_h.at[k], w1.at[:, pl.ds(1024 * k, 1024)]) for k in halves] + [(w2_h, w2)])
    pairs_out = ([(gqkv.at[:, pl.ds(768 * k, 768)], gqkv_h.at[k]) for k in halves] + [(go, go_h)]
                 + [(g1.at[:, pl.ds(1024 * k, 1024)], g1_h.at[k]) for k in halves] + [(g2, g2_h)])

    @pl.when(step == 0)
    def _():
        cps = [pltpu.make_async_copy(s, d, sem.at[i]) for i, (s, d) in enumerate(pairs_in)]
        for c in cps:
            c.start()
        for c in cps:
            c.wait()
        for j in range(3):
            wqkvt[pl.ds(512 * j, 512), :] = wqkv[:, pl.ds(512 * j, 512)].T
        wot[...] = wo[...].T
        for j in range(4):
            w1t[pl.ds(512 * j, 512), :] = w1[:, pl.ds(512 * j, 512)].T
            w2t[:, pl.ds(512 * j, 512)] = w2[pl.ds(512 * j, 512), :].T
        gqkv[...] = jnp.zeros_like(gqkv)
        go[...] = jnp.zeros_like(go)
        g1[...] = jnp.zeros_like(g1)
        g2[...] = jnp.zeros_like(g2)

    xs[0] = x_ref[0].T

    def fwd(l, carry):
        s = xs[l].astype(F32) + lanes4(emb_ref[l])
        u[...] = (s * rms_scale(s)).astype(BF16)
        for j in range(3):
            qkv[l, pl.ds(512 * j, 512), :] = dot_nn(wqkvt[pl.ds(512 * j, 512), :], u[...]).astype(BF16)
        for p in range(4):
            kp = qkv[l, pl.ds(qrow(2 * p) + 256, 128), :].T
            for hh in range(2):
                hd = 2 * p + hh
                qp = pad_head(qkv[l, pl.ds(qrow(hd), 64), :], hh)
                vt = qkv[l, pl.ds(qrow(hd) + 512, 64), :]
                for c in range(2):
                    cs = slice(256 * c, 256 * c + 256)
                    st = dot_nn(kp, qp[:, cs])
                    mx = jnp.max(st, axis=0, keepdims=True)
                    e = jnp.exp2((st - mx) * (SCALE * LOG2E))
                    sm = jnp.sum(e, axis=0, keepdims=True)
                    pr = (e * (1.0 / sm)).astype(BF16)
                    lse[l, pl.ds(hd, 1), pl.ds(256 * c, 256)] = mx * (SCALE * LOG2E) + jnp.log2(sm)
                    ctx[l, pl.ds(64 * hd, 64), pl.ds(256 * c, 256)] = dot_nn(vt, pr).astype(BF16)
        s = xs[l].astype(F32) + lanes4(emb_ref[l])
        hb = (s + dot_nn(wot[...], ctx[l])).astype(BF16)
        hs[l] = hb
        hf = hb.astype(F32)
        m[...] = (hf * rms_scale(hf)).astype(BF16)
        for j in range(4):
            z = dot_nn(w1t[pl.ds(512 * j, 512), :], m[...]).astype(BF16)
            zs[l, pl.ds(512 * j, 512), :] = z

        @pl.when(l < L - 1)
        def _():
            for j in range(4):
                act[pl.ds(512 * j, 512), :] = gelu_fwd(zs[l, pl.ds(512 * j, 512), :].astype(F32)).astype(BF16)
            xs[l + 1] = (hs[l].astype(F32) + dot_nn(w2t[...], act[...])).astype(BF16)
        return carry

    lax.fori_loop(0, L, fwd, 0)

    dn[...] = cot_ref[0].T

    def bwd(i, carry):
        l = L - 1 - i
        hf = hs[l].astype(F32)
        r = rms_scale(hf)
        m[...] = (hf * r).astype(BF16)
        for j in range(4):
            js = pl.ds(512 * j, 512)
            dg = dot_nn(w2[js, :], dn[...]).astype(BF16).astype(F32)
            g, gp = gelu_both(zs[l, js, :].astype(F32))
            act[js, :] = g.astype(BF16)
            dz[js, :] = (dg * gp).astype(BF16)
            g2[js, :] += dot_nt(act[js, :], dn[...])
            g1[:, js] += dot_nt(m[...], dz[js, :])
        dm = dot_nn(w1[...], dz[...]).astype(BF16).astype(F32)
        hf = hs[l].astype(F32)
        dmid[...] = (dn[...].astype(F32) + rms_pull(hf, rms_scale(hf), dm)).astype(BF16)
        go[...] += dot_nt(ctx[l], dmid[...])
        dctx[...] = dot_nn(wo[...], dmid[...]).astype(BF16)
        for p in range(4):
            kp = qkv[l, pl.ds(qrow(2 * p) + 256, 128), :].T
            vp = qkv[l, pl.ds(qrow(2 * p) + 512, 128), :].T
            for hh in range(2):
                hd = 2 * p + hh
                hsl = pl.ds(64 * hd, 64)
                qt = qkv[l, pl.ds(qrow(hd), 64), :]
                kt = qkv[l, pl.ds(qrow(hd) + 256, 64), :]
                dc = dctx[hsl, :]
                qp = pad_head(qt, hh)
                dcp = pad_head(dc, hh)
                delta = jnp.sum(dc.astype(F32) * ctx[l, hsl, :].astype(F32), axis=0, keepdims=True)
                dv = jnp.zeros((E, T), F32)
                dk = jnp.zeros((E, T), F32)
                for c in range(2):
                    cs = slice(256 * c, 256 * c + 256)
                    st = dot_nn(kp, qp[:, cs])
                    pr = jnp.exp2(st * (SCALE * LOG2E) - lse[l, pl.ds(hd, 1), pl.ds(256 * c, 256)])
                    dp = dot_nn(vp, dcp[:, cs]).astype(BF16).astype(F32)
                    ds = (pr * (dp - delta[:, cs])).astype(BF16)
                    dqkv[pl.ds(qrow(hd), 64), pl.ds(256 * c, 256)] = (dot_nn(kt, ds) * SCALE).astype(BF16)
                    dv += dot_nt(dc[:, cs], pr.astype(BF16))
                    dk += dot_nt(qt[:, cs], ds)
                dqkv[pl.ds(qrow(hd) + 256, 64), :] = (dk * SCALE).astype(BF16)
                dqkv[pl.ds(qrow(hd) + 512, 64), :] = dv.astype(BF16)
        s = xs[l].astype(F32) + lanes4(emb_ref[l])
        u[...] = (s * rms_scale(s)).astype(BF16)
        for j in range(3):
            js = pl.ds(512 * j, 512)
            gqkv[:, js] += dot_nt(u[...], dqkv[js, :])
        du = dot_nn(wqkv[...], dqkv[...]).astype(BF16).astype(F32)
        s = xs[l].astype(F32) + lanes4(emb_ref[l])
        dn[...] = (dmid[...].astype(F32) + rms_pull(s, rms_scale(s), du)).astype(BF16)
        return carry

    lax.fori_loop(0, L, bwd, 0)
    dx_ref[0] = dn[...].T

    @pl.when(step == nseq - 1)
    def _():
        cps = [pltpu.make_async_copy(s, d, sem.at[i]) for i, (s, d) in enumerate(pairs_out)]
        for c in cps:
            c.start()
        for c in cps:
            c.wait()


def run_kernel(x, cot, emb, wqkv, wo, w1, w2):
    nseq = x.shape[0]
    embb = jnp.broadcast_to(emb.astype(F32)[:, :, None], (L, D, 128))
    blk = pl.BlockSpec((1, T, D), lambda i: (i, 0, 0))
    anyspec = pl.BlockSpec(memory_space=pl.ANY)
    V = pltpu.VMEM
    return pl.pallas_call(
        functools.partial(kernel, nseq),
        grid=(nseq,),
        in_specs=[blk, blk, pl.BlockSpec(memory_space=pltpu.VMEM)] + [anyspec] * 4,
        out_specs=[blk] + [anyspec] * 4,
        out_shape=[jax.ShapeDtypeStruct((nseq, T, D), BF16), jax.ShapeDtypeStruct((2, D, 768), F32),
                   jax.ShapeDtypeStruct((D, D), F32), jax.ShapeDtypeStruct((2, D, 1024), F32), jax.ShapeDtypeStruct((FF, D), F32)],
        scratch_shapes=[V((D, 1536), BF16), V((D, D), BF16), V((D, FF), BF16), V((FF, D), BF16),
                        V((1536, D), BF16), V((D, D), BF16), V((FF, D), BF16), V((D, FF), BF16),
                        V((D, 1536), F32), V((D, D), F32), V((D, FF), F32), V((FF, D), F32),
                        V((L, D, T), BF16), V((L, 1536, T), BF16), V((L, D, T), BF16), V((L, D, T), BF16),
                        V((L, FF, T), BF16), V((L, H, T), F32), V((D, T), BF16), V((D, T), BF16), V((FF, T), BF16),
                        V((FF, T), BF16), V((D, T), BF16), V((D, T), BF16), V((D, T), BF16), V((1536, T), BF16),
                        pltpu.SemaphoreType.DMA((6,))],
        compiler_params=pltpu.CompilerParams(dimension_semantics=("arbitrary",), vmem_limit_bytes=67_000_000),
    )(x, cot, embb, wqkv, wo, w1, w2)


def solution(mesh):
    spec_col, spec_row, spec_act, spec_rep = P(None, 'model'), P('model', None), P('data', None, None), P(None, None)
    both = ('model', 'data')

    def part(w, d, parts):
        rows = w.shape[0] // parts
        return lax.dynamic_slice_in_dim(w, d * rows, rows, 0)

    def device_step(x_in, cot_out, step_emb, w_q, w_k, w_v, w_o, w_1, w_2):
        mi, di = lax.axis_index('model'), lax.axis_index('data')
        nd = mesh.shape['data']
        half = x_in.shape[0] // 2
        x = lax.dynamic_slice_in_dim(x_in, mi * half, half, 0)
        cot = lax.dynamic_slice_in_dim(cot_out, mi * half, half, 0)
        w_qkv = jnp.concatenate([part(w, di, nd) for w in (w_q, w_k, w_v)], axis=1)
        gat = lambda w: lax.all_gather(w, both, axis=0, tiled=True)
        wqkv = gat(w_qkv).reshape(2, D, 768)
        wo = gat(part(w_o, di, nd))
        w1 = gat(part(w_1, di, nd)).reshape(2, D, 1024)
        w2 = gat(part(w_2, di, nd))
        dx, gqkv, go, g1, g2 = run_kernel(x, cot, step_emb, wqkv, wo, w1, w2)
        red = lambda g: lax.all_gather(lax.psum_scatter(g, both, scatter_dimension=0, tiled=True), 'data', axis=0, tiled=True)
        gqkv = red(gqkv.reshape(2 * D, 768))
        go = red(go)
        g1 = red(g1.reshape(2 * D, 1024))
        g2 = red(g2)
        dx = lax.all_gather(dx, 'model', axis=0, tiled=True)
        return gqkv[:, :256], gqkv[:, 256:512], gqkv[:, 512:], go, g1, g2, dx

    return jax.shard_map(device_step, mesh=mesh,
                         in_specs=(spec_act, spec_act, spec_rep, spec_col, spec_col, spec_col, spec_row, spec_col, spec_row),
                         out_specs=(spec_col, spec_col, spec_col, spec_row, spec_col, spec_row, spec_act),
                         check_vma=False)
```

```python
import functools

import jax
import jax.numpy as jnp
from jax import lax
from jax.experimental import pallas as pl
from jax.experimental.pallas import tpu as pltpu
from jax.sharding import PartitionSpec as P

F32, BF16 = jnp.float32, jnp.bfloat16
T, D, FF, H, E, L = 512, 512, 2048, 8, 64, 4
EPS = 1e-6
CEXP = E ** -0.5 * 1.4426950408889634
SCALE = E ** -0.5
GK0 = 0.7978845608028654
GK1 = 0.044715
R = 16
LN = 128


def dot_nn(a, b):
    return lax.dot_general(a, b, (((1,), (0,)), ((), ())), preferred_element_type=F32)


def dot_nt(a, b):
    return lax.dot_general(a, b, (((1,), (1,)), ((), ())), preferred_element_type=F32)


def rows(r, n=R):
    return pl.ds(r, n)


def wide(e):
    return jnp.concatenate([e] * (T // LN), axis=1)


def fold8(v):
    return v[:8] + v[8:]


def col_sum(tile_fn):
    accs = [None, None]
    for i, r in enumerate(range(0, D, R)):
        v = fold8(tile_fn(r))
        accs[i % 2] = v if accs[i % 2] is None else accs[i % 2] + v
    return jnp.sum(accs[0] + accs[1], axis=0, keepdims=True)


def rms_of(tile_fn):
    def sq(r):
        v = tile_fn(r)
        return v * v
    return lax.rsqrt(col_sum(sq) * (1.0 / D) + EPS)


def weave(*streams):
    total = max(len(s) for s in streams)
    done = [0] * len(streams)
    for t in range(total):
        for k, s in enumerate(streams):
            upto = -(-len(s) * (t + 1) // total)
            while done[k] < upto:
                s[done[k]]()
                done[k] += 1


def gelu_fwd(z):
    t = jnp.tanh(z * (GK0 + (GK0 * GK1) * (z * z)))
    return (0.5 * z) * (1.0 + t)


def gelu_both(z):
    z2 = z * z
    t = jnp.tanh(z * (GK0 + (GK0 * GK1) * z2))
    up = 1.0 + t
    hz = 0.5 * z
    w = z * (GK0 + (3.0 * GK0 * GK1) * z2)
    return hz * up, (0.5 * up) * (1.0 + w * (1.0 - t))


def qrow(hd):
    return 768 * (hd // 4) + 64 * (hd % 4)


def pad_head(block, hh):
    zero = jnp.zeros_like(block)
    return jnp.concatenate([block, zero] if hh == 0 else [zero, block], axis=0)


def max_cols(ref, cols):
    accs = [None] * 4
    for i, r in enumerate(range(0, T, 8)):
        v = ref[rows(r, 8), cols]
        accs[i % 4] = v if accs[i % 4] is None else jnp.maximum(accs[i % 4], v)
    m = jnp.maximum(jnp.maximum(accs[0], accs[1]), jnp.maximum(accs[2], accs[3]))
    return jnp.max(m, axis=0, keepdims=True)

GL, GROWS = 256, 6144

def kernel(nseq, x_ref, cot_ref, emb_ref, wqkv_h, wo_h, w1_h, w2_h,
           dx_ref, grad_h,
           wqkv, wo, w1, w2, wqkvt, wot, w1t, w2t, gqkv, go, g1, g2,
           xs, qkv, ctx, ctxl, hs, zs, lse, u, m, act, dz, dn, dmid, dctx, dqkv, tmp, sbuf, sem):
    step = pl.program_id(0)
    halves = range(2)
    pairs_in = ([(wqkv_h.at[k], wqkv.at[:, pl.ds(768 * k, 768)]) for k in halves] + [(wo_h, wo)]
                + [(w1_h.at[k], w1.at[:, pl.ds(1024 * k, 1024)]) for k in halves] + [(w2_h, w2)])
    @pl.when(step == 0)
    def _():
        cps = [pltpu.make_async_copy(s, d, sem.at[i]) for i, (s, d) in enumerate(pairs_in)]
        for c in cps:
            c.start()
        for c in cps:
            c.wait()
        for j in range(3):
            wqkvt[pl.ds(512 * j, 512), :] = wqkv[:, pl.ds(512 * j, 512)].T
        wot[...] = wo[...].T
        for j in range(4):
            w1t[pl.ds(512 * j, 512), :] = w1[:, pl.ds(512 * j, 512)].T
            w2t[:, pl.ds(512 * j, 512)] = w2[pl.ds(512 * j, 512), :].T
        gqkv[...] = jnp.zeros_like(gqkv)
        go[...] = jnp.zeros_like(go)
        g1[...] = jnp.zeros_like(g1)
        g2[...] = jnp.zeros_like(g2)

    xs[0] = x_ref[0].T
    half = [pl.ds(0, 256), pl.ds(256, 256)]

    def s_tile(l):
        return lambda r: xs[l, rows(r), :].astype(F32) + wide(emb_ref[l, rows(r), :].astype(F32))

    def norm_into(dst, tile_fn):
        box = {}

        def stat():
            box['r'] = rms_of(tile_fn)

        def put(r):
            dst[rows(r), :] = (tile_fn(r) * box['r']).astype(BF16)

        return [stat] + [functools.partial(put, r) for r in range(0, D, R)]

    def pull_into(dst, base, tile_fn, dy):
        box = {}

        def stat():
            box['r'] = rms_of(tile_fn)

        def stat2():
            a = col_sum(lambda r: dy[rows(r), :].astype(F32) * tile_fn(r)) * (1.0 / D)
            rr = box['r']
            box['a'] = rr * rr * rr * a

        def put(r):
            g = dy[rows(r), :].astype(F32)
            dst[rows(r), :] = (base[rows(r), :].astype(F32) + (box['r'] * g - tile_fn(r) * box['a'])).astype(BF16)

        return [stat, stat2] + [functools.partial(put, r) for r in range(0, D, R)]

    def run(stream):
        for f in stream:
            f()

    def h_tile(l):
        return lambda r: hs[l, rows(r), :].astype(F32)

    def fwd(l, carry):
        run(norm_into(u, s_tile(l)))
        for j in range(3):
            qkv[l, pl.ds(512 * j, 512), :] = dot_nn(wqkvt[pl.ds(512 * j, 512), :], u[...]).astype(BF16)

        kps = {}
        inv = {}

        def stage_a(hd):
            p, hh = divmod(hd, 2)

            def first():
                if hh == 0:
                    kps[p] = qkv[l, pl.ds(qrow(hd) + 256, 128), :].T

            def part(c):
                qp = pad_head(qkv[l, pl.ds(qrow(hd), 64), half[c]], hh)
                sbuf[hd % 2, :, half[c]] = dot_nn(kps[p], qp)

            return [first, lambda: part(0), lambda: part(1)]

        def stage_b(hd):
            sref, eref = sbuf.at[hd % 2], act.at[pl.ds(512 * (hd % 2), 512), :]

            def group(g):
                cols = half[g]
                mx = max_cols(sref, cols) * CEXP
                accs = [None, None]
                for i, r in enumerate(range(0, T, 8)):
                    e = jnp.exp2(sref[rows(r, 8), cols] * CEXP - mx)
                    accs[i % 2] = e if accs[i % 2] is None else accs[i % 2] + e
                    eref[rows(r, 8), cols] = e.astype(BF16)
                sm = jnp.sum(accs[0] + accs[1], axis=0, keepdims=True)
                lse[l, pl.ds(hd, 1), cols] = mx + jnp.log2(sm)
                inv[hd, g] = 1.0 / sm

            return [functools.partial(group, g) for g in range(2)]

        def stage_c(hd):
            def part(c):
                cn = dot_nn(qkv[l, pl.ds(qrow(hd) + 512, 64), :], act[pl.ds(512 * (hd % 2), 512), half[c]])
                cn = cn * inv[hd, c]
                hi = cn.astype(BF16)
                ctx[l, pl.ds(64 * hd, 64), half[c]] = hi
                ctxl[l, pl.ds(64 * hd, 64), half[c]] = (cn - hi.astype(F32)).astype(BF16)

            return [lambda: part(0), lambda: part(1)]

        run(stage_a(0))
        for hd in range(H + 1):
            mx = (stage_a(hd + 1) if hd + 1 < H else []) + (stage_c(hd - 1) if hd >= 1 else [])
            va = stage_b(hd) if hd < H else []
            weave(mx, va)

        st = s_tile(l)
        for c in range(2):
            o = dot_nn(wot[...], ctx[l, :, half[c]])
            for r in range(0, D, R):
                sx = xs[l, rows(r), half[c]].astype(F32) + jnp.concatenate([emb_ref[l, rows(r), :].astype(F32)] * 2, axis=1)
                hs[l, rows(r), half[c]] = (sx + o[r:r + R]).astype(BF16)
        run(norm_into(m, h_tile(l)))

        def z_dot(j):
            def f(c):
                js = pl.ds(512 * j, 512)
                zs[l, js, half[c]] = dot_nn(w1t[js, :], m[:, half[c]]).astype(BF16)
            return [lambda: f(0), lambda: f(1)]

        def gelu_stream(j):
            def f(r):
                act[rows(r), :] = gelu_fwd(zs[l, rows(r), :].astype(F32)).astype(BF16)
            return [functools.partial(f, r) for r in range(512 * j, 512 * j + 512, R)]

        @pl.when(l < L - 1)
        def _():
            run(z_dot(0))
            for j in range(4):
                weave(z_dot(j + 1) if j < 3 else [], gelu_stream(j))
            for c in range(2):
                o = dot_nn(w2t[...], act[:, half[c]])
                for r in range(0, D, R):
                    xs[l + 1, rows(r), half[c]] = (hs[l, rows(r), half[c]].astype(F32) + o[r:r + R]).astype(BF16)

        @pl.when(l == L - 1)
        def _():
            for j in range(4):
                run(z_dot(j))
        return carry

    lax.fori_loop(0, L, fwd, 0)

    dn[...] = cot_ref[0].T

    def bwd(i, carry):
        l = L - 1 - i

        def dg_dot(j):
            def f(c):
                js = pl.ds(512 * j, 512)
                dz[js, half[c]] = dot_nn(w2[js, :], dn[:, half[c]]).astype(BF16)
            return [lambda: f(0), lambda: f(1)]

        def gelu_stream(j):
            def f(r):
                g, gp = gelu_both(zs[l, rows(r), :].astype(F32))
                act[rows(r), :] = g.astype(BF16)
                dz[rows(r), :] = (dz[rows(r), :].astype(F32) * gp).astype(BF16)
            return [functools.partial(f, r) for r in range(512 * j, 512 * j + 512, R)]

        def wgrad(j):
            js = pl.ds(512 * j, 512)

            def a(c):
                g2[js, half[c]] += dot_nt(act[js, :], dn[half[c], :])

            def b(c):
                jc = pl.ds(512 * j + 256 * c, 256)
                g1[:, jc] += dot_nt(m[...], dz[jc, :])
            return [lambda: a(0), lambda: a(1), lambda: b(0), lambda: b(1)]

        weave(dg_dot(0), norm_into(m, h_tile(l)))
        weave(dg_dot(1) + dg_dot(2), gelu_stream(0))
        weave(wgrad(0) + dg_dot(3), gelu_stream(1))
        weave(wgrad(1), gelu_stream(2))
        weave(wgrad(2), gelu_stream(3))
        for c in range(2):
            tmp[:, half[c]] = dot_nn(w1[...], dz[:, half[c]]).astype(BF16)
        weave(wgrad(3), pull_into(dmid, dn, h_tile(l), tmp))
        for c in range(2):
            dctx[:, half[c]] = dot_nn(wo[...], dmid[:, half[c]]).astype(BF16)

        kps, vps, delta = {}, {}, {}

        def stage_a(hd):
            p, hh = divmod(hd, 2)
            hsl = pl.ds(64 * hd, 64)

            def first():
                if hh == 0:
                    kps[p] = qkv[l, pl.ds(qrow(hd) + 256, 128), :].T
                    vps[p] = qkv[l, pl.ds(qrow(hd) + 512, 128), :].T
                c = ctx[l, hsl, :].astype(F32) + ctxl[l, hsl, :].astype(F32)
                delta[hd] = jnp.sum(dctx[hsl, :].astype(F32) * c, axis=0, keepdims=True)

            def s_part(c):
                qp = pad_head(qkv[l, pl.ds(qrow(hd), 64), half[c]], hh)
                sbuf[hd % 2, :, half[c]] = dot_nn(kps[p], qp)

            def p_part(c):
                dcp = pad_head(dctx[hsl, half[c]], hh)
                dz[pl.ds(512 * (hd % 2), 512), half[c]] = dot_nn(vps[p], dcp).astype(BF16)

            return [first, lambda: s_part(0), lambda: s_part(1), lambda: p_part(0), lambda: p_part(1)]

        def stage_b(hd):
            sl = 512 * (hd % 2)

            def group(g, r0):
                cols = half[g]
                ls = lse[l, pl.ds(hd, 1), cols]
                de = delta[hd][:, 256 * g:256 * g + 256]
                for r in range(r0, r0 + 128, 8):
                    pr = jnp.exp2(sbuf[hd % 2, rows(r, 8), cols] * CEXP - ls)
                    act[rows(sl + r, 8), cols] = pr.astype(BF16)
                    dp = dz[rows(sl + r, 8), cols].astype(F32)
                    act[rows(1024 + sl + r, 8), cols] = (pr * (dp - de)).astype(BF16)

            return [functools.partial(group, g, r0) for g in range(2) for r0 in range(0, T, 128)]

        def stage_c(hd):
            sl = 512 * (hd % 2)
            pb = act.at[pl.ds(sl, 512), :]
            db = act.at[pl.ds(1024 + sl, 512), :]
            hsl = pl.ds(64 * hd, 64)

            def f_v():
                dqkv[pl.ds(qrow(hd) + 512, 64), :] = dot_nt(dctx[hsl, :], pb[...]).astype(BF16)

            def f_k():
                dqkv[pl.ds(qrow(hd) + 256, 64), :] = (dot_nt(qkv[l, pl.ds(qrow(hd), 64), :], db[...]) * SCALE).astype(BF16)

            def f_q():
                dqkv[pl.ds(qrow(hd), 64), :] = (dot_nn(qkv[l, pl.ds(qrow(hd) + 256, 64), :], db[...]) * SCALE).astype(BF16)

            return [f_v, f_k, f_q]

        def wo_grad():
            go[...] += dot_nt(ctx[l], dmid[...])

        run(stage_a(0))
        for hd in range(H + 1):
            mx = (stage_a(hd + 1) if hd + 1 < H else []) + (stage_c(hd - 1) if hd >= 1 else [wo_grad])
            va = stage_b(hd) if hd < H else []
            weave(mx, va)

        for c in range(2):
            tmp[:, half[c]] = dot_nn(wqkv[...], dqkv[:, half[c]]).astype(BF16)

        def qkv_grad(j):
            js = pl.ds(256 * j, 256)
            gqkv[:, js] += dot_nt(u[...], dqkv[js, :])

        run(norm_into(u, s_tile(l)))
        weave([functools.partial(qkv_grad, j) for j in range(6)], pull_into(dn, dmid, s_tile(l), tmp))
        return carry

    lax.fori_loop(0, L, bwd, 0)
    dx_ref[0] = dn[...].T

    @pl.when(step == nseq - 1)
    def _():
        cps = []
        for m_ in range(2):
            g = grad_h.at[m_]
            for k in range(3):
                cps.append((gqkv.at[:, pl.ds(768 * m_ + 256 * k, 256)], g.at[pl.ds(512 * k, 512), :]))
            for k in range(4):
                cps.append((g1.at[:, pl.ds(1024 * m_ + 256 * k, 256)], g.at[pl.ds(1536 + 512 * k, 512), :]))
            for k in range(2):
                cps.append((g2.at[pl.ds(1024 * m_, 1024), pl.ds(256 * k, 256)], g.at[pl.ds(3584 + 1024 * k, 1024), :]))
            for k in range(2):
                cps.append((go.at[pl.ds(256 * m_, 256), pl.ds(256 * k, 256)], g.at[pl.ds(5632 + 256 * k, 256), :]))
        cps = [pltpu.make_async_copy(s, d, sem.at[i]) for i, (s, d) in enumerate(cps)]
        for c in cps:
            c.start()
        for c in cps:
            c.wait()


def run_kernel(x, cot, emb, wqkv, wo, w1, w2):
    nseq = x.shape[0] // 2
    embb = jnp.broadcast_to(emb[:, :, None], (L, D, LN))
    blk = pl.BlockSpec((1, T, D), lambda i: (lax.axis_index('model') * nseq + i, 0, 0))
    anyspec = pl.BlockSpec(memory_space=pl.ANY)
    V = pltpu.VMEM
    return pl.pallas_call(
        functools.partial(kernel, nseq),
        grid=(nseq,),
        in_specs=[blk, blk, pl.BlockSpec(memory_space=pltpu.VMEM)] + [anyspec] * 4,
        out_specs=[blk, anyspec],
        out_shape=[jax.ShapeDtypeStruct((2 * nseq, T, D), BF16), jax.ShapeDtypeStruct((2, GROWS, GL), F32)],
        scratch_shapes=[V((D, 1536), BF16), V((D, D), BF16), V((D, FF), BF16), V((FF, D), BF16),
                        V((1536, D), BF16), V((D, D), BF16), V((FF, D), BF16), V((D, FF), BF16),
                        V((D, 1536), F32), V((D, D), F32), V((D, FF), F32), V((FF, D), F32),
                        V((L, D, T), BF16), V((L, 1536, T), BF16), V((L, D, T), BF16), V((L, D, T), BF16), V((L, D, T), BF16),
                        V((L, FF, T), BF16), V((L, H, T), F32), V((D, T), BF16), V((D, T), BF16), V((FF, T), BF16),
                        V((FF, T), BF16), V((D, T), BF16), V((D, T), BF16), V((D, T), BF16), V((1536, T), BF16), V((D, T), BF16),
                        V((2, T, T), F32), pltpu.SemaphoreType.DMA((22,))],
        compiler_params=pltpu.CompilerParams(dimension_semantics=("arbitrary",), vmem_limit_bytes=67_000_000),
    )(x, cot, embb, wqkv, wo, w1, w2)


MESH_ID = pl.DeviceIdType.MESH
NCOL = 2
BR, GL = 384, 256
GROWS = NCOL * 8 * BR
ORDERS = ('xyz', 'yxz')
NW = 6


def neighbours():
    mi = lax.axis_index('model')
    di = lax.axis_index('data')
    core, x, y = di % 2, (di // 2) % 2, di // 4
    dev = {'x': {'model': mi, 'data': di + 2 - 4 * x}, 'y': {'model': mi, 'data': di + 4 - 8 * y},
           'z': {'model': 1 - mi, 'data': di}, 'c': {'model': mi, 'data': di + 1 - 2 * core}}
    return {'x': x, 'y': y, 'z': mi}, core, dev


def greet(dev, names):
    barrier = pltpu.get_barrier_semaphore()
    for d in names:
        pl.semaphore_signal(barrier, inc=1, device_id=dev[d], device_id_type=MESH_ID)
    pl.semaphore_wait(barrier, len(names))


def gather_kernel(*refs):
    w_in, (wqkv, wo, w1, w2), (stage, lsem, ssem, zsend, zrecv, csend, crecv) = refs[:NW], refs[NW:NW + 4], refs[NW + 4:]
    me, core, dev = neighbours()
    mi = me['z']
    greet(dev, 'zc')

    def place(k, m, r0, n):
        if k < 3:
            return wqkv.at[m, pl.ds(r0, n), pl.ds(256 * k, 256)]
        if k == 3:
            return wo.at[pl.ds(256 * m + r0, n), :]
        if k == 4:
            return w1.at[m, pl.ds(r0, n), :]
        return w2.at[pl.ds(1024 * m + r0, n), :]

    n_rows = (512, 512, 512, 256, 512, 1024)
    zc, cc, loc, put = [], [], [], []
    for k in range(NW):
        n = n_rows[k] // 2
        zc.append(pltpu.make_async_remote_copy(w_in[k].at[pl.ds(n * core, n), :], place(k, mi, n * core, n), zsend.at[k], zrecv.at[k],
                                               device_id=dev['z'], device_id_type=MESH_ID))
        zc[k].start()
    for k in range(NW):
        loc.append(pltpu.make_async_copy(w_in[k], stage.at[k, pl.ds(0, n_rows[k]), pl.ds(0, w_in[k].shape[1])], lsem.at[k]))
        loc[k].start()
    for k in range(NW):
        loc[k].wait()
        put.append(pltpu.make_async_copy(stage.at[k, pl.ds(0, n_rows[k]), pl.ds(0, w_in[k].shape[1])], place(k, mi, 0, n_rows[k]), ssem.at[k]))
        put[k].start()
    for k in range(NW):
        n = n_rows[k] // 2
        zc[k].wait_recv()
        got = place(k, 1 - mi, n * core, n)
        cc.append(pltpu.make_async_remote_copy(got, got, csend.at[k], crecv.at[k], device_id=dev['c'], device_id_type=MESH_ID))
        cc[k].start()
    for k in range(NW):
        put[k].wait()
        zc[k].wait_send()
        cc[k].wait()


def run_gather(ws):
    anyspec = pl.BlockSpec(memory_space=pl.ANY)
    S = pltpu.SemaphoreType.DMA
    return pl.pallas_call(
        gather_kernel,
        in_specs=[anyspec] * NW,
        out_specs=[anyspec] * 4,
        out_shape=[jax.ShapeDtypeStruct((2, D, 768), BF16), jax.ShapeDtypeStruct((D, D), BF16),
                   jax.ShapeDtypeStruct((2, D, 1024), BF16), jax.ShapeDtypeStruct((FF, D), BF16)],
        scratch_shapes=[pltpu.VMEM((NW, 1024, 1024), BF16)] + [S((NW,))] * 6,
        compiler_params=pltpu.CompilerParams(vmem_limit_bytes=60_000_000, collective_id=0, has_side_effects=True),
    )(*ws)


def reduce_kernel(g_h, dx_in, out, dx, acc, rd, r1, r2, r3, locsem, ds, dr, ps, pr, gs, gr, cs, cr, xs_, xr_):
    me, core, dev = neighbours()
    x, y, mi = me['x'], me['y'], me['z']
    nseq = dx.shape[0] // 2

    def rdma(src, dst, s, r, d):
        return pltpu.make_async_remote_copy(src, dst, s, r, device_id=dev[d], device_id_type=MESH_ID)

    greet(dev, 'xyzc')

    xc = []
    for s in range(nseq):
        here = dx.at[mi * nseq + s]
        xc.append(rdma(here, here, xs_.at[s], xr_.at[s], 'z'))

    def blk(color, pos):
        return (pos['z'] * NCOL + color) * 4 + pos['y'] * 2 + pos['x']

    def all_pos(fixed):
        out_ = [dict(fixed)]
        for ax in 'zyx':
            if ax not in fixed:
                out_ = [dict(p, **{ax: v}) for p in out_ for v in (0, 1)]
        return out_

    def add(dst, src):
        def body(i, c):
            r = pl.multiple_of(i * 32, 32)
            acc[dst, pl.ds(r, 32), :] += src[pl.ds(r, 32), :]
            return c
        lax.fori_loop(0, BR // 32, body, 0)

    first, rest = [], []
    for color in range(NCOL):
        a = ORDERS[color][0]
        first += [blk(color, p) for p in all_pos({a: 1 - me[a]})]
        rest += [blk(color, p) for p in all_pos({a: me[a]})]
    seq = first + rest
    nb = len(seq)
    dcp, lcp = [], []
    for i, b in enumerate(seq):
        dcp.append(rdma(g_h.at[b * 2 + (1 - core)], rd.at[b], ds.at[i], dr.at[i], 'c'))
        lcp.append(pltpu.make_async_copy(g_h.at[b * 2 + core], acc.at[b], locsem.at[i]))
    for i in range(nb):
        dcp[i].start()
        lcp[i].start()
    for s in range(4):
        xc[s].start()

    def fold_core(i):
        dcp[i].wait_recv()
        lcp[i].wait()
        add(seq[i], rd.at[seq[i]])

    p1, p2, p3 = [], [], []
    for j in range(4):
        for color in range(NCOL):
            a = ORDERS[color][0]
            i = 4 * color + j
            fold_core(i)
            cp = rdma(acc.at[blk(color, all_pos({a: 1 - me[a]})[j])], r1.at[i], ps.at[i], pr.at[i], a)
            cp.start()
            p1.append(cp)
    p1 = [p1[(i % 4) * NCOL + i // 4] for i in range(4 * NCOL)]
    for i in range(4 * NCOL, nb):
        fold_core(i)
    for color in range(NCOL):
        a, b = ORDERS[color][0], ORDERS[color][1]
        for j, p in enumerate(all_pos({a: me[a]})):
            p1[4 * color + j].wait_recv()
            add(blk(color, p), r1.at[4 * color + j])
        for j, p in enumerate(all_pos({a: me[a], b: 1 - me[b]})):
            i = 2 * color + j
            cp = rdma(acc.at[blk(color, p)], r2.at[i], ps.at[4 * NCOL + i], pr.at[4 * NCOL + i], b)
            cp.start()
            p2.append(cp)
    for color in range(NCOL):
        a, b, c = ORDERS[color]
        for j, p in enumerate(all_pos({a: me[a], b: me[b]})):
            p2[2 * color + j].wait_recv()
            add(blk(color, p), r2.at[2 * color + j])
        cp = rdma(acc.at[blk(color, dict(me, **{c: 1 - me[c]}))], r3.at[color], ps.at[6 * NCOL + color], pr.at[6 * NCOL + color], c)
        cp.start()
        p3.append(cp)
    for s in range(4, nseq):
        xc[s].start()

    cps, g1_, g2_ = [], [], []

    def out_at(color, yy, xx):
        return out.at[(color * 4 + yy * 2 + xx) * 2 + core]

    def to_sibling(color, yy, xx, i):
        o = out_at(color, yy, xx)
        cp = rdma(o, o, cs.at[i], cr.at[i], 'c')
        cp.start()
        cps.append(cp)

    for color in range(NCOL):
        p3[color].wait_recv()
        b = blk(color, me)
        o_blk = (color * 4 + y * 2 + x) * 2 + core

        def body(i, c, b=b, o_blk=o_blk, color=color):
            r = pl.multiple_of(i * 32, 32)
            out[o_blk, pl.ds(r, 32), :] = acc[b, pl.ds(r, 32), :] + r3[color, pl.ds(r, 32), :]
            return c
        lax.fori_loop(0, BR // 32, body, 0)
        o = out_at(color, y, x)
        cp = rdma(o, o, gs.at[color], gr.at[color], ORDERS[color][0])
        cp.start()
        g1_.append(cp)
        c2 = rdma(o, o, gs.at[NCOL + 2 * color], gr.at[NCOL + 2 * color], ORDERS[color][1])
        c2.start()
        g2_.append(c2)
        to_sibling(color, y, x, color)
    for color in range(NCOL):
        g1_[color].wait_recv()
        a, b = ORDERS[color][0], ORDERS[color][1]
        yy, xx = (y, 1 - x) if a == 'x' else (1 - y, x)
        o = out_at(color, yy, xx)
        c2 = rdma(o, o, gs.at[NCOL + 2 * color + 1], gr.at[NCOL + 2 * color + 1], b)
        c2.start()
        g2_.append(c2)
        to_sibling(color, yy, xx, NCOL + color)
    for k in range(2 * NCOL):
        color = k % NCOL
        b = ORDERS[color][1]
        g2_[k].wait_recv()
        if k < NCOL:
            ty, tx = (y, 1 - x) if b == 'x' else (1 - y, x)
        else:
            ty, tx = 1 - y, 1 - x
        to_sibling(color, ty, tx, 2 * NCOL + k)
    for cp in cps:
        cp.wait()
    for cp in dcp + p1 + p2 + p3 + g1_ + g2_:
        cp.wait_send()
    for s in range(nseq):
        xc[s].wait_send()
        there = dx.at[(1 - mi) * nseq + s]
        rdma(there, there, xs_.at[s], xr_.at[s], 'z').wait_recv()


def run_reduce(grad, dx):
    g = grad.reshape(2 * NCOL * 8, BR, GL)
    nb = NCOL * 8
    V = pltpu.VMEM
    S = pltpu.SemaphoreType.DMA
    anyspec = pl.BlockSpec(memory_space=pl.ANY)
    return pl.pallas_call(
        reduce_kernel,
        in_specs=[anyspec, anyspec],
        out_specs=[pl.BlockSpec(memory_space=pltpu.VMEM), anyspec],
        out_shape=[jax.ShapeDtypeStruct((nb, BR, GL), F32), jax.ShapeDtypeStruct(dx.shape, dx.dtype)],
        scratch_shapes=[V((nb, BR, GL), F32), V((nb, BR, GL), F32), V((4 * NCOL, BR, GL), F32), V((2 * NCOL, BR, GL), F32), V((NCOL, BR, GL), F32),
                        S((nb,)), S((nb,)), S((nb,)), S((7 * NCOL,)), S((7 * NCOL,)), S((3 * NCOL,)), S((3 * NCOL,)), S((4 * NCOL,)), S((4 * NCOL,)),
                        S((6,)), S((6,))],
        input_output_aliases={1: 1},
        compiler_params=pltpu.CompilerParams(vmem_limit_bytes=60_000_000, collective_id=1, has_side_effects=True),
    )(g, dx)


def solution(mesh):
    spec_col, spec_row, spec_act, spec_rep = P(None, 'model'), P('model', None), P('data', None, None), P(None, None)

    def device_step(x_in, cot_out, step_emb, w_q, w_k, w_v, w_o, w_1, w_2):
        wqkv, wo, w1, w2 = run_gather((w_q, w_k, w_v, w_o, w_1, w_2))
        dx, grad = run_kernel(x_in, cot_out, step_emb, wqkv, wo, w1, w2)
        g, dx = run_reduce(grad, dx)
        g = g.reshape(GROWS, GL)

        def join(r0, n, k):
            return jnp.concatenate([g[r0 + n * i:r0 + n * (i + 1)] for i in range(k)], axis=1)

        return g[:512], g[512:1024], g[1024:1536], join(5632, 256, 2), join(1536, 512, 4), join(3584, 1024, 2), dx

    return jax.shard_map(device_step, mesh=mesh,
                         in_specs=(spec_act, spec_act, spec_rep, spec_col, spec_col, spec_col, spec_row, spec_col, spec_row),
                         out_specs=(spec_col, spec_col, spec_col, spec_row, spec_col, spec_row, spec_act),
                         check_vma=False)
```

```python
import functools

import jax
import jax.numpy as jnp
from jax import lax
from jax.experimental import pallas as pl
from jax.experimental.pallas import tpu as pltpu
from jax.sharding import PartitionSpec as P

F32, BF16 = jnp.float32, jnp.bfloat16
T, D, FF, H, E, L = 512, 512, 2048, 8, 64, 4
EPS = 1e-6
CEXP = E ** -0.5 * 1.4426950408889634
SCALE = E ** -0.5
GK0 = 0.7978845608028654
GK1 = 0.044715
R = 8
LN = 128


def dot_nn(a, b):
    return lax.dot_general(a, b, (((1,), (0,)), ((), ())), preferred_element_type=F32)


def dot_nt(a, b):
    return lax.dot_general(a, b, (((1,), (1,)), ((), ())), preferred_element_type=F32)


def rows(r, n=R):
    return pl.ds(r, n)


def wide(e):
    return jnp.concatenate([e] * (T // LN), axis=1)


def col_sum(tile_fn):
    accs = [None, None]
    for i, r in enumerate(range(0, D, R)):
        v = tile_fn(r)
        accs[i % 2] = v if accs[i % 2] is None else accs[i % 2] + v
    return jnp.sum(accs[0] + accs[1], axis=0, keepdims=True)


def rms_of(tile_fn):
    def sq(r):
        v = tile_fn(r)
        return v * v
    return lax.rsqrt(col_sum(sq) * (1.0 / D) + EPS)


def weave(*streams):
    total = max(len(s) for s in streams)
    done = [0] * len(streams)
    for t in range(total):
        for k, s in enumerate(streams):
            upto = -(-len(s) * (t + 1) // total)
            while done[k] < upto:
                s[done[k]]()
                done[k] += 1


def gelu_fwd(z):
    return z * jax.nn.sigmoid(z * (2 * GK0 + (2 * GK0 * GK1) * (z * z)))


def gelu_both(z):
    z2 = z * z
    s = jax.nn.sigmoid(z * (2 * GK0 + (2 * GK0 * GK1) * z2))
    w = z * (2 * GK0 + (6 * GK0 * GK1) * z2)
    return z * s, s * (1.0 + w * (1.0 - s))


def qrow(hd):
    return 768 * (hd // 4) + 64 * (hd % 4)


def pad_head(block, hh):
    zero = jnp.zeros_like(block)
    return jnp.concatenate([block, zero] if hh == 0 else [zero, block], axis=0)


def zip_pad(a, b):
    return [(a[i:i + 1], b[i:i + 1]) for i in range(max(len(a), len(b)))]


def max_cols(ref, cols):
    accs = [None] * 4
    for i, r in enumerate(range(0, T, 8)):
        v = ref[rows(r, 8), cols]
        accs[i % 4] = v if accs[i % 4] is None else jnp.maximum(accs[i % 4], v)
    m = jnp.maximum(jnp.maximum(accs[0], accs[1]), jnp.maximum(accs[2], accs[3]))
    return jnp.max(m, axis=0, keepdims=True)

GL, GROWS = 256, 6144

def kernel(nseq, x_ref, cot_ref, emb_ref, wqkv_h, wo_h, w1_h, w2_h,
           dx_ref, grad_h,
           wqkv, wo, w1, w2, wqkvt, wot, w1t, w2t, gqkv, go, g1, g2,
           xs, qkv, ctx, ctxl, hs, zs, lse, rsc, u, m, act, dz, dn, dmid, dctx, dqkv, tmp, sbuf, lcol, dcol, sem):
    step = pl.program_id(0)
    halves = range(2)
    pairs_in = ([(wqkv_h.at[k], wqkv.at[:, pl.ds(768 * k, 768)]) for k in halves] + [(wo_h, wo)]
                + [(w1_h.at[k], w1.at[:, pl.ds(1024 * k, 1024)]) for k in halves] + [(w2_h, w2)])
    @pl.when(step == 0)
    def _():
        cps = [pltpu.make_async_copy(s, d, sem.at[i]) for i, (s, d) in enumerate(pairs_in)]
        for c in cps:
            c.start()
        for c in cps:
            c.wait()
        for j in range(3):
            wqkvt[pl.ds(512 * j, 512), :] = wqkv[:, pl.ds(512 * j, 512)].T
        wot[...] = wo[...].T
        for j in range(4):
            w1t[pl.ds(512 * j, 512), :] = w1[:, pl.ds(512 * j, 512)].T
            w2t[:, pl.ds(512 * j, 512)] = w2[pl.ds(512 * j, 512), :].T
        gqkv[...] = jnp.zeros_like(gqkv)
        go[...] = jnp.zeros_like(go)
        g1[...] = jnp.zeros_like(g1)
        g2[...] = jnp.zeros_like(g2)

    xs[0] = x_ref[0].T
    half = [pl.ds(0, 256), pl.ds(256, 256)]

    def s_tile(l):
        return lambda r: xs[l, rows(r), :].astype(F32) + wide(emb_ref[l, rows(r), :])

    def norm_into(dst, tile_fn, l, k, fresh):
        box = {}

        def stat():
            if fresh:
                box['r'] = rms_of(tile_fn)
                rsc[l, pl.ds(k, 1), :] = box['r']
            else:
                box['r'] = rsc[l, pl.ds(k, 1), :]

        def put(r):
            dst[rows(r), :] = (tile_fn(r) * box['r']).astype(BF16)

        return [stat] + [functools.partial(put, r) for r in range(0, D, R)]

    def pull_into(dst, base, tile_fn, dy, l, k):
        box = {}

        def stat():
            a = col_sum(lambda r: dy[rows(r), :].astype(F32) * tile_fn(r)) * (1.0 / D)
            rr = rsc[l, pl.ds(k, 1), :]
            box['r'] = rr
            box['a'] = rr * rr * rr * a

        def put(r):
            g = dy[rows(r), :].astype(F32)
            dst[rows(r), :] = (base[rows(r), :].astype(F32) + (box['r'] * g - tile_fn(r) * box['a'])).astype(BF16)

        return [stat] + [functools.partial(put, r) for r in range(0, D, R)]

    def run(stream):
        for f in stream:
            f()

    def h_tile(l):
        return lambda r: hs[l, rows(r), :].astype(F32)

    def fwd(l, carry):
        run(norm_into(u, s_tile(l), l, 0, True))
        for j in range(3):
            qkv[l, pl.ds(512 * j, 512), :] = dot_nn(wqkvt[pl.ds(512 * j, 512), :], u[...]).astype(BF16)

        kps = {}
        inv = {}

        def stage_a(hd):
            p, hh = divmod(hd, 2)

            def first():
                if hh == 0:
                    kps[p] = qkv[l, pl.ds(qrow(hd) + 256, 128), :].T

            def part(c):
                qp = pad_head(qkv[l, pl.ds(qrow(hd), 64), half[c]], hh)
                sbuf[hd % 2, :, half[c]] = dot_nn(kps[p], qp)

            return [first, lambda: part(0), lambda: part(1)]

        def stage_b(hd):
            sref, eref = sbuf.at[hd % 2], act.at[pl.ds(512 * (hd % 2), 512), :]

            def group(g):
                cols = half[g]
                mx = max_cols(sref, cols) * CEXP
                accs = [None, None]
                for i, r in enumerate(range(0, T, 8)):
                    e = jnp.exp2(sref[rows(r, 8), cols] * CEXP - mx)
                    accs[i % 2] = e if accs[i % 2] is None else accs[i % 2] + e
                    eref[rows(r, 8), cols] = e.astype(BF16)
                sm = jnp.sum(accs[0] + accs[1], axis=0, keepdims=True)
                lse[l, pl.ds(hd, 1), cols] = mx + jnp.log2(sm)
                inv[hd, g] = 1.0 / sm

            return [functools.partial(group, g) for g in range(2)]

        def stage_c(hd):
            def part(c):
                cn = dot_nn(qkv[l, pl.ds(qrow(hd) + 512, 64), :], act[pl.ds(512 * (hd % 2), 512), half[c]])
                cn = cn * inv[hd, c]
                hi = cn.astype(BF16)
                ctx[l, pl.ds(64 * hd, 64), half[c]] = hi
                ctxl[l, pl.ds(64 * hd, 64), half[c]] = (cn - hi.astype(F32)).astype(BF16)

            return [lambda: part(0), lambda: part(1)]

        run(stage_a(0))
        for hd in range(H + 1):
            mx = []
            for x_, y_ in zip_pad(stage_a(hd + 1) if hd + 1 < H else [], stage_c(hd - 1) if hd >= 1 else []):
                mx += x_ + y_
            va = stage_b(hd) if hd < H else []
            weave(mx, va)

        for c in range(2):
            o = dot_nn(wot[...], ctx[l, :, half[c]])
            for r in range(0, D, R):
                sx = xs[l, rows(r), half[c]].astype(F32) + jnp.concatenate([emb_ref[l, rows(r), :]] * 2, axis=1)
                hs[l, rows(r), half[c]] = (sx + o[r:r + R]).astype(BF16)
        run(norm_into(m, h_tile(l), l, 1, True))

        def z_dot(j):
            def f(c):
                js = pl.ds(512 * j, 512)
                zs[l, js, half[c]] = dot_nn(w1t[js, :], m[:, half[c]]).astype(BF16)
            return [lambda: f(0), lambda: f(1)]

        def gelu_stream(j):
            def f(r, c):
                act[rows(r), half[c]] = gelu_fwd(zs[l, rows(r), half[c]].astype(F32)).astype(BF16)
            return [functools.partial(f, r, c) for r in range(512 * j, 512 * j + 512, R) for c in range(2)]

        @pl.when(l < L - 1)
        def _():
            run(z_dot(0))
            for j in range(4):
                weave(z_dot(j + 1) if j < 3 else [], gelu_stream(j))
            for c in range(2):
                o = dot_nn(w2t[...], act[:, half[c]])
                for r in range(0, D, R):
                    xs[l + 1, rows(r), half[c]] = (hs[l, rows(r), half[c]].astype(F32) + o[r:r + R]).astype(BF16)

        @pl.when(l == L - 1)
        def _():
            for j in range(4):
                run(z_dot(j))
        return carry

    lax.fori_loop(0, L, fwd, 0)

    dn[...] = cot_ref[0].T

    def bwd(i, carry):
        l = L - 1 - i

        def dg_dot(j):
            def f(c):
                js = pl.ds(512 * j, 512)
                dz[js, half[c]] = dot_nn(w2[js, :], dn[:, half[c]]).astype(BF16)
            return [lambda: f(0), lambda: f(1)]

        def gelu_stream(j):
            def f(r, c):
                g, gp = gelu_both(zs[l, rows(r), half[c]].astype(F32))
                act[rows(r), half[c]] = g.astype(BF16)
                dz[rows(r), half[c]] = (dz[rows(r), half[c]].astype(F32) * gp).astype(BF16)
            return [functools.partial(f, r, c) for r in range(512 * j, 512 * j + 512, R) for c in range(2)]

        def wgrad(j):
            js = pl.ds(512 * j, 512)

            def a(c):
                g2[js, half[c]] += dot_nt(act[js, :], dn[half[c], :])

            def b(c):
                jc = pl.ds(512 * j + 256 * c, 256)
                g1[:, jc] += dot_nt(m[...], dz[jc, :])
            return [lambda: a(0), lambda: a(1), lambda: b(0), lambda: b(1)]

        weave(dg_dot(0), norm_into(m, h_tile(l), l, 1, False))
        def dm_part(k0, k1, last):
            def f(c):
                p = dot_nn(w1[:, 512 * k0:512 * k1], dz[pl.ds(512 * k0, 512 * (k1 - k0)), half[c]])
                if k0 > 0:
                    p = sbuf[0, :, half[c]] + p
                if last:
                    tmp[:, half[c]] = p.astype(BF16)
                else:
                    sbuf[0, :, half[c]] = p
            return [lambda: f(0), lambda: f(1)]

        weave(dg_dot(1) + dg_dot(2) + dg_dot(3), gelu_stream(0))
        weave(wgrad(0), gelu_stream(1))
        weave(wgrad(1) + dm_part(0, 2, False), gelu_stream(2))
        weave(wgrad(2), gelu_stream(3))
        run(dm_part(2, 4, True))
        weave(wgrad(3), pull_into(dmid, dn, h_tile(l), tmp, l, 1))
        for c in range(2):
            dctx[:, half[c]] = dot_nn(wo[...], dmid[:, half[c]]).astype(BF16)

        qps, dcs = {}, {}

        def column(row):
            return jnp.broadcast_to(row, (LN, T)).T

        def stage_a(hd):
            p, hh = divmod(hd, 2)
            hsl = pl.ds(64 * hd, 64)

            def first():
                if hh == 0:
                    qps[p] = qkv[l, pl.ds(qrow(hd), 128), :].T
                    dcs[p] = dctx[pl.ds(64 * hd, 128), :].T
                c = ctx[l, hsl, :].astype(F32) + ctxl[l, hsl, :].astype(F32)
                dcol[hd % 2] = column(jnp.sum(dctx[hsl, :].astype(F32) * c, axis=0, keepdims=True))
                lcol[hd % 2] = column(lse[l, pl.ds(hd, 1), :])

            def s_part(c):
                kp = pad_head(qkv[l, pl.ds(qrow(hd) + 256, 64), half[c]], hh)
                sbuf[hd % 2, :, half[c]] = dot_nn(qps[p], kp)

            def p_part(c):
                vp = pad_head(qkv[l, pl.ds(qrow(hd) + 512, 64), half[c]], hh)
                dz[pl.ds(512 * (hd % 2), 512), half[c]] = dot_nn(dcs[p], vp).astype(BF16)

            return [first] + [functools.partial(f, c) for f in (s_part, p_part) for c in range(2)]

        def merge(xs_, ys_):
            out = []
            for i in range(max(len(xs_), len(ys_))):
                out += xs_[i:i + 1] + ys_[i:i + 1]
            return out

        def stage_b(hd):
            sl = 512 * (hd % 2)

            def group(g, r0):
                cols = half[g]
                for r in range(r0, r0 + 64, 8):
                    lc = lcol[hd % 2, rows(r, 8), :]
                    dc = dcol[hd % 2, rows(r, 8), :]
                    pr = jnp.exp2(sbuf[hd % 2, rows(r, 8), cols] * CEXP - jnp.concatenate([lc, lc], axis=1))
                    act[rows(sl + r, 8), cols] = pr.astype(BF16)
                    dp = dz[rows(sl + r, 8), cols].astype(F32)
                    act[rows(1024 + sl + r, 8), cols] = (pr * (dp - jnp.concatenate([dc, dc], axis=1))).astype(BF16)

            return [functools.partial(group, g, r0) for r0 in range(0, T, 64) for g in range(2)]

        def stage_c(hd):
            sl = 512 * (hd % 2)
            pb = act.at[pl.ds(sl, 512), :]
            db = act.at[pl.ds(1024 + sl, 512), :]
            hsl = pl.ds(64 * hd, 64)

            def f_v(c):
                dqkv[pl.ds(qrow(hd) + 512, 64), half[c]] = dot_nn(dctx[hsl, :], pb[:, half[c]]).astype(BF16)

            def f_k(c):
                dk = dot_nn(qkv[l, pl.ds(qrow(hd), 64), :], db[:, half[c]]) * SCALE
                dqkv[pl.ds(qrow(hd) + 256, 64), half[c]] = dk.astype(BF16)

            def f_q(c):
                dq = dot_nt(qkv[l, pl.ds(qrow(hd) + 256, 64), :], db[half[c], :]) * SCALE
                dqkv[pl.ds(qrow(hd), 64), half[c]] = dq.astype(BF16)

            return [functools.partial(f, c) for f in (f_v, f_k, f_q) for c in range(2)]

        def wo_grad(c):
            go[:, half[c]] += dot_nt(ctx[l], dmid[half[c], :])

        def qkv_grad(j):
            js = pl.ds(256 * j, 256)
            gqkv[:, js] += dot_nt(u[...], dqkv[js, :])

        wo_parts = [functools.partial(wo_grad, c) for c in range(2)]
        qkv_parts = [functools.partial(qkv_grad, j) for j in range(6)]
        u_norm = norm_into(u, s_tile(l), l, 0, False)
        run(stage_a(0))
        for hd in range(H + 1):
            ma = stage_a(hd + 1) if hd + 1 < H else []
            mc = stage_c(hd - 1) if hd >= 1 else wo_parts
            if hd == H:
                ma = qkv_parts[:3]
            va = stage_b(hd) if hd < H else []
            if hd == H - 1:
                va = va + u_norm
            weave(merge(mc, ma), va)

        for c in range(2):
            tmp[:, half[c]] = dot_nn(wqkv[...], dqkv[:, half[c]]).astype(BF16)
        weave(qkv_parts[3:], pull_into(dn, dmid, s_tile(l), tmp, l, 0))
        return carry

    lax.fori_loop(0, L, bwd, 0)
    dx_ref[0] = dn[...].T

    @pl.when(step == nseq - 1)
    def _():
        cps = []
        for m_ in range(2):
            g = grad_h.at[m_]
            for k in range(3):
                cps.append((gqkv.at[:, pl.ds(768 * m_ + 256 * k, 256)], g.at[pl.ds(512 * k, 512), :]))
            for k in range(4):
                cps.append((g1.at[:, pl.ds(1024 * m_ + 256 * k, 256)], g.at[pl.ds(1536 + 512 * k, 512), :]))
            for k in range(2):
                cps.append((g2.at[pl.ds(1024 * m_, 1024), pl.ds(256 * k, 256)], g.at[pl.ds(3584 + 1024 * k, 1024), :]))
            for k in range(2):
                cps.append((go.at[pl.ds(256 * m_, 256), pl.ds(256 * k, 256)], g.at[pl.ds(5632 + 256 * k, 256), :]))
        cps = [pltpu.make_async_copy(s, d, sem.at[i]) for i, (s, d) in enumerate(cps)]
        for c in cps:
            c.start()
        for c in cps:
            c.wait()


def run_kernel(x, cot, emb, wqkv, wo, w1, w2):
    nseq = x.shape[0] // 2
    embb = jnp.broadcast_to(emb[:, :, None], (L, D, LN))
    blk = pl.BlockSpec((1, T, D), lambda i: (lax.axis_index('model') * nseq + i, 0, 0))
    anyspec = pl.BlockSpec(memory_space=pl.ANY)
    V = pltpu.VMEM
    return pl.pallas_call(
        functools.partial(kernel, nseq),
        grid=(nseq,),
        in_specs=[blk, blk, pl.BlockSpec(memory_space=pltpu.VMEM)] + [anyspec] * 4,
        out_specs=[blk, anyspec],
        out_shape=[jax.ShapeDtypeStruct((2 * nseq, T, D), BF16), jax.ShapeDtypeStruct((2, GROWS, GL), F32)],
        scratch_shapes=[V((D, 1536), BF16), V((D, D), BF16), V((D, FF), BF16), V((FF, D), BF16),
                        V((1536, D), BF16), V((D, D), BF16), V((FF, D), BF16), V((D, FF), BF16),
                        V((D, 1536), F32), V((D, D), F32), V((D, FF), F32), V((FF, D), F32),
                        V((L, D, T), BF16), V((L, 1536, T), BF16), V((L, D, T), BF16), V((L, D, T), BF16), V((L, D, T), BF16),
                        V((L, FF, T), BF16), V((L, H, T), F32), V((L, 2, T), F32), V((D, T), BF16), V((D, T), BF16), V((FF, T), BF16),
                        V((FF, T), BF16), V((D, T), BF16), V((D, T), BF16), V((D, T), BF16), V((1536, T), BF16), V((D, T), BF16),
                        V((2, T, T), F32), V((2, T, LN), F32), V((2, T, LN), F32), pltpu.SemaphoreType.DMA((22,))],
        compiler_params=pltpu.CompilerParams(dimension_semantics=("arbitrary",), vmem_limit_bytes=67_000_000),
    )(x, cot, embb, wqkv, wo, w1, w2)


MESH_ID = pl.DeviceIdType.MESH
NCOL = 2
BR, GL = 384, 256
GROWS = NCOL * 8 * BR
ORDERS = ('xyz', 'yxz')
NW = 6


def neighbours():
    mi = lax.axis_index('model')
    di = lax.axis_index('data')
    core, x, y = di % 2, (di // 2) % 2, di // 4
    dev = {'x': {'model': mi, 'data': di + 2 - 4 * x}, 'y': {'model': mi, 'data': di + 4 - 8 * y},
           'z': {'model': 1 - mi, 'data': di}, 'c': {'model': mi, 'data': di + 1 - 2 * core}}
    return {'x': x, 'y': y, 'z': mi}, core, dev


def greet(dev, names):
    barrier = pltpu.get_barrier_semaphore()
    for d in names:
        pl.semaphore_signal(barrier, inc=1, device_id=dev[d], device_id_type=MESH_ID)
    pl.semaphore_wait(barrier, len(names))


def gather_kernel(*refs):
    w_in, (wqkv, wo, w1, w2), (stage, lsem, ssem, zsend, zrecv, csend, crecv) = refs[:NW], refs[NW:NW + 4], refs[NW + 4:]
    me, core, dev = neighbours()
    mi = me['z']
    greet(dev, 'zc')

    def place(k, m, r0, n):
        if k < 3:
            return wqkv.at[m, pl.ds(r0, n), pl.ds(256 * k, 256)]
        if k == 3:
            return wo.at[pl.ds(256 * m + r0, n), :]
        if k == 4:
            return w1.at[m, pl.ds(r0, n), :]
        return w2.at[pl.ds(1024 * m + r0, n), :]

    n_rows = (512, 512, 512, 256, 512, 1024)
    zc, cc, loc, put = [], [], [], []
    for k in range(NW):
        n = n_rows[k] // 2
        zc.append(pltpu.make_async_remote_copy(w_in[k].at[pl.ds(n * core, n), :], place(k, mi, n * core, n), zsend.at[k], zrecv.at[k],
                                               device_id=dev['z'], device_id_type=MESH_ID))
        zc[k].start()
    for k in range(NW):
        loc.append(pltpu.make_async_copy(w_in[k], stage.at[k, pl.ds(0, n_rows[k]), pl.ds(0, w_in[k].shape[1])], lsem.at[k]))
        loc[k].start()
    for k in range(NW):
        loc[k].wait()
        put.append(pltpu.make_async_copy(stage.at[k, pl.ds(0, n_rows[k]), pl.ds(0, w_in[k].shape[1])], place(k, mi, 0, n_rows[k]), ssem.at[k]))
        put[k].start()
    for k in range(NW):
        n = n_rows[k] // 2
        zc[k].wait_recv()
        got = place(k, 1 - mi, n * core, n)
        cc.append(pltpu.make_async_remote_copy(got, got, csend.at[k], crecv.at[k], device_id=dev['c'], device_id_type=MESH_ID))
        cc[k].start()
    for k in range(NW):
        put[k].wait()
        zc[k].wait_send()
        cc[k].wait()


def run_gather(ws):
    anyspec = pl.BlockSpec(memory_space=pl.ANY)
    S = pltpu.SemaphoreType.DMA
    return pl.pallas_call(
        gather_kernel,
        in_specs=[anyspec] * NW,
        out_specs=[anyspec] * 4,
        out_shape=[jax.ShapeDtypeStruct((2, D, 768), BF16), jax.ShapeDtypeStruct((D, D), BF16),
                   jax.ShapeDtypeStruct((2, D, 1024), BF16), jax.ShapeDtypeStruct((FF, D), BF16)],
        scratch_shapes=[pltpu.VMEM((NW, 1024, 1024), BF16)] + [S((NW,))] * 6,
        compiler_params=pltpu.CompilerParams(vmem_limit_bytes=60_000_000, collective_id=0, has_side_effects=True),
    )(*ws)


def reduce_kernel(g_h, dx_in, out, dx, acc, rd, r1, r2, r3, locsem, ds, dr, ps, pr, gs, gr, cs, cr, xs_, xr_):
    me, core, dev = neighbours()
    x, y, mi = me['x'], me['y'], me['z']
    nseq = dx.shape[0] // 2

    def rdma(src, dst, s, r, d):
        return pltpu.make_async_remote_copy(src, dst, s, r, device_id=dev[d], device_id_type=MESH_ID)

    greet(dev, 'xyzc')

    xc = []
    for s in range(nseq):
        here = dx.at[mi * nseq + s]
        xc.append(rdma(here, here, xs_.at[s], xr_.at[s], 'z'))

    def blk(color, pos):
        return (pos['z'] * NCOL + color) * 4 + pos['y'] * 2 + pos['x']

    def all_pos(fixed):
        out_ = [dict(fixed)]
        for ax in 'zyx':
            if ax not in fixed:
                out_ = [dict(p, **{ax: v}) for p in out_ for v in (0, 1)]
        return out_

    def add(dst, src):
        def body(i, c):
            r = pl.multiple_of(i * 32, 32)
            acc[dst, pl.ds(r, 32), :] += src[pl.ds(r, 32), :]
            return c
        lax.fori_loop(0, BR // 32, body, 0)

    first, rest = [], []
    for color in range(NCOL):
        a = ORDERS[color][0]
        first += [blk(color, p) for p in all_pos({a: 1 - me[a]})]
        rest += [blk(color, p) for p in all_pos({a: me[a]})]
    seq = first + rest
    nb = len(seq)
    dcp, lcp = [], []
    for i, b in enumerate(seq):
        dcp.append(rdma(g_h.at[b * 2 + (1 - core)], rd.at[b], ds.at[i], dr.at[i], 'c'))
        lcp.append(pltpu.make_async_copy(g_h.at[b * 2 + core], acc.at[b], locsem.at[i]))
    for i in range(nb):
        dcp[i].start()
        lcp[i].start()
    for s in range(4):
        xc[s].start()

    def fold_core(i):
        dcp[i].wait_recv()
        lcp[i].wait()
        add(seq[i], rd.at[seq[i]])

    p1, p2, p3 = [], [], []
    for j in range(4):
        for color in range(NCOL):
            a = ORDERS[color][0]
            i = 4 * color + j
            fold_core(i)
            cp = rdma(acc.at[blk(color, all_pos({a: 1 - me[a]})[j])], r1.at[i], ps.at[i], pr.at[i], a)
            cp.start()
            p1.append(cp)
    p1 = [p1[(i % 4) * NCOL + i // 4] for i in range(4 * NCOL)]
    for i in range(4 * NCOL, nb):
        fold_core(i)
    for color in range(NCOL):
        a, b = ORDERS[color][0], ORDERS[color][1]
        for j, p in enumerate(all_pos({a: me[a]})):
            p1[4 * color + j].wait_recv()
            add(blk(color, p), r1.at[4 * color + j])
        for j, p in enumerate(all_pos({a: me[a], b: 1 - me[b]})):
            i = 2 * color + j
            cp = rdma(acc.at[blk(color, p)], r2.at[i], ps.at[4 * NCOL + i], pr.at[4 * NCOL + i], b)
            cp.start()
            p2.append(cp)
    for color in range(NCOL):
        a, b, c = ORDERS[color]
        for j, p in enumerate(all_pos({a: me[a], b: me[b]})):
            p2[2 * color + j].wait_recv()
            add(blk(color, p), r2.at[2 * color + j])
        cp = rdma(acc.at[blk(color, dict(me, **{c: 1 - me[c]}))], r3.at[color], ps.at[6 * NCOL + color], pr.at[6 * NCOL + color], c)
        cp.start()
        p3.append(cp)
    for s in range(4, nseq):
        xc[s].start()

    cps, g1_, g2_ = [], [], []

    def out_at(color, yy, xx):
        return out.at[(color * 4 + yy * 2 + xx) * 2 + core]

    def to_sibling(color, yy, xx, i):
        o = out_at(color, yy, xx)
        cp = rdma(o, o, cs.at[i], cr.at[i], 'c')
        cp.start()
        cps.append(cp)

    for color in range(NCOL):
        p3[color].wait_recv()
        b = blk(color, me)
        o_blk = (color * 4 + y * 2 + x) * 2 + core

        def body(i, c, b=b, o_blk=o_blk, color=color):
            r = pl.multiple_of(i * 32, 32)
            out[o_blk, pl.ds(r, 32), :] = acc[b, pl.ds(r, 32), :] + r3[color, pl.ds(r, 32), :]
            return c
        lax.fori_loop(0, BR // 32, body, 0)
        o = out_at(color, y, x)
        cp = rdma(o, o, gs.at[color], gr.at[color], ORDERS[color][0])
        cp.start()
        g1_.append(cp)
        c2 = rdma(o, o, gs.at[NCOL + 2 * color], gr.at[NCOL + 2 * color], ORDERS[color][1])
        c2.start()
        g2_.append(c2)
        to_sibling(color, y, x, color)
    for color in range(NCOL):
        g1_[color].wait_recv()
        a, b = ORDERS[color][0], ORDERS[color][1]
        yy, xx = (y, 1 - x) if a == 'x' else (1 - y, x)
        o = out_at(color, yy, xx)
        c2 = rdma(o, o, gs.at[NCOL + 2 * color + 1], gr.at[NCOL + 2 * color + 1], b)
        c2.start()
        g2_.append(c2)
        to_sibling(color, yy, xx, NCOL + color)
    for k in range(2 * NCOL):
        color = k % NCOL
        b = ORDERS[color][1]
        g2_[k].wait_recv()
        if k < NCOL:
            ty, tx = (y, 1 - x) if b == 'x' else (1 - y, x)
        else:
            ty, tx = 1 - y, 1 - x
        to_sibling(color, ty, tx, 2 * NCOL + k)
    for cp in cps:
        cp.wait()
    for cp in dcp + p1 + p2 + p3 + g1_ + g2_:
        cp.wait_send()
    for s in range(nseq):
        xc[s].wait_send()
        there = dx.at[(1 - mi) * nseq + s]
        rdma(there, there, xs_.at[s], xr_.at[s], 'z').wait_recv()


def run_reduce(grad, dx):
    g = grad.reshape(2 * NCOL * 8, BR, GL)
    nb = NCOL * 8
    V = pltpu.VMEM
    S = pltpu.SemaphoreType.DMA
    anyspec = pl.BlockSpec(memory_space=pl.ANY)
    return pl.pallas_call(
        reduce_kernel,
        in_specs=[anyspec, anyspec],
        out_specs=[pl.BlockSpec(memory_space=pltpu.VMEM), anyspec],
        out_shape=[jax.ShapeDtypeStruct((nb, BR, GL), F32), jax.ShapeDtypeStruct(dx.shape, dx.dtype)],
        scratch_shapes=[V((nb, BR, GL), F32), V((nb, BR, GL), F32), V((4 * NCOL, BR, GL), F32), V((2 * NCOL, BR, GL), F32), V((NCOL, BR, GL), F32),
                        S((nb,)), S((nb,)), S((nb,)), S((7 * NCOL,)), S((7 * NCOL,)), S((3 * NCOL,)), S((3 * NCOL,)), S((4 * NCOL,)), S((4 * NCOL,)),
                        S((6,)), S((6,))],
        input_output_aliases={1: 1},
        compiler_params=pltpu.CompilerParams(vmem_limit_bytes=60_000_000, collective_id=1, has_side_effects=True),
    )(g, dx)


def solution(mesh):
    spec_col, spec_row, spec_act, spec_rep = P(None, 'model'), P('model', None), P('data', None, None), P(None, None)

    def device_step(x_in, cot_out, step_emb, w_q, w_k, w_v, w_o, w_1, w_2):
        wqkv, wo, w1, w2 = run_gather((w_q, w_k, w_v, w_o, w_1, w_2))
        dx, grad = run_kernel(x_in, cot_out, step_emb, wqkv, wo, w1, w2)
        g, dx = run_reduce(grad, dx)
        g = g.reshape(GROWS, GL)

        def join(r0, n, k):
            return jnp.concatenate([g[r0 + n * i:r0 + n * (i + 1)] for i in range(k)], axis=1)

        return g[:512], g[512:1024], g[1024:1536], join(5632, 256, 2), join(1536, 512, 4), join(3584, 1024, 2), dx

    return jax.shard_map(device_step, mesh=mesh,
                         in_specs=(spec_act, spec_act, spec_rep, spec_col, spec_col, spec_col, spec_row, spec_col, spec_row),
                         out_specs=(spec_col, spec_col, spec_col, spec_row, spec_col, spec_row, spec_act),
                         check_vma=False)
```

```python
import functools

import jax
import jax.numpy as jnp
from jax import lax
from jax.experimental import pallas as pl
from jax.experimental.pallas import tpu as pltpu
from jax.sharding import PartitionSpec as P

F32, BF16 = jnp.float32, jnp.bfloat16
T, D, FF, H, E, L = 512, 512, 2048, 8, 64, 4
EPS = 1e-6
CEXP = E ** -0.5 * 1.4426950408889634
SCALE = E ** -0.5
GK0 = 0.7978845608028654
GK1 = 0.044715
R = 32
LN = 128


def dot_nn(a, b):
    return lax.dot_general(a, b, (((1,), (0,)), ((), ())), preferred_element_type=F32)


def dot_nt(a, b):
    return lax.dot_general(a, b, (((1,), (1,)), ((), ())), preferred_element_type=F32)


def rows(r, n=R):
    return pl.ds(r, n)


def wide(e):
    return jnp.concatenate([e] * (T // LN), axis=1)


def col_sum(tile_fn):
    accs = [None, None]
    for i, r in enumerate(range(0, D, R)):
        v = tile_fn(r)
        accs[i % 2] = v if accs[i % 2] is None else accs[i % 2] + v
    return jnp.sum(accs[0] + accs[1], axis=0, keepdims=True)


def rms_of(tile_fn):
    def sq(r):
        v = tile_fn(r)
        return v * v
    return lax.rsqrt(col_sum(sq) * (1.0 / D) + EPS)


def weave(*streams):
    total = max(len(s) for s in streams)
    done = [0] * len(streams)
    for t in range(total):
        for k, s in enumerate(streams):
            upto = -(-len(s) * (t + 1) // total)
            while done[k] < upto:
                s[done[k]]()
                done[k] += 1


def gelu_fwd(z):
    return z * jax.nn.sigmoid(z * (2 * GK0 + (2 * GK0 * GK1) * (z * z)))


def gelu_both(z):
    z2 = z * z
    s = jax.nn.sigmoid(z * (2 * GK0 + (2 * GK0 * GK1) * z2))
    w = z * (2 * GK0 + (6 * GK0 * GK1) * z2)
    return z * s, s * (1.0 + w * (1.0 - s))


def qrow(hd):
    return 768 * (hd // 4) + 64 * (hd % 4)


def pad_head(block, hh):
    zero = jnp.zeros_like(block)
    return jnp.concatenate([block, zero] if hh == 0 else [zero, block], axis=0)


def zip_pad(a, b):
    return [(a[i:i + 1], b[i:i + 1]) for i in range(max(len(a), len(b)))]


def max_cols(ref, cols):
    accs = [None] * 4
    for i, r in enumerate(range(0, T, 64)):
        v = ref[rows(r, 64), cols]
        accs[i % 4] = v if accs[i % 4] is None else jnp.maximum(accs[i % 4], v)
    m = jnp.maximum(jnp.maximum(accs[0], accs[1]), jnp.maximum(accs[2], accs[3]))
    return jnp.max(m, axis=0, keepdims=True)

GL, GROWS = 256, 6144


MESH_ID = pl.DeviceIdType.MESH
NW = 6


def other(i):
    return 1 - i


def kernel(nseq, x_ref, cot_ref, emb_ref, wq_h, wk_h, wv_h, wo_h, w1_h, w2_h,
           dx_h, grad_h,
           wqkv, wo, w1, w2, wqkvt, wot, w1t, w2t, gqkv, go, g1, g2,
           xs, qkv, ctx, ctxl, hs, zs, lse, rsc, u, m, act, dz, dn, dmid, dctx, dqkv, tmp, sbuf, lcol, dcol, dxs,
           sem, zsend, zrecv, csend, crecv, xloc, xsend, xrecv):
    step = pl.program_id(0)
    mi = lax.axis_index('model')
    di = lax.axis_index('data')
    core = di % 2
    zdev = {'model': 1 - mi, 'data': di}
    cdev = {'model': mi, 'data': di + 1 - 2 * core}

    def place(k, m, r0, n):
        if k < 3:
            return wqkv.at[pl.ds(r0, n), pl.ds(768 * m + 256 * k, 256)]
        if k == 3:
            return wo.at[pl.ds(256 * m + r0, n), :]
        if k == 4:
            return w1.at[pl.ds(r0, n), pl.ds(1024 * m, 1024)]
        return w2.at[pl.ds(1024 * m + r0, n), :]

    w_hbm = (wq_h, wk_h, wv_h, wo_h, w1_h, w2_h)
    w_rows = (512, 512, 512, 256, 512, 1024)

    def load_weights():
        barrier = pltpu.get_barrier_semaphore()
        for dev in (zdev, cdev):
            pl.semaphore_signal(barrier, inc=1, device_id=dev, device_id_type=MESH_ID)
        pl.semaphore_wait(barrier, 2)
        local, zs_, cs_ = [], [], []
        for k in range(NW):
            n = w_rows[k] // 2
            zs_.append(pltpu.make_async_remote_copy(
                w_hbm[k].at[pl.ds(n * core, n), :], place(k, mi, n * core, n),
                zsend.at[k], zrecv.at[k], device_id=zdev, device_id_type=MESH_ID))
            zs_[-1].start()
        for k in range(NW):
            local.append(pltpu.make_async_copy(w_hbm[k], place(k, mi, 0, w_rows[k]), sem.at[k]))
            local[-1].start()
        for k in range(NW):
            n = w_rows[k] // 2
            zs_[k].wait_recv()
            mine = place(k, 1 - mi, n * core, n)
            cs_.append(pltpu.make_async_remote_copy(
                mine, mine, csend.at[k], crecv.at[k], device_id=cdev, device_id_type=MESH_ID))
            cs_[-1].start()
        for k in range(NW):
            local[k].wait()
            zs_[k].wait_send()
            cs_[k].wait()

    @pl.when(step == 0)
    def _():
        load_weights()
        for j in range(3):
            wqkvt[pl.ds(512 * j, 512), :] = wqkv[:, pl.ds(512 * j, 512)].T
        wot[...] = wo[...].T
        for j in range(4):
            w1t[pl.ds(512 * j, 512), :] = w1[:, pl.ds(512 * j, 512)].T
            w2t[:, pl.ds(512 * j, 512)] = w2[pl.ds(512 * j, 512), :].T
        gqkv[...] = jnp.zeros_like(gqkv)
        go[...] = jnp.zeros_like(go)
        g1[...] = jnp.zeros_like(g1)
        g2[...] = jnp.zeros_like(g2)

    xs[0] = x_ref[0].T
    half = [pl.ds(0, 256), pl.ds(256, 256)]

    def s_tile(l):
        return lambda r: xs[l, rows(r), :].astype(F32) + wide(emb_ref[l, rows(r), :])

    def norm_into(dst, tile_fn, l, k, fresh):
        box = {}

        def stat():
            if fresh:
                box['r'] = rms_of(tile_fn)
                rsc[l, pl.ds(k, 1), :] = box['r']
            else:
                box['r'] = rsc[l, pl.ds(k, 1), :]

        def put(r):
            dst[rows(r), :] = (tile_fn(r) * box['r']).astype(BF16)

        return [stat] + [functools.partial(put, r) for r in range(0, D, R)]

    def pull_into(dst, base, tile_fn, dy, l, k):
        box = {}

        def stat():
            a = col_sum(lambda r: dy[rows(r), :].astype(F32) * tile_fn(r)) * (1.0 / D)
            rr = rsc[l, pl.ds(k, 1), :]
            box['r'] = rr
            box['a'] = rr * rr * rr * a

        def put(r):
            g = dy[rows(r), :].astype(F32)
            dst[rows(r), :] = (base[rows(r), :].astype(F32) + (box['r'] * g - tile_fn(r) * box['a'])).astype(BF16)

        return [stat] + [functools.partial(put, r) for r in range(0, D, R)]

    def run(stream):
        for f in stream:
            f()

    def h_tile(l):
        return lambda r: hs[l, rows(r), :].astype(F32)

    def fwd(l, carry):
        run(norm_into(u, s_tile(l), l, 0, True))
        for j in range(3):
            qkv[l, pl.ds(512 * j, 512), :] = dot_nn(wqkvt[pl.ds(512 * j, 512), :], u[...]).astype(BF16)

        kps = {}
        inv = {}

        def stage_a(hd):
            p, hh = divmod(hd, 2)

            def first():
                if hh == 0:
                    kps[p] = qkv[l, pl.ds(qrow(hd) + 256, 128), :].T

            def part(c):
                qp = pad_head(qkv[l, pl.ds(qrow(hd), 64), half[c]], hh)
                sbuf[hd % 2, :, half[c]] = dot_nn(kps[p], qp)

            return [first, lambda: part(0), lambda: part(1)]

        def stage_b(hd):
            sref, eref = sbuf.at[hd % 2], act.at[pl.ds(512 * (hd % 2), 512), :]

            def group(g):
                cols = half[g]
                mx = max_cols(sref, cols) * CEXP
                accs = [None, None]
                for i, r in enumerate(range(0, T, 64)):
                    e = jnp.exp2(sref[rows(r, 64), cols] * CEXP - mx)
                    accs[i % 2] = e if accs[i % 2] is None else accs[i % 2] + e
                    eref[rows(r, 64), cols] = e.astype(BF16)
                sm = jnp.sum(accs[0] + accs[1], axis=0, keepdims=True)
                lse[l, pl.ds(hd, 1), cols] = mx + jnp.log2(sm)
                inv[hd, g] = 1.0 / sm

            return [functools.partial(group, g) for g in range(2)]

        def stage_c(hd):
            def part(c):
                cn = dot_nn(qkv[l, pl.ds(qrow(hd) + 512, 64), :], act[pl.ds(512 * (hd % 2), 512), half[c]])
                cn = cn * inv[hd, c]
                hi = cn.astype(BF16)
                ctx[l, pl.ds(64 * hd, 64), half[c]] = hi
                ctxl[l, pl.ds(64 * hd, 64), half[c]] = (cn - hi.astype(F32)).astype(BF16)

            return [lambda: part(0), lambda: part(1)]

        run(stage_a(0))
        for hd in range(H + 1):
            mx = []
            for x_, y_ in zip_pad(stage_a(hd + 1) if hd + 1 < H else [], stage_c(hd - 1) if hd >= 1 else []):
                mx += x_ + y_
            va = stage_b(hd) if hd < H else []
            weave(mx, va)

        for c in range(2):
            o = dot_nn(wot[...], ctx[l, :, half[c]])
            for r in range(0, D, R):
                sx = xs[l, rows(r), half[c]].astype(F32) + jnp.concatenate([emb_ref[l, rows(r), :]] * 2, axis=1)
                hs[l, rows(r), half[c]] = (sx + o[r:r + R]).astype(BF16)
        run(norm_into(m, h_tile(l), l, 1, True))

        def z_dot(j):
            def f(c):
                js = pl.ds(512 * j, 512)
                zs[l, js, half[c]] = dot_nn(w1t[js, :], m[:, half[c]]).astype(BF16)
            return [lambda: f(0), lambda: f(1)]

        def gelu_stream(j):
            def f(r, c):
                act[rows(r, 64), half[c]] = gelu_fwd(zs[l, rows(r, 64), half[c]].astype(F32)).astype(BF16)
            return [functools.partial(f, r, c) for r in range(512 * j, 512 * j + 512, 64) for c in range(2)]

        @pl.when(l < L - 1)
        def _():
            run(z_dot(0))
            for j in range(4):
                weave(z_dot(j + 1) if j < 3 else [], gelu_stream(j))
            for c in range(2):
                o = dot_nn(w2t[...], act[:, half[c]])
                for r in range(0, D, R):
                    xs[l + 1, rows(r), half[c]] = (hs[l, rows(r), half[c]].astype(F32) + o[r:r + R]).astype(BF16)

        @pl.when(l == L - 1)
        def _():
            for j in range(4):
                run(z_dot(j))
        return carry

    lax.fori_loop(0, L, fwd, 0)

    dn[...] = cot_ref[0].T

    def bwd(i, carry):
        l = L - 1 - i

        def dg_dot(j):
            def f(c):
                js = pl.ds(512 * j, 512)
                dz[js, half[c]] = dot_nn(w2[js, :], dn[:, half[c]]).astype(BF16)
            return [lambda: f(0), lambda: f(1)]

        def gelu_stream(j):
            def f(r, c):
                g, gp = gelu_both(zs[l, rows(r, 64), half[c]].astype(F32))
                act[rows(r, 64), half[c]] = g.astype(BF16)
                dz[rows(r, 64), half[c]] = (dz[rows(r, 64), half[c]].astype(F32) * gp).astype(BF16)
            return [functools.partial(f, r, c) for r in range(512 * j, 512 * j + 512, 64) for c in range(2)]

        def wgrad(j):
            js = pl.ds(512 * j, 512)

            def a(c):
                g2[js, half[c]] += dot_nt(act[js, :], dn[half[c], :])

            def b(c):
                jc = pl.ds(512 * j + 256 * c, 256)
                g1[:, jc] += dot_nt(m[...], dz[jc, :])
            return [lambda: a(0), lambda: a(1), lambda: b(0), lambda: b(1)]

        weave(dg_dot(0), norm_into(m, h_tile(l), l, 1, False))
        def dm_part(k0, k1, last):
            def f(c):
                p = dot_nn(w1[:, 512 * k0:512 * k1], dz[pl.ds(512 * k0, 512 * (k1 - k0)), half[c]])
                if k0 > 0:
                    p = sbuf[0, :, half[c]] + p
                if last:
                    tmp[:, half[c]] = p.astype(BF16)
                else:
                    sbuf[0, :, half[c]] = p
            return [lambda: f(0), lambda: f(1)]

        weave(dg_dot(1) + dg_dot(2) + dg_dot(3), gelu_stream(0))
        weave(wgrad(0), gelu_stream(1))
        weave(wgrad(1) + dm_part(0, 2, False), gelu_stream(2))
        weave(wgrad(2), gelu_stream(3))
        run(dm_part(2, 4, True))
        weave(wgrad(3), pull_into(dmid, dn, h_tile(l), tmp, l, 1))
        for c in range(2):
            dctx[:, half[c]] = dot_nn(wo[...], dmid[:, half[c]]).astype(BF16)

        qps, dcs = {}, {}

        def column(row):
            return jnp.broadcast_to(row, (LN, T)).T

        def stage_a(hd):
            p, hh = divmod(hd, 2)
            hsl = pl.ds(64 * hd, 64)

            def first():
                if hh == 0:
                    qps[p] = qkv[l, pl.ds(qrow(hd), 128), :].T
                    dcs[p] = dctx[pl.ds(64 * hd, 128), :].T
                c = ctx[l, hsl, :].astype(F32) + ctxl[l, hsl, :].astype(F32)
                dcol[hd % 2] = column(jnp.sum(dctx[hsl, :].astype(F32) * c, axis=0, keepdims=True))
                lcol[hd % 2] = column(lse[l, pl.ds(hd, 1), :])

            def s_part(c):
                kp = pad_head(qkv[l, pl.ds(qrow(hd) + 256, 64), half[c]], hh)
                sbuf[hd % 2, :, half[c]] = dot_nn(qps[p], kp)

            def p_part(c):
                vp = pad_head(qkv[l, pl.ds(qrow(hd) + 512, 64), half[c]], hh)
                dz[pl.ds(512 * (hd % 2), 512), half[c]] = dot_nn(dcs[p], vp).astype(BF16)

            return [first] + [functools.partial(f, c) for f in (s_part, p_part) for c in range(2)]

        def merge(xs_, ys_):
            out = []
            for i in range(max(len(xs_), len(ys_))):
                out += xs_[i:i + 1] + ys_[i:i + 1]
            return out

        def stage_b(hd):
            sl = 512 * (hd % 2)

            def group(g, r0):
                cols = half[g]
                for r in range(r0, r0 + 64, 64):
                    lc = lcol[hd % 2, rows(r, 64), :]
                    dc = dcol[hd % 2, rows(r, 64), :]
                    pr = jnp.exp2(sbuf[hd % 2, rows(r, 64), cols] * CEXP - jnp.concatenate([lc, lc], axis=1))
                    act[rows(sl + r, 64), cols] = pr.astype(BF16)
                    dp = dz[rows(sl + r, 64), cols].astype(F32)
                    act[rows(1024 + sl + r, 64), cols] = (pr * (dp - jnp.concatenate([dc, dc], axis=1))).astype(BF16)

            return [functools.partial(group, g, r0) for r0 in range(0, T, 64) for g in range(2)]

        def stage_c(hd):
            sl = 512 * (hd % 2)
            pb = act.at[pl.ds(sl, 512), :]
            db = act.at[pl.ds(1024 + sl, 512), :]
            hsl = pl.ds(64 * hd, 64)

            def f_v(c):
                dqkv[pl.ds(qrow(hd) + 512, 64), half[c]] = dot_nn(dctx[hsl, :], pb[:, half[c]]).astype(BF16)

            def f_k(c):
                dk = dot_nn(qkv[l, pl.ds(qrow(hd), 64), :], db[:, half[c]]) * SCALE
                dqkv[pl.ds(qrow(hd) + 256, 64), half[c]] = dk.astype(BF16)

            def f_q(c):
                dq = dot_nt(qkv[l, pl.ds(qrow(hd) + 256, 64), :], db[half[c], :]) * SCALE
                dqkv[pl.ds(qrow(hd), 64), half[c]] = dq.astype(BF16)

            return [functools.partial(f, c) for f in (f_v, f_k, f_q) for c in range(2)]

        def wo_grad(c):
            go[:, half[c]] += dot_nt(ctx[l], dmid[half[c], :])

        def qkv_grad(j):
            js = pl.ds(256 * j, 256)
            gqkv[:, js] += dot_nt(u[...], dqkv[js, :])

        wo_parts = [functools.partial(wo_grad, c) for c in range(2)]
        qkv_parts = [functools.partial(qkv_grad, j) for j in range(6)]
        u_norm = norm_into(u, s_tile(l), l, 0, False)
        run(stage_a(0))
        for hd in range(H + 1):
            ma = stage_a(hd + 1) if hd + 1 < H else []
            mc = stage_c(hd - 1) if hd >= 1 else wo_parts
            if hd == H:
                ma = qkv_parts[:3]
            va = stage_b(hd) if hd < H else []
            if hd == H - 1:
                va = va + u_norm
            weave(merge(mc, ma), va)

        for c in range(2):
            tmp[:, half[c]] = dot_nn(wqkv[...], dqkv[:, half[c]]).astype(BF16)
        weave(qkv_parts[3:], pull_into(dn, dmid, s_tile(l), tmp, l, 0))
        return carry

    lax.fori_loop(0, L, bwd, 0)
    slot = step % 2

    def dx_copies(s, at):
        here = dx_h.at[mi * nseq + s]
        loc = pltpu.make_async_copy(dxs.at[at], here, xloc.at[at])
        rem = pltpu.make_async_remote_copy(dxs.at[at], here, xsend.at[at], xrecv.at[s], device_id=zdev, device_id_type=MESH_ID)
        return loc, rem

    def dx_drain(s, at):
        loc, rem = dx_copies(s, at)
        loc.wait()
        rem.wait_send()

    @pl.when(step >= 2)
    def _():
        dx_drain(step - 2, slot)

    dxs[slot] = dn[...].T
    for c in dx_copies(step, slot):
        c.start()

    @pl.when(step == nseq - 1)
    def _():
        cps = []
        for m_ in range(2):
            g = grad_h.at[m_]
            for k in range(3):
                cps.append((gqkv.at[:, pl.ds(768 * m_ + 256 * k, 256)], g.at[pl.ds(512 * k, 512), :]))
            for k in range(4):
                cps.append((g1.at[:, pl.ds(1024 * m_ + 256 * k, 256)], g.at[pl.ds(1536 + 512 * k, 512), :]))
            for k in range(2):
                cps.append((g2.at[pl.ds(1024 * m_, 1024), pl.ds(256 * k, 256)], g.at[pl.ds(3584 + 1024 * k, 1024), :]))
            for k in range(2):
                cps.append((go.at[pl.ds(256 * m_, 256), pl.ds(256 * k, 256)], g.at[pl.ds(5632 + 256 * k, 256), :]))
        cps = [pltpu.make_async_copy(s, d, sem.at[i]) for i, (s, d) in enumerate(cps)]
        for c in cps:
            c.start()
        dx_drain(nseq - 2, (nseq - 2) % 2)
        dx_drain(nseq - 1, (nseq - 1) % 2)
        for s in range(nseq):
            theirs = dx_h.at[(1 - mi) * nseq + s]
            pltpu.make_async_remote_copy(dxs.at[s % 2], theirs, xsend.at[s % 2], xrecv.at[s],
                                         device_id=zdev, device_id_type=MESH_ID).wait_recv()
        for c in cps:
            c.wait()


def run_kernel(x, cot, emb, ws, nseq):
    embb = jnp.broadcast_to(emb.astype(F32)[:, :, None], (L, D, LN))
    blk = pl.BlockSpec((1, T, D), lambda i: (lax.axis_index('model') * nseq + i, 0, 0))
    anyspec = pl.BlockSpec(memory_space=pl.ANY)
    V = pltpu.VMEM
    S = pltpu.SemaphoreType.DMA
    return pl.pallas_call(
        functools.partial(kernel, nseq),
        grid=(nseq,),
        in_specs=[blk, blk, pl.BlockSpec(memory_space=pltpu.VMEM)] + [anyspec] * NW,
        out_specs=[anyspec] * 2,
        out_shape=[jax.ShapeDtypeStruct((2 * nseq, T, D), BF16), jax.ShapeDtypeStruct((2, GROWS, GL), F32)],
        scratch_shapes=[V((D, 1536), BF16), V((D, D), BF16), V((D, FF), BF16), V((FF, D), BF16),
                        V((1536, D), BF16), V((D, D), BF16), V((FF, D), BF16), V((D, FF), BF16),
                        V((D, 1536), F32), V((D, D), F32), V((D, FF), F32), V((FF, D), F32),
                        V((L, D, T), BF16), V((L, 1536, T), BF16), V((L, D, T), BF16), V((L, D, T), BF16), V((L, D, T), BF16),
                        V((L, FF, T), BF16), V((L, H, T), F32), V((L, 2, T), F32), V((D, T), BF16), V((D, T), BF16), V((FF, T), BF16),
                        V((FF, T), BF16), V((D, T), BF16), V((D, T), BF16), V((D, T), BF16), V((1536, T), BF16), V((D, T), BF16),
                        V((2, T, T), F32), V((2, T, LN), F32), V((2, T, LN), F32), V((2, T, D), BF16),
                        S((22,)), S((NW,)), S((NW,)), S((NW,)), S((NW,)), S((2,)), S((2,)), S((nseq,))],
        compiler_params=pltpu.CompilerParams(dimension_semantics=("arbitrary",), vmem_limit_bytes=67_000_000,
                                             collective_id=0, has_side_effects=True),
    )(x, cot, embb, *ws)


NCOL = 3
BR = 256
GROWS = NCOL * 8 * BR
ORDERS = ('xyz', 'yzx', 'zxy')
SPREAD = ((0, 0, BR, 'xy'), (1, 0, BR, 'yx'), (2, 0, BR // 2, 'xy'), (2, BR // 2, BR // 2, 'yx'))


def reduce_kernel(g_h, out, acc, rd, r1, r2, r3, locsem, ds, dr, ps, pr, gs, gr, cs, cr):
    mi = lax.axis_index('model')
    di = lax.axis_index('data')
    core, x, y = di % 2, (di // 2) % 2, di // 4
    me = {'x': x, 'y': y, 'z': mi}
    dev = {'x': {'model': mi, 'data': di + 2 - 4 * x}, 'y': {'model': mi, 'data': di + 4 - 8 * y},
           'z': {'model': 1 - mi, 'data': di}, 'c': {'model': mi, 'data': di + 1 - 2 * core}}

    def rdma(src, dst, s, r, d):
        return pltpu.make_async_remote_copy(src, dst, s, r, device_id=dev[d], device_id_type=MESH_ID)

    barrier = pltpu.get_barrier_semaphore()
    for d in 'xyzc':
        pl.semaphore_signal(barrier, inc=1, device_id=dev[d], device_id_type=MESH_ID)
    pl.semaphore_wait(barrier, 4)

    def blk(color, far):
        pos = {ax: (1 - me[ax] if ax in far else me[ax]) for ax in 'xyz'}
        return (pos['z'] * NCOL + color) * 4 + pos['y'] * 2 + pos['x']

    def add(dst, src):
        def body(i, c):
            r = pl.multiple_of(i * 64, 64)
            acc[dst, pl.ds(r, 64), :] += src[pl.ds(r, 64), :]
            return c
        lax.fori_loop(0, BR // 64, body, 0)

    def places(color):
        a, b, c = ORDERS[color]
        keep = [b + c, b, c, '']
        return [a + k for k in keep], keep

    seq = ([blk(color, places(color)[0][j]) for j in range(4) for color in range(NCOL)]
           + [blk(color, places(color)[1][j]) for j in range(4) for color in range(NCOL)])
    nb = len(seq)
    dcp, lcp = [], []
    for i, b in enumerate(seq):
        dcp.append(rdma(g_h.at[b * 2 + (1 - core)], rd.at[b], ds.at[i], dr.at[i], 'c'))
        lcp.append(pltpu.make_async_copy(g_h.at[b * 2 + core], acc.at[b], locsem.at[i]))
    for i in range(nb):
        dcp[i].start()
        lcp[i].start()

    def fold_core(i):
        dcp[i].wait_recv()
        lcp[i].wait()
        add(seq[i], rd.at[seq[i]])

    p1, p2, p3 = {}, {}, {}
    for j in range(4):
        for color in range(NCOL):
            i = j * NCOL + color
            fold_core(i)
            p1[j, color] = rdma(acc.at[seq[i]], r1.at[i], ps.at[i], pr.at[i], ORDERS[color][0])
            p1[j, color].start()
    base2, base3 = 4 * NCOL, 6 * NCOL

    def fold_kept(j, color):
        i = j * NCOL + color
        fold_core(4 * NCOL + i)
        p1[j, color].wait_recv()
        add(seq[4 * NCOL + i], r1.at[i])
        return seq[4 * NCOL + i]

    for j in range(2):
        for color in range(NCOL):
            b = fold_kept(j, color)
            i = j * NCOL + color
            p2[j, color] = rdma(acc.at[b], r2.at[i], ps.at[base2 + i], pr.at[base2 + i], ORDERS[color][1])
            p2[j, color].start()
    for color in range(NCOL):
        b = fold_kept(2, color)
        p2[0, color].wait_recv()
        add(b, r2.at[color])
        p3[color] = rdma(acc.at[b], r3.at[color], ps.at[base3 + color], pr.at[base3 + color], ORDERS[color][2])
        p3[color].start()
    last = {}
    for color in range(NCOL):
        last[color] = fold_kept(3, color)
        p2[1, color].wait_recv()
        add(last[color], r2.at[NCOL + color])

    def out_at(color, far, r0, n):
        yy = 1 - y if 'y' in far else y
        xx = 1 - x if 'x' in far else x
        return out.at[(color * 4 + yy * 2 + xx) * 2 + core, pl.ds(r0, n), :]

    ns_ = len(SPREAD)
    cps, g1, g2, g3 = [], {}, {}, {}

    def to_sibling(k, far, i):
        color, r0, n, _ = SPREAD[k]
        o = out_at(color, far, r0, n)
        cp = rdma(o, o, cs.at[i], cr.at[i], 'c')
        cp.start()
        cps.append(cp)

    for color in range(NCOL):
        p3[color].wait_recv()
        b = last[color]
        o_blk = (color * 4 + y * 2 + x) * 2 + core

        def body(i, c, b=b, o_blk=o_blk, color=color):
            r = pl.multiple_of(i * 64, 64)
            out[o_blk, pl.ds(r, 64), :] = acc[b, pl.ds(r, 64), :] + r3[color, pl.ds(r, 64), :]
            return c
        lax.fori_loop(0, BR // 64, body, 0)
        for k, (col, r0, n, ab) in enumerate(SPREAD):
            if col != color:
                continue
            o = out_at(color, '', r0, n)
            g1[k] = rdma(o, o, gs.at[k], gr.at[k], ab[0])
            g2[k] = rdma(o, o, gs.at[ns_ + k], gr.at[ns_ + k], ab[1])
            g1[k].start()
            g2[k].start()
    for k in range(ns_):
        to_sibling(k, '', k)
    for k, (color, r0, n, ab) in enumerate(SPREAD):
        g1[k].wait_recv()
        o = out_at(color, ab[0], r0, n)
        g3[k] = rdma(o, o, gs.at[2 * ns_ + k], gr.at[2 * ns_ + k], ab[1])
        g3[k].start()
        to_sibling(k, ab[0], ns_ + k)
    for k, (color, r0, n, ab) in enumerate(SPREAD):
        g2[k].wait_recv()
        to_sibling(k, ab[1], 2 * ns_ + k)
    for k, (color, r0, n, ab) in enumerate(SPREAD):
        g3[k].wait_recv()
        to_sibling(k, 'xy', 3 * ns_ + k)
    for cp in cps:
        cp.wait()
    for cp in dcp + list(p1.values()) + list(p2.values()) + list(p3.values()) + list(g1.values()) + list(g2.values()) + list(g3.values()):
        cp.wait_send()


def run_reduce(grad):
    nb = NCOL * 8
    V = pltpu.VMEM
    S = pltpu.SemaphoreType.DMA
    return pl.pallas_call(
        reduce_kernel,
        in_specs=[pl.BlockSpec(memory_space=pl.ANY)],
        out_specs=pl.BlockSpec(memory_space=pltpu.VMEM),
        out_shape=jax.ShapeDtypeStruct((nb, BR, GL), F32),
        scratch_shapes=[V((nb, BR, GL), F32), V((nb, BR, GL), F32), V((4 * NCOL, BR, GL), F32), V((2 * NCOL, BR, GL), F32), V((NCOL, BR, GL), F32),
                        S((nb,)), S((nb,)), S((nb,)), S((7 * NCOL,)), S((7 * NCOL,)), S((12,)), S((12,)), S((16,)), S((16,))],
        compiler_params=pltpu.CompilerParams(vmem_limit_bytes=60_000_000, collective_id=1, has_side_effects=True),
    )(grad.reshape(2 * nb, BR, GL))


def solution(mesh):
    spec_col, spec_row, spec_act, spec_rep = P(None, 'model'), P('model', None), P('data', None, None), P(None, None)

    def device_step(x_in, cot_out, step_emb, w_q, w_k, w_v, w_o, w_1, w_2):
        dx, grad = run_kernel(x_in, cot_out, step_emb, (w_q, w_k, w_v, w_o, w_1, w_2), x_in.shape[0] // 2)
        g = run_reduce(grad).reshape(GROWS, GL)

        def join(r0, n, k):
            return jnp.concatenate([g[r0 + n * i:r0 + n * (i + 1)] for i in range(k)], axis=1)

        return g[:512], g[512:1024], g[1024:1536], join(5632, 256, 2), join(1536, 512, 4), join(3584, 1024, 2), dx

    return jax.shard_map(device_step, mesh=mesh,
                         in_specs=(spec_act, spec_act, spec_rep, spec_col, spec_col, spec_col, spec_row, spec_col, spec_row),
                         out_specs=(spec_col, spec_col, spec_col, spec_row, spec_col, spec_row, spec_act),
                         check_vma=False)
```

```python
import functools

import jax
import jax.numpy as jnp
from jax import lax
from jax.experimental import pallas as pl
from jax.experimental.pallas import tpu as pltpu
from jax.sharding import PartitionSpec as P

F32, BF16 = jnp.float32, jnp.bfloat16
T, D, FF, H, E, L = 512, 512, 2048, 8, 64, 4
EPS = 1e-6
CEXP = E ** -0.5 * 1.4426950408889634
SCALE = E ** -0.5
GK0 = 0.7978845608028654
GK1 = 0.044715
R = 32
LN = 128


def dot_nn(a, b):
    return lax.dot_general(a, b, (((1,), (0,)), ((), ())), preferred_element_type=F32)


def dot_nt(a, b):
    return lax.dot_general(a, b, (((1,), (1,)), ((), ())), preferred_element_type=F32)


def rows(r, n=R):
    return pl.ds(r, n)


def wide(e):
    return jnp.concatenate([e] * (T // LN), axis=1)


def col_sum(tile_fn):
    accs = [None, None]
    for i, r in enumerate(range(0, D, R)):
        v = tile_fn(r)
        accs[i % 2] = v if accs[i % 2] is None else accs[i % 2] + v
    return jnp.sum(accs[0] + accs[1], axis=0, keepdims=True)


def rms_of(tile_fn):
    def sq(r):
        v = tile_fn(r)
        return v * v
    return lax.rsqrt(col_sum(sq) * (1.0 / D) + EPS)


def weave(*streams):
    total = max(len(s) for s in streams)
    done = [0] * len(streams)
    for t in range(total):
        for k, s in enumerate(streams):
            upto = -(-len(s) * (t + 1) // total)
            while done[k] < upto:
                s[done[k]]()
                done[k] += 1


def gelu_fwd(z):
    return z * jax.nn.sigmoid(z * (2 * GK0 + (2 * GK0 * GK1) * (z * z)))


def gelu_both(z):
    z2 = z * z
    s = jax.nn.sigmoid(z * (2 * GK0 + (2 * GK0 * GK1) * z2))
    w = z * (2 * GK0 + (6 * GK0 * GK1) * z2)
    return z * s, s * (1.0 + w * (1.0 - s))


def qrow(hd):
    return 768 * (hd // 4) + 64 * (hd % 4)


def pad_head(block, hh):
    zero = jnp.zeros_like(block)
    return jnp.concatenate([block, zero] if hh == 0 else [zero, block], axis=0)


def zip_pad(a, b):
    return [(a[i:i + 1], b[i:i + 1]) for i in range(max(len(a), len(b)))]


def max_cols(ref, cols):
    accs = [None] * 4
    for i, r in enumerate(range(0, T, 64)):
        v = ref[rows(r, 64), cols]
        accs[i % 4] = v if accs[i % 4] is None else jnp.maximum(accs[i % 4], v)
    m = jnp.maximum(jnp.maximum(accs[0], accs[1]), jnp.maximum(accs[2], accs[3]))
    return jnp.max(m, axis=0, keepdims=True)

GL, GROWS = 256, 6144


MESH_ID = pl.DeviceIdType.MESH
NW = 6


def other(i):
    return 1 - i


def kernel(nseq, x_ref, cot_ref, emb_ref, wq_h, wk_h, wv_h, wo_h, w1_h, w2_h,
           dx_h, grad_h,
           wqkv, wo, w1, w2, wqkvt, wot, w1t, w2t, gqkv, go, g1, g2,
           xs, qkv, ctx, ctxl, hs, zs, lse, rsc, u, m, act, dz, dn, dmid, dctx, dqkv, tmp, sbuf, lcol, dcol, dxs,
           embv, sem, zsend, zrecv, gsend, grecv, xloc, xsend, xrecv):
    step = pl.program_id(0)
    mi = lax.axis_index('model')
    di = lax.axis_index('data')
    core = di % 2
    zdev = {'model': 1 - mi, 'data': di}
    cdev = {'model': mi, 'data': di + 1 - 2 * core}

    def place(k, m, r0, n):
        if k < 3:
            return wqkv.at[pl.ds(r0, n), pl.ds(768 * m + 256 * k, 256)]
        if k == 3:
            return wo.at[pl.ds(256 * m + r0, n), :]
        if k == 4:
            return w1.at[pl.ds(r0, n), pl.ds(1024 * m, 1024)]
        return w2.at[pl.ds(1024 * m + r0, n), :]

    xx, yy = (di // 2) % 2, di // 4
    dev = {'x': {'model': mi, 'data': di + 2 - 4 * xx}, 'y': {'model': mi, 'data': di + 4 - 8 * yy}, 'z': zdev, 'c': cdev}

    w_hbm = (wq_h, wk_h, wv_h, wo_h, w1_h, w2_h)
    w_rows = (512, 512, 512, 256, 512, 1024)
    groups = ((0, 1, 2), (3,), (4,), (5,))

    def region(g, far, color):
        k = groups[g][0]
        pr = w_rows[k] // 8
        py = 1 - yy if 'y' in far else yy
        px = 1 - xx if 'x' in far else xx
        r0, n = (py * 4 + px * 2 + core) * pr, pr
        if color is not None:
            r0, n = r0 + color * (pr // 2), pr // 2
        if g == 0:
            return wqkv.at[pl.ds(r0, n), pl.ds(768 * (1 - mi), 768)]
        return place(k, 1 - mi, r0, n)

    def load_weights():
        barrier = pltpu.get_barrier_semaphore()
        for d in 'xyzc':
            pl.semaphore_signal(barrier, inc=1, device_id=dev[d], device_id_type=MESH_ID)
        pl.semaphore_wait(barrier, 4)
        zc, local, plane, sib = {}, [], {}, []

        def hand(g, far, color, d, i):
            o = region(g, far, color)
            cp = pltpu.make_async_remote_copy(o, o, gsend.at[g, i], grecv.at[g, i], device_id=dev[d], device_id_type=MESH_ID)
            cp.start()
            return cp

        for k in range(NW):
            pr = w_rows[k] // 8
            zc[k] = pltpu.make_async_remote_copy(w_hbm[k].at[pl.ds(di * pr, pr), :], place(k, mi, di * pr, pr),
                                                 zsend.at[k], zrecv.at[k], device_id=zdev, device_id_type=MESH_ID)
            zc[k].start()
        for k in range(NW):
            local.append(pltpu.make_async_copy(w_hbm[k], place(k, mi, 0, w_rows[k]), sem.at[k]))
            local[-1].start()

        def own(g):
            for k in groups[g]:
                zc[k].wait_recv()
            for color, ab in enumerate(('xy', 'yx')):
                plane[g, color, 0] = hand(g, '', color, ab[0], 3 * color)
                plane[g, color, 1] = hand(g, '', color, ab[1], 3 * color + 1)
            sib.append(hand(g, '', None, 'c', 6))

        def forward(g):
            for color, ab in enumerate(('xy', 'yx')):
                plane[g, color, 0].wait_recv()
                plane[g, color, 2] = hand(g, ab[0], color, ab[1], 3 * color + 2)
                sib.append(hand(g, ab[0], color, 'c', 7 + 3 * color))

        def finish(g):
            for color, ab in enumerate(('xy', 'yx')):
                plane[g, color, 1].wait_recv()
                sib.append(hand(g, ab[1], color, 'c', 8 + 3 * color))
            for color in range(2):
                plane[g, color, 2].wait_recv()
                sib.append(hand(g, 'xy', color, 'c', 9 + 3 * color))

        own(0)
        own(1)
        own(2)
        forward(0)
        forward(1)
        own(3)
        forward(2)
        finish(0)
        finish(1)
        forward(3)
        finish(2)
        finish(3)
        for k in range(NW):
            local[k].wait()
            zc[k].wait_send()
        for cp in plane.values():
            cp.wait_send()
        for cp in sib:
            cp.wait()

    @pl.when(step == 0)
    def _():
        load_weights()
        for l_ in range(L):
            embv[l_] = jnp.broadcast_to(emb_ref[l_:l_ + 1, :].astype(F32), (LN, D)).T
        for j in range(3):
            wqkvt[pl.ds(512 * j, 512), :] = wqkv[:, pl.ds(512 * j, 512)].T
        wot[...] = wo[...].T
        for j in range(4):
            w1t[pl.ds(512 * j, 512), :] = w1[:, pl.ds(512 * j, 512)].T
            w2t[:, pl.ds(512 * j, 512)] = w2[pl.ds(512 * j, 512), :].T
        gqkv[...] = jnp.zeros_like(gqkv)
        go[...] = jnp.zeros_like(go)
        g1[...] = jnp.zeros_like(g1)
        g2[...] = jnp.zeros_like(g2)

    xs[0] = x_ref[0].T
    half = [pl.ds(0, 256), pl.ds(256, 256)]

    def s_tile(l):
        return lambda r: xs[l, rows(r), :].astype(F32) + wide(embv[l, rows(r), :])

    def norm_into(dst, tile_fn, l, k, fresh):
        box = {}

        def stat():
            if fresh:
                box['r'] = rms_of(tile_fn)
                rsc[l, pl.ds(k, 1), :] = box['r']
            else:
                box['r'] = rsc[l, pl.ds(k, 1), :]

        def put(r):
            dst[rows(r), :] = (tile_fn(r) * box['r']).astype(BF16)

        return [stat] + [functools.partial(put, r) for r in range(0, D, R)]

    def pull_into(dst, base, tile_fn, dy, l, k):
        box = {}

        def stat():
            a = col_sum(lambda r: dy[rows(r), :].astype(F32) * tile_fn(r)) * (1.0 / D)
            rr = rsc[l, pl.ds(k, 1), :]
            box['r'] = rr
            box['a'] = rr * rr * rr * a

        def put(r):
            g = dy[rows(r), :].astype(F32)
            dst[rows(r), :] = (base[rows(r), :].astype(F32) + (box['r'] * g - tile_fn(r) * box['a'])).astype(BF16)

        return [stat] + [functools.partial(put, r) for r in range(0, D, R)]

    def run(stream):
        for f in stream:
            f()

    def h_tile(l):
        return lambda r: hs[l, rows(r), :].astype(F32)

    def fwd(l, carry):
        run(norm_into(u, s_tile(l), l, 0, True))
        for j in range(3):
            qkv[l, pl.ds(512 * j, 512), :] = dot_nn(wqkvt[pl.ds(512 * j, 512), :], u[...]).astype(BF16)

        kps = {}
        inv = {}

        def stage_a(hd):
            p, hh = divmod(hd, 2)

            def first():
                if hh == 0:
                    kps[p] = qkv[l, pl.ds(qrow(hd) + 256, 128), :].T

            def part(c):
                qp = pad_head(qkv[l, pl.ds(qrow(hd), 64), half[c]], hh)
                sbuf[hd % 2, :, half[c]] = dot_nn(kps[p], qp)

            return [first, lambda: part(0), lambda: part(1)]

        def stage_b(hd):
            sref, eref = sbuf.at[hd % 2], act.at[pl.ds(512 * (hd % 2), 512), :]

            def group(g):
                cols = half[g]
                mx = max_cols(sref, cols) * CEXP
                accs = [None, None]
                for i, r in enumerate(range(0, T, 64)):
                    e = jnp.exp2(sref[rows(r, 64), cols] * CEXP - mx)
                    accs[i % 2] = e if accs[i % 2] is None else accs[i % 2] + e
                    eref[rows(r, 64), cols] = e.astype(BF16)
                sm = jnp.sum(accs[0] + accs[1], axis=0, keepdims=True)
                lse[l, pl.ds(hd, 1), cols] = mx + jnp.log2(sm)
                inv[hd, g] = 1.0 / sm

            return [functools.partial(group, g) for g in range(2)]

        def stage_c(hd):
            def part(c):
                cn = dot_nn(qkv[l, pl.ds(qrow(hd) + 512, 64), :], act[pl.ds(512 * (hd % 2), 512), half[c]])
                cn = cn * inv[hd, c]
                hi = cn.astype(BF16)
                ctx[l, pl.ds(64 * hd, 64), half[c]] = hi
                ctxl[l, pl.ds(64 * hd, 64), half[c]] = (cn - hi.astype(F32)).astype(BF16)

            return [lambda: part(0), lambda: part(1)]

        run(stage_a(0))
        for hd in range(H + 1):
            mx = []
            for x_, y_ in zip_pad(stage_a(hd + 1) if hd + 1 < H else [], stage_c(hd - 1) if hd >= 1 else []):
                mx += x_ + y_
            va = stage_b(hd) if hd < H else []
            weave(mx, va)

        for c in range(2):
            o = dot_nn(wot[...], ctx[l, :, half[c]])
            for r in range(0, D, R):
                sx = xs[l, rows(r), half[c]].astype(F32) + jnp.concatenate([embv[l, rows(r), :]] * 2, axis=1)
                hs[l, rows(r), half[c]] = (sx + o[r:r + R]).astype(BF16)
        run(norm_into(m, h_tile(l), l, 1, True))

        def z_dot(j):
            def f(c):
                js = pl.ds(512 * j, 512)
                zs[l, js, half[c]] = dot_nn(w1t[js, :], m[:, half[c]]).astype(BF16)
            return [lambda: f(0), lambda: f(1)]

        def gelu_stream(j):
            def f(r, c):
                act[rows(r, 64), half[c]] = gelu_fwd(zs[l, rows(r, 64), half[c]].astype(F32)).astype(BF16)
            return [functools.partial(f, r, c) for r in range(512 * j, 512 * j + 512, 64) for c in range(2)]

        @pl.when(l < L - 1)
        def _():
            run(z_dot(0))
            for j in range(4):
                weave(z_dot(j + 1) if j < 3 else [], gelu_stream(j))
            for c in range(2):
                o = dot_nn(w2t[...], act[:, half[c]])
                for r in range(0, D, R):
                    xs[l + 1, rows(r), half[c]] = (hs[l, rows(r), half[c]].astype(F32) + o[r:r + R]).astype(BF16)

        @pl.when(l == L - 1)
        def _():
            for j in range(4):
                run(z_dot(j))
        return carry

    lax.fori_loop(0, L, fwd, 0)

    dn[...] = cot_ref[0].T

    def bwd(i, carry):
        l = L - 1 - i

        def dg_dot(j):
            def f(c):
                js = pl.ds(512 * j, 512)
                dz[js, half[c]] = dot_nn(w2[js, :], dn[:, half[c]]).astype(BF16)
            return [lambda: f(0), lambda: f(1)]

        def gelu_stream(j):
            def f(r, c):
                g, gp = gelu_both(zs[l, rows(r, 64), half[c]].astype(F32))
                act[rows(r, 64), half[c]] = g.astype(BF16)
                dz[rows(r, 64), half[c]] = (dz[rows(r, 64), half[c]].astype(F32) * gp).astype(BF16)
            return [functools.partial(f, r, c) for r in range(512 * j, 512 * j + 512, 64) for c in range(2)]

        def wgrad(j):
            js = pl.ds(512 * j, 512)

            def a(c):
                g2[js, half[c]] += dot_nt(act[js, :], dn[half[c], :])

            def b(c):
                jc = pl.ds(512 * j + 256 * c, 256)
                g1[:, jc] += dot_nt(m[...], dz[jc, :])
            return [lambda: a(0), lambda: a(1), lambda: b(0), lambda: b(1)]

        weave(dg_dot(0), norm_into(m, h_tile(l), l, 1, False))
        def dm_part(k0, k1, last):
            def f(c):
                p = dot_nn(w1[:, 512 * k0:512 * k1], dz[pl.ds(512 * k0, 512 * (k1 - k0)), half[c]])
                if k0 > 0:
                    p = sbuf[0, :, half[c]] + p
                if last:
                    tmp[:, half[c]] = p.astype(BF16)
                else:
                    sbuf[0, :, half[c]] = p
            return [lambda: f(0), lambda: f(1)]

        weave(dg_dot(1) + dg_dot(2) + dg_dot(3), gelu_stream(0))
        weave(wgrad(0), gelu_stream(1))
        weave(wgrad(1) + dm_part(0, 2, False), gelu_stream(2))
        weave(wgrad(2), gelu_stream(3))
        run(dm_part(2, 4, True))
        weave(wgrad(3), pull_into(dmid, dn, h_tile(l), tmp, l, 1))
        for c in range(2):
            dctx[:, half[c]] = dot_nn(wo[...], dmid[:, half[c]]).astype(BF16)

        qps, dcs = {}, {}

        def column(row):
            return jnp.broadcast_to(row, (LN, T)).T

        def stage_a(hd):
            p, hh = divmod(hd, 2)
            hsl = pl.ds(64 * hd, 64)

            def first():
                if hh == 0:
                    qps[p] = qkv[l, pl.ds(qrow(hd), 128), :].T
                    dcs[p] = dctx[pl.ds(64 * hd, 128), :].T
                c = ctx[l, hsl, :].astype(F32) + ctxl[l, hsl, :].astype(F32)
                dcol[hd % 2] = column(jnp.sum(dctx[hsl, :].astype(F32) * c, axis=0, keepdims=True))
                lcol[hd % 2] = column(lse[l, pl.ds(hd, 1), :])

            def s_part(c):
                kp = pad_head(qkv[l, pl.ds(qrow(hd) + 256, 64), half[c]], hh)
                sbuf[hd % 2, :, half[c]] = dot_nn(qps[p], kp)

            def p_part(c):
                vp = pad_head(qkv[l, pl.ds(qrow(hd) + 512, 64), half[c]], hh)
                dz[pl.ds(512 * (hd % 2), 512), half[c]] = dot_nn(dcs[p], vp).astype(BF16)

            return [first] + [functools.partial(f, c) for f in (s_part, p_part) for c in range(2)]

        def merge(xs_, ys_):
            out = []
            for i in range(max(len(xs_), len(ys_))):
                out += xs_[i:i + 1] + ys_[i:i + 1]
            return out

        def stage_b(hd):
            sl = 512 * (hd % 2)

            def group(g, r0):
                cols = half[g]
                for r in range(r0, r0 + 64, 64):
                    lc = lcol[hd % 2, rows(r, 64), :]
                    dc = dcol[hd % 2, rows(r, 64), :]
                    pr = jnp.exp2(sbuf[hd % 2, rows(r, 64), cols] * CEXP - jnp.concatenate([lc, lc], axis=1))
                    act[rows(sl + r, 64), cols] = pr.astype(BF16)
                    dp = dz[rows(sl + r, 64), cols].astype(F32)
                    act[rows(1024 + sl + r, 64), cols] = (pr * (dp - jnp.concatenate([dc, dc], axis=1))).astype(BF16)

            return [functools.partial(group, g, r0) for r0 in range(0, T, 64) for g in range(2)]

        def stage_c(hd):
            sl = 512 * (hd % 2)
            pb = act.at[pl.ds(sl, 512), :]
            db = act.at[pl.ds(1024 + sl, 512), :]
            hsl = pl.ds(64 * hd, 64)

            def f_v(c):
                dqkv[pl.ds(qrow(hd) + 512, 64), half[c]] = dot_nn(dctx[hsl, :], pb[:, half[c]]).astype(BF16)

            def f_k(c):
                dk = dot_nn(qkv[l, pl.ds(qrow(hd), 64), :], db[:, half[c]]) * SCALE
                dqkv[pl.ds(qrow(hd) + 256, 64), half[c]] = dk.astype(BF16)

            def f_q(c):
                dq = dot_nt(qkv[l, pl.ds(qrow(hd) + 256, 64), :], db[half[c], :]) * SCALE
                dqkv[pl.ds(qrow(hd), 64), half[c]] = dq.astype(BF16)

            return [functools.partial(f, c) for f in (f_v, f_k, f_q) for c in range(2)]

        def wo_grad(c):
            go[:, half[c]] += dot_nt(ctx[l], dmid[half[c], :])

        def qkv_grad(j):
            js = pl.ds(256 * j, 256)
            gqkv[:, js] += dot_nt(u[...], dqkv[js, :])

        wo_parts = [functools.partial(wo_grad, c) for c in range(2)]
        qkv_parts = [functools.partial(qkv_grad, j) for j in range(6)]
        u_norm = norm_into(u, s_tile(l), l, 0, False)
        run(stage_a(0))
        for hd in range(H + 1):
            ma = stage_a(hd + 1) if hd + 1 < H else []
            mc = stage_c(hd - 1) if hd >= 1 else wo_parts
            if hd == H:
                ma = qkv_parts[:3]
            va = stage_b(hd) if hd < H else []
            if hd == H - 1:
                va = va + u_norm
            weave(merge(mc, ma), va)

        for c in range(2):
            tmp[:, half[c]] = dot_nn(wqkv[...], dqkv[:, half[c]]).astype(BF16)
        weave(qkv_parts[3:], pull_into(dn, dmid, s_tile(l), tmp, l, 0))
        return carry

    lax.fori_loop(0, L, bwd, 0)
    slot = step % 2

    def dx_copies(s, at):
        here = dx_h.at[mi * nseq + s]
        loc = pltpu.make_async_copy(dxs.at[at], here, xloc.at[at])
        rem = pltpu.make_async_remote_copy(dxs.at[at], here, xsend.at[at], xrecv.at[s], device_id=zdev, device_id_type=MESH_ID)
        return loc, rem

    def dx_drain(s, at):
        loc, rem = dx_copies(s, at)
        loc.wait()
        rem.wait_send()

    @pl.when(step >= 2)
    def _():
        dx_drain(step - 2, slot)

    dxs[slot] = dn[...].T
    dx_copies(step, slot)[0].start()

    @pl.when(step < nseq - 1)
    def _():
        dx_copies(step, slot)[1].start()

    @pl.when(step == nseq - 1)
    def _():
        cps = []
        for m_ in range(2):
            g = grad_h.at[m_]
            for k in range(3):
                cps.append((gqkv.at[:, pl.ds(768 * m_ + 256 * k, 256)], g.at[pl.ds(512 * k, 512), :]))
            for k in range(4):
                cps.append((g1.at[:, pl.ds(1024 * m_ + 256 * k, 256)], g.at[pl.ds(1536 + 512 * k, 512), :]))
            for k in range(2):
                cps.append((g2.at[pl.ds(1024 * m_, 1024), pl.ds(256 * k, 256)], g.at[pl.ds(3584 + 1024 * k, 1024), :]))
            for k in range(2):
                cps.append((go.at[pl.ds(256 * m_, 256), pl.ds(256 * k, 256)], g.at[pl.ds(5632 + 256 * k, 256), :]))
        cps = [pltpu.make_async_copy(s, d, sem.at[i]) for i, (s, d) in enumerate(cps)]
        for c in cps:
            c.start()
        dx_drain(nseq - 2, (nseq - 2) % 2)
        dx_copies(nseq - 1, (nseq - 1) % 2)[0].wait()
        for s in range(nseq - 1):
            theirs = dx_h.at[(1 - mi) * nseq + s]
            pltpu.make_async_remote_copy(dxs.at[s % 2], theirs, xsend.at[s % 2], xrecv.at[s],
                                         device_id=zdev, device_id_type=MESH_ID).wait_recv()
        for c in cps:
            c.wait()


def run_kernel(x, cot, emb, ws, nseq):
    blk = pl.BlockSpec((1, T, D), lambda i: (lax.axis_index('model') * nseq + i, 0, 0))
    anyspec = pl.BlockSpec(memory_space=pl.ANY)
    V = pltpu.VMEM
    S = pltpu.SemaphoreType.DMA
    return pl.pallas_call(
        functools.partial(kernel, nseq),
        grid=(nseq,),
        in_specs=[blk, blk, pl.BlockSpec(memory_space=pltpu.VMEM)] + [anyspec] * NW,
        out_specs=[anyspec] * 2,
        out_shape=[jax.ShapeDtypeStruct((2 * nseq, T, D), BF16), jax.ShapeDtypeStruct((2, GROWS, GL), F32)],
        scratch_shapes=[V((D, 1536), BF16), V((D, D), BF16), V((D, FF), BF16), V((FF, D), BF16),
                        V((1536, D), BF16), V((D, D), BF16), V((FF, D), BF16), V((D, FF), BF16),
                        V((D, 1536), F32), V((D, D), F32), V((D, FF), F32), V((FF, D), F32),
                        V((L, D, T), BF16), V((L, 1536, T), BF16), V((L, D, T), BF16), V((L, D, T), BF16), V((L, D, T), BF16),
                        V((L, FF, T), BF16), V((L, H, T), F32), V((L, 2, T), F32), V((D, T), BF16), V((D, T), BF16), V((FF, T), BF16),
                        V((FF, T), BF16), V((D, T), BF16), V((D, T), BF16), V((D, T), BF16), V((1536, T), BF16), V((D, T), BF16),
                        V((2, T, T), F32), V((2, T, LN), F32), V((2, T, LN), F32), V((2, T, D), BF16),
                        V((L, D, LN), F32), S((22,)), S((NW,)), S((NW,)), S((4, 13)), S((4, 13)), S((2,)), S((2,)), S((nseq,))],
        compiler_params=pltpu.CompilerParams(dimension_semantics=("arbitrary",), vmem_limit_bytes=67_000_000,
                                             collective_id=0, has_side_effects=True),
    )(x, cot, emb, *ws)


NCOL = 3
BR = 256
GROWS = NCOL * 8 * BR
ORDERS = ('xyz', 'yzx', 'zxy')
SPREAD = ((0, 0, BR, 'xy'), (1, 0, BR, 'yx'), (2, 0, BR // 2, 'xy'), (2, BR // 2, BR // 2, 'yx'))


def reduce_kernel(g_h, dx_in, out, dx, acc, rd, r1, r2, r3, locsem, ds, dr, ps, pr, gs, gr, cs, cr, xs_, xr_):
    mi = lax.axis_index('model')
    di = lax.axis_index('data')
    core, x, y = di % 2, (di // 2) % 2, di // 4
    me = {'x': x, 'y': y, 'z': mi}
    dev = {'x': {'model': mi, 'data': di + 2 - 4 * x}, 'y': {'model': mi, 'data': di + 4 - 8 * y},
           'z': {'model': 1 - mi, 'data': di}, 'c': {'model': mi, 'data': di + 1 - 2 * core}}

    def rdma(src, dst, s, r, d):
        return pltpu.make_async_remote_copy(src, dst, s, r, device_id=dev[d], device_id_type=MESH_ID)

    barrier = pltpu.get_barrier_semaphore()
    for d in 'xyzc':
        pl.semaphore_signal(barrier, inc=1, device_id=dev[d], device_id_type=MESH_ID)
    pl.semaphore_wait(barrier, 4)

    def blk(color, far):
        pos = {ax: (1 - me[ax] if ax in far else me[ax]) for ax in 'xyz'}
        return (pos['z'] * NCOL + color) * 4 + pos['y'] * 2 + pos['x']

    def add(dst, src):
        def body(i, c):
            r = pl.multiple_of(i * 64, 64)
            acc[dst, pl.ds(r, 64), :] += src[pl.ds(r, 64), :]
            return c
        lax.fori_loop(0, BR // 64, body, 0)

    def places(color):
        a, b, c = ORDERS[color]
        keep = [b + c, b, c, '']
        return [a + k for k in keep], keep

    seq = ([blk(color, places(color)[0][j]) for j in range(4) for color in range(NCOL)]
           + [blk(color, places(color)[1][j]) for j in range(4) for color in range(NCOL)])
    nb = len(seq)
    dcp, lcp = [], []
    for i, b in enumerate(seq):
        dcp.append(rdma(g_h.at[b * 2 + (1 - core)], rd.at[b], ds.at[i], dr.at[i], 'c'))
        lcp.append(pltpu.make_async_copy(g_h.at[b * 2 + core], acc.at[b], locsem.at[i]))
    for i in range(nb):
        dcp[i].start()
        lcp[i].start()

    def fold_core(i):
        dcp[i].wait_recv()
        lcp[i].wait()
        add(seq[i], rd.at[seq[i]])

    p1, p2, p3 = {}, {}, {}
    for j in range(4):
        for color in range(NCOL):
            i = j * NCOL + color
            fold_core(i)
            p1[j, color] = rdma(acc.at[seq[i]], r1.at[i], ps.at[i], pr.at[i], ORDERS[color][0])
            p1[j, color].start()
    base2, base3 = 4 * NCOL, 6 * NCOL

    def fold_kept(j, color):
        i = j * NCOL + color
        fold_core(4 * NCOL + i)
        p1[j, color].wait_recv()
        add(seq[4 * NCOL + i], r1.at[i])
        return seq[4 * NCOL + i]

    for j in range(2):
        for color in range(NCOL):
            b = fold_kept(j, color)
            i = j * NCOL + color
            p2[j, color] = rdma(acc.at[b], r2.at[i], ps.at[base2 + i], pr.at[base2 + i], ORDERS[color][1])
            p2[j, color].start()
    for color in range(NCOL):
        b = fold_kept(2, color)
        p2[0, color].wait_recv()
        add(b, r2.at[color])
        p3[color] = rdma(acc.at[b], r3.at[color], ps.at[base3 + color], pr.at[base3 + color], ORDERS[color][2])
        p3[color].start()
    nseq = dx.shape[0] // 2
    mine, theirs = dx.at[mi * nseq + nseq - 1], dx.at[(1 - mi) * nseq + nseq - 1]
    dx_out = rdma(mine, mine, xs_.at[0], xr_.at[0], 'z')
    dx_out.start()
    last = {}
    for color in range(NCOL):
        last[color] = fold_kept(3, color)
        p2[1, color].wait_recv()
        add(last[color], r2.at[NCOL + color])

    def out_at(color, far, r0, n):
        yy = 1 - y if 'y' in far else y
        xx = 1 - x if 'x' in far else x
        return out.at[(color * 4 + yy * 2 + xx) * 2 + core, pl.ds(r0, n), :]

    ns_ = len(SPREAD)
    cps, g1, g2, g3 = [], {}, {}, {}

    def to_sibling(k, far, i):
        color, r0, n, _ = SPREAD[k]
        o = out_at(color, far, r0, n)
        cp = rdma(o, o, cs.at[i], cr.at[i], 'c')
        cp.start()
        cps.append(cp)

    for color in range(NCOL):
        p3[color].wait_recv()
        b = last[color]
        o_blk = (color * 4 + y * 2 + x) * 2 + core

        def body(i, c, b=b, o_blk=o_blk, color=color):
            r = pl.multiple_of(i * 64, 64)
            out[o_blk, pl.ds(r, 64), :] = acc[b, pl.ds(r, 64), :] + r3[color, pl.ds(r, 64), :]
            return c
        lax.fori_loop(0, BR // 64, body, 0)
        for k, (col, r0, n, ab) in enumerate(SPREAD):
            if col != color:
                continue
            o = out_at(color, '', r0, n)
            g1[k] = rdma(o, o, gs.at[k], gr.at[k], ab[0])
            g2[k] = rdma(o, o, gs.at[ns_ + k], gr.at[ns_ + k], ab[1])
            g1[k].start()
            g2[k].start()
    for k in range(ns_):
        to_sibling(k, '', k)
    for k, (color, r0, n, ab) in enumerate(SPREAD):
        g1[k].wait_recv()
        o = out_at(color, ab[0], r0, n)
        g3[k] = rdma(o, o, gs.at[2 * ns_ + k], gr.at[2 * ns_ + k], ab[1])
        g3[k].start()
        to_sibling(k, ab[0], ns_ + k)
    for k, (color, r0, n, ab) in enumerate(SPREAD):
        g2[k].wait_recv()
        to_sibling(k, ab[1], 2 * ns_ + k)
    for k, (color, r0, n, ab) in enumerate(SPREAD):
        g3[k].wait_recv()
        to_sibling(k, 'xy', 3 * ns_ + k)
    for cp in cps:
        cp.wait()
    dx_out.wait_send()
    rdma(theirs, theirs, xs_.at[0], xr_.at[0], 'z').wait_recv()
    for cp in dcp + list(p1.values()) + list(p2.values()) + list(p3.values()) + list(g1.values()) + list(g2.values()) + list(g3.values()):
        cp.wait_send()


def run_reduce(grad, dx):
    nb = NCOL * 8
    V = pltpu.VMEM
    S = pltpu.SemaphoreType.DMA
    return pl.pallas_call(
        reduce_kernel,
        in_specs=[pl.BlockSpec(memory_space=pl.ANY)] * 2,
        out_specs=[pl.BlockSpec(memory_space=pltpu.VMEM), pl.BlockSpec(memory_space=pl.ANY)],
        out_shape=[jax.ShapeDtypeStruct((nb, BR, GL), F32), jax.ShapeDtypeStruct(dx.shape, dx.dtype)],
        scratch_shapes=[V((nb, BR, GL), F32), V((nb, BR, GL), F32), V((4 * NCOL, BR, GL), F32), V((2 * NCOL, BR, GL), F32), V((NCOL, BR, GL), F32),
                        S((nb,)), S((nb,)), S((nb,)), S((7 * NCOL,)), S((7 * NCOL,)), S((12,)), S((12,)), S((16,)), S((16,)), S((1,)), S((1,))],
        input_output_aliases={1: 1},
        compiler_params=pltpu.CompilerParams(vmem_limit_bytes=60_000_000, collective_id=1, has_side_effects=True),
    )(grad.reshape(2 * nb, BR, GL), dx)


def solution(mesh):
    spec_col, spec_row, spec_act, spec_rep = P(None, 'model'), P('model', None), P('data', None, None), P(None, None)

    def device_step(x_in, cot_out, step_emb, w_q, w_k, w_v, w_o, w_1, w_2):
        dx, grad = run_kernel(x_in, cot_out, step_emb, (w_q, w_k, w_v, w_o, w_1, w_2), x_in.shape[0] // 2)
        g, dx = run_reduce(grad, dx)
        g = g.reshape(GROWS, GL)

        def join(r0, n, k):
            return jnp.concatenate([g[r0 + n * i:r0 + n * (i + 1)] for i in range(k)], axis=1)

        return g[:512], g[512:1024], g[1024:1536], join(5632, 256, 2), join(1536, 512, 4), join(3584, 1024, 2), dx

    return jax.shard_map(device_step, mesh=mesh,
                         in_specs=(spec_act, spec_act, spec_rep, spec_col, spec_col, spec_col, spec_row, spec_col, spec_row),
                         out_specs=(spec_col, spec_col, spec_col, spec_row, spec_col, spec_row, spec_act),
                         check_vma=False)
```

```python
import functools

import jax
import jax.numpy as jnp
from jax import lax
from jax.experimental import pallas as pl
from jax.experimental.pallas import tpu as pltpu
from jax.sharding import PartitionSpec as P

F32, BF16 = jnp.float32, jnp.bfloat16
T, D, FF, H, E, L = 512, 512, 2048, 8, 64, 4
EPS = 1e-6
CEXP = E ** -0.5 * 1.4426950408889634
SCALE = E ** -0.5
GK0 = 0.7978845608028654
GK1 = 0.044715
R = 32
LN = 128


def dot_nn(a, b):
    return lax.dot_general(a, b, (((1,), (0,)), ((), ())), preferred_element_type=F32)


def dot_nt(a, b):
    return lax.dot_general(a, b, (((1,), (1,)), ((), ())), preferred_element_type=F32)


def rows(r, n=R):
    return pl.ds(r, n)


def wide(e):
    return jnp.concatenate([e] * (T // LN), axis=1)


def col_sum(tile_fn):
    accs = [None, None]
    for i, r in enumerate(range(0, D, R)):
        v = tile_fn(r)
        accs[i % 2] = v if accs[i % 2] is None else accs[i % 2] + v
    return jnp.sum(accs[0] + accs[1], axis=0, keepdims=True)


def rms_of(tile_fn):
    def sq(r):
        v = tile_fn(r)
        return v * v
    return lax.rsqrt(col_sum(sq) * (1.0 / D) + EPS)


def weave(*streams):
    total = max(len(s) for s in streams)
    done = [0] * len(streams)
    for t in range(total):
        for k, s in enumerate(streams):
            upto = -(-len(s) * (t + 1) // total)
            while done[k] < upto:
                s[done[k]]()
                done[k] += 1


def gelu_fwd(z):
    return z * jax.nn.sigmoid(z * (2 * GK0 + (2 * GK0 * GK1) * (z * z)))


def gelu_both(z):
    z2 = z * z
    s = jax.nn.sigmoid(z * (2 * GK0 + (2 * GK0 * GK1) * z2))
    w = z * (2 * GK0 + (6 * GK0 * GK1) * z2)
    return z * s, s * (1.0 + w * (1.0 - s))


def qrow(hd):
    return 768 * (hd // 4) + 64 * (hd % 4)


def pad_head(block, hh):
    zero = jnp.zeros_like(block)
    return jnp.concatenate([block, zero] if hh == 0 else [zero, block], axis=0)


def zip_pad(a, b):
    return [(a[i:i + 1], b[i:i + 1]) for i in range(max(len(a), len(b)))]


def max_cols(ref, cols):
    accs = [None] * 4
    for i, r in enumerate(range(0, T, 64)):
        v = ref[rows(r, 64), cols]
        accs[i % 4] = v if accs[i % 4] is None else jnp.maximum(accs[i % 4], v)
    m = jnp.maximum(jnp.maximum(accs[0], accs[1]), jnp.maximum(accs[2], accs[3]))
    return jnp.max(m, axis=0, keepdims=True)

GL, GROWS = 256, 6144


MESH_ID = pl.DeviceIdType.MESH
NW = 6


def other(i):
    return 1 - i


def kernel(nseq, x_ref, cot_ref, emb_ref, wq_h, wk_h, wv_h, wo_h, w1_h, w2_h,
           dx_h, grad_h,
           wqkv, wo, w1, w2, wqkvt, wot, w1t, w2t, gqkv, go, g1, g2,
           xs, qkv, ctx, ctxl, hs, zs, lse, rsc, u, m, act, dz, dn, dmid, dctx, dqkv, tmp, sbuf, lcol, dcol, dxs,
           embv, sem, zsend, zrecv, gsend, grecv, xloc, xsend, xrecv):
    step = pl.program_id(0)
    mi = lax.axis_index('model')
    di = lax.axis_index('data')
    core = di % 2
    zdev = {'model': 1 - mi, 'data': di}
    cdev = {'model': mi, 'data': di + 1 - 2 * core}

    def place(k, m, r0, n):
        if k < 3:
            return wqkv.at[pl.ds(r0, n), pl.ds(768 * m + 256 * k, 256)]
        if k == 3:
            return wo.at[pl.ds(256 * m + r0, n), :]
        if k == 4:
            return w1.at[pl.ds(r0, n), pl.ds(1024 * m, 1024)]
        return w2.at[pl.ds(1024 * m + r0, n), :]

    xx, yy = (di // 2) % 2, di // 4
    dev = {'x': {'model': mi, 'data': di + 2 - 4 * xx}, 'y': {'model': mi, 'data': di + 4 - 8 * yy}, 'z': zdev, 'c': cdev}

    w_hbm = (wq_h, wk_h, wv_h, wo_h, w1_h, w2_h)
    w_rows = (512, 512, 512, 256, 512, 1024)
    groups = ((0, 1, 2), (3,), (4,), (5,))

    def region(g, far, color):
        k = groups[g][0]
        pr = w_rows[k] // 8
        py = 1 - yy if 'y' in far else yy
        px = 1 - xx if 'x' in far else xx
        r0, n = (py * 4 + px * 2 + core) * pr, pr
        if color is not None:
            r0, n = r0 + color * (pr // 2), pr // 2
        if g == 0:
            return wqkv.at[pl.ds(r0, n), pl.ds(768 * (1 - mi), 768)]
        return place(k, 1 - mi, r0, n)

    def load_weights():
        barrier = pltpu.get_barrier_semaphore()
        for d in 'xyzc':
            pl.semaphore_signal(barrier, inc=1, device_id=dev[d], device_id_type=MESH_ID)
        pl.semaphore_wait(barrier, 4)
        zc, local, plane, sib = {}, [], {}, []

        def hand(g, far, color, d, i):
            o = region(g, far, color)
            cp = pltpu.make_async_remote_copy(o, o, gsend.at[g, i], grecv.at[g, i], device_id=dev[d], device_id_type=MESH_ID)
            cp.start()
            return cp

        for k in range(NW):
            pr = w_rows[k] // 8
            zc[k] = pltpu.make_async_remote_copy(w_hbm[k].at[pl.ds(di * pr, pr), :], place(k, mi, di * pr, pr),
                                                 zsend.at[k], zrecv.at[k], device_id=zdev, device_id_type=MESH_ID)
            zc[k].start()
        for k in range(NW):
            local.append(pltpu.make_async_copy(w_hbm[k], place(k, mi, 0, w_rows[k]), sem.at[k]))
            local[-1].start()

        def own(g):
            for k in groups[g]:
                zc[k].wait_recv()
            for color, ab in enumerate(('xy', 'yx')):
                plane[g, color, 0] = hand(g, '', color, ab[0], 3 * color)
                plane[g, color, 1] = hand(g, '', color, ab[1], 3 * color + 1)
            sib.append(hand(g, '', None, 'c', 6))

        def forward(g):
            for color, ab in enumerate(('xy', 'yx')):
                plane[g, color, 0].wait_recv()
                plane[g, color, 2] = hand(g, ab[0], color, ab[1], 3 * color + 2)
                sib.append(hand(g, ab[0], color, 'c', 7 + 3 * color))

        def finish(g):
            for color, ab in enumerate(('xy', 'yx')):
                plane[g, color, 1].wait_recv()
                sib.append(hand(g, ab[1], color, 'c', 8 + 3 * color))
            for color in range(2):
                plane[g, color, 2].wait_recv()
                sib.append(hand(g, 'xy', color, 'c', 9 + 3 * color))

        own(0)
        own(1)
        own(2)
        forward(0)
        forward(1)
        own(3)
        forward(2)
        finish(0)
        finish(1)
        forward(3)
        finish(2)
        finish(3)
        for k in range(NW):
            local[k].wait()
            zc[k].wait_send()
        for cp in plane.values():
            cp.wait_send()
        for cp in sib:
            cp.wait()

    @pl.when(step == 0)
    def _():
        load_weights()
        for l_ in range(L):
            embv[l_] = jnp.broadcast_to(emb_ref[l_:l_ + 1, :].astype(F32), (LN, D)).T
        for j in range(3):
            wqkvt[pl.ds(512 * j, 512), :] = wqkv[:, pl.ds(512 * j, 512)].T
        wot[...] = wo[...].T
        for j in range(4):
            w1t[pl.ds(512 * j, 512), :] = w1[:, pl.ds(512 * j, 512)].T
            w2t[:, pl.ds(512 * j, 512)] = w2[pl.ds(512 * j, 512), :].T
        gqkv[...] = jnp.zeros_like(gqkv)
        go[...] = jnp.zeros_like(go)
        g1[...] = jnp.zeros_like(g1)
        g2[...] = jnp.zeros_like(g2)

    xs[0] = x_ref[0].T
    half = [pl.ds(0, 256), pl.ds(256, 256)]

    def s_tile(l, cols=slice(None)):
        w = 4 if cols == slice(None) else 2
        return lambda r: xs[l, rows(r), cols].astype(F32) + jnp.concatenate([embv[l, rows(r), :]] * w, axis=1)

    def norm_into(dst, tile_fn, l, k, fresh, cols=slice(None)):
        box = {}

        def stat():
            if fresh:
                box['r'] = rms_of(tile_fn)
                rsc[l, pl.ds(k, 1), cols] = box['r']
            else:
                box['r'] = rsc[l, pl.ds(k, 1), cols]

        def put(r):
            dst[rows(r), cols] = (tile_fn(r) * box['r']).astype(BF16)

        return [stat] + [functools.partial(put, r) for r in range(0, D, R)]

    def pull_into(dst, base, tile_of, dy, l, k):
        out = []
        for cols in half:
            tile_fn = tile_of(l, cols)
            box = {}

            def stat(cols=cols, tile_fn=tile_fn, box=box):
                a = col_sum(lambda r: dy[rows(r), cols].astype(F32) * tile_fn(r)) * (1.0 / D)
                rr = rsc[l, pl.ds(k, 1), cols]
                box['r'] = rr
                box['a'] = rr * rr * rr * a

            def put(r, cols=cols, tile_fn=tile_fn, box=box):
                g = dy[rows(r), cols].astype(F32)
                dst[rows(r), cols] = (base[rows(r), cols].astype(F32) + (box['r'] * g - tile_fn(r) * box['a'])).astype(BF16)

            out += [stat] + [functools.partial(put, r) for r in range(0, D, R)]
        return out

    def run(stream):
        for f in stream:
            f()

    def h_tile(l, cols=slice(None)):
        return lambda r: hs[l, rows(r), cols].astype(F32)

    def fwd(l, carry):
        for c in range(2):
            run(norm_into(u, s_tile(l, half[c]), l, 0, True, half[c]))
        for j in range(3):
            qkv[l, pl.ds(512 * j, 512), :] = dot_nn(wqkvt[pl.ds(512 * j, 512), :], u[...]).astype(BF16)

        kps = {}
        inv = {}

        def stage_a(hd):
            p, hh = divmod(hd, 2)

            def first():
                if hh == 0:
                    kps[p] = qkv[l, pl.ds(qrow(hd) + 256, 128), :].T

            def part(c):
                qp = pad_head(qkv[l, pl.ds(qrow(hd), 64), half[c]], hh)
                sbuf[hd % 2, :, half[c]] = dot_nn(kps[p], qp)

            return [first, lambda: part(0), lambda: part(1)]

        def stage_b(hd):
            sref, eref = sbuf.at[hd % 2], act.at[pl.ds(512 * (hd % 2), 512), :]

            def group(g):
                cols = half[g]
                mx = max_cols(sref, cols) * CEXP
                accs = [None, None]
                for i, r in enumerate(range(0, T, 64)):
                    e = jnp.exp2(sref[rows(r, 64), cols] * CEXP - mx)
                    accs[i % 2] = e if accs[i % 2] is None else accs[i % 2] + e
                    eref[rows(r, 64), cols] = e.astype(BF16)
                sm = jnp.sum(accs[0] + accs[1], axis=0, keepdims=True)
                lse[l, pl.ds(hd, 1), cols] = mx + jnp.log2(sm)
                inv[hd, g] = 1.0 / sm

            return [functools.partial(group, g) for g in range(2)]

        def stage_c(hd):
            def part(c):
                cn = dot_nn(qkv[l, pl.ds(qrow(hd) + 512, 64), :], act[pl.ds(512 * (hd % 2), 512), half[c]])
                cn = cn * inv[hd, c]
                hi = cn.astype(BF16)
                ctx[l, pl.ds(64 * hd, 64), half[c]] = hi
                ctxl[l, pl.ds(64 * hd, 64), half[c]] = (cn - hi.astype(F32)).astype(BF16)

            return [lambda: part(0), lambda: part(1)]

        run(stage_a(0))
        for hd in range(H + 1):
            mx = []
            for x_, y_ in zip_pad(stage_a(hd + 1) if hd + 1 < H else [], stage_c(hd - 1) if hd >= 1 else []):
                mx += x_ + y_
            va = stage_b(hd) if hd < H else []
            weave(mx, va)

        for c in range(2):
            o = dot_nn(wot[...], ctx[l, :, half[c]])
            for r in range(0, D, R):
                sx = xs[l, rows(r), half[c]].astype(F32) + jnp.concatenate([embv[l, rows(r), :]] * 2, axis=1)
                hs[l, rows(r), half[c]] = (sx + o[r:r + R]).astype(BF16)
        for c in range(2):
            run(norm_into(m, h_tile(l, half[c]), l, 1, True, half[c]))

        def z_dot(j):
            def f(c):
                js = pl.ds(512 * j, 512)
                zs[l, js, half[c]] = dot_nn(w1t[js, :], m[:, half[c]]).astype(BF16)
            return [lambda: f(0), lambda: f(1)]

        def gelu_stream(j):
            def f(r, c):
                act[rows(r, 64), half[c]] = gelu_fwd(zs[l, rows(r, 64), half[c]].astype(F32)).astype(BF16)
            return [functools.partial(f, r, c) for r in range(512 * j, 512 * j + 512, 64) for c in range(2)]

        @pl.when(l < L - 1)
        def _():
            run(z_dot(0))
            for j in range(4):
                weave(z_dot(j + 1) if j < 3 else [], gelu_stream(j))
            for c in range(2):
                o = dot_nn(w2t[...], act[:, half[c]])
                for r in range(0, D, R):
                    xs[l + 1, rows(r), half[c]] = (hs[l, rows(r), half[c]].astype(F32) + o[r:r + R]).astype(BF16)

        @pl.when(l == L - 1)
        def _():
            for j in range(4):
                run(z_dot(j))
        return carry

    lax.fori_loop(0, L, fwd, 0)

    dn[...] = cot_ref[0].T

    def bwd(i, carry):
        l = L - 1 - i

        def dg_dot(j):
            def f(c):
                js = pl.ds(512 * j, 512)
                dz[js, half[c]] = dot_nn(w2[js, :], dn[:, half[c]]).astype(BF16)
            return [lambda: f(0), lambda: f(1)]

        def gelu_stream(j):
            def f(r, c):
                g, gp = gelu_both(zs[l, rows(r, 64), half[c]].astype(F32))
                act[rows(r, 64), half[c]] = g.astype(BF16)
                dz[rows(r, 64), half[c]] = (dz[rows(r, 64), half[c]].astype(F32) * gp).astype(BF16)
            return [functools.partial(f, r, c) for r in range(512 * j, 512 * j + 512, 64) for c in range(2)]

        def wgrad(j):
            js = pl.ds(512 * j, 512)

            def a(c):
                g2[js, half[c]] += dot_nt(act[js, :], dn[half[c], :])

            def b(c):
                jc = pl.ds(512 * j + 256 * c, 256)
                g1[:, jc] += dot_nt(m[...], dz[jc, :])
            return [lambda: a(0), lambda: a(1), lambda: b(0), lambda: b(1)]

        weave(dg_dot(0), norm_into(m, h_tile(l, half[0]), l, 1, False, half[0]) + norm_into(m, h_tile(l, half[1]), l, 1, False, half[1]))
        def dm_part(k0, k1, last):
            def f(c):
                p = dot_nn(w1[:, 512 * k0:512 * k1], dz[pl.ds(512 * k0, 512 * (k1 - k0)), half[c]])
                if k0 > 0:
                    p = sbuf[0, :, half[c]] + p
                if last:
                    tmp[:, half[c]] = p.astype(BF16)
                else:
                    sbuf[0, :, half[c]] = p
            return [lambda: f(0), lambda: f(1)]

        weave(dg_dot(1) + dg_dot(2) + dg_dot(3), gelu_stream(0))
        weave(wgrad(0), gelu_stream(1))
        weave(wgrad(1) + dm_part(0, 2, False), gelu_stream(2))
        weave(wgrad(2), gelu_stream(3))
        run(dm_part(2, 4, True))
        weave(wgrad(3), pull_into(dmid, dn, h_tile, tmp, l, 1))
        for c in range(2):
            dctx[:, half[c]] = dot_nn(wo[...], dmid[:, half[c]]).astype(BF16)

        qps, dcs = {}, {}

        def column(row):
            return jnp.broadcast_to(row, (LN, T)).T

        def stage_a(hd):
            p, hh = divmod(hd, 2)
            hsl = pl.ds(64 * hd, 64)

            def first():
                if hh == 0:
                    qps[p] = qkv[l, pl.ds(qrow(hd), 128), :].T
                    dcs[p] = dctx[pl.ds(64 * hd, 128), :].T
                c = ctx[l, hsl, :].astype(F32) + ctxl[l, hsl, :].astype(F32)
                dcol[hd % 2] = column(jnp.sum(dctx[hsl, :].astype(F32) * c, axis=0, keepdims=True))
                lcol[hd % 2] = column(lse[l, pl.ds(hd, 1), :])

            def s_part(c):
                kp = pad_head(qkv[l, pl.ds(qrow(hd) + 256, 64), half[c]], hh)
                sbuf[hd % 2, :, half[c]] = dot_nn(qps[p], kp)

            def p_part(c):
                vp = pad_head(qkv[l, pl.ds(qrow(hd) + 512, 64), half[c]], hh)
                dz[pl.ds(512 * (hd % 2), 512), half[c]] = dot_nn(dcs[p], vp).astype(BF16)

            return [first] + [functools.partial(f, c) for f in (s_part, p_part) for c in range(2)]

        def merge(xs_, ys_):
            out = []
            for i in range(max(len(xs_), len(ys_))):
                out += xs_[i:i + 1] + ys_[i:i + 1]
            return out

        def stage_b(hd):
            sl = 512 * (hd % 2)

            def group(g, r0):
                cols = half[g]
                for r in range(r0, r0 + 64, 64):
                    lc = lcol[hd % 2, rows(r, 64), :]
                    dc = dcol[hd % 2, rows(r, 64), :]
                    pr = jnp.exp2(sbuf[hd % 2, rows(r, 64), cols] * CEXP - jnp.concatenate([lc, lc], axis=1))
                    act[rows(sl + r, 64), cols] = pr.astype(BF16)
                    dp = dz[rows(sl + r, 64), cols].astype(F32)
                    act[rows(1024 + sl + r, 64), cols] = (pr * (dp - jnp.concatenate([dc, dc], axis=1))).astype(BF16)

            return [functools.partial(group, g, r0) for r0 in range(0, T, 64) for g in range(2)]

        def stage_c(hd):
            sl = 512 * (hd % 2)
            pb = act.at[pl.ds(sl, 512), :]
            db = act.at[pl.ds(1024 + sl, 512), :]
            hsl = pl.ds(64 * hd, 64)

            def f_v(c):
                dqkv[pl.ds(qrow(hd) + 512, 64), half[c]] = dot_nn(dctx[hsl, :], pb[:, half[c]]).astype(BF16)

            def f_k(c):
                dk = dot_nn(qkv[l, pl.ds(qrow(hd), 64), :], db[:, half[c]]) * SCALE
                dqkv[pl.ds(qrow(hd) + 256, 64), half[c]] = dk.astype(BF16)

            def f_q(c):
                dq = dot_nt(qkv[l, pl.ds(qrow(hd) + 256, 64), :], db[half[c], :]) * SCALE
                dqkv[pl.ds(qrow(hd), 64), half[c]] = dq.astype(BF16)

            return [functools.partial(f, c) for f in (f_v, f_k, f_q) for c in range(2)]

        def wo_grad(c):
            go[:, half[c]] += dot_nt(ctx[l], dmid[half[c], :])

        def qkv_grad(j):
            js = pl.ds(256 * j, 256)
            gqkv[:, js] += dot_nt(u[...], dqkv[js, :])

        wo_parts = [functools.partial(wo_grad, c) for c in range(2)]
        qkv_parts = [functools.partial(qkv_grad, j) for j in range(6)]
        u_norm = sum([norm_into(u, s_tile(l, cc), l, 0, False, cc) for cc in half], [])
        run(stage_a(0))
        for hd in range(H + 1):
            ma = stage_a(hd + 1) if hd + 1 < H else []
            mc = stage_c(hd - 1) if hd >= 1 else wo_parts
            if hd == H:
                ma = qkv_parts[:3]
            va = stage_b(hd) if hd < H else []
            if hd == H - 1:
                va = va + u_norm
            weave(merge(mc, ma), va)

        for c in range(2):
            tmp[:, half[c]] = dot_nn(wqkv[...], dqkv[:, half[c]]).astype(BF16)
        weave(qkv_parts[3:], pull_into(dn, dmid, s_tile, tmp, l, 0))
        return carry

    lax.fori_loop(0, L, bwd, 0)
    slot = step % 2

    def dx_copies(s, at):
        here = dx_h.at[mi * nseq + s]
        loc = pltpu.make_async_copy(dxs.at[at], here, xloc.at[at])
        rem = pltpu.make_async_remote_copy(dxs.at[at], here, xsend.at[at], xrecv.at[s], device_id=zdev, device_id_type=MESH_ID)
        return loc, rem

    def dx_drain(s, at):
        loc, rem = dx_copies(s, at)
        loc.wait()
        rem.wait_send()

    @pl.when(step >= 2)
    def _():
        dx_drain(step - 2, slot)

    dxs[slot] = dn[...].T
    dx_copies(step, slot)[0].start()

    @pl.when(step < nseq - 1)
    def _():
        dx_copies(step, slot)[1].start()

    @pl.when(step == nseq - 1)
    def _():
        cps = []
        for m_ in range(2):
            g = grad_h.at[m_]
            for k in range(3):
                cps.append((gqkv.at[:, pl.ds(768 * m_ + 256 * k, 256)], g.at[pl.ds(512 * k, 512), :]))
            for k in range(4):
                cps.append((g1.at[:, pl.ds(1024 * m_ + 256 * k, 256)], g.at[pl.ds(1536 + 512 * k, 512), :]))
            for k in range(2):
                cps.append((g2.at[pl.ds(1024 * m_, 1024), pl.ds(256 * k, 256)], g.at[pl.ds(3584 + 1024 * k, 1024), :]))
            for k in range(2):
                cps.append((go.at[pl.ds(256 * m_, 256), pl.ds(256 * k, 256)], g.at[pl.ds(5632 + 256 * k, 256), :]))
        cps = [pltpu.make_async_copy(s, d, sem.at[i]) for i, (s, d) in enumerate(cps)]
        for c in cps:
            c.start()
        dx_drain(nseq - 2, (nseq - 2) % 2)
        dx_copies(nseq - 1, (nseq - 1) % 2)[0].wait()
        for s in range(nseq - 1):
            theirs = dx_h.at[(1 - mi) * nseq + s]
            pltpu.make_async_remote_copy(dxs.at[s % 2], theirs, xsend.at[s % 2], xrecv.at[s],
                                         device_id=zdev, device_id_type=MESH_ID).wait_recv()
        for c in cps:
            c.wait()


def run_kernel(x, cot, emb, ws, nseq):
    blk = pl.BlockSpec((1, T, D), lambda i: (lax.axis_index('model') * nseq + i, 0, 0))
    anyspec = pl.BlockSpec(memory_space=pl.ANY)
    V = pltpu.VMEM
    S = pltpu.SemaphoreType.DMA
    return pl.pallas_call(
        functools.partial(kernel, nseq),
        grid=(nseq,),
        in_specs=[blk, blk, pl.BlockSpec(memory_space=pltpu.VMEM)] + [anyspec] * NW,
        out_specs=[anyspec] * 2,
        out_shape=[jax.ShapeDtypeStruct((2 * nseq, T, D), BF16), jax.ShapeDtypeStruct((2, GROWS, GL), F32)],
        scratch_shapes=[V((D, 1536), BF16), V((D, D), BF16), V((D, FF), BF16), V((FF, D), BF16),
                        V((1536, D), BF16), V((D, D), BF16), V((FF, D), BF16), V((D, FF), BF16),
                        V((D, 1536), F32), V((D, D), F32), V((D, FF), F32), V((FF, D), F32),
                        V((L, D, T), BF16), V((L, 1536, T), BF16), V((L, D, T), BF16), V((L, D, T), BF16), V((L, D, T), BF16),
                        V((L, FF, T), BF16), V((L, H, T), F32), V((L, 2, T), F32), V((D, T), BF16), V((D, T), BF16), V((FF, T), BF16),
                        V((FF, T), BF16), V((D, T), BF16), V((D, T), BF16), V((D, T), BF16), V((1536, T), BF16), V((D, T), BF16),
                        V((2, T, T), F32), V((2, T, LN), F32), V((2, T, LN), F32), V((2, T, D), BF16),
                        V((L, D, LN), F32), S((22,)), S((NW,)), S((NW,)), S((4, 13)), S((4, 13)), S((2,)), S((2,)), S((nseq,))],
        compiler_params=pltpu.CompilerParams(dimension_semantics=("arbitrary",), vmem_limit_bytes=67_000_000,
                                             collective_id=0, has_side_effects=True),
    )(x, cot, emb, *ws)


NCOL = 3
BR = 256
GROWS = NCOL * 8 * BR
ORDERS = ('xyz', 'yzx', 'zxy')
SPREAD = ((0, 0, BR, 'xy'), (1, 0, BR, 'yx'), (2, 0, BR // 2, 'xy'), (2, BR // 2, BR // 2, 'yx'))


def reduce_kernel(g_h, dx_in, out, dx, acc, rd, r1, r2, r3, locsem, ds, dr, ps, pr, gs, gr, cs, cr, xs_, xr_):
    mi = lax.axis_index('model')
    di = lax.axis_index('data')
    core, x, y = di % 2, (di // 2) % 2, di // 4
    me = {'x': x, 'y': y, 'z': mi}
    dev = {'x': {'model': mi, 'data': di + 2 - 4 * x}, 'y': {'model': mi, 'data': di + 4 - 8 * y},
           'z': {'model': 1 - mi, 'data': di}, 'c': {'model': mi, 'data': di + 1 - 2 * core}}

    def rdma(src, dst, s, r, d):
        return pltpu.make_async_remote_copy(src, dst, s, r, device_id=dev[d], device_id_type=MESH_ID)

    barrier = pltpu.get_barrier_semaphore()
    for d in 'xyzc':
        pl.semaphore_signal(barrier, inc=1, device_id=dev[d], device_id_type=MESH_ID)
    pl.semaphore_wait(barrier, 4)

    def blk(color, far):
        pos = {ax: (1 - me[ax] if ax in far else me[ax]) for ax in 'xyz'}
        return (pos['z'] * NCOL + color) * 4 + pos['y'] * 2 + pos['x']

    def add(dst, src):
        def body(i, c):
            r = pl.multiple_of(i * 64, 64)
            acc[dst, pl.ds(r, 64), :] += src[pl.ds(r, 64), :]
            return c
        lax.fori_loop(0, BR // 64, body, 0)

    def places(color):
        a, b, c = ORDERS[color]
        keep = [b + c, b, c, '']
        return [a + k for k in keep], keep

    seq = ([blk(color, places(color)[0][j]) for j in range(4) for color in range(NCOL)]
           + [blk(color, places(color)[1][j]) for j in range(4) for color in range(NCOL)])
    nb = len(seq)
    dcp, lcp = [], []
    for i, b in enumerate(seq):
        dcp.append(rdma(g_h.at[b * 2 + (1 - core)], rd.at[b], ds.at[i], dr.at[i], 'c'))
        lcp.append(pltpu.make_async_copy(g_h.at[b * 2 + core], acc.at[b], locsem.at[i]))
    for i in range(nb):
        dcp[i].start()
        lcp[i].start()

    def fold_core(i):
        dcp[i].wait_recv()
        lcp[i].wait()
        add(seq[i], rd.at[seq[i]])

    p1, p2, p3 = {}, {}, {}
    for j in range(4):
        for color in range(NCOL):
            i = j * NCOL + color
            fold_core(i)
            p1[j, color] = rdma(acc.at[seq[i]], r1.at[i], ps.at[i], pr.at[i], ORDERS[color][0])
            p1[j, color].start()
    base2, base3 = 4 * NCOL, 6 * NCOL

    def fold_kept(j, color):
        i = j * NCOL + color
        fold_core(4 * NCOL + i)
        p1[j, color].wait_recv()
        add(seq[4 * NCOL + i], r1.at[i])
        return seq[4 * NCOL + i]

    for j in range(2):
        for color in range(NCOL):
            b = fold_kept(j, color)
            i = j * NCOL + color
            p2[j, color] = rdma(acc.at[b], r2.at[i], ps.at[base2 + i], pr.at[base2 + i], ORDERS[color][1])
            p2[j, color].start()
    for color in range(NCOL):
        b = fold_kept(2, color)
        p2[0, color].wait_recv()
        add(b, r2.at[color])
        p3[color] = rdma(acc.at[b], r3.at[color], ps.at[base3 + color], pr.at[base3 + color], ORDERS[color][2])
        p3[color].start()
    nseq = dx.shape[0] // 2
    mine, theirs = dx.at[mi * nseq + nseq - 1], dx.at[(1 - mi) * nseq + nseq - 1]
    dx_out = rdma(mine, mine, xs_.at[0], xr_.at[0], 'z')
    dx_out.start()
    last = {}
    for color in range(NCOL):
        last[color] = fold_kept(3, color)
        p2[1, color].wait_recv()
        add(last[color], r2.at[NCOL + color])

    def out_at(color, far, r0, n):
        yy = 1 - y if 'y' in far else y
        xx = 1 - x if 'x' in far else x
        return out.at[(color * 4 + yy * 2 + xx) * 2 + core, pl.ds(r0, n), :]

    ns_ = len(SPREAD)
    cps, g1, g2, g3 = [], {}, {}, {}

    def to_sibling(k, far, i):
        color, r0, n, _ = SPREAD[k]
        o = out_at(color, far, r0, n)
        cp = rdma(o, o, cs.at[i], cr.at[i], 'c')
        cp.start()
        cps.append(cp)

    for color in range(NCOL):
        p3[color].wait_recv()
        b = last[color]
        o_blk = (color * 4 + y * 2 + x) * 2 + core

        def body(i, c, b=b, o_blk=o_blk, color=color):
            r = pl.multiple_of(i * 64, 64)
            out[o_blk, pl.ds(r, 64), :] = acc[b, pl.ds(r, 64), :] + r3[color, pl.ds(r, 64), :]
            return c
        lax.fori_loop(0, BR // 64, body, 0)
        for k, (col, r0, n, ab) in enumerate(SPREAD):
            if col != color:
                continue
            o = out_at(color, '', r0, n)
            g1[k] = rdma(o, o, gs.at[k], gr.at[k], ab[0])
            g2[k] = rdma(o, o, gs.at[ns_ + k], gr.at[ns_ + k], ab[1])
            g1[k].start()
            g2[k].start()
    for k in range(ns_):
        to_sibling(k, '', k)
    for k, (color, r0, n, ab) in enumerate(SPREAD):
        g1[k].wait_recv()
        o = out_at(color, ab[0], r0, n)
        g3[k] = rdma(o, o, gs.at[2 * ns_ + k], gr.at[2 * ns_ + k], ab[1])
        g3[k].start()
        to_sibling(k, ab[0], ns_ + k)
    for k, (color, r0, n, ab) in enumerate(SPREAD):
        g2[k].wait_recv()
        to_sibling(k, ab[1], 2 * ns_ + k)
    for k, (color, r0, n, ab) in enumerate(SPREAD):
        g3[k].wait_recv()
        to_sibling(k, 'xy', 3 * ns_ + k)
    for cp in cps:
        cp.wait()
    dx_out.wait_send()
    rdma(theirs, theirs, xs_.at[0], xr_.at[0], 'z').wait_recv()
    for cp in dcp + list(p1.values()) + list(p2.values()) + list(p3.values()) + list(g1.values()) + list(g2.values()) + list(g3.values()):
        cp.wait_send()


def run_reduce(grad, dx):
    nb = NCOL * 8
    V = pltpu.VMEM
    S = pltpu.SemaphoreType.DMA
    return pl.pallas_call(
        reduce_kernel,
        in_specs=[pl.BlockSpec(memory_space=pl.ANY)] * 2,
        out_specs=[pl.BlockSpec(memory_space=pltpu.VMEM), pl.BlockSpec(memory_space=pl.ANY)],
        out_shape=[jax.ShapeDtypeStruct((nb, BR, GL), F32), jax.ShapeDtypeStruct(dx.shape, dx.dtype)],
        scratch_shapes=[V((nb, BR, GL), F32), V((nb, BR, GL), F32), V((4 * NCOL, BR, GL), F32), V((2 * NCOL, BR, GL), F32), V((NCOL, BR, GL), F32),
                        S((nb,)), S((nb,)), S((nb,)), S((7 * NCOL,)), S((7 * NCOL,)), S((12,)), S((12,)), S((16,)), S((16,)), S((1,)), S((1,))],
        input_output_aliases={1: 1},
        compiler_params=pltpu.CompilerParams(vmem_limit_bytes=60_000_000, collective_id=1, has_side_effects=True),
    )(grad.reshape(2 * nb, BR, GL), dx)


def place_kernel(g, o_q, o_k, o_v, o_o, o_1, o_2, sem):
    cps = []

    def move(b, dst):
        cps.append(pltpu.make_async_copy(g.at[b], dst, sem.at[b]))
        cps[-1].start()

    for j, o in enumerate((o_q, o_k, o_v)):
        for i in range(2):
            move(2 * j + i, o.at[pl.ds(256 * i, 256), :])
    for k in range(4):
        for i in range(2):
            move(6 + 2 * k + i, o_1.at[pl.ds(256 * i, 256), pl.ds(256 * k, 256)])
    for k in range(2):
        for i in range(4):
            move(14 + 4 * k + i, o_2.at[pl.ds(256 * i, 256), pl.ds(256 * k, 256)])
    for k in range(2):
        move(22 + k, o_o.at[:, pl.ds(256 * k, 256)])
    for c in cps:
        c.wait()


def run_place(g):
    shapes = [(512, 256)] * 3 + [(256, 512), (512, 1024), (1024, 512)]
    return pl.pallas_call(
        place_kernel,
        in_specs=[pl.BlockSpec(memory_space=pltpu.VMEM)],
        out_specs=[pl.BlockSpec(memory_space=pl.ANY)] * 6,
        out_shape=[jax.ShapeDtypeStruct(s, F32) for s in shapes],
        scratch_shapes=[pltpu.SemaphoreType.DMA((24,))],
        compiler_params=pltpu.CompilerParams(vmem_limit_bytes=20_000_000),
    )(g)


def solution(mesh):
    spec_col, spec_row, spec_act, spec_rep = P(None, 'model'), P('model', None), P('data', None, None), P(None, None)

    def device_step(x_in, cot_out, step_emb, w_q, w_k, w_v, w_o, w_1, w_2):
        dx, grad = run_kernel(x_in, cot_out, step_emb, (w_q, w_k, w_v, w_o, w_1, w_2), x_in.shape[0] // 2)
        g, dx = run_reduce(grad, dx)
        return (*run_place(g), dx)

    return jax.shard_map(device_step, mesh=mesh,
                         in_specs=(spec_act, spec_act, spec_rep, spec_col, spec_col, spec_col, spec_row, spec_col, spec_row),
                         out_specs=(spec_col, spec_col, spec_col, spec_row, spec_col, spec_row, spec_act),
                         check_vma=False)
```

```python
import functools

import jax
import jax.numpy as jnp
from jax import lax
from jax.experimental import pallas as pl
from jax.experimental.pallas import tpu as pltpu
from jax.sharding import PartitionSpec as P

F32, BF16 = jnp.float32, jnp.bfloat16
T, D, FF, H, E, L = 512, 512, 2048, 8, 64, 4
EPS = 1e-6
CEXP = E ** -0.5 * 1.4426950408889634
SCALE = E ** -0.5
GK0 = 0.7978845608028654
GK1 = 0.044715
R = 32
LN = 128


def dot_nn(a, b):
    return lax.dot_general(a, b, (((1,), (0,)), ((), ())), preferred_element_type=F32)


def dot_nt(a, b):
    return lax.dot_general(a, b, (((1,), (1,)), ((), ())), preferred_element_type=F32)


def rows(r, n=R):
    return pl.ds(r, n)


def wide(e):
    return jnp.concatenate([e] * (T // LN), axis=1)


def col_sum(tile_fn):
    accs = [None, None]
    for i, r in enumerate(range(0, D, R)):
        v = tile_fn(r)
        accs[i % 2] = v if accs[i % 2] is None else accs[i % 2] + v
    return jnp.sum(accs[0] + accs[1], axis=0, keepdims=True)


def rms_of(tile_fn):
    def sq(r):
        v = tile_fn(r)
        return v * v
    return lax.rsqrt(col_sum(sq) * (1.0 / D) + EPS)


def weave(*streams):
    total = max(len(s) for s in streams)
    done = [0] * len(streams)
    for t in range(total):
        for k, s in enumerate(streams):
            upto = -(-len(s) * (t + 1) // total)
            while done[k] < upto:
                s[done[k]]()
                done[k] += 1


def gelu_fwd(z):
    return z * jax.nn.sigmoid(z * (2 * GK0 + (2 * GK0 * GK1) * (z * z)))


def gelu_both(z):
    z2 = z * z
    s = jax.nn.sigmoid(z * (2 * GK0 + (2 * GK0 * GK1) * z2))
    w = z * (2 * GK0 + (6 * GK0 * GK1) * z2)
    return z * s, s * (1.0 + w * (1.0 - s))


def qrow(hd):
    return 768 * (hd // 4) + 64 * (hd % 4)


def pad_head(block, hh):
    zero = jnp.zeros_like(block)
    return jnp.concatenate([block, zero] if hh == 0 else [zero, block], axis=0)


def zip_pad(a, b):
    return [(a[i:i + 1], b[i:i + 1]) for i in range(max(len(a), len(b)))]


def max_cols(ref, cols):
    accs = [None] * 4
    for i, r in enumerate(range(0, T, 64)):
        v = ref[rows(r, 64), cols]
        accs[i % 4] = v if accs[i % 4] is None else jnp.maximum(accs[i % 4], v)
    m = jnp.maximum(jnp.maximum(accs[0], accs[1]), jnp.maximum(accs[2], accs[3]))
    return jnp.max(m, axis=0, keepdims=True)

GL, PR1, PR2 = 256, 512, 256


MESH_ID = pl.DeviceIdType.MESH
NW = 6


def other(i):
    return 1 - i


def kernel(nseq, x_ref, cot_ref, emb_ref, wq_h, wk_h, wv_h, wo_h, w1_h, w2_h,
           dx_h, grad_h, u_h, dmid_h, ctx_h, dqkv_h,
           wqkv, wo, w1, w2, wqkvt, wot, w1t, w2t, g1, g2,
           xs, qkv, ctx, ctxl, hs, zs, lse, rsc, u, m, act, dz, dn, dmid, dctx, dqkv, tmp, sbuf, lcol, dcol, dxs,
           embv, ssem, sem, zsend, zrecv, gsend, grecv, xloc, xsend, xrecv):
    step = pl.program_id(0)
    mi = lax.axis_index('model')
    di = lax.axis_index('data')
    core = di % 2
    zdev = {'model': 1 - mi, 'data': di}
    cdev = {'model': mi, 'data': di + 1 - 2 * core}

    def place(k, m, r0, n):
        if k < 3:
            return wqkv.at[pl.ds(r0, n), pl.ds(768 * m + 256 * k, 256)]
        if k == 3:
            return wo.at[pl.ds(256 * m + r0, n), :]
        if k == 4:
            return w1.at[pl.ds(r0, n), pl.ds(1024 * m, 1024)]
        return w2.at[pl.ds(1024 * m + r0, n), :]

    xx, yy = (di // 2) % 2, di // 4
    dev = {'x': {'model': mi, 'data': di + 2 - 4 * xx}, 'y': {'model': mi, 'data': di + 4 - 8 * yy}, 'z': zdev, 'c': cdev}

    w_hbm = (wq_h, wk_h, wv_h, wo_h, w1_h, w2_h)
    w_rows = (512, 512, 512, 256, 512, 1024)
    groups = ((0, 1, 2), (3,), (4,), (5,))

    def region(g, far, color):
        k = groups[g][0]
        pr = w_rows[k] // 8
        py = 1 - yy if 'y' in far else yy
        px = 1 - xx if 'x' in far else xx
        r0, n = (py * 4 + px * 2 + core) * pr, pr
        if color is not None:
            r0, n = r0 + color * (pr // 2), pr // 2
        if g == 0:
            return wqkv.at[pl.ds(r0, n), pl.ds(768 * (1 - mi), 768)]
        return place(k, 1 - mi, r0, n)

    def load_weights():
        barrier = pltpu.get_barrier_semaphore()
        for d in 'xyzc':
            pl.semaphore_signal(barrier, inc=1, device_id=dev[d], device_id_type=MESH_ID)
        pl.semaphore_wait(barrier, 4)
        zc, local, plane, sib = {}, [], {}, []

        def hand(g, far, color, d, i):
            o = region(g, far, color)
            cp = pltpu.make_async_remote_copy(o, o, gsend.at[g, i], grecv.at[g, i], device_id=dev[d], device_id_type=MESH_ID)
            cp.start()
            return cp

        for k in range(NW):
            pr = w_rows[k] // 8
            zc[k] = pltpu.make_async_remote_copy(w_hbm[k].at[pl.ds(di * pr, pr), :], place(k, mi, di * pr, pr),
                                                 zsend.at[k], zrecv.at[k], device_id=zdev, device_id_type=MESH_ID)
            zc[k].start()
        for k in range(NW):
            local.append(pltpu.make_async_copy(w_hbm[k], place(k, mi, 0, w_rows[k]), sem.at[k]))
            local[-1].start()

        def own(g):
            for k in groups[g]:
                zc[k].wait_recv()
            for color, ab in enumerate(('xy', 'yx')):
                plane[g, color, 0] = hand(g, '', color, ab[0], 3 * color)
                plane[g, color, 1] = hand(g, '', color, ab[1], 3 * color + 1)
            sib.append(hand(g, '', None, 'c', 6))

        def forward(g):
            for color, ab in enumerate(('xy', 'yx')):
                plane[g, color, 0].wait_recv()
                plane[g, color, 2] = hand(g, ab[0], color, ab[1], 3 * color + 2)
                sib.append(hand(g, ab[0], color, 'c', 7 + 3 * color))

        def finish(g):
            for color, ab in enumerate(('xy', 'yx')):
                plane[g, color, 1].wait_recv()
                sib.append(hand(g, ab[1], color, 'c', 8 + 3 * color))
            for color in range(2):
                plane[g, color, 2].wait_recv()
                sib.append(hand(g, 'xy', color, 'c', 9 + 3 * color))

        own(0)
        own(1)
        own(2)
        forward(0)
        forward(1)
        own(3)
        forward(2)
        finish(0)
        finish(1)
        forward(3)
        finish(2)
        finish(3)
        for k in range(NW):
            local[k].wait()
            zc[k].wait_send()
        for cp in plane.values():
            cp.wait_send()
        for cp in sib:
            cp.wait()

    @pl.when(step == 0)
    def _():
        load_weights()
        for l_ in range(L):
            embv[l_] = jnp.broadcast_to(emb_ref[l_:l_ + 1, :].astype(F32), (LN, D)).T
        for j in range(3):
            wqkvt[pl.ds(512 * j, 512), :] = wqkv[:, pl.ds(512 * j, 512)].T
        wot[...] = wo[...].T
        for j in range(4):
            w1t[pl.ds(512 * j, 512), :] = w1[:, pl.ds(512 * j, 512)].T
            w2t[:, pl.ds(512 * j, 512)] = w2[pl.ds(512 * j, 512), :].T
        g1[...] = jnp.zeros_like(g1)
        g2[...] = jnp.zeros_like(g2)

    def stash(k, names):
        pairs = dict(ctx=(ctx.at[k % L], ctx_h), u=(u, u_h), dmid=(dmid, dmid_h), dqkv=(dqkv, dqkv_h))
        return [pltpu.make_async_copy(pairs[n][0], pairs[n][1].at[k], ssem.at[list(pairs).index(n)]) for n in names]

    def start_all(cs):
        for c in cs:
            c.start()

    def wait_all(cs):
        for c in cs:
            c.wait()

    @pl.when(step == 0)
    def _():
        start_all(stash(L - 1, ('u', 'dmid', 'dqkv')))

    xs[0] = x_ref[0].T
    half = [pl.ds(0, 256), pl.ds(256, 256)]

    def s_tile(l, cols=slice(None)):
        w = 4 if cols == slice(None) else 2
        return lambda r: xs[l, rows(r), cols].astype(F32) + jnp.concatenate([embv[l, rows(r), :]] * w, axis=1)

    def norm_into(dst, tile_fn, l, k, fresh, cols=slice(None)):
        box = {}

        def stat():
            if fresh:
                box['r'] = rms_of(tile_fn)
                rsc[l, pl.ds(k, 1), cols] = box['r']
            else:
                box['r'] = rsc[l, pl.ds(k, 1), cols]

        def put(r):
            dst[rows(r), cols] = (tile_fn(r) * box['r']).astype(BF16)

        return [stat] + [functools.partial(put, r) for r in range(0, D, R)]

    def pull_into(dst, base, tile_of, dy, l, k):
        out = []
        for cols in half:
            tile_fn = tile_of(l, cols)
            box = {}

            def stat(cols=cols, tile_fn=tile_fn, box=box):
                a = col_sum(lambda r: dy[rows(r), cols].astype(F32) * tile_fn(r)) * (1.0 / D)
                rr = rsc[l, pl.ds(k, 1), cols]
                box['r'] = rr
                box['a'] = rr * rr * rr * a

            def put(r, cols=cols, tile_fn=tile_fn, box=box):
                g = dy[rows(r), cols].astype(F32)
                dst[rows(r), cols] = (base[rows(r), cols].astype(F32) + (box['r'] * g - tile_fn(r) * box['a'])).astype(BF16)

            out += [stat] + [functools.partial(put, r) for r in range(0, D, R)]
        return out

    def run(stream):
        for f in stream:
            f()

    def h_tile(l, cols=slice(None)):
        return lambda r: hs[l, rows(r), cols].astype(F32)

    def fwd(l, carry):
        for c in range(2):
            run(norm_into(tmp, s_tile(l, half[c]), l, 0, True, half[c]))
        for j in range(3):
            qkv[l, pl.ds(512 * j, 512), :] = dot_nn(wqkvt[pl.ds(512 * j, 512), :], tmp[...]).astype(BF16)

        kps = {}
        inv = {}

        def stage_a(hd):
            p, hh = divmod(hd, 2)

            def first():
                if hh == 0:
                    kps[p] = qkv[l, pl.ds(qrow(hd) + 256, 128), :].T

            def part(c):
                qp = pad_head(qkv[l, pl.ds(qrow(hd), 64), half[c]], hh)
                sbuf[hd % 2, :, half[c]] = dot_nn(kps[p], qp)

            return [first, lambda: part(0), lambda: part(1)]

        def stage_b(hd):
            sref, eref = sbuf.at[hd % 2], act.at[pl.ds(512 * (hd % 2), 512), :]

            def group(g):
                cols = half[g]
                mx = max_cols(sref, cols) * CEXP
                accs = [None, None]
                for i, r in enumerate(range(0, T, 64)):
                    e = jnp.exp2(sref[rows(r, 64), cols] * CEXP - mx)
                    accs[i % 2] = e if accs[i % 2] is None else accs[i % 2] + e
                    eref[rows(r, 64), cols] = e.astype(BF16)
                sm = jnp.sum(accs[0] + accs[1], axis=0, keepdims=True)
                lse[l, pl.ds(hd, 1), cols] = mx + jnp.log2(sm)
                inv[hd, g] = 1.0 / sm

            return [functools.partial(group, g) for g in range(2)]

        def stage_c(hd):
            def part(c):
                cn = dot_nn(qkv[l, pl.ds(qrow(hd) + 512, 64), :], act[pl.ds(512 * (hd % 2), 512), half[c]])
                cn = cn * inv[hd, c]
                hi = cn.astype(BF16)
                ctx[l, pl.ds(64 * hd, 64), half[c]] = hi
                ctxl[l, pl.ds(64 * hd, 64), half[c]] = (cn - hi.astype(F32)).astype(BF16)

            return [lambda: part(0), lambda: part(1)]

        run(stage_a(0))
        for hd in range(H + 1):
            mx = []
            for x_, y_ in zip_pad(stage_a(hd + 1) if hd + 1 < H else [], stage_c(hd - 1) if hd >= 1 else []):
                mx += x_ + y_
            va = stage_b(hd) if hd < H else []
            weave(mx, va)

        for c in range(2):
            o = dot_nn(wot[...], ctx[l, :, half[c]])
            for r in range(0, D, R):
                sx = xs[l, rows(r), half[c]].astype(F32) + jnp.concatenate([embv[l, rows(r), :]] * 2, axis=1)
                hs[l, rows(r), half[c]] = (sx + o[r:r + R]).astype(BF16)
        for c in range(2):
            run(norm_into(m, h_tile(l, half[c]), l, 1, True, half[c]))

        def z_dot(j):
            def f(c):
                js = pl.ds(512 * j, 512)
                zs[l, js, half[c]] = dot_nn(w1t[js, :], m[:, half[c]]).astype(BF16)
            return [lambda: f(0), lambda: f(1)]

        def gelu_stream(j):
            def f(r, c):
                act[rows(r, 64), half[c]] = gelu_fwd(zs[l, rows(r, 64), half[c]].astype(F32)).astype(BF16)
            return [functools.partial(f, r, c) for r in range(512 * j, 512 * j + 512, 64) for c in range(2)]

        @pl.when(l < L - 1)
        def _():
            run(z_dot(0))
            for j in range(4):
                weave(z_dot(j + 1) if j < 3 else [], gelu_stream(j))
            for c in range(2):
                o = dot_nn(w2t[...], act[:, half[c]])
                for r in range(0, D, R):
                    xs[l + 1, rows(r), half[c]] = (hs[l, rows(r), half[c]].astype(F32) + o[r:r + R]).astype(BF16)

        @pl.when(l == L - 1)
        def _():
            for j in range(4):
                run(z_dot(j))
        return carry

    lax.fori_loop(0, L, fwd, 0)

    dn[...] = cot_ref[0].T

    def bwd(i, carry):
        l = L - 1 - i
        k = step * L + l
        start_all(stash(k, ('ctx',)))

        def dg_dot(j):
            def f(c):
                js = pl.ds(512 * j, 512)
                dz[js, half[c]] = dot_nn(w2[js, :], dn[:, half[c]]).astype(BF16)
            return [lambda: f(0), lambda: f(1)]

        def gelu_stream(j):
            def f(r, c):
                g, gp = gelu_both(zs[l, rows(r, 64), half[c]].astype(F32))
                act[rows(r, 64), half[c]] = g.astype(BF16)
                dz[rows(r, 64), half[c]] = (dz[rows(r, 64), half[c]].astype(F32) * gp).astype(BF16)
            return [functools.partial(f, r, c) for r in range(512 * j, 512 * j + 512, 64) for c in range(2)]

        def wgrad(j):
            js = pl.ds(512 * j, 512)

            def a(c):
                g2[js, half[c]] += dot_nt(act[js, :], dn[half[c], :])

            def b(c):
                jc = pl.ds(512 * j + 256 * c, 256)
                g1[:, jc] += dot_nt(m[...], dz[jc, :])
            return [lambda: a(0), lambda: a(1), lambda: b(0), lambda: b(1)]

        weave(dg_dot(0), norm_into(m, h_tile(l, half[0]), l, 1, False, half[0]) + norm_into(m, h_tile(l, half[1]), l, 1, False, half[1]))
        def dm_part(k0, k1, last):
            def f(c):
                p = dot_nn(w1[:, 512 * k0:512 * k1], dz[pl.ds(512 * k0, 512 * (k1 - k0)), half[c]])
                if k0 > 0:
                    p = sbuf[0, :, half[c]] + p
                if last:
                    tmp[:, half[c]] = p.astype(BF16)
                else:
                    sbuf[0, :, half[c]] = p
            return [lambda: f(0), lambda: f(1)]

        weave(dg_dot(1) + dg_dot(2) + dg_dot(3), gelu_stream(0))
        weave(wgrad(0), gelu_stream(1))
        weave(wgrad(1) + dm_part(0, 2, False), gelu_stream(2))
        weave(wgrad(2), gelu_stream(3))
        run(dm_part(2, 4, True))
        wait_all(stash(k, ('ctx', 'u', 'dmid', 'dqkv')))
        weave(wgrad(3), pull_into(dmid, dn, h_tile, tmp, l, 1))
        for c in range(2):
            dctx[:, half[c]] = dot_nn(wo[...], dmid[:, half[c]]).astype(BF16)

        qps, dcs = {}, {}

        def column(row):
            return jnp.broadcast_to(row, (LN, T)).T

        def stage_a(hd):
            p, hh = divmod(hd, 2)
            hsl = pl.ds(64 * hd, 64)

            def first():
                if hh == 0:
                    qps[p] = qkv[l, pl.ds(qrow(hd), 128), :].T
                    dcs[p] = dctx[pl.ds(64 * hd, 128), :].T
                c = ctx[l, hsl, :].astype(F32) + ctxl[l, hsl, :].astype(F32)
                dcol[hd % 2] = column(jnp.sum(dctx[hsl, :].astype(F32) * c, axis=0, keepdims=True))
                lcol[hd % 2] = column(lse[l, pl.ds(hd, 1), :])

            def s_part(c):
                kp = pad_head(qkv[l, pl.ds(qrow(hd) + 256, 64), half[c]], hh)
                sbuf[hd % 2, :, half[c]] = dot_nn(qps[p], kp)

            def p_part(c):
                vp = pad_head(qkv[l, pl.ds(qrow(hd) + 512, 64), half[c]], hh)
                dz[pl.ds(512 * (hd % 2), 512), half[c]] = dot_nn(dcs[p], vp).astype(BF16)

            return [first] + [functools.partial(f, c) for f in (s_part, p_part) for c in range(2)]

        def merge(xs_, ys_):
            out = []
            for i in range(max(len(xs_), len(ys_))):
                out += xs_[i:i + 1] + ys_[i:i + 1]
            return out

        def stage_b(hd):
            sl = 512 * (hd % 2)

            def group(g, r0):
                cols = half[g]
                for r in range(r0, r0 + 64, 64):
                    lc = lcol[hd % 2, rows(r, 64), :]
                    dc = dcol[hd % 2, rows(r, 64), :]
                    pr = jnp.exp2(sbuf[hd % 2, rows(r, 64), cols] * CEXP - jnp.concatenate([lc, lc], axis=1))
                    act[rows(sl + r, 64), cols] = pr.astype(BF16)
                    dp = dz[rows(sl + r, 64), cols].astype(F32)
                    act[rows(1024 + sl + r, 64), cols] = (pr * (dp - jnp.concatenate([dc, dc], axis=1))).astype(BF16)

            return [functools.partial(group, g, r0) for r0 in range(0, T, 64) for g in range(2)]

        def stage_c(hd):
            sl = 512 * (hd % 2)
            pb = act.at[pl.ds(sl, 512), :]
            db = act.at[pl.ds(1024 + sl, 512), :]
            hsl = pl.ds(64 * hd, 64)

            def f_v(c):
                dqkv[pl.ds(qrow(hd) + 512, 64), half[c]] = dot_nn(dctx[hsl, :], pb[:, half[c]]).astype(BF16)

            def f_k(c):
                dk = dot_nn(qkv[l, pl.ds(qrow(hd), 64), :], db[:, half[c]]) * SCALE
                dqkv[pl.ds(qrow(hd) + 256, 64), half[c]] = dk.astype(BF16)

            def f_q(c):
                dq = dot_nt(qkv[l, pl.ds(qrow(hd) + 256, 64), :], db[half[c], :]) * SCALE
                dqkv[pl.ds(qrow(hd), 64), half[c]] = dq.astype(BF16)

            return [functools.partial(f, c) for f in (f_v, f_k, f_q) for c in range(2)]

        u_norm = sum([norm_into(u, s_tile(l, cc), l, 0, False, cc) for cc in half], [])
        run(stage_a(0))
        for hd in range(H + 1):
            ma = stage_a(hd + 1) if hd + 1 < H else []
            mc = stage_c(hd - 1) if hd >= 1 else []
            va = stage_b(hd) if hd < H else []
            if hd == H - 1:
                va = va + u_norm
            weave(merge(mc, ma), va)

        for c in range(2):
            tmp[:, half[c]] = dot_nn(wqkv[...], dqkv[:, half[c]]).astype(BF16)
        weave([], pull_into(dn, dmid, s_tile, tmp, l, 0))
        start_all(stash(k, ('u', 'dmid', 'dqkv')))
        return carry

    lax.fori_loop(0, L, bwd, 0)
    slot = step % 2

    def dx_copies(s, at):
        here = dx_h.at[mi * nseq + s]
        loc = pltpu.make_async_copy(dxs.at[at], here, xloc.at[at])
        rem = pltpu.make_async_remote_copy(dxs.at[at], here, xsend.at[at], xrecv.at[s], device_id=zdev, device_id_type=MESH_ID)
        return loc, rem

    def dx_drain(s, at):
        loc, rem = dx_copies(s, at)
        loc.wait()
        rem.wait_send()

    @pl.when(step >= 2)
    def _():
        dx_drain(step - 2, slot)

    dxs[slot] = dn[...].T
    dx_copies(step, slot)[0].start()

    @pl.when(step < nseq - 1)
    def _():
        dx_copies(step, slot)[1].start()

    @pl.when(step == nseq - 1)
    def _():
        wait_all(stash(0, ('u', 'dmid', 'dqkv')))
        cps = []
        for m_ in range(2):
            for k in range(4):
                cps.append((g1.at[:, pl.ds(1024 * m_ + 256 * k, 256)], grad_h.at[m_, k]))
                cps.append((g2.at[pl.ds(1024 * m_ + 512 * (k % 2), 512), pl.ds(256 * (k // 2), 256)], grad_h.at[m_, 4 + k]))
        cps = [pltpu.make_async_copy(s, d, sem.at[i]) for i, (s, d) in enumerate(cps)]
        for c in cps:
            c.start()
        dx_drain(nseq - 2, (nseq - 2) % 2)
        dx_copies(nseq - 1, (nseq - 1) % 2)[0].wait()
        for s in range(nseq - 1):
            theirs = dx_h.at[(1 - mi) * nseq + s]
            pltpu.make_async_remote_copy(dxs.at[s % 2], theirs, xsend.at[s % 2], xrecv.at[s],
                                         device_id=zdev, device_id_type=MESH_ID).wait_recv()
        for c in cps:
            c.wait()


def run_kernel(x, cot, emb, ws, nseq):
    blk = pl.BlockSpec((1, T, D), lambda i: (lax.axis_index('model') * nseq + i, 0, 0))
    anyspec = pl.BlockSpec(memory_space=pl.ANY)
    V = pltpu.VMEM
    S = pltpu.SemaphoreType.DMA
    return pl.pallas_call(
        functools.partial(kernel, nseq),
        grid=(nseq,),
        in_specs=[blk, blk, pl.BlockSpec(memory_space=pltpu.VMEM)] + [anyspec] * NW,
        out_specs=[anyspec] * 6,
        out_shape=[jax.ShapeDtypeStruct((2 * nseq, T, D), BF16), jax.ShapeDtypeStruct((2, 8, PR1, GL), F32)]
                  + [jax.ShapeDtypeStruct((nseq * L, n, T), BF16) for n in (D, D, D, 1536)],
        scratch_shapes=[V((D, 1536), BF16), V((D, D), BF16), V((D, FF), BF16), V((FF, D), BF16),
                        V((1536, D), BF16), V((D, D), BF16), V((FF, D), BF16), V((D, FF), BF16),
                        V((D, FF), F32), V((FF, D), F32),
                        V((L, D, T), BF16), V((L, 1536, T), BF16), V((L, D, T), BF16), V((L, D, T), BF16), V((L, D, T), BF16),
                        V((L, FF, T), BF16), V((L, H, T), F32), V((L, 2, T), F32), V((D, T), BF16), V((D, T), BF16), V((FF, T), BF16),
                        V((FF, T), BF16), V((D, T), BF16), V((D, T), BF16), V((D, T), BF16), V((1536, T), BF16), V((D, T), BF16),
                        V((2, T, T), F32), V((2, T, LN), F32), V((2, T, LN), F32), V((2, T, D), BF16),
                        V((L, D, LN), F32), S((4,)), S((16,)), S((NW,)), S((NW,)), S((4, 13)), S((4, 13)), S((2,)), S((2,)), S((nseq,))],
        compiler_params=pltpu.CompilerParams(dimension_semantics=("arbitrary",), vmem_limit_bytes=67_000_000,
                                             collective_id=0, has_side_effects=True),
    )(x, cot, emb, *ws)


ORDERS = ('xyz', 'yzx', 'zxy')
SPREAD = ('xy', 'yx', None)
CUTS = {PR1: ((0, 176), (176, 168), (344, 168)), PR2: ((0, 88), (88, 88), (176, 80))}
NB = 12


class Later:
    def __init__(self, make):
        self.make = make

    def start(self):
        self.make().start()

    def wait(self):
        self.make().wait()

    def wait_recv(self):
        self.make().wait_recv()

    def wait_send(self):
        self.make().wait_send()


class Summed:
    def __init__(self, pr, mine, other, load, out, rd, r1, r2, r3, sems, me, core, rdma):
        self.pr, self.mine, self.other, self.load, self.out = pr, mine, other, load, out
        self.rd, self.r1, self.r2, self.r3, self.me, self.core, self.rdma = rd, r1, r2, r3, me, core, rdma
        self.ds, self.dr, self.ls, self.ps, self.prv, self.gs, self.gr, self.cs, self.cr = sems
        self.sends, self.sib = [], []

    def piece(self, far):
        pos = {ax: (1 - v if ax in far else v) for ax, v in self.me.items()}
        return (pos['z'] * 2 + pos['y']) * 2 + pos['x']

    def kept(self, color):
        a, b, c = ORDERS[color]
        return [b + c, b, c, '']

    def go(self, ends, d):
        cp = self.rdma(ends, d)
        cp.start()
        self.sends.append(cp)
        return cp

    def rows(self, color):
        return pl.ds(*CUTS[self.pr][color])

    def add(self, dst, src, color):
        r0, n = CUTS[self.pr][color]

        def body(i, c):
            r = pl.multiple_of(r0 + i * 8, 8)
            dst[pl.ds(r, 8), :] += src[pl.ds(r, 8), :]
            return c
        lax.fori_loop(0, n // 8, body, 0, unroll=2)

    def start(self):
        self.d, self.l = {}, {}
        i = 0
        for first in (True, False):
            for j in range(4):
                for color in range(3):
                    k = self.kept(color)[j]
                    e = self.piece(ORDERS[color][0] + k if first else k)
                    r = self.rows(color)
                    self.d[first, j, color] = (e, self.go(
                        lambda e=e, r=r, i=i: (self.other(e).at[r, :], self.rd.at[e, r, :], self.ds.at[i], self.dr.at[i]), 'c'))
                    if self.load is not None:
                        cp = Later(lambda e=e, r=r, i=i: pltpu.make_async_copy(self.load(e).at[r, :], self.mine(e).at[r, :], self.ls.at[i]))
                        cp.start()
                        self.l[first, j, color] = cp
                    i += 1

    def fold(self, first, j, color):
        e, cp = self.d[first, j, color]
        cp.wait_recv()
        if self.load is not None:
            self.l[first, j, color].wait()
        self.add(self.mine(e), self.rd.at[e], color)
        return e

    def phase1(self):
        self.p1, self.p2, self.p3 = {}, {}, {}
        for j in range(4):
            for color in range(3):
                e, r, i = self.fold(True, j, color), self.rows(color), 3 * j + color
                self.p1[j, color] = self.go(
                    lambda e=e, r=r, i=i, j=j: (self.mine(e).at[r, :], self.r1.at[j, r, :], self.ps.at[i], self.prv.at[i]), ORDERS[color][0])

    def fold_kept(self):
        self.e = {(j, color): self.fold(False, j, color) for j in range(4) for color in range(3)}

    def take1(self, j, color):
        self.p1[j, color].wait_recv()
        e = self.e[j, color]
        self.add(self.mine(e), self.r1.at[j], color)
        return e

    def phase2(self):
        for j in range(2):
            for color in range(3):
                e, r, i = self.take1(j, color), self.rows(color), 12 + 3 * j + color
                self.p2[j, color] = self.go(
                    lambda e=e, r=r, i=i, j=j: (self.mine(e).at[r, :], self.r2.at[j, r, :], self.ps.at[i], self.prv.at[i]), ORDERS[color][1])

    def phase3(self):
        for color in range(3):
            e, r, i = self.take1(2, color), self.rows(color), 18 + color
            self.p2[0, color].wait_recv()
            self.add(self.mine(e), self.r2.at[0], color)
            self.p3[color] = self.go(
                lambda e=e, r=r, i=i: (self.mine(e).at[r, :], self.r3.at[r, :], self.ps.at[i], self.prv.at[i]), ORDERS[color][2])
        for color in range(3):
            e = self.take1(3, color)
            self.p2[1, color].wait_recv()
            self.add(self.mine(e), self.r2.at[1], color)

    def at(self, far, r0, n):
        y = 1 - self.me['y'] if 'y' in far else self.me['y']
        x = 1 - self.me['x'] if 'x' in far else self.me['x']
        return self.out.at[(y * 2 + x) * 2 + self.core, pl.ds(r0, n), :]

    def parts(self):
        out = []
        for color, (r0, n) in enumerate(CUTS[self.pr]):
            if SPREAD[color]:
                out.append((color, r0, n, SPREAD[color]))
            else:
                h = n // 16 * 8
                out += [(color, r0, h, 'xy'), (color, r0 + h, n - h, 'yx')]
        return out

    def sibling(self, far, r0, n, i):
        cp = self.rdma(lambda: (self.at(far, r0, n), self.at(far, r0, n), self.cs.at[i], self.cr.at[i]), 'c')
        cp.start()
        self.sib.append(cp)

    def hand(self, far, r0, n, i, d):
        return self.go(lambda: (self.at(far, r0, n), self.at(far, r0, n), self.gs.at[i], self.gr.at[i]), d)

    def spread(self):
        self.g1, self.g2, self.g3 = {}, {}, {}
        for color, (r0, n) in enumerate(CUTS[self.pr]):
            self.p3[color].wait_recv()
            m = self.mine(self.e[3, color])
            o = self.out.at[(self.me['y'] * 2 + self.me['x']) * 2 + self.core]

            def body(i, c, r0=r0, m=m, o=o):
                r = pl.multiple_of(r0 + i * 8, 8)
                o[pl.ds(r, 8), :] = m[pl.ds(r, 8), :] + self.r3[pl.ds(r, 8), :]
                return c
            lax.fori_loop(0, n // 8, body, 0, unroll=2)
            for k, (col, q0, qn, ab) in enumerate(self.parts()):
                if col == color:
                    self.g1[k] = self.hand('', q0, qn, k, ab[0])
                    self.g2[k] = self.hand('', q0, qn, 4 + k, ab[1])
        for k, (col, r0, n, ab) in enumerate(self.parts()):
            self.sibling('', r0, n, k)

    def forward(self):
        for k, (col, r0, n, ab) in enumerate(self.parts()):
            self.g1[k].wait_recv()
            self.g3[k] = self.hand(ab[0], r0, n, 8 + k, ab[1])
            self.sibling(ab[0], r0, n, 4 + k)

    def collect(self):
        for k, (col, r0, n, ab) in enumerate(self.parts()):
            self.g2[k].wait_recv()
            self.sibling(ab[1], r0, n, 8 + k)
        for k, (col, r0, n, ab) in enumerate(self.parts()):
            self.g3[k].wait_recv()
            self.sibling('xy', r0, n, 12 + k)

    def finish(self):
        for cp in self.sib:
            cp.wait()
        for cp in self.sends:
            cp.wait_send()


def reduce_kernel(g_h, dx_in, u_h, dmid_h, ctx_h, dqkv_h, out1, out2, dx, acc, full, ub, qb, cb, mb, ra, r1, r2, r3, rb, s1, s2, s3, bsem,
                  ds1, dr1, ls1, ps1, pr1, gs1, gr1, cs1, cr1, ds2, dr2, ls2, ps2, pr2, gs2, gr2, cs2, cr2, xs_, xr_):
    mi = lax.axis_index('model')
    di = lax.axis_index('data')
    core, x, y = di % 2, (di // 2) % 2, di // 4
    me = {'x': x, 'y': y, 'z': mi}
    dev = {'x': {'model': mi, 'data': di + 2 - 4 * x}, 'y': {'model': mi, 'data': di + 4 - 8 * y},
           'z': {'model': 1 - mi, 'data': di}, 'c': {'model': mi, 'data': di + 1 - 2 * core}}

    def rdma(ends, d):
        return Later(lambda: pltpu.make_async_remote_copy(*ends(), device_id=dev[d], device_id_type=MESH_ID))

    barrier = pltpu.get_barrier_semaphore()
    for d in 'xyzc':
        pl.semaphore_signal(barrier, inc=1, device_id=dev[d], device_id_type=MESH_ID)
    pl.semaphore_wait(barrier, 4)

    def g_at(e, c):
        return g_h.at[e // 4, (e % 4) * 2 + c]

    mlp = Summed(PR1, lambda e: acc.at[e], lambda e: g_at(e, 1 - core), lambda e: g_at(e, core), out1, ra, r1, r2, r3,
                 (ds1, dr1, ls1, ps1, pr1, gs1, gr1, cs1, cr1), me, core, rdma)
    att = Summed(PR2, lambda e: full.at[e * 2 + core], lambda e: full.at[e * 2 + 1 - core], None, out2, rb, s1, s2, s3,
                 (ds2, dr2, ls2, ps2, pr2, gs2, gr2, cs2, cr2), me, core, rdma)

    def fetch(i, slot):
        two = pl.ds(2 * i, 2)
        return [pltpu.make_async_copy(u_h.at[two], ub.at[slot], bsem.at[slot, 0]),
                pltpu.make_async_copy(dqkv_h.at[two], qb.at[slot], bsem.at[slot, 1])]

    def fetch_o(i, slot):
        two = pl.ds(2 * i, 2)
        return [pltpu.make_async_copy(ctx_h.at[two], cb.at[slot], bsem.at[2 + slot, 0]),
                pltpu.make_async_copy(dmid_h.at[two], mb.at[slot], bsem.at[2 + slot, 1])]

    def begin(cs):
        for c in cs:
            c.start()

    def end(cs):
        for c in cs:
            c.wait()

    mlp.start()
    begin(fetch(0, 0))
    begin(fetch_o(0, 0))
    full[...] = jnp.zeros_like(full)

    def loop(fetch_fn, products, hooks):
        def body(i, carry):
            slot = i % 2
            end(fetch_fn(i, slot))

            @pl.when(i < NB - 1)
            def _():
                begin(fetch_fn(i + 1, 1 - slot))

            products(slot)
            for at, hook in hooks.items():
                pl.when(i == at)(hook)
            return carry
        lax.fori_loop(0, NB, body, 0)

    def qkv_products(slot):
        for j in range(6):
            p = None
            for k in range(2):
                d = dot_nt(ub[slot, k], qb[slot, k, pl.ds(256 * j, 256), :])
                p = d if p is None else p + d
            t = (j // 3) * 8 + 2 * (j % 3)
            full[t] += p[:256]
            full[t + 1] += p[256:]

    def o_products(slot):
        for z in range(2):
            for c in range(2):
                p = None
                for k in range(2):
                    d = dot_nt(cb[slot, k, pl.ds(256 * z, 256), :], mb[slot, k, pl.ds(256 * c, 256), :])
                    p = d if p is None else p + d
                full[z * 8 + 6 + c] += p

    nseq = dx.shape[0] // 2
    mine_x, theirs_x = dx.at[mi * nseq + nseq - 1], dx.at[(1 - mi) * nseq + nseq - 1]
    dx_out = rdma(lambda: (mine_x, mine_x, xs_.at[0], xr_.at[0]), 'z')

    loop(fetch, qkv_products, {2: mlp.phase1, 4: mlp.fold_kept, 8: mlp.phase2})
    loop(fetch_o, o_products, {6: mlp.phase3})
    att.start()
    dx_out.start()
    mlp.spread()
    att.phase1()
    att.fold_kept()
    mlp.forward()
    att.phase2()
    mlp.collect()
    att.phase3()
    att.spread()
    att.forward()
    att.collect()
    mlp.finish()
    att.finish()
    dx_out.wait_send()
    rdma(lambda: (theirs_x, theirs_x, xs_.at[0], xr_.at[0]), 'z').wait_recv()


def run_reduce(grad, dx, u, dmid, ctx, dqkv):
    V = pltpu.VMEM
    S = pltpu.SemaphoreType.DMA
    anyspec = pl.BlockSpec(memory_space=pl.ANY)
    sems = [S((24,)), S((24,)), S((24,)), S((21,)), S((21,)), S((12,)), S((12,)), S((16,)), S((16,))]
    return pl.pallas_call(
        reduce_kernel,
        in_specs=[anyspec] * 6,
        out_specs=[pl.BlockSpec(memory_space=pltpu.VMEM)] * 2 + [anyspec],
        out_shape=[jax.ShapeDtypeStruct((8, PR1, GL), F32), jax.ShapeDtypeStruct((8, PR2, GL), F32), jax.ShapeDtypeStruct(dx.shape, dx.dtype)],
        scratch_shapes=[V((8, PR1, GL), F32), V((16, PR2, GL), F32),
                        V((2, 2, D, T), BF16), V((2, 2, 1536, T), BF16), V((2, 2, D, T), BF16), V((2, 2, D, T), BF16),
                        V((8, PR1, GL), F32), V((4, PR1, GL), F32), V((2, PR1, GL), F32), V((PR1, GL), F32),
                        V((8, PR2, GL), F32), V((4, PR2, GL), F32), V((2, PR2, GL), F32), V((PR2, GL), F32), S((4, 2))]
                       + sems + sems + [S((1,)), S((1,))],
        input_output_aliases={1: 2},
        compiler_params=pltpu.CompilerParams(vmem_limit_bytes=47_000_000, collective_id=1, has_side_effects=True),
    )(grad, dx, u, dmid, ctx, dqkv)


def place_kernel(a, b, o_q, o_k, o_v, o_o, o_1, o_2, sem):
    cps = []

    def move(src, dst):
        cps.append(pltpu.make_async_copy(src, dst, sem.at[len(cps)]))
        cps[-1].start()

    for k in range(4):
        move(a.at[k], o_1.at[:, pl.ds(256 * k, 256)])
        move(a.at[4 + k], o_2.at[pl.ds(512 * (k % 2), 512), pl.ds(256 * (k // 2), 256)])
    for j, o in enumerate((o_q, o_k, o_v)):
        for i in range(2):
            move(b.at[2 * j + i], o.at[pl.ds(256 * i, 256), :])
    for k in range(2):
        move(b.at[6 + k], o_o.at[:, pl.ds(256 * k, 256)])
    for c in cps:
        c.wait()


def run_place(a, b):
    shapes = [(512, 256)] * 3 + [(256, 512), (512, 1024), (1024, 512)]
    return pl.pallas_call(
        place_kernel,
        in_specs=[pl.BlockSpec(memory_space=pltpu.VMEM)] * 2,
        out_specs=[pl.BlockSpec(memory_space=pltpu.HBM)] * 6,
        out_shape=[jax.ShapeDtypeStruct(s, F32) for s in shapes],
        scratch_shapes=[pltpu.SemaphoreType.DMA((16,))],
        compiler_params=pltpu.CompilerParams(vmem_limit_bytes=2_000_000),
    )(a, b)


def solution(mesh):
    spec_col, spec_row, spec_act, spec_rep = P(None, 'model'), P('model', None), P('data', None, None), P(None, None)

    def device_step(x_in, cot_out, step_emb, w_q, w_k, w_v, w_o, w_1, w_2):
        dx, grad, *rest = run_kernel(x_in, cot_out, step_emb, (w_q, w_k, w_v, w_o, w_1, w_2), x_in.shape[0] // 2)
        a, b, dx = run_reduce(grad, dx, *rest)
        return (*run_place(a, b), dx)

    return jax.shard_map(device_step, mesh=mesh,
                         in_specs=(spec_act, spec_act, spec_rep, spec_col, spec_col, spec_col, spec_row, spec_col, spec_row),
                         out_specs=(spec_col, spec_col, spec_col, spec_row, spec_col, spec_row, spec_act),
                         check_vma=False)
```

```python
import functools

import jax
import jax.numpy as jnp
from jax import lax
from jax.experimental import pallas as pl
from jax.experimental.pallas import tpu as pltpu
from jax.sharding import PartitionSpec as P

F32, BF16 = jnp.float32, jnp.bfloat16
T, D, FF, H, E, L = 512, 512, 2048, 8, 64, 4
EPS = 1e-6
CEXP = E ** -0.5 * 1.4426950408889634
SCALE = E ** -0.5
GK0 = 0.7978845608028654
GK1 = 0.044715
R = 32
LN = 128


def dot_nn(a, b):
    return lax.dot_general(a, b, (((1,), (0,)), ((), ())), preferred_element_type=F32)


def dot_nt(a, b):
    return lax.dot_general(a, b, (((1,), (1,)), ((), ())), preferred_element_type=F32)


def rows(r, n=R):
    return pl.ds(r, n)


def wide(e):
    return jnp.concatenate([e] * (T // LN), axis=1)


def col_sum(tile_fn):
    accs = [None, None]
    for i, r in enumerate(range(0, D, R)):
        v = tile_fn(r)
        accs[i % 2] = v if accs[i % 2] is None else accs[i % 2] + v
    return jnp.sum(accs[0] + accs[1], axis=0, keepdims=True)


def rms_of(tile_fn):
    def sq(r):
        v = tile_fn(r)
        return v * v
    return lax.rsqrt(col_sum(sq) * (1.0 / D) + EPS)


def weave(*streams):
    total = max(len(s) for s in streams)
    done = [0] * len(streams)
    for t in range(total):
        for k, s in enumerate(streams):
            upto = -(-len(s) * (t + 1) // total)
            while done[k] < upto:
                s[done[k]]()
                done[k] += 1


def gelu_fwd(z):
    return z * jax.nn.sigmoid(z * (2 * GK0 + (2 * GK0 * GK1) * (z * z)))


def gelu_both(z):
    z2 = z * z
    s = jax.nn.sigmoid(z * (2 * GK0 + (2 * GK0 * GK1) * z2))
    w = z * (2 * GK0 + (6 * GK0 * GK1) * z2)
    return z * s, s * (1.0 + w * (1.0 - s))


def qrow(hd):
    return 768 * (hd // 4) + 64 * (hd % 4)


def pad_head(block, hh):
    zero = jnp.zeros_like(block)
    return jnp.concatenate([block, zero] if hh == 0 else [zero, block], axis=0)


def zip_pad(a, b):
    return [(a[i:i + 1], b[i:i + 1]) for i in range(max(len(a), len(b)))]


def max_cols(ref, cols):
    accs = [None] * 4
    for i, r in enumerate(range(0, T, 64)):
        v = ref[rows(r, 64), cols]
        accs[i % 4] = v if accs[i % 4] is None else jnp.maximum(accs[i % 4], v)
    m = jnp.maximum(jnp.maximum(accs[0], accs[1]), jnp.maximum(accs[2], accs[3]))
    return jnp.max(m, axis=0, keepdims=True)

GL, PR1, PR2 = 256, 512, 256


MESH_ID = pl.DeviceIdType.MESH
NW = 6


def other(i):
    return 1 - i


def kernel(nseq, x_ref, cot_ref, emb_ref, wq_h, wk_h, wv_h, wo_h, w1_h, w2_h,
           dx_h, grad_h, u_h, dmid_h, ctx_h, dqkv_h,
           wqkv, wo, w1, w2, wqkvt, wot, w1t, w2t, g1, g2,
           xs, qkv, ctx, ctxl, hs, zs, lse, rsc, u, m, act, dz, dn, dmid, dctx, dqkv, tmp, sbuf, lcol, dcol, dxs,
           embv, ssem, sem, zsend, zrecv, gsend, grecv, xloc, xsend, xrecv):
    step = pl.program_id(0)
    mi = lax.axis_index('model')
    di = lax.axis_index('data')
    core = di % 2
    zdev = {'model': 1 - mi, 'data': di}
    cdev = {'model': mi, 'data': di + 1 - 2 * core}

    def place(k, m, r0, n):
        if k < 3:
            return wqkv.at[pl.ds(r0, n), pl.ds(768 * m + 256 * k, 256)]
        if k == 3:
            return wo.at[pl.ds(256 * m + r0, n), :]
        if k == 4:
            return w1.at[pl.ds(r0, n), pl.ds(1024 * m, 1024)]
        return w2.at[pl.ds(1024 * m + r0, n), :]

    xx, yy = (di // 2) % 2, di // 4
    dev = {'x': {'model': mi, 'data': di + 2 - 4 * xx}, 'y': {'model': mi, 'data': di + 4 - 8 * yy}, 'z': zdev, 'c': cdev}

    w_hbm = (wq_h, wk_h, wv_h, wo_h, w1_h, w2_h)
    w_rows = (512, 512, 512, 256, 512, 1024)
    groups = ((0, 1, 2), (3,), (4,), (5,))

    def region(g, far, color):
        k = groups[g][0]
        pr = w_rows[k] // 8
        py = 1 - yy if 'y' in far else yy
        px = 1 - xx if 'x' in far else xx
        r0, n = (py * 4 + px * 2 + core) * pr, pr
        if color is not None:
            r0, n = r0 + color * (pr // 2), pr // 2
        if g == 0:
            return wqkv.at[pl.ds(r0, n), pl.ds(768 * (1 - mi), 768)]
        return place(k, 1 - mi, r0, n)

    def load_weights():
        barrier = pltpu.get_barrier_semaphore()
        for d in 'xyzc':
            pl.semaphore_signal(barrier, inc=1, device_id=dev[d], device_id_type=MESH_ID)
        pl.semaphore_wait(barrier, 4)
        zc, local, plane, sib = {}, [], {}, []

        def hand(g, far, color, d, i):
            o = region(g, far, color)
            cp = pltpu.make_async_remote_copy(o, o, gsend.at[g, i], grecv.at[g, i], device_id=dev[d], device_id_type=MESH_ID)
            cp.start()
            return cp

        for k in range(NW):
            pr = w_rows[k] // 8
            zc[k] = pltpu.make_async_remote_copy(w_hbm[k].at[pl.ds(di * pr, pr), :], place(k, mi, di * pr, pr),
                                                 zsend.at[k], zrecv.at[k], device_id=zdev, device_id_type=MESH_ID)
            zc[k].start()
        for k in range(NW):
            local.append(pltpu.make_async_copy(w_hbm[k], place(k, mi, 0, w_rows[k]), sem.at[k]))
            local[-1].start()

        def own(g):
            for k in groups[g]:
                zc[k].wait_recv()
            for color, ab in enumerate(('xy', 'yx')):
                plane[g, color, 0] = hand(g, '', color, ab[0], 3 * color)
                plane[g, color, 1] = hand(g, '', color, ab[1], 3 * color + 1)
            sib.append(hand(g, '', None, 'c', 6))

        def forward(g):
            for color, ab in enumerate(('xy', 'yx')):
                plane[g, color, 0].wait_recv()
                plane[g, color, 2] = hand(g, ab[0], color, ab[1], 3 * color + 2)
                sib.append(hand(g, ab[0], color, 'c', 7 + 3 * color))

        def finish(g):
            for color, ab in enumerate(('xy', 'yx')):
                plane[g, color, 1].wait_recv()
                sib.append(hand(g, ab[1], color, 'c', 8 + 3 * color))
            for color in range(2):
                plane[g, color, 2].wait_recv()
                sib.append(hand(g, 'xy', color, 'c', 9 + 3 * color))

        own(0)
        own(1)
        own(2)
        forward(0)
        forward(1)
        own(3)
        forward(2)
        finish(0)
        finish(1)
        forward(3)
        finish(2)
        finish(3)
        for k in range(NW):
            local[k].wait()
            zc[k].wait_send()
        for cp in plane.values():
            cp.wait_send()
        for cp in sib:
            cp.wait()

    @pl.when(step == 0)
    def _():
        load_weights()
        for l_ in range(L):
            embv[l_] = jnp.broadcast_to(emb_ref[l_:l_ + 1, :].astype(F32), (LN, D)).T
        for j in range(3):
            wqkvt[pl.ds(512 * j, 512), :] = wqkv[:, pl.ds(512 * j, 512)].T
        wot[...] = wo[...].T
        for j in range(4):
            w1t[pl.ds(512 * j, 512), :] = w1[:, pl.ds(512 * j, 512)].T
            w2t[:, pl.ds(512 * j, 512)] = w2[pl.ds(512 * j, 512), :].T
        g1[...] = jnp.zeros_like(g1)
        g2[...] = jnp.zeros_like(g2)

    def stash(k, names):
        pairs = dict(ctx=(ctx.at[k % L], ctx_h), u=(u, u_h), dmid=(dmid, dmid_h), dqkv=(dqkv, dqkv_h))
        return [pltpu.make_async_copy(pairs[n][0], pairs[n][1].at[k], ssem.at[list(pairs).index(n)]) for n in names]

    def start_all(cs):
        for c in cs:
            c.start()

    def wait_all(cs):
        for c in cs:
            c.wait()

    @pl.when(step == 0)
    def _():
        start_all(stash(L - 1, ('u', 'dmid', 'dqkv')))

    xs[0] = x_ref[0].T
    half = [pl.ds(0, 256), pl.ds(256, 256)]

    def s_tile(l, cols=slice(None)):
        w = 4 if cols == slice(None) else 2
        return lambda r: xs[l, rows(r), cols].astype(F32) + jnp.concatenate([embv[l, rows(r), :]] * w, axis=1)

    def norm_into(dst, tile_fn, l, k, fresh, cols=slice(None)):
        box = {}

        def stat():
            if fresh:
                box['r'] = rms_of(tile_fn)
                rsc[l, pl.ds(k, 1), cols] = box['r']
            else:
                box['r'] = rsc[l, pl.ds(k, 1), cols]

        def put(r):
            dst[rows(r), cols] = (tile_fn(r) * box['r']).astype(BF16)

        return [stat] + [functools.partial(put, r) for r in range(0, D, R)]

    def pull_into(dst, base, tile_of, dy, l, k):
        out = []
        for cols in half:
            tile_fn = tile_of(l, cols)
            box = {}

            def stat(cols=cols, tile_fn=tile_fn, box=box):
                a = col_sum(lambda r: dy[rows(r), cols].astype(F32) * tile_fn(r)) * (1.0 / D)
                rr = rsc[l, pl.ds(k, 1), cols]
                box['r'] = rr
                box['a'] = rr * rr * rr * a

            def put(r, cols=cols, tile_fn=tile_fn, box=box):
                g = dy[rows(r), cols].astype(F32)
                dst[rows(r), cols] = (base[rows(r), cols].astype(F32) + (box['r'] * g - tile_fn(r) * box['a'])).astype(BF16)

            out += [stat] + [functools.partial(put, r) for r in range(0, D, R)]
        return out

    def run(stream):
        for f in stream:
            f()

    def h_tile(l, cols=slice(None)):
        return lambda r: hs[l, rows(r), cols].astype(F32)

    def fwd(l, carry):
        for c in range(2):
            run(norm_into(tmp, s_tile(l, half[c]), l, 0, True, half[c]))
        for j in range(3):
            qkv[l, pl.ds(512 * j, 512), :] = dot_nn(wqkvt[pl.ds(512 * j, 512), :], tmp[...]).astype(BF16)

        kps = {}
        inv = {}

        def stage_a(hd):
            p, hh = divmod(hd, 2)

            def first():
                if hh == 0:
                    kps[p] = qkv[l, pl.ds(qrow(hd) + 256, 128), :].T

            def part(c):
                qp = pad_head(qkv[l, pl.ds(qrow(hd), 64), half[c]], hh)
                sbuf[hd % 2, :, half[c]] = dot_nn(kps[p], qp)

            return [first, lambda: part(0), lambda: part(1)]

        def stage_b(hd):
            sref, eref = sbuf.at[hd % 2], act.at[pl.ds(512 * (hd % 2), 512), :]

            def group(g):
                cols = half[g]
                mx = max_cols(sref, cols) * CEXP
                accs = [None, None]
                for i, r in enumerate(range(0, T, 64)):
                    e = jnp.exp2(sref[rows(r, 64), cols] * CEXP - mx)
                    accs[i % 2] = e if accs[i % 2] is None else accs[i % 2] + e
                    eref[rows(r, 64), cols] = e.astype(BF16)
                sm = jnp.sum(accs[0] + accs[1], axis=0, keepdims=True)
                lse[l, pl.ds(hd, 1), cols] = mx + jnp.log2(sm)
                inv[hd, g] = 1.0 / sm

            return [functools.partial(group, g) for g in range(2)]

        def stage_c(hd):
            def part(c):
                cn = dot_nn(qkv[l, pl.ds(qrow(hd) + 512, 64), :], act[pl.ds(512 * (hd % 2), 512), half[c]])
                cn = cn * inv[hd, c]
                hi = cn.astype(BF16)
                ctx[l, pl.ds(64 * hd, 64), half[c]] = hi
                ctxl[l, pl.ds(64 * hd, 64), half[c]] = (cn - hi.astype(F32)).astype(BF16)

            return [lambda: part(0), lambda: part(1)]

        run(stage_a(0))
        for hd in range(H + 1):
            mx = []
            for x_, y_ in zip_pad(stage_a(hd + 1) if hd + 1 < H else [], stage_c(hd - 1) if hd >= 1 else []):
                mx += x_ + y_
            va = stage_b(hd) if hd < H else []
            weave(mx, va)

        for c in range(2):
            o = dot_nn(wot[...], ctx[l, :, half[c]])
            for r in range(0, D, R):
                sx = xs[l, rows(r), half[c]].astype(F32) + jnp.concatenate([embv[l, rows(r), :]] * 2, axis=1)
                hs[l, rows(r), half[c]] = (sx + o[r:r + R]).astype(BF16)
        for c in range(2):
            run(norm_into(m, h_tile(l, half[c]), l, 1, True, half[c]))

        def z_dot(j):
            def f(c):
                js = pl.ds(512 * j, 512)
                zs[l, js, half[c]] = dot_nn(w1t[js, :], m[:, half[c]]).astype(BF16)
            return [lambda: f(0), lambda: f(1)]

        def gelu_stream(j):
            def f(r, c):
                act[rows(r, 64), half[c]] = gelu_fwd(zs[l, rows(r, 64), half[c]].astype(F32)).astype(BF16)
            return [functools.partial(f, r, c) for r in range(512 * j, 512 * j + 512, 64) for c in range(2)]

        @pl.when(l < L - 1)
        def _():
            run(z_dot(0))
            for j in range(4):
                weave(z_dot(j + 1) if j < 3 else [], gelu_stream(j))
            for c in range(2):
                o = dot_nn(w2t[...], act[:, half[c]])
                for r in range(0, D, R):
                    xs[l + 1, rows(r), half[c]] = (hs[l, rows(r), half[c]].astype(F32) + o[r:r + R]).astype(BF16)

        @pl.when(l == L - 1)
        def _():
            for j in range(4):
                run(z_dot(j))
        return carry

    lax.fori_loop(0, L, fwd, 0)

    dn[...] = cot_ref[0].T

    def bwd(i, carry):
        l = L - 1 - i
        k = step * L + l
        start_all(stash(k, ('ctx',)))

        def dg_dot(j):
            def f(c):
                js = pl.ds(512 * j, 512)
                dz[js, half[c]] = dot_nn(w2[js, :], dn[:, half[c]]).astype(BF16)
            return [lambda: f(0), lambda: f(1)]

        def gelu_stream(j):
            def f(r, c):
                g, gp = gelu_both(zs[l, rows(r, 64), half[c]].astype(F32))
                act[rows(r, 64), half[c]] = g.astype(BF16)
                dz[rows(r, 64), half[c]] = (dz[rows(r, 64), half[c]].astype(F32) * gp).astype(BF16)
            return [functools.partial(f, r, c) for r in range(512 * j, 512 * j + 512, 64) for c in range(2)]

        def wgrad(j):
            js = pl.ds(512 * j, 512)

            def a(c):
                g2[js, half[c]] += dot_nt(act[js, :], dn[half[c], :])

            def b(c):
                jc = pl.ds(512 * j + 256 * c, 256)
                g1[:, jc] += dot_nt(m[...], dz[jc, :])
            return [lambda: a(0), lambda: a(1), lambda: b(0), lambda: b(1)]

        weave(dg_dot(0), norm_into(m, h_tile(l, half[0]), l, 1, False, half[0]) + norm_into(m, h_tile(l, half[1]), l, 1, False, half[1]))
        def dm_part(k0, k1, last):
            def f(c):
                p = dot_nn(w1[:, 512 * k0:512 * k1], dz[pl.ds(512 * k0, 512 * (k1 - k0)), half[c]])
                if k0 > 0:
                    p = sbuf[0, :, half[c]] + p
                if last:
                    tmp[:, half[c]] = p.astype(BF16)
                else:
                    sbuf[0, :, half[c]] = p
            return [lambda: f(0), lambda: f(1)]

        weave(dg_dot(1) + dg_dot(2) + dg_dot(3), gelu_stream(0))
        weave(wgrad(0), gelu_stream(1))
        weave(wgrad(1) + dm_part(0, 2, False), gelu_stream(2))
        weave(wgrad(2), gelu_stream(3))
        run(dm_part(2, 4, True))
        wait_all(stash(k, ('ctx', 'u', 'dmid', 'dqkv')))
        weave(wgrad(3), pull_into(dmid, dn, h_tile, tmp, l, 1))
        for c in range(2):
            dctx[:, half[c]] = dot_nn(wo[...], dmid[:, half[c]]).astype(BF16)

        qps, dcs = {}, {}

        def column(row):
            return jnp.broadcast_to(row, (LN, T)).T

        def stage_a(hd):
            p, hh = divmod(hd, 2)
            hsl = pl.ds(64 * hd, 64)

            def first():
                if hh == 0:
                    qps[p] = qkv[l, pl.ds(qrow(hd), 128), :].T
                    dcs[p] = dctx[pl.ds(64 * hd, 128), :].T
                c = ctx[l, hsl, :].astype(F32) + ctxl[l, hsl, :].astype(F32)
                dcol[hd % 2] = column(jnp.sum(dctx[hsl, :].astype(F32) * c, axis=0, keepdims=True))
                lcol[hd % 2] = column(lse[l, pl.ds(hd, 1), :])

            def s_part(c):
                kp = pad_head(qkv[l, pl.ds(qrow(hd) + 256, 64), half[c]], hh)
                sbuf[hd % 2, :, half[c]] = dot_nn(qps[p], kp)

            def p_part(c):
                vp = pad_head(qkv[l, pl.ds(qrow(hd) + 512, 64), half[c]], hh)
                dz[pl.ds(512 * (hd % 2), 512), half[c]] = dot_nn(dcs[p], vp).astype(BF16)

            return [first] + [functools.partial(f, c) for f in (s_part, p_part) for c in range(2)]

        def merge(xs_, ys_):
            out = []
            for i in range(max(len(xs_), len(ys_))):
                out += xs_[i:i + 1] + ys_[i:i + 1]
            return out

        def stage_b(hd):
            sl = 512 * (hd % 2)

            def group(g, r0):
                cols = half[g]
                for r in range(r0, r0 + 64, 64):
                    lc = lcol[hd % 2, rows(r, 64), :]
                    dc = dcol[hd % 2, rows(r, 64), :]
                    pr = jnp.exp2(sbuf[hd % 2, rows(r, 64), cols] * CEXP - jnp.concatenate([lc, lc], axis=1))
                    act[rows(sl + r, 64), cols] = pr.astype(BF16)
                    dp = dz[rows(sl + r, 64), cols].astype(F32)
                    act[rows(1024 + sl + r, 64), cols] = (pr * (dp - jnp.concatenate([dc, dc], axis=1))).astype(BF16)

            return [functools.partial(group, g, r0) for r0 in range(0, T, 64) for g in range(2)]

        def stage_c(hd):
            sl = 512 * (hd % 2)
            pb = act.at[pl.ds(sl, 512), :]
            db = act.at[pl.ds(1024 + sl, 512), :]
            hsl = pl.ds(64 * hd, 64)

            def f_v(c):
                dqkv[pl.ds(qrow(hd) + 512, 64), half[c]] = dot_nn(dctx[hsl, :], pb[:, half[c]]).astype(BF16)

            def f_k(c):
                dk = dot_nn(qkv[l, pl.ds(qrow(hd), 64), :], db[:, half[c]]) * SCALE
                dqkv[pl.ds(qrow(hd) + 256, 64), half[c]] = dk.astype(BF16)

            def f_q(c):
                dq = dot_nt(qkv[l, pl.ds(qrow(hd) + 256, 64), :], db[half[c], :]) * SCALE
                dqkv[pl.ds(qrow(hd), 64), half[c]] = dq.astype(BF16)

            return [functools.partial(f, c) for f in (f_v, f_k, f_q) for c in range(2)]

        u_norm = sum([norm_into(u, s_tile(l, cc), l, 0, False, cc) for cc in half], [])
        run(stage_a(0))
        for hd in range(H + 1):
            ma = stage_a(hd + 1) if hd + 1 < H else []
            mc = stage_c(hd - 1) if hd >= 1 else []
            va = stage_b(hd) if hd < H else []
            if hd == H - 1:
                va = va + u_norm
            weave(merge(mc, ma), va)

        for c in range(2):
            tmp[:, half[c]] = dot_nn(wqkv[...], dqkv[:, half[c]]).astype(BF16)
        weave([], pull_into(dn, dmid, s_tile, tmp, l, 0))
        start_all(stash(k, ('u', 'dmid', 'dqkv')))
        return carry

    lax.fori_loop(0, L, bwd, 0)
    slot = step % 2

    def dx_copies(s, at):
        here = dx_h.at[mi * nseq + s]
        loc = pltpu.make_async_copy(dxs.at[at], here, xloc.at[at])
        rem = pltpu.make_async_remote_copy(dxs.at[at], here, xsend.at[at], xrecv.at[s], device_id=zdev, device_id_type=MESH_ID)
        return loc, rem

    def dx_drain(s, at):
        loc, rem = dx_copies(s, at)
        loc.wait()
        rem.wait_send()

    @pl.when(step >= 2)
    def _():
        dx_drain(step - 2, slot)

    dxs[slot] = dn[...].T
    dx_copies(step, slot)[0].start()

    @pl.when(step < nseq - 1)
    def _():
        dx_copies(step, slot)[1].start()

    @pl.when(step == nseq - 1)
    def _():
        wait_all(stash(0, ('u', 'dmid', 'dqkv')))
        cps = []
        for m_ in range(2):
            for k in range(4):
                cps.append((g1.at[:, pl.ds(1024 * m_ + 256 * k, 256)], grad_h.at[m_, k]))
                cps.append((g2.at[pl.ds(1024 * m_ + 512 * (k % 2), 512), pl.ds(256 * (k // 2), 256)], grad_h.at[m_, 4 + k]))
        cps = [pltpu.make_async_copy(s, d, sem.at[i]) for i, (s, d) in enumerate(cps)]
        for c in cps:
            c.start()
        dx_drain(nseq - 2, (nseq - 2) % 2)
        dx_copies(nseq - 1, (nseq - 1) % 2)[0].wait()
        for s in range(nseq - 1):
            theirs = dx_h.at[(1 - mi) * nseq + s]
            pltpu.make_async_remote_copy(dxs.at[s % 2], theirs, xsend.at[s % 2], xrecv.at[s],
                                         device_id=zdev, device_id_type=MESH_ID).wait_recv()
        for c in cps:
            c.wait()


def run_kernel(x, cot, emb, ws, nseq):
    blk = pl.BlockSpec((1, T, D), lambda i: (lax.axis_index('model') * nseq + i, 0, 0))
    anyspec = pl.BlockSpec(memory_space=pl.ANY)
    V = pltpu.VMEM
    S = pltpu.SemaphoreType.DMA
    return pl.pallas_call(
        functools.partial(kernel, nseq),
        grid=(nseq,),
        in_specs=[blk, blk, pl.BlockSpec(memory_space=pltpu.VMEM)] + [anyspec] * NW,
        out_specs=[anyspec] * 6,
        out_shape=[jax.ShapeDtypeStruct((2 * nseq, T, D), BF16), jax.ShapeDtypeStruct((2, 8, PR1, GL), F32)]
                  + [jax.ShapeDtypeStruct((nseq * L, n, T), BF16) for n in (D, D, D, 1536)],
        scratch_shapes=[V((D, 1536), BF16), V((D, D), BF16), V((D, FF), BF16), V((FF, D), BF16),
                        V((1536, D), BF16), V((D, D), BF16), V((FF, D), BF16), V((D, FF), BF16),
                        V((D, FF), F32), V((FF, D), F32),
                        V((L, D, T), BF16), V((L, 1536, T), BF16), V((L, D, T), BF16), V((L, D, T), BF16), V((L, D, T), BF16),
                        V((L, FF, T), BF16), V((L, H, T), F32), V((L, 2, T), F32), V((D, T), BF16), V((D, T), BF16), V((FF, T), BF16),
                        V((FF, T), BF16), V((D, T), BF16), V((D, T), BF16), V((D, T), BF16), V((1536, T), BF16), V((D, T), BF16),
                        V((2, T, T), F32), V((2, T, LN), F32), V((2, T, LN), F32), V((2, T, D), BF16),
                        V((L, D, LN), F32), S((4,)), S((16,)), S((NW,)), S((NW,)), S((4, 13)), S((4, 13)), S((2,)), S((2,)), S((nseq,))],
        compiler_params=pltpu.CompilerParams(dimension_semantics=("arbitrary",), vmem_limit_bytes=67_000_000,
                                             collective_id=0, has_side_effects=True),
    )(x, cot, emb, *ws)


ORDERS = ('xyz', 'yzx', 'zxy')
SPREAD = ('xy', 'yx', None)
CUTS = {PR1: ((0, 176), (176, 168), (344, 168)), PR2: ((0, 88), (88, 88), (176, 80))}
NB = 12


class Later:
    def __init__(self, make):
        self.make = make

    def start(self):
        self.make().start()

    def wait(self):
        self.make().wait()

    def wait_recv(self):
        self.make().wait_recv()

    def wait_send(self):
        self.make().wait_send()


class Summed:
    def __init__(self, pr, mine, other, load, out, rd, r1, r2, r3, sems, me, core, rdma):
        self.pr, self.mine, self.other, self.load, self.out = pr, mine, other, load, out
        self.rd, self.r1, self.r2, self.r3, self.me, self.core, self.rdma = rd, r1, r2, r3, me, core, rdma
        self.ds, self.dr, self.ls, self.ps, self.prv, self.gs, self.gr, self.cs, self.cr = sems
        self.sends, self.sib = [], []

    def piece(self, far):
        pos = {ax: (1 - v if ax in far else v) for ax, v in self.me.items()}
        return (pos['z'] * 2 + pos['y']) * 2 + pos['x']

    def kept(self, color):
        a, b, c = ORDERS[color]
        return [b + c, b, c, '']

    def go(self, ends, d):
        cp = self.rdma(ends, d)
        cp.start()
        self.sends.append(cp)
        return cp

    def rows(self, color):
        return pl.ds(*CUTS[self.pr][color])

    def add(self, dst, src, color):
        r = self.rows(color)
        dst[r, :] += src[r, :]

    def start(self):
        self.d, self.l = {}, {}
        i = 0
        for first in (True, False):
            for j in range(4):
                for color in range(3):
                    k = self.kept(color)[j]
                    e = self.piece(ORDERS[color][0] + k if first else k)
                    r = self.rows(color)
                    self.d[first, j, color] = (e, self.go(
                        lambda e=e, r=r, i=i: (self.other(e).at[r, :], self.rd.at[e, r, :], self.ds.at[i], self.dr.at[i]), 'c'))
                    if self.load is not None:
                        cp = Later(lambda e=e, r=r, i=i: pltpu.make_async_copy(self.load(e).at[r, :], self.mine(e).at[r, :], self.ls.at[i]))
                        cp.start()
                        self.l[first, j, color] = cp
                    i += 1

    def fold(self, first, j, color):
        e, cp = self.d[first, j, color]
        cp.wait_recv()
        if self.load is not None:
            self.l[first, j, color].wait()
        self.add(self.mine(e), self.rd.at[e], color)
        return e

    def phase1(self):
        self.p1, self.p2, self.p3 = {}, {}, {}
        for j in range(4):
            for color in range(3):
                e, r, i = self.fold(True, j, color), self.rows(color), 3 * j + color
                self.p1[j, color] = self.go(
                    lambda e=e, r=r, i=i, j=j: (self.mine(e).at[r, :], self.r1.at[j, r, :], self.ps.at[i], self.prv.at[i]), ORDERS[color][0])

    def fold_kept(self):
        self.e = {(j, color): self.fold(False, j, color) for j in range(4) for color in range(3)}

    def take1(self, j, color):
        self.p1[j, color].wait_recv()
        e = self.e[j, color]
        self.add(self.mine(e), self.r1.at[j], color)
        return e

    def phase2(self):
        for j in range(2):
            for color in range(3):
                e, r, i = self.take1(j, color), self.rows(color), 12 + 3 * j + color
                self.p2[j, color] = self.go(
                    lambda e=e, r=r, i=i, j=j: (self.mine(e).at[r, :], self.r2.at[j, r, :], self.ps.at[i], self.prv.at[i]), ORDERS[color][1])

    def phase3(self):
        for color in range(3):
            e, r, i = self.take1(2, color), self.rows(color), 18 + color
            self.p2[0, color].wait_recv()
            self.add(self.mine(e), self.r2.at[0], color)
            self.p3[color] = self.go(
                lambda e=e, r=r, i=i: (self.mine(e).at[r, :], self.r3.at[r, :], self.ps.at[i], self.prv.at[i]), ORDERS[color][2])
        for color in range(3):
            e = self.take1(3, color)
            self.p2[1, color].wait_recv()
            self.add(self.mine(e), self.r2.at[1], color)

    def at(self, far, r0, n):
        y = 1 - self.me['y'] if 'y' in far else self.me['y']
        x = 1 - self.me['x'] if 'x' in far else self.me['x']
        return self.out.at[(y * 2 + x) * 2 + self.core, pl.ds(r0, n), :]

    def parts(self):
        out = []
        for color, (r0, n) in enumerate(CUTS[self.pr]):
            if SPREAD[color]:
                out.append((color, r0, n, SPREAD[color]))
            else:
                h = n // 16 * 8
                out += [(color, r0, h, 'xy'), (color, r0 + h, n - h, 'yx')]
        return out

    def sibling(self, far, r0, n, i):
        cp = self.rdma(lambda: (self.at(far, r0, n), self.at(far, r0, n), self.cs.at[i], self.cr.at[i]), 'c')
        cp.start()
        self.sib.append(cp)

    def hand(self, far, r0, n, i, d):
        return self.go(lambda: (self.at(far, r0, n), self.at(far, r0, n), self.gs.at[i], self.gr.at[i]), d)

    def spread(self):
        self.g1, self.g2, self.g3 = {}, {}, {}
        for color, (r0, n) in enumerate(CUTS[self.pr]):
            self.p3[color].wait_recv()
            self.at('', r0, n)[...] = self.mine(self.e[3, color])[pl.ds(r0, n), :] + self.r3[pl.ds(r0, n), :]
            for k, (col, q0, qn, ab) in enumerate(self.parts()):
                if col == color:
                    self.g1[k] = self.hand('', q0, qn, k, ab[0])
                    self.g2[k] = self.hand('', q0, qn, 4 + k, ab[1])
        for k, (col, r0, n, ab) in enumerate(self.parts()):
            self.sibling('', r0, n, k)

    def forward(self):
        for k, (col, r0, n, ab) in enumerate(self.parts()):
            self.g1[k].wait_recv()
            self.g3[k] = self.hand(ab[0], r0, n, 8 + k, ab[1])
            self.sibling(ab[0], r0, n, 4 + k)

    def collect(self):
        for k, (col, r0, n, ab) in enumerate(self.parts()):
            self.g2[k].wait_recv()
            self.sibling(ab[1], r0, n, 8 + k)
        for k, (col, r0, n, ab) in enumerate(self.parts()):
            self.g3[k].wait_recv()
            self.sibling('xy', r0, n, 12 + k)

    def finish(self):
        for cp in self.sib:
            cp.wait()
        for cp in self.sends:
            cp.wait_send()


def reduce_kernel(g_h, dx_in, u_h, dmid_h, ctx_h, dqkv_h, out1, out2, dx, acc, full, ub, qb, cb, mb, ra, r1, r2, r3, rb, s1, s2, s3, bsem,
                  ds1, dr1, ls1, ps1, pr1, gs1, gr1, cs1, cr1, ds2, dr2, ls2, ps2, pr2, gs2, gr2, cs2, cr2, xs_, xr_):
    mi = lax.axis_index('model')
    di = lax.axis_index('data')
    core, x, y = di % 2, (di // 2) % 2, di // 4
    me = {'x': x, 'y': y, 'z': mi}
    dev = {'x': {'model': mi, 'data': di + 2 - 4 * x}, 'y': {'model': mi, 'data': di + 4 - 8 * y},
           'z': {'model': 1 - mi, 'data': di}, 'c': {'model': mi, 'data': di + 1 - 2 * core}}

    def rdma(ends, d):
        return Later(lambda: pltpu.make_async_remote_copy(*ends(), device_id=dev[d], device_id_type=MESH_ID))

    barrier = pltpu.get_barrier_semaphore()
    for d in 'xyzc':
        pl.semaphore_signal(barrier, inc=1, device_id=dev[d], device_id_type=MESH_ID)
    pl.semaphore_wait(barrier, 4)

    def g_at(e, c):
        return g_h.at[e // 4, (e % 4) * 2 + c]

    mlp = Summed(PR1, lambda e: acc.at[e], lambda e: g_at(e, 1 - core), lambda e: g_at(e, core), out1, ra, r1, r2, r3,
                 (ds1, dr1, ls1, ps1, pr1, gs1, gr1, cs1, cr1), me, core, rdma)
    att = Summed(PR2, lambda e: full.at[e * 2 + core], lambda e: full.at[e * 2 + 1 - core], None, out2, rb, s1, s2, s3,
                 (ds2, dr2, ls2, ps2, pr2, gs2, gr2, cs2, cr2), me, core, rdma)

    def fetch(i, slot):
        two = pl.ds(2 * i, 2)
        return [pltpu.make_async_copy(u_h.at[two], ub.at[slot], bsem.at[slot, 0]),
                pltpu.make_async_copy(dqkv_h.at[two], qb.at[slot], bsem.at[slot, 1])]

    def fetch_o(i, slot):
        two = pl.ds(2 * i, 2)
        return [pltpu.make_async_copy(ctx_h.at[two], cb.at[slot], bsem.at[3 + slot, 0]),
                pltpu.make_async_copy(dmid_h.at[two], mb.at[slot], bsem.at[3 + slot, 1])]

    def begin(cs):
        for c in cs:
            c.start()

    def end(cs):
        for c in cs:
            c.wait()

    mlp.start()
    for i in range(2):
        begin(fetch(i, i))
    for i in range(2):
        begin(fetch_o(i, i))
    full[...] = jnp.zeros_like(full)

    def loop(fetch_fn, products, hooks):
        def body(i, carry):
            slot = i % 3
            end(fetch_fn(i, slot))

            @pl.when(i < NB - 2)
            def _():
                begin(fetch_fn(i + 2, (i + 2) % 3))

            products(slot)
            for at, hook in hooks.items():
                pl.when(i == at)(hook)
            return carry
        lax.fori_loop(0, NB, body, 0)

    def qkv_products(slot):
        for j in range(6):
            p = None
            for k in range(2):
                d = dot_nt(ub[slot, k], qb[slot, k, pl.ds(256 * j, 256), :])
                p = d if p is None else p + d
            t = (j // 3) * 8 + 2 * (j % 3)
            full[t] += p[:256]
            full[t + 1] += p[256:]

    def o_products(slot):
        for z in range(2):
            for c in range(2):
                p = None
                for k in range(2):
                    d = dot_nt(cb[slot, k, pl.ds(256 * z, 256), :], mb[slot, k, pl.ds(256 * c, 256), :])
                    p = d if p is None else p + d
                full[z * 8 + 6 + c] += p

    nseq = dx.shape[0] // 2
    mine_x, theirs_x = dx.at[mi * nseq + nseq - 1], dx.at[(1 - mi) * nseq + nseq - 1]
    dx_out = rdma(lambda: (mine_x, mine_x, xs_.at[0], xr_.at[0]), 'z')

    loop(fetch, qkv_products, {2: mlp.phase1, 4: mlp.fold_kept, 8: mlp.phase2})
    loop(fetch_o, o_products, {6: mlp.phase3})
    att.start()
    dx_out.start()
    mlp.spread()
    att.phase1()
    att.fold_kept()
    mlp.forward()
    att.phase2()
    mlp.collect()
    att.phase3()
    att.spread()
    att.forward()
    att.collect()
    mlp.finish()
    att.finish()
    dx_out.wait_send()
    rdma(lambda: (theirs_x, theirs_x, xs_.at[0], xr_.at[0]), 'z').wait_recv()


def run_reduce(grad, dx, u, dmid, ctx, dqkv):
    V = pltpu.VMEM
    S = pltpu.SemaphoreType.DMA
    anyspec = pl.BlockSpec(memory_space=pl.ANY)
    sems = [S((24,)), S((24,)), S((24,)), S((21,)), S((21,)), S((12,)), S((12,)), S((16,)), S((16,))]
    return pl.pallas_call(
        reduce_kernel,
        in_specs=[anyspec] * 6,
        out_specs=[pl.BlockSpec(memory_space=pltpu.VMEM)] * 2 + [anyspec],
        out_shape=[jax.ShapeDtypeStruct((8, PR1, GL), F32), jax.ShapeDtypeStruct((8, PR2, GL), F32), jax.ShapeDtypeStruct(dx.shape, dx.dtype)],
        scratch_shapes=[V((8, PR1, GL), F32), V((16, PR2, GL), F32),
                        V((3, 2, D, T), BF16), V((3, 2, 1536, T), BF16), V((3, 2, D, T), BF16), V((3, 2, D, T), BF16),
                        V((8, PR1, GL), F32), V((4, PR1, GL), F32), V((2, PR1, GL), F32), V((PR1, GL), F32),
                        V((8, PR2, GL), F32), V((4, PR2, GL), F32), V((2, PR2, GL), F32), V((PR2, GL), F32), S((6, 2))]
                       + sems + sems + [S((1,)), S((1,))],
        input_output_aliases={1: 2},
        compiler_params=pltpu.CompilerParams(vmem_limit_bytes=47_000_000, collective_id=1, has_side_effects=True),
    )(grad, dx, u, dmid, ctx, dqkv)


def place_kernel(a, b, o_q, o_k, o_v, o_o, o_1, o_2, sem):
    cps = []

    def move(src, dst):
        cps.append(pltpu.make_async_copy(src, dst, sem.at[len(cps)]))
        cps[-1].start()

    for k in range(4):
        move(a.at[k], o_1.at[:, pl.ds(256 * k, 256)])
        move(a.at[4 + k], o_2.at[pl.ds(512 * (k % 2), 512), pl.ds(256 * (k // 2), 256)])
    for j, o in enumerate((o_q, o_k, o_v)):
        for i in range(2):
            move(b.at[2 * j + i], o.at[pl.ds(256 * i, 256), :])
    for k in range(2):
        move(b.at[6 + k], o_o.at[:, pl.ds(256 * k, 256)])
    for c in cps:
        c.wait()


def run_place(a, b):
    shapes = [(512, 256)] * 3 + [(256, 512), (512, 1024), (1024, 512)]
    return pl.pallas_call(
        place_kernel,
        in_specs=[pl.BlockSpec(memory_space=pltpu.VMEM)] * 2,
        out_specs=[pl.BlockSpec(memory_space=pltpu.HBM)] * 6,
        out_shape=[jax.ShapeDtypeStruct(s, F32) for s in shapes],
        scratch_shapes=[pltpu.SemaphoreType.DMA((16,))],
        compiler_params=pltpu.CompilerParams(vmem_limit_bytes=2_000_000),
    )(a, b)


def solution(mesh):
    spec_col, spec_row, spec_act, spec_rep = P(None, 'model'), P('model', None), P('data', None, None), P(None, None)

    def device_step(x_in, cot_out, step_emb, w_q, w_k, w_v, w_o, w_1, w_2):
        dx, grad, *rest = run_kernel(x_in, cot_out, step_emb, (w_q, w_k, w_v, w_o, w_1, w_2), x_in.shape[0] // 2)
        a, b, dx = run_reduce(grad, dx, *rest)
        return (*run_place(a, b), dx)

    return jax.shard_map(device_step, mesh=mesh,
                         in_specs=(spec_act, spec_act, spec_rep, spec_col, spec_col, spec_col, spec_row, spec_col, spec_row),
                         out_specs=(spec_col, spec_col, spec_col, spec_row, spec_col, spec_row, spec_act),
                         check_vma=False)
```

```python
import functools

import jax
import jax.numpy as jnp
from jax import lax
from jax.experimental import pallas as pl
from jax.experimental.pallas import tpu as pltpu
from jax.sharding import PartitionSpec as P

F32, BF16 = jnp.float32, jnp.bfloat16
T, D, FF, H, E, L = 512, 512, 2048, 8, 64, 4
EPS = 1e-6
CEXP = E ** -0.5 * 1.4426950408889634
SCALE = E ** -0.5
GK0 = 0.7978845608028654
GK1 = 0.044715
R = 32
LN = 128


def dot_nn(a, b):
    return lax.dot_general(a, b, (((1,), (0,)), ((), ())), preferred_element_type=F32)


def dot_nt(a, b):
    return lax.dot_general(a, b, (((1,), (1,)), ((), ())), preferred_element_type=F32)


def rows(r, n=R):
    return pl.ds(r, n)


def wide(e):
    return jnp.concatenate([e] * (T // LN), axis=1)


def col_sum(tile_fn):
    accs = [None, None]
    for i, r in enumerate(range(0, D, R)):
        v = tile_fn(r)
        accs[i % 2] = v if accs[i % 2] is None else accs[i % 2] + v
    return jnp.sum(accs[0] + accs[1], axis=0, keepdims=True)


def rms_of(tile_fn):
    def sq(r):
        v = tile_fn(r)
        return v * v
    return lax.rsqrt(col_sum(sq) * (1.0 / D) + EPS)


def weave(*streams):
    total = max(len(s) for s in streams)
    done = [0] * len(streams)
    for t in range(total):
        for k, s in enumerate(streams):
            upto = -(-len(s) * (t + 1) // total)
            while done[k] < upto:
                s[done[k]]()
                done[k] += 1


def gelu_fwd(z):
    return z * jax.nn.sigmoid(z * (2 * GK0 + (2 * GK0 * GK1) * (z * z)))


def gelu_both(z):
    z2 = z * z
    s = jax.nn.sigmoid(z * (2 * GK0 + (2 * GK0 * GK1) * z2))
    w = z * (2 * GK0 + (6 * GK0 * GK1) * z2)
    return z * s, s * (1.0 + w * (1.0 - s))


def qrow(hd):
    return 768 * (hd // 4) + 64 * (hd % 4)


def pad_head(block, hh):
    zero = jnp.zeros_like(block)
    return jnp.concatenate([block, zero] if hh == 0 else [zero, block], axis=0)


def zip_pad(a, b):
    return [(a[i:i + 1], b[i:i + 1]) for i in range(max(len(a), len(b)))]


def max_cols(ref, cols):
    accs = [None] * 4
    for i, r in enumerate(range(0, T, 64)):
        v = ref[rows(r, 64), cols]
        accs[i % 4] = v if accs[i % 4] is None else jnp.maximum(accs[i % 4], v)
    m = jnp.maximum(jnp.maximum(accs[0], accs[1]), jnp.maximum(accs[2], accs[3]))
    return jnp.max(m, axis=0, keepdims=True)

GL, PR1, PR2 = 256, 512, 256


MESH_ID = pl.DeviceIdType.MESH
NW = 6


def other(i):
    return 1 - i


def kernel(nseq, x_ref, cot_ref, emb_ref, wq_h, wk_h, wv_h, wo_h, w1_h, w2_h,
           dx_h, grad_h, u_h, dmid_h, ctx_h, dqkv_h,
           wqkv, wo, w1, w2, wqkvt, wot, w1t, w2t, g1, g2,
           xs, qkv, ctx, ctxl, hs, zs, lse, rsc, us, ms, act, dz, dn, dmid2, dctx, dqkv2, tmp, sbuf, lcol, dcol, dxs,
           embv, ssem, sem, zsend, zrecv, gsend, grecv, xloc, xsend, xrecv):
    step = pl.program_id(0)
    mi = lax.axis_index('model')
    di = lax.axis_index('data')
    core = di % 2
    zdev = {'model': 1 - mi, 'data': di}
    cdev = {'model': mi, 'data': di + 1 - 2 * core}

    def place(k, m, r0, n):
        if k < 3:
            return wqkv.at[pl.ds(r0, n), pl.ds(768 * m + 256 * k, 256)]
        if k == 3:
            return wo.at[pl.ds(256 * m + r0, n), :]
        if k == 4:
            return w1.at[pl.ds(r0, n), pl.ds(1024 * m, 1024)]
        return w2.at[pl.ds(1024 * m + r0, n), :]

    xx, yy = (di // 2) % 2, di // 4
    dev = {'x': {'model': mi, 'data': di + 2 - 4 * xx}, 'y': {'model': mi, 'data': di + 4 - 8 * yy}, 'z': zdev, 'c': cdev}

    w_hbm = (wq_h, wk_h, wv_h, wo_h, w1_h, w2_h)
    w_rows = (512, 512, 512, 256, 512, 1024)
    groups = ((0, 1, 2), (3,), (4,), (5,))

    def region(g, far, color):
        k = groups[g][0]
        pr = w_rows[k] // 8
        py = 1 - yy if 'y' in far else yy
        px = 1 - xx if 'x' in far else xx
        r0, n = (py * 4 + px * 2 + core) * pr, pr
        if color is not None:
            r0, n = r0 + color * (pr // 2), pr // 2
        if g == 0:
            return wqkv.at[pl.ds(r0, n), pl.ds(768 * (1 - mi), 768)]
        return place(k, 1 - mi, r0, n)

    def turn(m_):
        for j in range(3):
            c = pl.ds(pl.multiple_of(768 * m_ + 256 * j, 256), 256)
            wqkvt[c, :] = wqkv[:, c].T
        c = pl.ds(pl.multiple_of(256 * m_, 256), 256)
        wot[:, c] = wo[c, :].T
        for j in range(2):
            c = pl.ds(pl.multiple_of(1024 * m_ + 512 * j, 512), 512)
            w1t[c, :] = w1[:, c].T
            w2t[:, c] = w2[c, :].T

    def load_weights():
        barrier = pltpu.get_barrier_semaphore()
        for d in 'xyzc':
            pl.semaphore_signal(barrier, inc=1, device_id=dev[d], device_id_type=MESH_ID)
        pl.semaphore_wait(barrier, 4)
        zc, local, plane, sib = {}, [], {}, []

        def hand(g, far, color, d, i):
            o = region(g, far, color)
            cp = pltpu.make_async_remote_copy(o, o, gsend.at[g, i], grecv.at[g, i], device_id=dev[d], device_id_type=MESH_ID)
            cp.start()
            return cp

        for k in range(NW):
            pr = w_rows[k] // 8
            zc[k] = pltpu.make_async_remote_copy(w_hbm[k].at[pl.ds(di * pr, pr), :], place(k, mi, di * pr, pr),
                                                 zsend.at[k], zrecv.at[k], device_id=zdev, device_id_type=MESH_ID)
            zc[k].start()
        for k in range(NW):
            local.append(pltpu.make_async_copy(w_hbm[k], place(k, mi, 0, w_rows[k]), sem.at[k]))
            local[-1].start()

        def own(g):
            for k in groups[g]:
                zc[k].wait_recv()
            for color, ab in enumerate(('xy', 'yx')):
                plane[g, color, 0] = hand(g, '', color, ab[0], 3 * color)
                plane[g, color, 1] = hand(g, '', color, ab[1], 3 * color + 1)
            sib.append(hand(g, '', None, 'c', 6))

        def forward(g):
            for color, ab in enumerate(('xy', 'yx')):
                plane[g, color, 0].wait_recv()
                plane[g, color, 2] = hand(g, ab[0], color, ab[1], 3 * color + 2)
                sib.append(hand(g, ab[0], color, 'c', 7 + 3 * color))

        def finish(g):
            for color, ab in enumerate(('xy', 'yx')):
                plane[g, color, 1].wait_recv()
                sib.append(hand(g, ab[1], color, 'c', 8 + 3 * color))
            for color in range(2):
                plane[g, color, 2].wait_recv()
                sib.append(hand(g, 'xy', color, 'c', 9 + 3 * color))

        for cp in local:
            cp.wait()
        turn(mi)
        for l_ in range(L):
            embv[l_] = jnp.broadcast_to(emb_ref[l_:l_ + 1, :].astype(F32), (LN, D)).T
        own(0)
        own(1)
        own(2)
        forward(0)
        forward(1)
        own(3)
        forward(2)
        finish(0)
        finish(1)
        forward(3)
        finish(2)
        finish(3)
        for k in range(NW):
            zc[k].wait_send()
        for cp in plane.values():
            cp.wait_send()
        for cp in sib:
            cp.wait()

    @pl.when(step == 0)
    def _():
        load_weights()
        turn(1 - mi)
        g1[...] = jnp.zeros_like(g1)
        g2[...] = jnp.zeros_like(g2)

    def stash(k, names, at=0):
        pairs = dict(ctx=(ctx.at[k % L], ctx_h), u=(us.at[k % L], u_h), dmid=(dmid2.at[at], dmid_h), dqkv=(dqkv2.at[at], dqkv_h))
        return [pltpu.make_async_copy(pairs[n][0], pairs[n][1].at[k], ssem.at[at, list(pairs).index(n)]) for n in names]

    def start_all(cs):
        for c in cs:
            c.start()

    def wait_all(cs):
        for c in cs:
            c.wait()

    @pl.when(step == 0)
    def _():
        start_all(stash(L - 1, ('dmid', 'dqkv'), 0))
        start_all(stash(L - 2, ('dmid', 'dqkv'), 1))

    xs[0] = x_ref[0].T
    half = [pl.ds(0, 256), pl.ds(256, 256)]

    def s_tile(l, cols=slice(None)):
        w = 4 if cols == slice(None) else 2
        return lambda r: xs[l, rows(r), cols].astype(F32) + jnp.concatenate([embv[l, rows(r), :]] * w, axis=1)

    def norm_into(dst, tile_fn, l, k, fresh, cols=slice(None)):
        box = {}

        def stat():
            if fresh:
                box['r'] = rms_of(tile_fn)
                rsc[l, pl.ds(k, 1), cols] = box['r']
            else:
                box['r'] = rsc[l, pl.ds(k, 1), cols]

        def put(r):
            dst[rows(r), cols] = (tile_fn(r) * box['r']).astype(BF16)

        return [stat] + [functools.partial(put, r) for r in range(0, D, R)]

    def pull_into(dst, base, tile_of, dy, l, k):
        out = []
        for cols in half:
            tile_fn = tile_of(l, cols)
            box = {}

            def stat(cols=cols, tile_fn=tile_fn, box=box):
                a = col_sum(lambda r: dy[rows(r), cols].astype(F32) * tile_fn(r)) * (1.0 / D)
                rr = rsc[l, pl.ds(k, 1), cols]
                box['r'] = rr
                box['a'] = rr * rr * rr * a

            def put(r, cols=cols, tile_fn=tile_fn, box=box):
                g = dy[rows(r), cols].astype(F32)
                dst[rows(r), cols] = (base[rows(r), cols].astype(F32) + (box['r'] * g - tile_fn(r) * box['a'])).astype(BF16)

            out += [stat] + [functools.partial(put, r) for r in range(0, D, R)]
        return out

    def run(stream):
        for f in stream:
            f()

    def h_tile(l, cols=slice(None)):
        return lambda r: hs[l, rows(r), cols].astype(F32)

    def fwd(l, carry):
        for c in range(2):
            run(norm_into(us.at[l], s_tile(l, half[c]), l, 0, True, half[c]))
        for j in range(3):
            qkv[l, pl.ds(512 * j, 512), :] = dot_nn(wqkvt[pl.ds(512 * j, 512), :], us[l]).astype(BF16)

        kps = {}
        inv = {}

        def stage_a(hd):
            p, hh = divmod(hd, 2)

            def first():
                if hh == 0:
                    kps[p] = qkv[l, pl.ds(qrow(hd) + 256, 128), :].T

            def part(c):
                qp = pad_head(qkv[l, pl.ds(qrow(hd), 64), half[c]], hh)
                sbuf[hd % 2, :, half[c]] = dot_nn(kps[p], qp)

            return [first, lambda: part(0), lambda: part(1)]

        def stage_b(hd):
            sref, eref = sbuf.at[hd % 2], act.at[pl.ds(512 * (hd % 2), 512), :]

            def group(g):
                cols = half[g]
                mx = max_cols(sref, cols) * CEXP
                accs = [None, None]
                for i, r in enumerate(range(0, T, 64)):
                    e = jnp.exp2(sref[rows(r, 64), cols] * CEXP - mx)
                    accs[i % 2] = e if accs[i % 2] is None else accs[i % 2] + e
                    eref[rows(r, 64), cols] = e.astype(BF16)
                sm = jnp.sum(accs[0] + accs[1], axis=0, keepdims=True)
                lse[l, pl.ds(hd, 1), cols] = mx + jnp.log2(sm)
                inv[hd, g] = 1.0 / sm

            return [functools.partial(group, g) for g in range(2)]

        def stage_c(hd):
            def part(c):
                cn = dot_nn(qkv[l, pl.ds(qrow(hd) + 512, 64), :], act[pl.ds(512 * (hd % 2), 512), half[c]])
                cn = cn * inv[hd, c]
                hi = cn.astype(BF16)
                ctx[l, pl.ds(64 * hd, 64), half[c]] = hi
                ctxl[l, pl.ds(64 * hd, 64), half[c]] = (cn - hi.astype(F32)).astype(BF16)

            return [lambda: part(0), lambda: part(1)]

        run(stage_a(0))
        for hd in range(H + 1):
            mx = []
            for x_, y_ in zip_pad(stage_a(hd + 1) if hd + 1 < H else [], stage_c(hd - 1) if hd >= 1 else []):
                mx += x_ + y_
            va = stage_b(hd) if hd < H else []
            weave(mx, va)

        for c in range(2):
            o = dot_nn(wot[...], ctx[l, :, half[c]])
            for r in range(0, D, R):
                sx = xs[l, rows(r), half[c]].astype(F32) + jnp.concatenate([embv[l, rows(r), :]] * 2, axis=1)
                hs[l, rows(r), half[c]] = (sx + o[r:r + R]).astype(BF16)
        for c in range(2):
            run(norm_into(ms.at[l], h_tile(l, half[c]), l, 1, True, half[c]))

        def z_dot(j):
            def f(c):
                js = pl.ds(512 * j, 512)
                zs[l, js, half[c]] = dot_nn(w1t[js, :], ms[l, :, half[c]]).astype(BF16)
            return [lambda: f(0), lambda: f(1)]

        def gelu_stream(j):
            def f(r, c):
                act[rows(r, 64), half[c]] = gelu_fwd(zs[l, rows(r, 64), half[c]].astype(F32)).astype(BF16)
            return [functools.partial(f, r, c) for r in range(512 * j, 512 * j + 512, 64) for c in range(2)]

        @pl.when(l < L - 1)
        def _():
            run(z_dot(0))
            for j in range(4):
                weave(z_dot(j + 1) if j < 3 else [], gelu_stream(j))
            for c in range(2):
                o = dot_nn(w2t[...], act[:, half[c]])
                for r in range(0, D, R):
                    xs[l + 1, rows(r), half[c]] = (hs[l, rows(r), half[c]].astype(F32) + o[r:r + R]).astype(BF16)

        @pl.when(l == L - 1)
        def _():
            for j in range(4):
                run(z_dot(j))
                dn[:, pl.ds(128 * j, 128)] = cot_ref[0, pl.ds(128 * j, 128), :].T
        return carry

    lax.fori_loop(0, L, fwd, 0)


    def bwd(i, carry):
        l = L - 1 - i
        k = step * L + l
        dmid, dqkv = dmid2.at[i % 2], dqkv2.at[i % 2]
        wait_all(stash(k, ('dmid', 'dqkv'), i % 2))
        start_all(stash(k, ('ctx', 'u')))

        def dg_dot(j):
            def f(c):
                js = pl.ds(512 * j, 512)
                dz[js, half[c]] = dot_nn(w2[js, :], dn[:, half[c]]).astype(BF16)
            return [lambda: f(0), lambda: f(1)]

        def gelu_stream(j):
            def f(r, c):
                g, gp = gelu_both(zs[l, rows(r, 64), half[c]].astype(F32))
                act[rows(r, 64), half[c]] = g.astype(BF16)
                dz[rows(r, 64), half[c]] = (dz[rows(r, 64), half[c]].astype(F32) * gp).astype(BF16)
            return [functools.partial(f, r, c) for r in range(512 * j, 512 * j + 512, 64) for c in range(2)]

        def wgrad(j):
            js = pl.ds(512 * j, 512)

            def a(c):
                g2[js, half[c]] += dot_nt(act[js, :], dn[half[c], :])

            def b(c):
                jc = pl.ds(512 * j + 256 * c, 256)
                g1[:, jc] += dot_nt(ms[l], dz[jc, :])
            return [lambda: a(0), lambda: a(1), lambda: b(0), lambda: b(1)]

        run(dg_dot(0))
        def dm_part(k0, k1, last):
            def f(c):
                p = dot_nn(w1[:, 512 * k0:512 * k1], dz[pl.ds(512 * k0, 512 * (k1 - k0)), half[c]])
                if k0 > 0:
                    p = sbuf[0, :, half[c]] + p
                if last:
                    tmp[:, half[c]] = p.astype(BF16)
                else:
                    sbuf[0, :, half[c]] = p
            return [lambda: f(0), lambda: f(1)]

        weave(dg_dot(1) + dg_dot(2) + dg_dot(3), gelu_stream(0))
        weave(wgrad(0), gelu_stream(1))
        weave(wgrad(1) + dm_part(0, 2, False), gelu_stream(2))
        weave(wgrad(2), gelu_stream(3))
        run(dm_part(2, 4, True))
        weave(wgrad(3), pull_into(dmid, dn, h_tile, tmp, l, 1))
        for c in range(2):
            dctx[:, half[c]] = dot_nn(wo[...], dmid[:, half[c]]).astype(BF16)

        qps, dcs = {}, {}

        def column(row):
            return jnp.broadcast_to(row, (LN, T)).T

        def stage_a(hd):
            p, hh = divmod(hd, 2)
            hsl = pl.ds(64 * hd, 64)

            def first():
                if hh == 0:
                    qps[p] = qkv[l, pl.ds(qrow(hd), 128), :].T
                    dcs[p] = dctx[pl.ds(64 * hd, 128), :].T
                c = ctx[l, hsl, :].astype(F32) + ctxl[l, hsl, :].astype(F32)
                dcol[hd % 2] = column(jnp.sum(dctx[hsl, :].astype(F32) * c, axis=0, keepdims=True))
                lcol[hd % 2] = column(lse[l, pl.ds(hd, 1), :])

            def s_part(c):
                kp = pad_head(qkv[l, pl.ds(qrow(hd) + 256, 64), half[c]], hh)
                sbuf[hd % 2, :, half[c]] = dot_nn(qps[p], kp)

            def p_part(c):
                vp = pad_head(qkv[l, pl.ds(qrow(hd) + 512, 64), half[c]], hh)
                dz[pl.ds(512 * (hd % 2), 512), half[c]] = dot_nn(dcs[p], vp).astype(BF16)

            return [first] + [functools.partial(f, c) for f in (s_part, p_part) for c in range(2)]

        def merge(xs_, ys_):
            out = []
            for i in range(max(len(xs_), len(ys_))):
                out += xs_[i:i + 1] + ys_[i:i + 1]
            return out

        def stage_b(hd):
            sl = 512 * (hd % 2)

            def group(g, r0):
                cols = half[g]
                for r in range(r0, r0 + 64, 64):
                    lc = lcol[hd % 2, rows(r, 64), :]
                    dc = dcol[hd % 2, rows(r, 64), :]
                    pr = jnp.exp2(sbuf[hd % 2, rows(r, 64), cols] * CEXP - jnp.concatenate([lc, lc], axis=1))
                    act[rows(sl + r, 64), cols] = pr.astype(BF16)
                    dp = dz[rows(sl + r, 64), cols].astype(F32)
                    act[rows(1024 + sl + r, 64), cols] = (pr * (dp - jnp.concatenate([dc, dc], axis=1))).astype(BF16)

            return [functools.partial(group, g, r0) for r0 in range(0, T, 64) for g in range(2)]

        def stage_c(hd):
            sl = 512 * (hd % 2)
            pb = act.at[pl.ds(sl, 512), :]
            db = act.at[pl.ds(1024 + sl, 512), :]
            hsl = pl.ds(64 * hd, 64)

            def f_v(c):
                dqkv[pl.ds(qrow(hd) + 512, 64), half[c]] = dot_nn(dctx[hsl, :], pb[:, half[c]]).astype(BF16)

            def f_k(c):
                dk = dot_nn(qkv[l, pl.ds(qrow(hd), 64), :], db[:, half[c]]) * SCALE
                dqkv[pl.ds(qrow(hd) + 256, 64), half[c]] = dk.astype(BF16)

            def f_q(c):
                dq = dot_nt(qkv[l, pl.ds(qrow(hd) + 256, 64), :], db[half[c], :]) * SCALE
                dqkv[pl.ds(qrow(hd), 64), half[c]] = dq.astype(BF16)

            return [functools.partial(f, c) for f in (f_v, f_k, f_q) for c in range(2)]

        run(stage_a(0))
        for hd in range(H + 1):
            ma = stage_a(hd + 1) if hd + 1 < H else []
            mc = stage_c(hd - 1) if hd >= 1 else []
            va = stage_b(hd) if hd < H else []
            weave(merge(mc, ma), va)

        for c in range(2):
            tmp[:, half[c]] = dot_nn(wqkv[...], dqkv[:, half[c]]).astype(BF16)
        weave([], pull_into(dn, dmid, s_tile, tmp, l, 0))
        wait_all(stash(k, ('ctx', 'u')))
        start_all(stash(k, ('dmid', 'dqkv'), i % 2))
        return carry

    lax.fori_loop(0, L, bwd, 0)
    slot = step % 2

    def dx_copies(s, at):
        here = dx_h.at[mi * nseq + s]
        loc = pltpu.make_async_copy(dxs.at[at], here, xloc.at[at])
        rem = pltpu.make_async_remote_copy(dxs.at[at], here, xsend.at[at], xrecv.at[s], device_id=zdev, device_id_type=MESH_ID)
        return loc, rem

    def dx_drain(s, at):
        loc, rem = dx_copies(s, at)
        loc.wait()
        rem.wait_send()

    @pl.when(step >= 2)
    def _():
        dx_drain(step - 2, slot)

    dxs[slot] = dn[...].T
    dx_copies(step, slot)[0].start()

    @pl.when(step < nseq - 1)
    def _():
        dx_copies(step, slot)[1].start()

    @pl.when(step == nseq - 1)
    def _():
        for at in range(2):
            wait_all(stash(0, ('dmid', 'dqkv'), at))
        cps = []
        for m_ in range(2):
            for k in range(4):
                cps.append((g1.at[:, pl.ds(1024 * m_ + 256 * k, 256)], grad_h.at[m_, k]))
                cps.append((g2.at[pl.ds(1024 * m_ + 512 * (k % 2), 512), pl.ds(256 * (k // 2), 256)], grad_h.at[m_, 4 + k]))
        cps = [pltpu.make_async_copy(s, d, sem.at[i]) for i, (s, d) in enumerate(cps)]
        for c in cps:
            c.start()
        dx_drain(nseq - 2, (nseq - 2) % 2)
        dx_copies(nseq - 1, (nseq - 1) % 2)[0].wait()
        for s in range(nseq - 1):
            theirs = dx_h.at[(1 - mi) * nseq + s]
            pltpu.make_async_remote_copy(dxs.at[s % 2], theirs, xsend.at[s % 2], xrecv.at[s],
                                         device_id=zdev, device_id_type=MESH_ID).wait_recv()
        for c in cps:
            c.wait()


def run_kernel(x, cot, emb, ws, nseq):
    blk = pl.BlockSpec((1, T, D), lambda i: (lax.axis_index('model') * nseq + i, 0, 0))
    anyspec = pl.BlockSpec(memory_space=pl.ANY)
    V = pltpu.VMEM
    S = pltpu.SemaphoreType.DMA
    return pl.pallas_call(
        functools.partial(kernel, nseq),
        grid=(nseq,),
        in_specs=[blk, blk, pl.BlockSpec(memory_space=pltpu.VMEM)] + [anyspec] * NW,
        out_specs=[anyspec] * 6,
        out_shape=[jax.ShapeDtypeStruct((2 * nseq, T, D), BF16), jax.ShapeDtypeStruct((2, 8, PR1, GL), F32)]
                  + [jax.ShapeDtypeStruct((nseq * L, n, T), BF16) for n in (D, D, D, 1536)],
        scratch_shapes=[V((D, 1536), BF16), V((D, D), BF16), V((D, FF), BF16), V((FF, D), BF16),
                        V((1536, D), BF16), V((D, D), BF16), V((FF, D), BF16), V((D, FF), BF16),
                        V((D, FF), F32), V((FF, D), F32),
                        V((L, D, T), BF16), V((L, 1536, T), BF16), V((L, D, T), BF16), V((L, D, T), BF16), V((L, D, T), BF16),
                        V((L, FF, T), BF16), V((L, H, T), F32), V((L, 2, T), F32), V((L, D, T), BF16), V((L, D, T), BF16), V((FF, T), BF16),
                        V((FF, T), BF16), V((D, T), BF16), V((2, D, T), BF16), V((D, T), BF16), V((2, 1536, T), BF16), V((D, T), BF16),
                        V((2, T, T), F32), V((2, T, LN), F32), V((2, T, LN), F32), V((2, T, D), BF16),
                        V((L, D, LN), F32), S((2, 4)), S((16,)), S((NW,)), S((NW,)), S((4, 13)), S((4, 13)), S((2,)), S((2,)), S((nseq,))],
        compiler_params=pltpu.CompilerParams(dimension_semantics=("arbitrary",), vmem_limit_bytes=67_000_000,
                                             collective_id=0, has_side_effects=True),
    )(x, cot, emb, *ws)


ORDERS = ('xyz', 'yzx', 'zxy')
SPREAD = ('xy', 'yx', None)
CUTS = {PR1: ((0, 176), (176, 168), (344, 168)), PR2: ((0, 88), (88, 88), (176, 80))}
NB = 12


class Later:
    def __init__(self, make):
        self.make = make

    def start(self):
        self.make().start()

    def wait(self):
        self.make().wait()

    def wait_recv(self):
        self.make().wait_recv()

    def wait_send(self):
        self.make().wait_send()


class Summed:
    def __init__(self, pr, mine, other, load, out, rd, r1, r2, r3, sems, me, core, rdma):
        self.pr, self.mine, self.other, self.load, self.out = pr, mine, other, load, out
        self.rd, self.r1, self.r2, self.r3, self.me, self.core, self.rdma = rd, r1, r2, r3, me, core, rdma
        self.ds, self.dr, self.ls, self.ps, self.prv, self.gs, self.gr, self.cs, self.cr = sems
        self.sends, self.sib = [], []

    def piece(self, far):
        pos = {ax: (1 - v if ax in far else v) for ax, v in self.me.items()}
        return (pos['z'] * 2 + pos['y']) * 2 + pos['x']

    def kept(self, color):
        a, b, c = ORDERS[color]
        return [b + c, b, c, '']

    def go(self, ends, d):
        cp = self.rdma(ends, d)
        cp.start()
        self.sends.append(cp)
        return cp

    def rows(self, color):
        return pl.ds(*CUTS[self.pr][color])

    def add(self, dst, src, color):
        r = self.rows(color)
        dst[r, :] += src[r, :]

    def start(self):
        self.d, self.l = {}, {}
        i = 0
        for first in (True, False):
            for j in range(4):
                for color in range(3):
                    k = self.kept(color)[j]
                    e = self.piece(ORDERS[color][0] + k if first else k)
                    r = self.rows(color)
                    self.d[first, j, color] = (e, self.go(
                        lambda e=e, r=r, i=i: (self.other(e).at[r, :], self.rd.at[e, r, :], self.ds.at[i], self.dr.at[i]), 'c'))
                    if self.load is not None:
                        cp = Later(lambda e=e, r=r, i=i: pltpu.make_async_copy(self.load(e).at[r, :], self.mine(e).at[r, :], self.ls.at[i]))
                        cp.start()
                        self.l[first, j, color] = cp
                    i += 1

    def fold(self, first, j, color):
        e, cp = self.d[first, j, color]
        cp.wait_recv()
        if self.load is not None:
            self.l[first, j, color].wait()
        self.add(self.mine(e), self.rd.at[e], color)
        return e

    def phase1(self):
        self.p1, self.p2, self.p3 = {}, {}, {}
        for j in range(4):
            for color in range(3):
                e, r, i = self.fold(True, j, color), self.rows(color), 3 * j + color
                self.p1[j, color] = self.go(
                    lambda e=e, r=r, i=i, j=j: (self.mine(e).at[r, :], self.r1.at[j, r, :], self.ps.at[i], self.prv.at[i]), ORDERS[color][0])

    def fold_kept(self):
        self.e = {(j, color): self.fold(False, j, color) for j in range(4) for color in range(3)}

    def take1(self, j, color):
        self.p1[j, color].wait_recv()
        e = self.e[j, color]
        self.add(self.mine(e), self.r1.at[j], color)
        return e

    def phase2(self):
        for j in range(2):
            for color in range(3):
                e, r, i = self.take1(j, color), self.rows(color), 12 + 3 * j + color
                self.p2[j, color] = self.go(
                    lambda e=e, r=r, i=i, j=j: (self.mine(e).at[r, :], self.r2.at[j, r, :], self.ps.at[i], self.prv.at[i]), ORDERS[color][1])

    def phase3(self):
        for color in range(3):
            e, r, i = self.take1(2, color), self.rows(color), 18 + color
            self.p2[0, color].wait_recv()
            self.add(self.mine(e), self.r2.at[0], color)
            self.p3[color] = self.go(
                lambda e=e, r=r, i=i: (self.mine(e).at[r, :], self.r3.at[r, :], self.ps.at[i], self.prv.at[i]), ORDERS[color][2])
        for color in range(3):
            e = self.take1(3, color)
            self.p2[1, color].wait_recv()
            self.add(self.mine(e), self.r2.at[1], color)

    def at(self, far, r0, n):
        y = 1 - self.me['y'] if 'y' in far else self.me['y']
        x = 1 - self.me['x'] if 'x' in far else self.me['x']
        return self.out.at[(y * 2 + x) * 2 + self.core, pl.ds(r0, n), :]

    def parts(self):
        out = []
        for color, (r0, n) in enumerate(CUTS[self.pr]):
            if SPREAD[color]:
                out.append((color, r0, n, SPREAD[color]))
            else:
                h = n // 16 * 8
                out += [(color, r0, h, 'xy'), (color, r0 + h, n - h, 'yx')]
        return out

    def sibling(self, far, r0, n, i):
        cp = self.rdma(lambda: (self.at(far, r0, n), self.at(far, r0, n), self.cs.at[i], self.cr.at[i]), 'c')
        cp.start()
        self.sib.append(cp)

    def hand(self, far, r0, n, i, d):
        return self.go(lambda: (self.at(far, r0, n), self.at(far, r0, n), self.gs.at[i], self.gr.at[i]), d)

    def spread(self):
        self.g1, self.g2, self.g3 = {}, {}, {}
        for color, (r0, n) in enumerate(CUTS[self.pr]):
            self.p3[color].wait_recv()
            self.at('', r0, n)[...] = self.mine(self.e[3, color])[pl.ds(r0, n), :] + self.r3[pl.ds(r0, n), :]
            for k, (col, q0, qn, ab) in enumerate(self.parts()):
                if col == color:
                    self.g1[k] = self.hand('', q0, qn, k, ab[0])
                    self.g2[k] = self.hand('', q0, qn, 4 + k, ab[1])
        for k, (col, r0, n, ab) in enumerate(self.parts()):
            self.sibling('', r0, n, k)

    def forward(self):
        for k, (col, r0, n, ab) in enumerate(self.parts()):
            self.g1[k].wait_recv()
            self.g3[k] = self.hand(ab[0], r0, n, 8 + k, ab[1])
            self.sibling(ab[0], r0, n, 4 + k)

    def collect(self):
        for k, (col, r0, n, ab) in enumerate(self.parts()):
            self.g2[k].wait_recv()
            self.sibling(ab[1], r0, n, 8 + k)
        for k, (col, r0, n, ab) in enumerate(self.parts()):
            self.g3[k].wait_recv()
            self.sibling('xy', r0, n, 12 + k)

    def finish(self):
        for cp in self.sib:
            cp.wait()
        for cp in self.sends:
            cp.wait_send()


def reduce_kernel(g_h, dx_in, u_h, dmid_h, ctx_h, dqkv_h, out1, out2, dx, acc, full, ub, qb, cb, mb, ra, r1, r2, r3, rb, s1, s2, s3, bsem,
                  ds1, dr1, ls1, ps1, pr1, gs1, gr1, cs1, cr1, ds2, dr2, ls2, ps2, pr2, gs2, gr2, cs2, cr2, xs_, xr_):
    mi = lax.axis_index('model')
    di = lax.axis_index('data')
    core, x, y = di % 2, (di // 2) % 2, di // 4
    me = {'x': x, 'y': y, 'z': mi}
    dev = {'x': {'model': mi, 'data': di + 2 - 4 * x}, 'y': {'model': mi, 'data': di + 4 - 8 * y},
           'z': {'model': 1 - mi, 'data': di}, 'c': {'model': mi, 'data': di + 1 - 2 * core}}

    def rdma(ends, d):
        return Later(lambda: pltpu.make_async_remote_copy(*ends(), device_id=dev[d], device_id_type=MESH_ID))

    barrier = pltpu.get_barrier_semaphore()
    for d in 'xyzc':
        pl.semaphore_signal(barrier, inc=1, device_id=dev[d], device_id_type=MESH_ID)
    pl.semaphore_wait(barrier, 4)

    def g_at(e, c):
        return g_h.at[e // 4, (e % 4) * 2 + c]

    mlp = Summed(PR1, lambda e: acc.at[e], lambda e: g_at(e, 1 - core), lambda e: g_at(e, core), out1, ra, r1, r2, r3,
                 (ds1, dr1, ls1, ps1, pr1, gs1, gr1, cs1, cr1), me, core, rdma)
    att = Summed(PR2, lambda e: full.at[e * 2 + core], lambda e: full.at[e * 2 + 1 - core], None, out2, rb, s1, s2, s3,
                 (ds2, dr2, ls2, ps2, pr2, gs2, gr2, cs2, cr2), me, core, rdma)

    def fetch(i, slot):
        two = pl.ds(2 * i, 2)
        return [pltpu.make_async_copy(u_h.at[two], ub.at[slot], bsem.at[slot, 0]),
                pltpu.make_async_copy(dqkv_h.at[two], qb.at[slot], bsem.at[slot, 1])]

    def fetch_o(i, slot):
        two = pl.ds(2 * i, 2)
        return [pltpu.make_async_copy(ctx_h.at[two], cb.at[slot], bsem.at[3 + slot, 0]),
                pltpu.make_async_copy(dmid_h.at[two], mb.at[slot], bsem.at[3 + slot, 1])]

    def begin(cs):
        for c in cs:
            c.start()

    def end(cs):
        for c in cs:
            c.wait()

    mlp.start()
    for i in range(2):
        begin(fetch(i, i))
    for i in range(2):
        begin(fetch_o(i, i))
    full[...] = jnp.zeros_like(full)

    def loop(fetch_fn, products, hooks):
        def body(i, carry):
            slot = i % 3
            end(fetch_fn(i, slot))

            @pl.when(i < NB - 2)
            def _():
                begin(fetch_fn(i + 2, (i + 2) % 3))

            products(slot)
            for at, hook in hooks.items():
                pl.when(i == at)(hook)
            return carry
        lax.fori_loop(0, NB, body, 0)

    def qkv_products(slot):
        for j in range(6):
            p = None
            for k in range(2):
                d = dot_nt(ub[slot, k], qb[slot, k, pl.ds(256 * j, 256), :])
                p = d if p is None else p + d
            t = (j // 3) * 8 + 2 * (j % 3)
            full[t] += p[:256]
            full[t + 1] += p[256:]

    def o_products(slot):
        for z in range(2):
            for c in range(2):
                p = None
                for k in range(2):
                    d = dot_nt(cb[slot, k, pl.ds(256 * z, 256), :], mb[slot, k, pl.ds(256 * c, 256), :])
                    p = d if p is None else p + d
                full[z * 8 + 6 + c] += p

    nseq = dx.shape[0] // 2
    mine_x, theirs_x = dx.at[mi * nseq + nseq - 1], dx.at[(1 - mi) * nseq + nseq - 1]
    dx_out = rdma(lambda: (mine_x, mine_x, xs_.at[0], xr_.at[0]), 'z')

    loop(fetch, qkv_products, {2: mlp.phase1, 4: mlp.fold_kept, 8: mlp.phase2})
    loop(fetch_o, o_products, {6: mlp.phase3})
    att.start()
    dx_out.start()
    mlp.spread()
    att.phase1()
    att.fold_kept()
    mlp.forward()
    att.phase2()
    mlp.collect()
    att.phase3()
    att.spread()
    att.forward()
    att.collect()
    mlp.finish()
    att.finish()
    dx_out.wait_send()
    rdma(lambda: (theirs_x, theirs_x, xs_.at[0], xr_.at[0]), 'z').wait_recv()


def run_reduce(grad, dx, u, dmid, ctx, dqkv):
    V = pltpu.VMEM
    S = pltpu.SemaphoreType.DMA
    anyspec = pl.BlockSpec(memory_space=pl.ANY)
    sems = [S((24,)), S((24,)), S((24,)), S((21,)), S((21,)), S((12,)), S((12,)), S((16,)), S((16,))]
    return pl.pallas_call(
        reduce_kernel,
        in_specs=[anyspec] * 6,
        out_specs=[pl.BlockSpec(memory_space=pltpu.VMEM)] * 2 + [anyspec],
        out_shape=[jax.ShapeDtypeStruct((8, PR1, GL), F32), jax.ShapeDtypeStruct((8, PR2, GL), F32), jax.ShapeDtypeStruct(dx.shape, dx.dtype)],
        scratch_shapes=[V((8, PR1, GL), F32), V((16, PR2, GL), F32),
                        V((3, 2, D, T), BF16), V((3, 2, 1536, T), BF16), V((3, 2, D, T), BF16), V((3, 2, D, T), BF16),
                        V((8, PR1, GL), F32), V((4, PR1, GL), F32), V((2, PR1, GL), F32), V((PR1, GL), F32),
                        V((8, PR2, GL), F32), V((4, PR2, GL), F32), V((2, PR2, GL), F32), V((PR2, GL), F32), S((6, 2))]
                       + sems + sems + [S((1,)), S((1,))],
        input_output_aliases={1: 2},
        compiler_params=pltpu.CompilerParams(vmem_limit_bytes=47_000_000, collective_id=1, has_side_effects=True),
    )(grad, dx, u, dmid, ctx, dqkv)


def place_kernel(a, b, o_q, o_k, o_v, o_o, o_1, o_2, sem):
    cps = []

    def move(src, dst):
        cps.append(pltpu.make_async_copy(src, dst, sem.at[len(cps)]))
        cps[-1].start()

    for k in range(4):
        move(a.at[k], o_1.at[:, pl.ds(256 * k, 256)])
        move(a.at[4 + k], o_2.at[pl.ds(512 * (k % 2), 512), pl.ds(256 * (k // 2), 256)])
    for j, o in enumerate((o_q, o_k, o_v)):
        for i in range(2):
            move(b.at[2 * j + i], o.at[pl.ds(256 * i, 256), :])
    for k in range(2):
        move(b.at[6 + k], o_o.at[:, pl.ds(256 * k, 256)])
    for c in cps:
        c.wait()


def run_place(a, b):
    shapes = [(512, 256)] * 3 + [(256, 512), (512, 1024), (1024, 512)]
    return pl.pallas_call(
        place_kernel,
        in_specs=[pl.BlockSpec(memory_space=pltpu.VMEM)] * 2,
        out_specs=[pl.BlockSpec(memory_space=pltpu.HBM)] * 6,
        out_shape=[jax.ShapeDtypeStruct(s, F32) for s in shapes],
        scratch_shapes=[pltpu.SemaphoreType.DMA((16,))],
        compiler_params=pltpu.CompilerParams(vmem_limit_bytes=2_000_000),
    )(a, b)


def solution(mesh):
    spec_col, spec_row, spec_act, spec_rep = P(None, 'model'), P('model', None), P('data', None, None), P(None, None)

    def device_step(x_in, cot_out, step_emb, w_q, w_k, w_v, w_o, w_1, w_2):
        dx, grad, *rest = run_kernel(x_in, cot_out, step_emb, (w_q, w_k, w_v, w_o, w_1, w_2), x_in.shape[0] // 2)
        a, b, dx = run_reduce(grad, dx, *rest)
        return (*run_place(a, b), dx)

    return jax.shard_map(device_step, mesh=mesh,
                         in_specs=(spec_act, spec_act, spec_rep, spec_col, spec_col, spec_col, spec_row, spec_col, spec_row),
                         out_specs=(spec_col, spec_col, spec_col, spec_row, spec_col, spec_row, spec_act),
                         check_vma=False)
```

```python
import functools

import jax
import jax.numpy as jnp
from jax import lax
from jax.experimental import pallas as pl
from jax.experimental.pallas import tpu as pltpu
from jax.sharding import PartitionSpec as P

F32, BF16 = jnp.float32, jnp.bfloat16
T, D, FF, H, E, L = 512, 512, 2048, 8, 64, 4
EPS = 1e-6
CEXP = E ** -0.5 * 1.4426950408889634
SCALE = E ** -0.5
GK0 = 0.7978845608028654
GK1 = 0.044715
R = 32
LN = 128


def dot_nn(a, b):
    return lax.dot_general(a, b, (((1,), (0,)), ((), ())), preferred_element_type=F32)


def dot_nt(a, b):
    return lax.dot_general(a, b, (((1,), (1,)), ((), ())), preferred_element_type=F32)


def rows(r, n=R):
    return pl.ds(r, n)


def wide(e):
    return jnp.concatenate([e] * (T // LN), axis=1)


def col_sum(tile_fn):
    accs = [None, None]
    for i, r in enumerate(range(0, D, R)):
        v = tile_fn(r)
        accs[i % 2] = v if accs[i % 2] is None else accs[i % 2] + v
    return jnp.sum(accs[0] + accs[1], axis=0, keepdims=True)


def rms_of(tile_fn):
    def sq(r):
        v = tile_fn(r)
        return v * v
    return lax.rsqrt(col_sum(sq) * (1.0 / D) + EPS)


def weave(*streams):
    total = max(len(s) for s in streams)
    done = [0] * len(streams)
    for t in range(total):
        for k, s in enumerate(streams):
            upto = -(-len(s) * (t + 1) // total)
            while done[k] < upto:
                s[done[k]]()
                done[k] += 1


def gelu_fwd(z):
    return z * jax.nn.sigmoid(z * (2 * GK0 + (2 * GK0 * GK1) * (z * z)))


def gelu_both(z):
    z2 = z * z
    s = jax.nn.sigmoid(z * (2 * GK0 + (2 * GK0 * GK1) * z2))
    g = z * s
    return g, s + (g * (1.0 - s)) * (2 * GK0 + (6 * GK0 * GK1) * z2)


def qrow(hd):
    return 768 * (hd // 4) + 64 * (hd % 4)


def pad_head(block, hh):
    zero = jnp.zeros_like(block)
    return jnp.concatenate([block, zero] if hh == 0 else [zero, block], axis=0)


def zip_pad(a, b):
    return [(a[i:i + 1], b[i:i + 1]) for i in range(max(len(a), len(b)))]


def max_cols(ref, cols):
    accs = [None] * 4
    for i, r in enumerate(range(0, T, 64)):
        v = ref[rows(r, 64), cols]
        accs[i % 4] = v if accs[i % 4] is None else jnp.maximum(accs[i % 4], v)
    m = jnp.maximum(jnp.maximum(accs[0], accs[1]), jnp.maximum(accs[2], accs[3]))
    return jnp.max(m, axis=0, keepdims=True)

GL, PR1, PR2 = 256, 512, 256


MESH_ID = pl.DeviceIdType.MESH
NW = 6


def other(i):
    return 1 - i


def kernel(nseq, x_ref, cot_ref, emb_ref, wq_h, wk_h, wv_h, wo_h, w1_h, w2_h,
           dx_h, grad_h, u_h, dmid_h, ctx_h, dqkv_h,
           wqkv, wo, w1, w2, wqkvt, wot, w1t, w2t, g1, g2,
           xs, qkv, ctx, ctxl, hs, zs, lse, rsc, us, ms, act, dz, dn, dmid2, dctx, dqkv2, tmp, sbuf, lcol, dcol, dxs,
           embv, ssem, sem, zsend, zrecv, gsend, grecv, xloc, xsend, xrecv):
    step = pl.program_id(0)
    mi = lax.axis_index('model')
    di = lax.axis_index('data')
    core = di % 2
    zdev = {'model': 1 - mi, 'data': di}
    cdev = {'model': mi, 'data': di + 1 - 2 * core}

    def place(k, m, r0, n):
        if k < 3:
            return wqkv.at[pl.ds(r0, n), pl.ds(768 * m + 256 * k, 256)]
        if k == 3:
            return wo.at[pl.ds(256 * m + r0, n), :]
        if k == 4:
            return w1.at[pl.ds(r0, n), pl.ds(1024 * m, 1024)]
        return w2.at[pl.ds(1024 * m + r0, n), :]

    xx, yy = (di // 2) % 2, di // 4
    dev = {'x': {'model': mi, 'data': di + 2 - 4 * xx}, 'y': {'model': mi, 'data': di + 4 - 8 * yy}, 'z': zdev, 'c': cdev}

    w_hbm = (wq_h, wk_h, wv_h, wo_h, w1_h, w2_h)
    w_rows = (512, 512, 512, 256, 512, 1024)
    groups = ((0, 1, 2), (3,), (4,), (5,))

    def region(g, far, color):
        k = groups[g][0]
        pr = w_rows[k] // 8
        py = 1 - yy if 'y' in far else yy
        px = 1 - xx if 'x' in far else xx
        r0, n = (py * 4 + px * 2 + core) * pr, pr
        if color is not None:
            r0, n = r0 + color * (pr // 2), pr // 2
        if g == 0:
            return wqkv.at[pl.ds(r0, n), pl.ds(768 * (1 - mi), 768)]
        return place(k, 1 - mi, r0, n)

    def turn(m_):
        for j in range(3):
            c = pl.ds(pl.multiple_of(768 * m_ + 256 * j, 256), 256)
            wqkvt[c, :] = wqkv[:, c].T
        c = pl.ds(pl.multiple_of(256 * m_, 256), 256)
        wot[:, c] = wo[c, :].T
        for j in range(2):
            c = pl.ds(pl.multiple_of(1024 * m_ + 512 * j, 512), 512)
            w1t[c, :] = w1[:, c].T
            w2t[:, c] = w2[c, :].T

    def load_weights():
        barrier = pltpu.get_barrier_semaphore()
        for d in 'xyzc':
            pl.semaphore_signal(barrier, inc=1, device_id=dev[d], device_id_type=MESH_ID)
        pl.semaphore_wait(barrier, 4)
        zc, local, plane, sib = {}, [], {}, []

        def hand(g, far, color, d, i):
            o = region(g, far, color)
            cp = pltpu.make_async_remote_copy(o, o, gsend.at[g, i], grecv.at[g, i], device_id=dev[d], device_id_type=MESH_ID)
            cp.start()
            return cp

        for k in range(NW):
            pr = w_rows[k] // 8
            zc[k] = pltpu.make_async_remote_copy(w_hbm[k].at[pl.ds(di * pr, pr), :], place(k, mi, di * pr, pr),
                                                 zsend.at[k], zrecv.at[k], device_id=zdev, device_id_type=MESH_ID)
            zc[k].start()
        for k in range(NW):
            local.append(pltpu.make_async_copy(w_hbm[k], place(k, mi, 0, w_rows[k]), sem.at[k]))
            local[-1].start()

        def own(g):
            for k in groups[g]:
                zc[k].wait_recv()
            for color, ab in enumerate(('xy', 'yx')):
                plane[g, color, 0] = hand(g, '', color, ab[0], 3 * color)
                plane[g, color, 1] = hand(g, '', color, ab[1], 3 * color + 1)
            sib.append(hand(g, '', None, 'c', 6))

        def forward(g):
            for color, ab in enumerate(('xy', 'yx')):
                plane[g, color, 0].wait_recv()
                plane[g, color, 2] = hand(g, ab[0], color, ab[1], 3 * color + 2)
                sib.append(hand(g, ab[0], color, 'c', 7 + 3 * color))

        def finish(g):
            for color, ab in enumerate(('xy', 'yx')):
                plane[g, color, 1].wait_recv()
                sib.append(hand(g, ab[1], color, 'c', 8 + 3 * color))
            for color in range(2):
                plane[g, color, 2].wait_recv()
                sib.append(hand(g, 'xy', color, 'c', 9 + 3 * color))

        for cp in local:
            cp.wait()
        turn(mi)
        for l_ in range(L):
            embv[l_] = jnp.broadcast_to(emb_ref[l_:l_ + 1, :].astype(F32), (LN, D)).T
        own(0)
        own(1)
        own(2)
        forward(0)
        forward(1)
        own(3)
        forward(2)
        finish(0)
        finish(1)
        forward(3)
        finish(2)
        finish(3)
        for k in range(NW):
            zc[k].wait_send()
        for cp in plane.values():
            cp.wait_send()
        for cp in sib:
            cp.wait()

    @pl.when(step == 0)
    def _():
        load_weights()
        turn(1 - mi)
        g1[...] = jnp.zeros_like(g1)
        g2[...] = jnp.zeros_like(g2)

    def stash(k, names, at=0):
        pairs = dict(ctx=(ctx.at[k % L], ctx_h), u=(us.at[k % L], u_h), dmid=(dmid2.at[at], dmid_h), dqkv=(dqkv2.at[at], dqkv_h))
        return [pltpu.make_async_copy(pairs[n][0], pairs[n][1].at[k], ssem.at[at, list(pairs).index(n)]) for n in names]

    def start_all(cs):
        for c in cs:
            c.start()

    def wait_all(cs):
        for c in cs:
            c.wait()

    @pl.when(step == 0)
    def _():
        start_all(stash(L - 1, ('dmid', 'dqkv'), 0))
        start_all(stash(L - 2, ('dmid', 'dqkv'), 1))

    xs[0] = x_ref[0].T
    half = [pl.ds(0, 256), pl.ds(256, 256)]

    def s_tile(l, cols=slice(None)):
        w = 4 if cols == slice(None) else 2
        return lambda r: xs[l, rows(r), cols].astype(F32) + jnp.concatenate([embv[l, rows(r), :]] * w, axis=1)

    def norm_into(dst, tile_fn, l, k, fresh, cols=slice(None)):
        box = {}

        def stat():
            if fresh:
                box['r'] = rms_of(tile_fn)
                rsc[l, pl.ds(k, 1), cols] = box['r']
            else:
                box['r'] = rsc[l, pl.ds(k, 1), cols]

        def put(r):
            dst[rows(r), cols] = (tile_fn(r) * box['r']).astype(BF16)

        return [stat] + [functools.partial(put, r) for r in range(0, D, R)]

    def pull_into(dst, base, tile_of, dy, l, k):
        out = []
        for cols in half:
            tile_fn = tile_of(l, cols)
            box = {}

            def stat(cols=cols, tile_fn=tile_fn, box=box):
                a = col_sum(lambda r: dy[rows(r), cols].astype(F32) * tile_fn(r)) * (1.0 / D)
                rr = rsc[l, pl.ds(k, 1), cols]
                box['r'] = rr
                box['a'] = rr * rr * rr * a

            def put(r, cols=cols, tile_fn=tile_fn, box=box):
                g = dy[rows(r), cols].astype(F32)
                dst[rows(r), cols] = (base[rows(r), cols].astype(F32) + (box['r'] * g - tile_fn(r) * box['a'])).astype(BF16)

            out += [stat] + [functools.partial(put, r) for r in range(0, D, R)]
        return out

    def run(stream):
        for f in stream:
            f()

    def h_tile(l, cols=slice(None)):
        return lambda r: hs[l, rows(r), cols].astype(F32)

    def fwd(l, carry):
        for c in range(2):
            run(norm_into(us.at[l], s_tile(l, half[c]), l, 0, True, half[c]))
        for j in range(3):
            qkv[l, pl.ds(512 * j, 512), :] = dot_nn(wqkvt[pl.ds(512 * j, 512), :], us[l]).astype(BF16)

        kps = {}
        inv = {}

        def stage_a(hd):
            p, hh = divmod(hd, 2)

            def first():
                if hh == 0:
                    kps[p] = qkv[l, pl.ds(qrow(hd) + 256, 128), :].T

            def part(c):
                qp = pad_head(qkv[l, pl.ds(qrow(hd), 64), half[c]], hh)
                sbuf[hd % 2, :, half[c]] = dot_nn(kps[p], qp)

            return [first, lambda: part(0), lambda: part(1)]

        def stage_b(hd):
            sref, eref = sbuf.at[hd % 2], act.at[pl.ds(512 * (hd % 2), 512), :]

            def group(g):
                cols = half[g]
                mx = max_cols(sref, cols)
                accs = [None, None]
                for i, r in enumerate(range(0, T, 64)):
                    e = jnp.exp2((sref[rows(r, 64), cols] - mx) * CEXP)
                    accs[i % 2] = e if accs[i % 2] is None else accs[i % 2] + e
                    eref[rows(r, 64), cols] = e.astype(BF16)
                sm = jnp.sum(accs[0] + accs[1], axis=0, keepdims=True)
                lse[l, pl.ds(hd, 1), cols] = mx + jnp.log2(sm) * (1.0 / CEXP)
                inv[hd, g] = 1.0 / sm

            return [functools.partial(group, g) for g in range(2)]

        def stage_c(hd):
            def part(c):
                cn = dot_nn(qkv[l, pl.ds(qrow(hd) + 512, 64), :], act[pl.ds(512 * (hd % 2), 512), half[c]])
                cn = cn * inv[hd, c]
                hi = cn.astype(BF16)
                ctx[l, pl.ds(64 * hd, 64), half[c]] = hi
                ctxl[l, pl.ds(64 * hd, 64), half[c]] = (cn - hi.astype(F32)).astype(BF16)

            return [lambda: part(0), lambda: part(1)]

        run(stage_a(0))
        for hd in range(H + 1):
            mx = []
            for x_, y_ in zip_pad(stage_a(hd + 1) if hd + 1 < H else [], stage_c(hd - 1) if hd >= 1 else []):
                mx += x_ + y_
            va = stage_b(hd) if hd < H else []
            weave(mx, va)

        for c in range(2):
            o = dot_nn(wot[...], ctx[l, :, half[c]])
            for r in range(0, D, R):
                sx = xs[l, rows(r), half[c]].astype(F32) + jnp.concatenate([embv[l, rows(r), :]] * 2, axis=1)
                hs[l, rows(r), half[c]] = (sx + o[r:r + R]).astype(BF16)
        for c in range(2):
            run(norm_into(ms.at[l], h_tile(l, half[c]), l, 1, True, half[c]))

        def z_dot(j):
            def f(c):
                js = pl.ds(512 * j, 512)
                zs[l, js, half[c]] = dot_nn(w1t[js, :], ms[l, :, half[c]]).astype(BF16)
            return [lambda: f(0), lambda: f(1)]

        def gelu_stream(j):
            def f(r, c):
                act[rows(r, 64), half[c]] = gelu_fwd(zs[l, rows(r, 64), half[c]].astype(F32)).astype(BF16)
            return [functools.partial(f, r, c) for r in range(512 * j, 512 * j + 512, 64) for c in range(2)]

        @pl.when(l < L - 1)
        def _():
            run(z_dot(0))
            for j in range(4):
                weave(z_dot(j + 1) if j < 3 else [], gelu_stream(j))
            for c in range(2):
                o = dot_nn(w2t[...], act[:, half[c]])
                for r in range(0, D, R):
                    xs[l + 1, rows(r), half[c]] = (hs[l, rows(r), half[c]].astype(F32) + o[r:r + R]).astype(BF16)

        @pl.when(l == L - 1)
        def _():
            for j in range(4):
                run(z_dot(j))
                dn[:, pl.ds(128 * j, 128)] = cot_ref[0, pl.ds(128 * j, 128), :].T
        return carry

    lax.fori_loop(0, L, fwd, 0)


    def bwd(i, carry):
        l = L - 1 - i
        k = step * L + l
        dmid, dqkv = dmid2.at[i % 2], dqkv2.at[i % 2]
        wait_all(stash(k, ('dmid', 'dqkv'), i % 2))
        start_all(stash(k, ('ctx', 'u')))

        def dg_dot(j):
            def f(c):
                js = pl.ds(512 * j, 512)
                dz[js, half[c]] = dot_nn(w2[js, :], dn[:, half[c]]).astype(BF16)
            return [lambda: f(0), lambda: f(1)]

        def gelu_stream(j):
            def f(r, c):
                g, gp = gelu_both(zs[l, rows(r, 64), half[c]].astype(F32))
                act[rows(r, 64), half[c]] = g.astype(BF16)
                dz[rows(r, 64), half[c]] = (dz[rows(r, 64), half[c]].astype(F32) * gp).astype(BF16)
            return [functools.partial(f, r, c) for r in range(512 * j, 512 * j + 512, 64) for c in range(2)]

        def wgrad(j):
            js = pl.ds(512 * j, 512)

            def a(c):
                g2[js, half[c]] += dot_nt(act[js, :], dn[half[c], :])

            def b(c):
                jc = pl.ds(512 * j + 256 * c, 256)
                g1[:, jc] += dot_nt(ms[l], dz[jc, :])
            return [lambda: a(0), lambda: a(1), lambda: b(0), lambda: b(1)]

        run(dg_dot(0))
        def dm_part(k0, k1, last):
            def f(c):
                p = dot_nn(w1[:, 512 * k0:512 * k1], dz[pl.ds(512 * k0, 512 * (k1 - k0)), half[c]])
                if k0 > 0:
                    p = sbuf[0, :, half[c]] + p
                if last:
                    tmp[:, half[c]] = p.astype(BF16)
                else:
                    sbuf[0, :, half[c]] = p
            return [lambda: f(0), lambda: f(1)]

        weave(dg_dot(1) + dg_dot(2) + dg_dot(3), gelu_stream(0))
        weave(wgrad(0), gelu_stream(1))
        weave(wgrad(1) + dm_part(0, 2, False), gelu_stream(2))
        weave(wgrad(2), gelu_stream(3))
        run(dm_part(2, 4, True))
        weave(wgrad(3), pull_into(dmid, dn, h_tile, tmp, l, 1))
        for c in range(2):
            dctx[:, half[c]] = dot_nn(wo[...], dmid[:, half[c]]).astype(BF16)

        qps, dcs = {}, {}

        def column(row):
            return jnp.broadcast_to(row, (LN, T)).T

        def stage_a(hd):
            p, hh = divmod(hd, 2)
            hsl = pl.ds(64 * hd, 64)

            def first():
                if hh == 0:
                    qps[p] = qkv[l, pl.ds(qrow(hd), 128), :].T
                    dcs[p] = dctx[pl.ds(64 * hd, 128), :].T
                c = ctx[l, hsl, :].astype(F32) + ctxl[l, hsl, :].astype(F32)
                dcol[hd % 2] = column(jnp.sum(dctx[hsl, :].astype(F32) * c, axis=0, keepdims=True))
                lcol[hd % 2] = column(lse[l, pl.ds(hd, 1), :])

            def s_part(c):
                kp = pad_head(qkv[l, pl.ds(qrow(hd) + 256, 64), half[c]], hh)
                sbuf[hd % 2, :, half[c]] = dot_nn(qps[p], kp)

            def p_part(c):
                vp = pad_head(qkv[l, pl.ds(qrow(hd) + 512, 64), half[c]], hh)
                dz[pl.ds(512 * (hd % 2), 512), half[c]] = dot_nn(dcs[p], vp).astype(BF16)

            return [first] + [functools.partial(f, c) for f in (s_part, p_part) for c in range(2)]

        def merge(xs_, ys_):
            out = []
            for i in range(max(len(xs_), len(ys_))):
                out += xs_[i:i + 1] + ys_[i:i + 1]
            return out

        def stage_b(hd):
            sl = 512 * (hd % 2)

            def group(g, r0):
                cols = half[g]
                for r in range(r0, r0 + 64, 64):
                    lc = lcol[hd % 2, rows(r, 64), :]
                    dc = dcol[hd % 2, rows(r, 64), :]
                    pr = jnp.exp2((sbuf[hd % 2, rows(r, 64), cols] - jnp.concatenate([lc, lc], axis=1)) * CEXP)
                    act[rows(sl + r, 64), cols] = pr.astype(BF16)
                    dp = dz[rows(sl + r, 64), cols].astype(F32)
                    act[rows(1024 + sl + r, 64), cols] = (pr * (dp - jnp.concatenate([dc, dc], axis=1))).astype(BF16)

            return [functools.partial(group, g, r0) for r0 in range(0, T, 64) for g in range(2)]

        def stage_c(hd):
            sl = 512 * (hd % 2)
            pb = act.at[pl.ds(sl, 512), :]
            db = act.at[pl.ds(1024 + sl, 512), :]
            hsl = pl.ds(64 * hd, 64)

            def f_v(c):
                dqkv[pl.ds(qrow(hd) + 512, 64), half[c]] = dot_nn(dctx[hsl, :], pb[:, half[c]]).astype(BF16)

            def f_k(c):
                dk = dot_nn(qkv[l, pl.ds(qrow(hd), 64), :], db[:, half[c]]) * SCALE
                dqkv[pl.ds(qrow(hd) + 256, 64), half[c]] = dk.astype(BF16)

            def f_q(c):
                dq = dot_nt(qkv[l, pl.ds(qrow(hd) + 256, 64), :], db[half[c], :]) * SCALE
                dqkv[pl.ds(qrow(hd), 64), half[c]] = dq.astype(BF16)

            return [functools.partial(f, c) for f in (f_v, f_k, f_q) for c in range(2)]

        run(stage_a(0))
        for hd in range(H + 1):
            ma = stage_a(hd + 1) if hd + 1 < H else []
            mc = stage_c(hd - 1) if hd >= 1 else []
            va = stage_b(hd) if hd < H else []
            weave(merge(mc, ma), va)

        for c in range(2):
            tmp[:, half[c]] = dot_nn(wqkv[...], dqkv[:, half[c]]).astype(BF16)
        weave([], pull_into(dn, dmid, s_tile, tmp, l, 0))
        wait_all(stash(k, ('ctx', 'u')))
        start_all(stash(k, ('dmid', 'dqkv'), i % 2))
        return carry

    lax.fori_loop(0, L, bwd, 0)
    slot = step % 2

    def dx_copies(s, at):
        here = dx_h.at[mi * nseq + s]
        loc = pltpu.make_async_copy(dxs.at[at], here, xloc.at[at])
        rem = pltpu.make_async_remote_copy(dxs.at[at], here, xsend.at[at], xrecv.at[s], device_id=zdev, device_id_type=MESH_ID)
        return loc, rem

    def dx_drain(s, at):
        loc, rem = dx_copies(s, at)
        loc.wait()
        rem.wait_send()

    @pl.when(step >= 2)
    def _():
        dx_drain(step - 2, slot)

    dxs[slot] = dn[...].T
    dx_copies(step, slot)[0].start()

    @pl.when(step < nseq - 1)
    def _():
        dx_copies(step, slot)[1].start()

    @pl.when(step == nseq - 1)
    def _():
        for at in range(2):
            wait_all(stash(0, ('dmid', 'dqkv'), at))
        cps = []
        for m_ in range(2):
            for k in range(4):
                cps.append((g1.at[:, pl.ds(1024 * m_ + 256 * k, 256)], grad_h.at[m_, k]))
                cps.append((g2.at[pl.ds(1024 * m_ + 512 * (k % 2), 512), pl.ds(256 * (k // 2), 256)], grad_h.at[m_, 4 + k]))
        cps = [pltpu.make_async_copy(s, d, sem.at[i]) for i, (s, d) in enumerate(cps)]
        for c in cps:
            c.start()
        dx_drain(nseq - 2, (nseq - 2) % 2)
        dx_copies(nseq - 1, (nseq - 1) % 2)[0].wait()
        for s in range(nseq - 1):
            theirs = dx_h.at[(1 - mi) * nseq + s]
            pltpu.make_async_remote_copy(dxs.at[s % 2], theirs, xsend.at[s % 2], xrecv.at[s],
                                         device_id=zdev, device_id_type=MESH_ID).wait_recv()
        for c in cps:
            c.wait()


def run_kernel(x, cot, emb, ws, nseq):
    blk = pl.BlockSpec((1, T, D), lambda i: (lax.axis_index('model') * nseq + i, 0, 0))
    anyspec = pl.BlockSpec(memory_space=pl.ANY)
    V = pltpu.VMEM
    S = pltpu.SemaphoreType.DMA
    return pl.pallas_call(
        functools.partial(kernel, nseq),
        grid=(nseq,),
        in_specs=[blk, blk, pl.BlockSpec(memory_space=pltpu.VMEM)] + [anyspec] * NW,
        out_specs=[anyspec] * 6,
        out_shape=[jax.ShapeDtypeStruct((2 * nseq, T, D), BF16), jax.ShapeDtypeStruct((2, 8, PR1, GL), F32)]
                  + [jax.ShapeDtypeStruct((nseq * L, n, T), BF16) for n in (D, D, D, 1536)],
        scratch_shapes=[V((D, 1536), BF16), V((D, D), BF16), V((D, FF), BF16), V((FF, D), BF16),
                        V((1536, D), BF16), V((D, D), BF16), V((FF, D), BF16), V((D, FF), BF16),
                        V((D, FF), F32), V((FF, D), F32),
                        V((L, D, T), BF16), V((L, 1536, T), BF16), V((L, D, T), BF16), V((L, D, T), BF16), V((L, D, T), BF16),
                        V((L, FF, T), BF16), V((L, H, T), F32), V((L, 2, T), F32), V((L, D, T), BF16), V((L, D, T), BF16), V((FF, T), BF16),
                        V((FF, T), BF16), V((D, T), BF16), V((2, D, T), BF16), V((D, T), BF16), V((2, 1536, T), BF16), V((D, T), BF16),
                        V((2, T, T), F32), V((2, T, LN), F32), V((2, T, LN), F32), V((2, T, D), BF16),
                        V((L, D, LN), F32), S((2, 4)), S((16,)), S((NW,)), S((NW,)), S((4, 13)), S((4, 13)), S((2,)), S((2,)), S((nseq,))],
        compiler_params=pltpu.CompilerParams(dimension_semantics=("arbitrary",), vmem_limit_bytes=67_000_000,
                                             collective_id=0, has_side_effects=True),
    )(x, cot, emb, *ws)


ORDERS = ('xyz', 'yzx', 'zxy')
SPREAD = ('xy', 'yx', None)
CUTS = {PR1: ((0, 176), (176, 168), (344, 168)), PR2: ((0, 88), (88, 88), (176, 80))}
NB = 12


class Later:
    def __init__(self, make):
        self.make = make

    def start(self):
        self.make().start()

    def wait(self):
        self.make().wait()

    def wait_recv(self):
        self.make().wait_recv()

    def wait_send(self):
        self.make().wait_send()


class Summed:
    def __init__(self, pr, mine, other, load, out, rd, r1, r2, r3, sems, me, core, rdma):
        self.pr, self.mine, self.other, self.load, self.out = pr, mine, other, load, out
        self.rd, self.r1, self.r2, self.r3, self.me, self.core, self.rdma = rd, r1, r2, r3, me, core, rdma
        self.ds, self.dr, self.ls, self.ps, self.prv, self.gs, self.gr, self.cs, self.cr = sems
        self.sends, self.sib = [], []

    def piece(self, far):
        pos = {ax: (1 - v if ax in far else v) for ax, v in self.me.items()}
        return (pos['z'] * 2 + pos['y']) * 2 + pos['x']

    def kept(self, color):
        a, b, c = ORDERS[color]
        return [b + c, b, c, '']

    def go(self, ends, d):
        cp = self.rdma(ends, d)
        cp.start()
        self.sends.append(cp)
        return cp

    def rows(self, color):
        return pl.ds(*CUTS[self.pr][color])

    def add(self, dst, src, color):
        r = self.rows(color)
        dst[r, :] += src[r, :]

    def start(self):
        self.d, self.l = {}, {}
        i = 0
        for first in (True, False):
            for j in range(4):
                for color in range(3):
                    k = self.kept(color)[j]
                    e = self.piece(ORDERS[color][0] + k if first else k)
                    r = self.rows(color)
                    self.d[first, j, color] = (e, self.go(
                        lambda e=e, r=r, i=i: (self.other(e).at[r, :], self.rd.at[e, r, :], self.ds.at[i], self.dr.at[i]), 'c'))
                    if self.load is not None:
                        cp = Later(lambda e=e, r=r, i=i: pltpu.make_async_copy(self.load(e).at[r, :], self.mine(e).at[r, :], self.ls.at[i]))
                        cp.start()
                        self.l[first, j, color] = cp
                    i += 1

    def fold(self, first, j, color):
        e, cp = self.d[first, j, color]
        cp.wait_recv()
        if self.load is not None:
            self.l[first, j, color].wait()
        self.add(self.mine(e), self.rd.at[e], color)
        return e

    def phase1(self):
        self.p1, self.p2, self.p3 = {}, {}, {}
        for j in range(4):
            for color in range(3):
                e, r, i = self.fold(True, j, color), self.rows(color), 3 * j + color
                self.p1[j, color] = self.go(
                    lambda e=e, r=r, i=i, j=j: (self.mine(e).at[r, :], self.r1.at[j, r, :], self.ps.at[i], self.prv.at[i]), ORDERS[color][0])

    def fold_kept(self):
        self.e = {(j, color): self.fold(False, j, color) for j in range(4) for color in range(3)}

    def take1(self, j, color):
        self.p1[j, color].wait_recv()
        e = self.e[j, color]
        self.add(self.mine(e), self.r1.at[j], color)
        return e

    def phase2(self):
        for j in range(2):
            for color in range(3):
                e, r, i = self.take1(j, color), self.rows(color), 12 + 3 * j + color
                self.p2[j, color] = self.go(
                    lambda e=e, r=r, i=i, j=j: (self.mine(e).at[r, :], self.r2.at[j, r, :], self.ps.at[i], self.prv.at[i]), ORDERS[color][1])

    def phase3(self):
        for color in range(3):
            e, r, i = self.take1(2, color), self.rows(color), 18 + color
            self.p2[0, color].wait_recv()
            self.add(self.mine(e), self.r2.at[0], color)
            self.p3[color] = self.go(
                lambda e=e, r=r, i=i: (self.mine(e).at[r, :], self.r3.at[r, :], self.ps.at[i], self.prv.at[i]), ORDERS[color][2])
        for color in range(3):
            e = self.take1(3, color)
            self.p2[1, color].wait_recv()
            self.add(self.mine(e), self.r2.at[1], color)

    def at(self, far, r0, n):
        y = 1 - self.me['y'] if 'y' in far else self.me['y']
        x = 1 - self.me['x'] if 'x' in far else self.me['x']
        return self.out.at[(y * 2 + x) * 2 + self.core, pl.ds(r0, n), :]

    def parts(self):
        out = []
        for color, (r0, n) in enumerate(CUTS[self.pr]):
            if SPREAD[color]:
                out.append((color, r0, n, SPREAD[color]))
            else:
                h = n // 16 * 8
                out += [(color, r0, h, 'xy'), (color, r0 + h, n - h, 'yx')]
        return out

    def sibling(self, far, r0, n, i):
        cp = self.rdma(lambda: (self.at(far, r0, n), self.at(far, r0, n), self.cs.at[i], self.cr.at[i]), 'c')
        cp.start()
        self.sib.append(cp)

    def hand(self, far, r0, n, i, d):
        return self.go(lambda: (self.at(far, r0, n), self.at(far, r0, n), self.gs.at[i], self.gr.at[i]), d)

    def spread(self):
        self.g1, self.g2, self.g3 = {}, {}, {}
        for color, (r0, n) in enumerate(CUTS[self.pr]):
            self.p3[color].wait_recv()
            self.at('', r0, n)[...] = self.mine(self.e[3, color])[pl.ds(r0, n), :] + self.r3[pl.ds(r0, n), :]
            for k, (col, q0, qn, ab) in enumerate(self.parts()):
                if col == color:
                    self.g1[k] = self.hand('', q0, qn, k, ab[0])
                    self.g2[k] = self.hand('', q0, qn, 4 + k, ab[1])
        for k, (col, r0, n, ab) in enumerate(self.parts()):
            self.sibling('', r0, n, k)

    def forward(self):
        for k, (col, r0, n, ab) in enumerate(self.parts()):
            self.g1[k].wait_recv()
            self.g3[k] = self.hand(ab[0], r0, n, 8 + k, ab[1])
            self.sibling(ab[0], r0, n, 4 + k)

    def collect(self):
        for k, (col, r0, n, ab) in enumerate(self.parts()):
            self.g2[k].wait_recv()
            self.sibling(ab[1], r0, n, 8 + k)
        for k, (col, r0, n, ab) in enumerate(self.parts()):
            self.g3[k].wait_recv()
            self.sibling('xy', r0, n, 12 + k)

    def finish(self):
        for cp in self.sib:
            cp.wait()
        for cp in self.sends:
            cp.wait_send()


def reduce_kernel(g_h, dx_in, u_h, dmid_h, ctx_h, dqkv_h, out1, out2, dx, acc, full, ub, qb, cb, mb, ra, r1, r2, r3, rb, s1, s2, s3, bsem,
                  ds1, dr1, ls1, ps1, pr1, gs1, gr1, cs1, cr1, ds2, dr2, ls2, ps2, pr2, gs2, gr2, cs2, cr2, xs_, xr_):
    mi = lax.axis_index('model')
    di = lax.axis_index('data')
    core, x, y = di % 2, (di // 2) % 2, di // 4
    me = {'x': x, 'y': y, 'z': mi}
    dev = {'x': {'model': mi, 'data': di + 2 - 4 * x}, 'y': {'model': mi, 'data': di + 4 - 8 * y},
           'z': {'model': 1 - mi, 'data': di}, 'c': {'model': mi, 'data': di + 1 - 2 * core}}

    def rdma(ends, d):
        return Later(lambda: pltpu.make_async_remote_copy(*ends(), device_id=dev[d], device_id_type=MESH_ID))

    barrier = pltpu.get_barrier_semaphore()
    for d in 'xyzc':
        pl.semaphore_signal(barrier, inc=1, device_id=dev[d], device_id_type=MESH_ID)
    pl.semaphore_wait(barrier, 4)

    def g_at(e, c):
        return g_h.at[e // 4, (e % 4) * 2 + c]

    mlp = Summed(PR1, lambda e: acc.at[e], lambda e: g_at(e, 1 - core), lambda e: g_at(e, core), out1, ra, r1, r2, r3,
                 (ds1, dr1, ls1, ps1, pr1, gs1, gr1, cs1, cr1), me, core, rdma)
    att = Summed(PR2, lambda e: full.at[e * 2 + core], lambda e: full.at[e * 2 + 1 - core], None, out2, rb, s1, s2, s3,
                 (ds2, dr2, ls2, ps2, pr2, gs2, gr2, cs2, cr2), me, core, rdma)

    def fetch(i, slot):
        two = pl.ds(2 * i, 2)
        return [pltpu.make_async_copy(u_h.at[two], ub.at[slot], bsem.at[slot, 0]),
                pltpu.make_async_copy(dqkv_h.at[two], qb.at[slot], bsem.at[slot, 1])]

    def fetch_o(i, slot):
        two = pl.ds(2 * i, 2)
        return [pltpu.make_async_copy(ctx_h.at[two], cb.at[slot], bsem.at[3 + slot, 0]),
                pltpu.make_async_copy(dmid_h.at[two], mb.at[slot], bsem.at[3 + slot, 1])]

    def begin(cs):
        for c in cs:
            c.start()

    def end(cs):
        for c in cs:
            c.wait()

    mlp.start()
    for i in range(2):
        begin(fetch(i, i))
    for i in range(2):
        begin(fetch_o(i, i))
    full[...] = jnp.zeros_like(full)

    def loop(fetch_fn, products, hooks):
        def body(i, carry):
            slot = i % 3
            end(fetch_fn(i, slot))

            @pl.when(i < NB - 2)
            def _():
                begin(fetch_fn(i + 2, (i + 2) % 3))

            products(slot)
            for at, hook in hooks.items():
                pl.when(i == at)(hook)
            return carry
        lax.fori_loop(0, NB, body, 0)

    def qkv_products(slot):
        for j in range(6):
            p = None
            for k in range(2):
                d = dot_nt(ub[slot, k], qb[slot, k, pl.ds(256 * j, 256), :])
                p = d if p is None else p + d
            t = (j // 3) * 8 + 2 * (j % 3)
            full[t] += p[:256]
            full[t + 1] += p[256:]

    def o_products(slot):
        for z in range(2):
            for c in range(2):
                p = None
                for k in range(2):
                    d = dot_nt(cb[slot, k, pl.ds(256 * z, 256), :], mb[slot, k, pl.ds(256 * c, 256), :])
                    p = d if p is None else p + d
                full[z * 8 + 6 + c] += p

    nseq = dx.shape[0] // 2
    mine_x, theirs_x = dx.at[mi * nseq + nseq - 1], dx.at[(1 - mi) * nseq + nseq - 1]
    dx_out = rdma(lambda: (mine_x, mine_x, xs_.at[0], xr_.at[0]), 'z')

    loop(fetch, qkv_products, {2: mlp.phase1, 4: mlp.fold_kept, 8: mlp.phase2})
    loop(fetch_o, o_products, {6: mlp.phase3})
    att.start()
    dx_out.start()
    mlp.spread()
    att.phase1()
    att.fold_kept()
    mlp.forward()
    att.phase2()
    mlp.collect()
    att.phase3()
    att.spread()
    att.forward()
    att.collect()
    mlp.finish()
    att.finish()
    dx_out.wait_send()
    rdma(lambda: (theirs_x, theirs_x, xs_.at[0], xr_.at[0]), 'z').wait_recv()


def run_reduce(grad, dx, u, dmid, ctx, dqkv):
    V = pltpu.VMEM
    S = pltpu.SemaphoreType.DMA
    anyspec = pl.BlockSpec(memory_space=pl.ANY)
    sems = [S((24,)), S((24,)), S((24,)), S((21,)), S((21,)), S((12,)), S((12,)), S((16,)), S((16,))]
    return pl.pallas_call(
        reduce_kernel,
        in_specs=[anyspec] * 6,
        out_specs=[pl.BlockSpec(memory_space=pltpu.VMEM)] * 2 + [anyspec],
        out_shape=[jax.ShapeDtypeStruct((8, PR1, GL), F32), jax.ShapeDtypeStruct((8, PR2, GL), F32), jax.ShapeDtypeStruct(dx.shape, dx.dtype)],
        scratch_shapes=[V((8, PR1, GL), F32), V((16, PR2, GL), F32),
                        V((3, 2, D, T), BF16), V((3, 2, 1536, T), BF16), V((3, 2, D, T), BF16), V((3, 2, D, T), BF16),
                        V((8, PR1, GL), F32), V((4, PR1, GL), F32), V((2, PR1, GL), F32), V((PR1, GL), F32),
                        V((8, PR2, GL), F32), V((4, PR2, GL), F32), V((2, PR2, GL), F32), V((PR2, GL), F32), S((6, 2))]
                       + sems + sems + [S((1,)), S((1,))],
        input_output_aliases={1: 2},
        compiler_params=pltpu.CompilerParams(vmem_limit_bytes=47_000_000, collective_id=1, has_side_effects=True),
    )(grad, dx, u, dmid, ctx, dqkv)


def place_kernel(a, b, o_q, o_k, o_v, o_o, o_1, o_2, sem):
    cps = []

    def move(src, dst):
        cps.append(pltpu.make_async_copy(src, dst, sem.at[len(cps)]))
        cps[-1].start()

    for k in range(4):
        move(a.at[k], o_1.at[:, pl.ds(256 * k, 256)])
        move(a.at[4 + k], o_2.at[pl.ds(512 * (k % 2), 512), pl.ds(256 * (k // 2), 256)])
    for j, o in enumerate((o_q, o_k, o_v)):
        for i in range(2):
            move(b.at[2 * j + i], o.at[pl.ds(256 * i, 256), :])
    for k in range(2):
        move(b.at[6 + k], o_o.at[:, pl.ds(256 * k, 256)])
    for c in cps:
        c.wait()


def run_place(a, b):
    shapes = [(512, 256)] * 3 + [(256, 512), (512, 1024), (1024, 512)]
    return pl.pallas_call(
        place_kernel,
        in_specs=[pl.BlockSpec(memory_space=pltpu.VMEM)] * 2,
        out_specs=[pl.BlockSpec(memory_space=pltpu.HBM)] * 6,
        out_shape=[jax.ShapeDtypeStruct(s, F32) for s in shapes],
        scratch_shapes=[pltpu.SemaphoreType.DMA((16,))],
        compiler_params=pltpu.CompilerParams(vmem_limit_bytes=2_000_000),
    )(a, b)


def solution(mesh):
    spec_col, spec_row, spec_act, spec_rep = P(None, 'model'), P('model', None), P('data', None, None), P(None, None)

    def device_step(x_in, cot_out, step_emb, w_q, w_k, w_v, w_o, w_1, w_2):
        dx, grad, *rest = run_kernel(x_in, cot_out, step_emb, (w_q, w_k, w_v, w_o, w_1, w_2), x_in.shape[0] // 2)
        a, b, dx = run_reduce(grad, dx, *rest)
        return (*run_place(a, b), dx)

    return jax.shard_map(device_step, mesh=mesh,
                         in_specs=(spec_act, spec_act, spec_rep, spec_col, spec_col, spec_col, spec_row, spec_col, spec_row),
                         out_specs=(spec_col, spec_col, spec_col, spec_row, spec_col, spec_row, spec_act),
                         check_vma=False)
```

```python
import functools

import jax
import jax.numpy as jnp
from jax import lax
from jax.experimental import pallas as pl
from jax.experimental.pallas import tpu as pltpu
from jax.sharding import PartitionSpec as P

F32, BF16 = jnp.float32, jnp.bfloat16
T, D, FF, H, E, L = 512, 512, 2048, 8, 64, 4
EPS = 1e-6
CEXP = E ** -0.5 * 1.4426950408889634
SCALE = E ** -0.5
GK0 = 0.7978845608028654
GK1 = 0.044715
R = 32
LN = 128


def dot_nn(a, b):
    return lax.dot_general(a, b, (((1,), (0,)), ((), ())), preferred_element_type=F32)


def dot_nt(a, b):
    return lax.dot_general(a, b, (((1,), (1,)), ((), ())), preferred_element_type=F32)


def rows(r, n=R):
    return pl.ds(r, n)


def wide(e):
    return jnp.concatenate([e] * (T // LN), axis=1)


def col_sum(tile_fn):
    accs = [None, None]
    for i, r in enumerate(range(0, D, R)):
        v = tile_fn(r)
        accs[i % 2] = v if accs[i % 2] is None else accs[i % 2] + v
    return jnp.sum(accs[0] + accs[1], axis=0, keepdims=True)


def rms_of(tile_fn):
    def sq(r):
        v = tile_fn(r)
        return v * v
    return lax.rsqrt(col_sum(sq) * (1.0 / D) + EPS)


def weave(*streams):
    total = max(len(s) for s in streams)
    done = [0] * len(streams)
    for t in range(total):
        for k, s in enumerate(streams):
            upto = -(-len(s) * (t + 1) // total)
            while done[k] < upto:
                s[done[k]]()
                done[k] += 1


def gelu_fwd(z):
    return z * jax.nn.sigmoid(z * (2 * GK0 + (2 * GK0 * GK1) * (z * z)))


def gelu_both(z):
    z2 = z * z
    s = jax.nn.sigmoid(z * (2 * GK0 + (2 * GK0 * GK1) * z2))
    g = z * s
    return g, s + (g * (1.0 - s)) * (2 * GK0 + (6 * GK0 * GK1) * z2)


def qrow(hd):
    return 768 * (hd // 4) + 64 * (hd % 4)


def pad_head(block, hh):
    zero = jnp.zeros_like(block)
    return jnp.concatenate([block, zero] if hh == 0 else [zero, block], axis=0)


def zip_pad(a, b):
    return [(a[i:i + 1], b[i:i + 1]) for i in range(max(len(a), len(b)))]


def max_cols(ref, cols):
    accs = [None] * 4
    for i, r in enumerate(range(0, T, 64)):
        v = ref[rows(r, 64), cols]
        accs[i % 4] = v if accs[i % 4] is None else jnp.maximum(accs[i % 4], v)
    m = jnp.maximum(jnp.maximum(accs[0], accs[1]), jnp.maximum(accs[2], accs[3]))
    return jnp.max(m, axis=0, keepdims=True)

GL, PR1, PR2 = 256, 512, 256


MESH_ID = pl.DeviceIdType.MESH
NW = 6


def other(i):
    return 1 - i


def kernel(nseq, x_ref, cot_ref, emb_ref, wq_h, wk_h, wv_h, wo_h, w1_h, w2_h,
           dx_h, grad_h, u_h, dmid_h, ctx_h, dqkv_h,
           wqkv, wo, w1, w2, wqkvt, wot, w1t, w2t, g1, g2,
           xs, qkv, ctx, ctxl, hs, zs, lse, rsc, us, ms, act, dz, dn, dmid2, dctx, dqkv2, tmp, sbuf, lcol, dcol, dxs,
           embv, ssem, sem, zsend, zrecv, gsend, grecv, xloc, xsend, xrecv):
    step = pl.program_id(0)
    mi = lax.axis_index('model')
    di = lax.axis_index('data')
    core = di % 2
    zdev = {'model': 1 - mi, 'data': di}
    cdev = {'model': mi, 'data': di + 1 - 2 * core}

    def place(k, m, r0, n):
        if k < 3:
            return wqkv.at[pl.ds(r0, n), pl.ds(768 * m + 256 * k, 256)]
        if k == 3:
            return wo.at[pl.ds(256 * m + r0, n), :]
        if k == 4:
            return w1.at[pl.ds(r0, n), pl.ds(1024 * m, 1024)]
        return w2.at[pl.ds(1024 * m + r0, n), :]

    xx, yy = (di // 2) % 2, di // 4
    dev = {'x': {'model': mi, 'data': di + 2 - 4 * xx}, 'y': {'model': mi, 'data': di + 4 - 8 * yy}, 'z': zdev, 'c': cdev}

    w_hbm = (wq_h, wk_h, wv_h, wo_h, w1_h, w2_h)
    w_rows = (512, 512, 512, 256, 512, 1024)
    groups = ((0, 1, 2), (3,), (4,), (5,))

    def region(g, far, color):
        k = groups[g][0]
        pr = w_rows[k] // 8
        py = 1 - yy if 'y' in far else yy
        px = 1 - xx if 'x' in far else xx
        r0, n = (py * 4 + px * 2 + core) * pr, pr
        if color is not None:
            r0, n = r0 + color * (pr // 2), pr // 2
        if g == 0:
            return wqkv.at[pl.ds(r0, n), pl.ds(768 * (1 - mi), 768)]
        return place(k, 1 - mi, r0, n)

    def turn(m_):
        for j in range(3):
            c = pl.ds(pl.multiple_of(768 * m_ + 256 * j, 256), 256)
            wqkvt[c, :] = wqkv[:, c].T
        c = pl.ds(pl.multiple_of(256 * m_, 256), 256)
        wot[:, c] = wo[c, :].T
        for j in range(2):
            c = pl.ds(pl.multiple_of(1024 * m_ + 512 * j, 512), 512)
            w1t[c, :] = w1[:, c].T
            w2t[:, c] = w2[c, :].T

    def load_weights():
        barrier = pltpu.get_barrier_semaphore()
        for d in 'xyzc':
            pl.semaphore_signal(barrier, inc=1, device_id=dev[d], device_id_type=MESH_ID)
        pl.semaphore_wait(barrier, 4)
        zc, local, plane, sib = {}, [], {}, []

        def hand(g, far, color, d, i):
            o = region(g, far, color)
            cp = pltpu.make_async_remote_copy(o, o, gsend.at[g, i], grecv.at[g, i], device_id=dev[d], device_id_type=MESH_ID)
            cp.start()
            return cp

        for k in range(NW):
            pr = w_rows[k] // 8
            zc[k] = pltpu.make_async_remote_copy(w_hbm[k].at[pl.ds(di * pr, pr), :], place(k, mi, di * pr, pr),
                                                 zsend.at[k], zrecv.at[k], device_id=zdev, device_id_type=MESH_ID)
            zc[k].start()
        for k in range(NW):
            local.append(pltpu.make_async_copy(w_hbm[k], place(k, mi, 0, w_rows[k]), sem.at[k]))
            local[-1].start()

        def own(g):
            for k in groups[g]:
                zc[k].wait_recv()
            for color, ab in enumerate(('xy', 'yx')):
                plane[g, color, 0] = hand(g, '', color, ab[0], 3 * color)
                plane[g, color, 1] = hand(g, '', color, ab[1], 3 * color + 1)
            sib.append(hand(g, '', None, 'c', 6))

        def forward(g):
            for color, ab in enumerate(('xy', 'yx')):
                plane[g, color, 0].wait_recv()
                plane[g, color, 2] = hand(g, ab[0], color, ab[1], 3 * color + 2)
                sib.append(hand(g, ab[0], color, 'c', 7 + 3 * color))

        def finish(g):
            for color, ab in enumerate(('xy', 'yx')):
                plane[g, color, 1].wait_recv()
                sib.append(hand(g, ab[1], color, 'c', 8 + 3 * color))
            for color in range(2):
                plane[g, color, 2].wait_recv()
                sib.append(hand(g, 'xy', color, 'c', 9 + 3 * color))

        for cp in local:
            cp.wait()
        turn(mi)
        for l_ in range(L):
            embv[l_] = jnp.broadcast_to(emb_ref[l_:l_ + 1, :].astype(F32), (LN, D)).T
        own(0)
        own(1)
        own(2)
        forward(0)
        forward(1)
        own(3)
        forward(2)
        finish(0)
        finish(1)
        forward(3)
        finish(2)
        finish(3)
        for k in range(NW):
            zc[k].wait_send()
        for cp in plane.values():
            cp.wait_send()
        for cp in sib:
            cp.wait()

    @pl.when(step == 0)
    def _():
        load_weights()
        turn(1 - mi)
        g1[...] = jnp.zeros_like(g1)
        g2[...] = jnp.zeros_like(g2)

    def stash(k, names, at=0):
        pairs = dict(ctx=(ctx.at[k % L], ctx_h), u=(us.at[k % L], u_h), dmid=(dmid2.at[at], dmid_h), dqkv=(dqkv2.at[at], dqkv_h))
        return [pltpu.make_async_copy(pairs[n][0], pairs[n][1].at[k], ssem.at[at, list(pairs).index(n)]) for n in names]

    def start_all(cs):
        for c in cs:
            c.start()

    def wait_all(cs):
        for c in cs:
            c.wait()

    @pl.when(step == 0)
    def _():
        start_all(stash(L - 1, ('dmid', 'dqkv'), 0))
        start_all(stash(L - 2, ('dmid', 'dqkv'), 1))

    xs[0] = x_ref[0].T
    half = [pl.ds(0, 256), pl.ds(256, 256)]

    def s_tile(l, cols=slice(None)):
        w = 4 if cols == slice(None) else 2
        return lambda r: xs[l, rows(r), cols].astype(F32) + jnp.concatenate([embv[l, rows(r), :]] * w, axis=1)

    def norm_into(dst, tile_fn, l, k, fresh, cols=slice(None)):
        box = {}

        def stat():
            if fresh:
                box['r'] = rms_of(tile_fn)
                rsc[l, pl.ds(k, 1), cols] = box['r']
            else:
                box['r'] = rsc[l, pl.ds(k, 1), cols]

        def put(r):
            dst[rows(r), cols] = (tile_fn(r) * box['r']).astype(BF16)

        return [stat] + [functools.partial(put, r) for r in range(0, D, R)]

    def pull_into(dst, base, tile_of, dy, l, k):
        out = []
        for cols in half:
            tile_fn = tile_of(l, cols)
            box = {}

            def stat(cols=cols, tile_fn=tile_fn, box=box):
                a = col_sum(lambda r: dy[rows(r), cols].astype(F32) * tile_fn(r)) * (1.0 / D)
                rr = rsc[l, pl.ds(k, 1), cols]
                box['r'] = rr
                box['a'] = rr * rr * rr * a

            def put(r, cols=cols, tile_fn=tile_fn, box=box):
                g = dy[rows(r), cols].astype(F32)
                dst[rows(r), cols] = (base[rows(r), cols].astype(F32) + (box['r'] * g - tile_fn(r) * box['a'])).astype(BF16)

            out += [stat] + [functools.partial(put, r) for r in range(0, D, R)]
        return out

    def run(stream):
        for f in stream:
            f()

    def h_tile(l, cols=slice(None)):
        return lambda r: hs[l, rows(r), cols].astype(F32)

    def fwd(l, carry):
        for c in range(2):
            run(norm_into(us.at[l], s_tile(l, half[c]), l, 0, True, half[c]))
        for j in range(3):
            qkv[l, pl.ds(512 * j, 512), :] = dot_nn(wqkvt[pl.ds(512 * j, 512), :], us[l]).astype(BF16)

        kps, mxs = {}, {}
        inv = {}

        def stage_a(hd):
            p, hh = divmod(hd, 2)

            def first():
                if hh == 0:
                    kps[p] = qkv[l, pl.ds(qrow(hd) + 256, 128), :].T

            def part(c):
                qp = pad_head(qkv[l, pl.ds(qrow(hd), 64), half[c]], hh)
                st = dot_nn(kps[p], qp)
                sbuf[hd % 2, :, half[c]] = st
                mxs[hd, c] = jnp.max(st.reshape(64, 8, 256), axis=0)

            return [first, lambda: part(0), lambda: part(1)]

        def stage_b(hd):
            sref, eref = sbuf.at[hd % 2], act.at[pl.ds(512 * (hd % 2), 512), :]

            def group(g):
                cols = half[g]
                mx = jnp.max(mxs[hd, g], axis=0, keepdims=True)
                accs = [None, None]
                for i, r in enumerate(range(0, T, 32)):
                    e = jnp.exp2((sref[rows(r, 32), cols] - mx) * CEXP)
                    accs[i % 2] = e if accs[i % 2] is None else accs[i % 2] + e
                    eref[rows(r, 32), cols] = e.astype(BF16)
                sm = jnp.sum(accs[0] + accs[1], axis=0, keepdims=True)
                lse[l, pl.ds(hd, 1), cols] = mx + jnp.log2(sm) * (1.0 / CEXP)
                inv[hd, g] = 1.0 / sm

            return [functools.partial(group, g) for g in range(2)]

        def stage_c(hd):
            def part(c):
                cn = dot_nn(qkv[l, pl.ds(qrow(hd) + 512, 64), :], act[pl.ds(512 * (hd % 2), 512), half[c]])
                cn = cn * inv[hd, c]
                hi = cn.astype(BF16)
                ctx[l, pl.ds(64 * hd, 64), half[c]] = hi
                ctxl[l, pl.ds(64 * hd, 64), half[c]] = (cn - hi.astype(F32)).astype(BF16)

            return [lambda: part(0), lambda: part(1)]

        run(stage_a(0))
        for hd in range(H + 1):
            mx = []
            for x_, y_ in zip_pad(stage_a(hd + 1) if hd + 1 < H else [], stage_c(hd - 1) if hd >= 1 else []):
                mx += x_ + y_
            va = stage_b(hd) if hd < H else []
            weave(mx, va)

        for c in range(2):
            o = dot_nn(wot[...], ctx[l, :, half[c]])
            for r in range(0, D, R):
                sx = xs[l, rows(r), half[c]].astype(F32) + jnp.concatenate([embv[l, rows(r), :]] * 2, axis=1)
                hs[l, rows(r), half[c]] = (sx + o[r:r + R]).astype(BF16)
        for c in range(2):
            run(norm_into(ms.at[l], h_tile(l, half[c]), l, 1, True, half[c]))

        def z_dot(j):
            def f(c):
                js = pl.ds(512 * j, 512)
                zs[l, js, half[c]] = dot_nn(w1t[js, :], ms[l, :, half[c]]).astype(BF16)
            return [lambda: f(0), lambda: f(1)]

        def gelu_stream(j):
            def f(r, c):
                act[rows(r, 64), half[c]] = gelu_fwd(zs[l, rows(r, 64), half[c]].astype(F32)).astype(BF16)
            return [functools.partial(f, r, c) for r in range(512 * j, 512 * j + 512, 64) for c in range(2)]

        @pl.when(l < L - 1)
        def _():
            run(z_dot(0))
            for j in range(4):
                weave(z_dot(j + 1) if j < 3 else [], gelu_stream(j))
            for c in range(2):
                o = dot_nn(w2t[...], act[:, half[c]])
                for r in range(0, D, R):
                    xs[l + 1, rows(r), half[c]] = (hs[l, rows(r), half[c]].astype(F32) + o[r:r + R]).astype(BF16)

        @pl.when(l == L - 1)
        def _():
            for j in range(4):
                run(z_dot(j))
                dn[:, pl.ds(128 * j, 128)] = cot_ref[0, pl.ds(128 * j, 128), :].T
        return carry

    lax.fori_loop(0, L, fwd, 0)


    def bwd(i, carry):
        l = L - 1 - i
        k = step * L + l
        dmid, dqkv = dmid2.at[i % 2], dqkv2.at[i % 2]
        wait_all(stash(k, ('dmid', 'dqkv'), i % 2))
        start_all(stash(k, ('ctx', 'u')))

        def dg_dot(j):
            def f(c):
                js = pl.ds(512 * j, 512)
                dz[js, half[c]] = dot_nn(w2[js, :], dn[:, half[c]]).astype(BF16)
            return [lambda: f(0), lambda: f(1)]

        def gelu_stream(j):
            def f(r, c):
                g, gp = gelu_both(zs[l, rows(r, 64), half[c]].astype(F32))
                act[rows(r, 64), half[c]] = g.astype(BF16)
                dz[rows(r, 64), half[c]] = (dz[rows(r, 64), half[c]].astype(F32) * gp).astype(BF16)
            return [functools.partial(f, r, c) for r in range(512 * j, 512 * j + 512, 64) for c in range(2)]

        def wgrad(j):
            js = pl.ds(512 * j, 512)

            def a(c):
                g2[js, half[c]] += dot_nt(act[js, :], dn[half[c], :])

            def b(c):
                jc = pl.ds(512 * j + 256 * c, 256)
                g1[:, jc] += dot_nt(ms[l], dz[jc, :])
            return [lambda: a(0), lambda: a(1), lambda: b(0), lambda: b(1)]

        run(dg_dot(0))
        def dm_part(k0, k1, last):
            def f(c):
                p = dot_nn(w1[:, 512 * k0:512 * k1], dz[pl.ds(512 * k0, 512 * (k1 - k0)), half[c]])
                if k0 > 0:
                    p = sbuf[0, :, half[c]] + p
                if last:
                    tmp[:, half[c]] = p.astype(BF16)
                else:
                    sbuf[0, :, half[c]] = p
            return [lambda: f(0), lambda: f(1)]

        weave(dg_dot(1) + dg_dot(2) + dg_dot(3), gelu_stream(0))
        weave(wgrad(0), gelu_stream(1))
        weave(wgrad(1) + dm_part(0, 2, False), gelu_stream(2))
        weave(wgrad(2), gelu_stream(3))
        run(dm_part(2, 4, True))
        weave(wgrad(3), pull_into(dmid, dn, h_tile, tmp, l, 1))
        for c in range(2):
            dctx[:, half[c]] = dot_nn(wo[...], dmid[:, half[c]]).astype(BF16)

        qps, dcs = {}, {}

        def column(row):
            return jnp.broadcast_to(row, (LN, T)).T

        def stage_a(hd):
            p, hh = divmod(hd, 2)
            hsl = pl.ds(64 * hd, 64)

            def first():
                if hh == 0:
                    qps[p] = qkv[l, pl.ds(qrow(hd), 128), :].T
                    dcs[p] = dctx[pl.ds(64 * hd, 128), :].T
                c = ctx[l, hsl, :].astype(F32) + ctxl[l, hsl, :].astype(F32)
                dcol[hd % 2] = column(jnp.sum(dctx[hsl, :].astype(F32) * c, axis=0, keepdims=True))
                lcol[hd % 2] = column(lse[l, pl.ds(hd, 1), :])

            def s_part(c):
                kp = pad_head(qkv[l, pl.ds(qrow(hd) + 256, 64), half[c]], hh)
                sbuf[hd % 2, :, half[c]] = dot_nn(qps[p], kp)

            def p_part(c):
                vp = pad_head(qkv[l, pl.ds(qrow(hd) + 512, 64), half[c]], hh)
                dz[pl.ds(512 * (hd % 2), 512), half[c]] = dot_nn(dcs[p], vp).astype(BF16)

            return [first] + [functools.partial(f, c) for f in (s_part, p_part) for c in range(2)]

        def merge(xs_, ys_):
            out = []
            for i in range(max(len(xs_), len(ys_))):
                out += xs_[i:i + 1] + ys_[i:i + 1]
            return out

        def stage_b(hd):
            sl = 512 * (hd % 2)

            def group(g, r0):
                cols = half[g]
                for r in range(r0, r0 + 64, 64):
                    lc = lcol[hd % 2, rows(r, 64), :]
                    dc = dcol[hd % 2, rows(r, 64), :]
                    pr = jnp.exp2((sbuf[hd % 2, rows(r, 64), cols] - jnp.concatenate([lc, lc], axis=1)) * CEXP)
                    act[rows(sl + r, 64), cols] = pr.astype(BF16)
                    dp = dz[rows(sl + r, 64), cols].astype(F32)
                    act[rows(1024 + sl + r, 64), cols] = (pr * (dp - jnp.concatenate([dc, dc], axis=1))).astype(BF16)

            return [functools.partial(group, g, r0) for r0 in range(0, T, 64) for g in range(2)]

        def stage_c(hd):
            sl = 512 * (hd % 2)
            pb = act.at[pl.ds(sl, 512), :]
            db = act.at[pl.ds(1024 + sl, 512), :]
            hsl = pl.ds(64 * hd, 64)

            def f_v(c):
                dqkv[pl.ds(qrow(hd) + 512, 64), half[c]] = dot_nn(dctx[hsl, :], pb[:, half[c]]).astype(BF16)

            def f_k(c):
                dk = dot_nn(qkv[l, pl.ds(qrow(hd), 64), :], db[:, half[c]]) * SCALE
                dqkv[pl.ds(qrow(hd) + 256, 64), half[c]] = dk.astype(BF16)

            def f_q(c):
                dq = dot_nt(qkv[l, pl.ds(qrow(hd) + 256, 64), :], db[half[c], :]) * SCALE
                dqkv[pl.ds(qrow(hd), 64), half[c]] = dq.astype(BF16)

            return [functools.partial(f, c) for f in (f_v, f_k, f_q) for c in range(2)]

        run(stage_a(0))
        for hd in range(H + 1):
            ma = stage_a(hd + 1) if hd + 1 < H else []
            mc = stage_c(hd - 1) if hd >= 1 else []
            va = stage_b(hd) if hd < H else []
            weave(merge(mc, ma), va)

        for c in range(2):
            tmp[:, half[c]] = dot_nn(wqkv[...], dqkv[:, half[c]]).astype(BF16)
        weave([], pull_into(dn, dmid, s_tile, tmp, l, 0))
        wait_all(stash(k, ('ctx', 'u')))
        start_all(stash(k, ('dmid', 'dqkv'), i % 2))
        return carry

    lax.fori_loop(0, L, bwd, 0)
    slot = step % 2

    def dx_copies(s, at):
        here = dx_h.at[mi * nseq + s]
        loc = pltpu.make_async_copy(dxs.at[at], here, xloc.at[at])
        rem = pltpu.make_async_remote_copy(dxs.at[at], here, xsend.at[at], xrecv.at[s], device_id=zdev, device_id_type=MESH_ID)
        return loc, rem

    def dx_drain(s, at):
        loc, rem = dx_copies(s, at)
        loc.wait()
        rem.wait_send()

    @pl.when(step >= 2)
    def _():
        dx_drain(step - 2, slot)

    dxs[slot] = dn[...].T
    dx_copies(step, slot)[0].start()

    @pl.when(step < nseq - 1)
    def _():
        dx_copies(step, slot)[1].start()

    @pl.when(step == nseq - 1)
    def _():
        for at in range(2):
            wait_all(stash(0, ('dmid', 'dqkv'), at))
        cps = []
        for m_ in range(2):
            for k in range(4):
                cps.append((g1.at[:, pl.ds(1024 * m_ + 256 * k, 256)], grad_h.at[m_, k]))
                cps.append((g2.at[pl.ds(1024 * m_ + 512 * (k % 2), 512), pl.ds(256 * (k // 2), 256)], grad_h.at[m_, 4 + k]))
        cps = [pltpu.make_async_copy(s, d, sem.at[i]) for i, (s, d) in enumerate(cps)]
        for c in cps:
            c.start()
        dx_drain(nseq - 2, (nseq - 2) % 2)
        dx_copies(nseq - 1, (nseq - 1) % 2)[0].wait()
        for s in range(nseq - 1):
            theirs = dx_h.at[(1 - mi) * nseq + s]
            pltpu.make_async_remote_copy(dxs.at[s % 2], theirs, xsend.at[s % 2], xrecv.at[s],
                                         device_id=zdev, device_id_type=MESH_ID).wait_recv()
        for c in cps:
            c.wait()


def run_kernel(x, cot, emb, ws, nseq):
    blk = pl.BlockSpec((1, T, D), lambda i: (lax.axis_index('model') * nseq + i, 0, 0))
    anyspec = pl.BlockSpec(memory_space=pl.ANY)
    V = pltpu.VMEM
    S = pltpu.SemaphoreType.DMA
    return pl.pallas_call(
        functools.partial(kernel, nseq),
        grid=(nseq,),
        in_specs=[blk, blk, pl.BlockSpec(memory_space=pltpu.VMEM)] + [anyspec] * NW,
        out_specs=[anyspec] * 6,
        out_shape=[jax.ShapeDtypeStruct((2 * nseq, T, D), BF16), jax.ShapeDtypeStruct((2, 8, PR1, GL), F32)]
                  + [jax.ShapeDtypeStruct((nseq * L, n, T), BF16) for n in (D, D, D, 1536)],
        scratch_shapes=[V((D, 1536), BF16), V((D, D), BF16), V((D, FF), BF16), V((FF, D), BF16),
                        V((1536, D), BF16), V((D, D), BF16), V((FF, D), BF16), V((D, FF), BF16),
                        V((D, FF), F32), V((FF, D), F32),
                        V((L, D, T), BF16), V((L, 1536, T), BF16), V((L, D, T), BF16), V((L, D, T), BF16), V((L, D, T), BF16),
                        V((L, FF, T), BF16), V((L, H, T), F32), V((L, 2, T), F32), V((L, D, T), BF16), V((L, D, T), BF16), V((FF, T), BF16),
                        V((FF, T), BF16), V((D, T), BF16), V((2, D, T), BF16), V((D, T), BF16), V((2, 1536, T), BF16), V((D, T), BF16),
                        V((2, T, T), F32), V((2, T, LN), F32), V((2, T, LN), F32), V((2, T, D), BF16),
                        V((L, D, LN), F32), S((2, 4)), S((16,)), S((NW,)), S((NW,)), S((4, 13)), S((4, 13)), S((2,)), S((2,)), S((nseq,))],
        compiler_params=pltpu.CompilerParams(dimension_semantics=("arbitrary",), vmem_limit_bytes=67_000_000, collective_id=0, has_side_effects=True),
    )(x, cot, emb, *ws)


ORDERS = ('xyz', 'yzx', 'zxy')
SPREAD = ('xy', 'yx', None)
CUTS = {PR1: ((0, 176), (176, 168), (344, 168)), PR2: ((0, 88), (88, 88), (176, 80))}
NB = 12


class Later:
    def __init__(self, make):
        self.make = make

    def start(self):
        self.make().start()

    def wait(self):
        self.make().wait()

    def wait_recv(self):
        self.make().wait_recv()

    def wait_send(self):
        self.make().wait_send()


class Summed:
    def __init__(self, pr, mine, other, load, out, rd, r1, r2, r3, sems, me, core, rdma):
        self.pr, self.mine, self.other, self.load, self.out = pr, mine, other, load, out
        self.rd, self.r1, self.r2, self.r3, self.me, self.core, self.rdma = rd, r1, r2, r3, me, core, rdma
        self.ds, self.dr, self.ls, self.ps, self.prv, self.gs, self.gr, self.cs, self.cr = sems
        self.sends, self.sib = [], []

    def piece(self, far):
        pos = {ax: (1 - v if ax in far else v) for ax, v in self.me.items()}
        return (pos['z'] * 2 + pos['y']) * 2 + pos['x']

    def kept(self, color):
        a, b, c = ORDERS[color]
        return [b + c, b, c, '']

    def go(self, ends, d):
        cp = self.rdma(ends, d)
        cp.start()
        self.sends.append(cp)
        return cp

    def rows(self, color):
        return pl.ds(*CUTS[self.pr][color])

    def add(self, dst, src, color):
        r = self.rows(color)
        dst[r, :] += src[r, :]

    def start(self):
        self.d, self.l = {}, {}
        i = 0
        for first in (True, False):
            for j in range(4):
                for color in range(3):
                    k = self.kept(color)[j]
                    e = self.piece(ORDERS[color][0] + k if first else k)
                    r = self.rows(color)
                    self.d[first, j, color] = (e, self.go(
                        lambda e=e, r=r, i=i: (self.other(e).at[r, :], self.rd.at[e, r, :], self.ds.at[i], self.dr.at[i]), 'c'))
                    if self.load is not None:
                        cp = Later(lambda e=e, r=r, i=i: pltpu.make_async_copy(self.load(e).at[r, :], self.mine(e).at[r, :], self.ls.at[i]))
                        cp.start()
                        self.l[first, j, color] = cp
                    i += 1

    def fold(self, first, j, color):
        e, cp = self.d[first, j, color]
        cp.wait_recv()
        if self.load is not None:
            self.l[first, j, color].wait()
        self.add(self.mine(e), self.rd.at[e], color)
        return e

    def phase1(self):
        self.p1, self.p2, self.p3 = {}, {}, {}
        for j in range(4):
            for color in range(3):
                e, r, i = self.fold(True, j, color), self.rows(color), 3 * j + color
                self.p1[j, color] = self.go(
                    lambda e=e, r=r, i=i, j=j: (self.mine(e).at[r, :], self.r1.at[j, r, :], self.ps.at[i], self.prv.at[i]), ORDERS[color][0])

    def fold_kept(self):
        self.e = {(j, color): self.fold(False, j, color) for j in range(4) for color in range(3)}

    def take1(self, j, color):
        self.p1[j, color].wait_recv()
        e = self.e[j, color]
        self.add(self.mine(e), self.r1.at[j], color)
        return e

    def phase2(self):
        for j in range(2):
            for color in range(3):
                e, r, i = self.take1(j, color), self.rows(color), 12 + 3 * j + color
                self.p2[j, color] = self.go(
                    lambda e=e, r=r, i=i, j=j: (self.mine(e).at[r, :], self.r2.at[j, r, :], self.ps.at[i], self.prv.at[i]), ORDERS[color][1])

    def phase3(self):
        for color in range(3):
            e, r, i = self.take1(2, color), self.rows(color), 18 + color
            self.p2[0, color].wait_recv()
            self.add(self.mine(e), self.r2.at[0], color)
            self.p3[color] = self.go(
                lambda e=e, r=r, i=i: (self.mine(e).at[r, :], self.r3.at[r, :], self.ps.at[i], self.prv.at[i]), ORDERS[color][2])
        for color in range(3):
            e = self.take1(3, color)
            self.p2[1, color].wait_recv()
            self.add(self.mine(e), self.r2.at[1], color)

    def at(self, far, r0, n):
        y = 1 - self.me['y'] if 'y' in far else self.me['y']
        x = 1 - self.me['x'] if 'x' in far else self.me['x']
        return self.out.at[(y * 2 + x) * 2 + self.core, pl.ds(r0, n), :]

    def parts(self):
        out = []
        for color, (r0, n) in enumerate(CUTS[self.pr]):
            if SPREAD[color]:
                out.append((color, r0, n, SPREAD[color]))
            else:
                h = n // 16 * 8
                out += [(color, r0, h, 'xy'), (color, r0 + h, n - h, 'yx')]
        return out

    def sibling(self, far, r0, n, i):
        cp = self.rdma(lambda: (self.at(far, r0, n), self.at(far, r0, n), self.cs.at[i], self.cr.at[i]), 'c')
        cp.start()
        self.sib.append(cp)

    def hand(self, far, r0, n, i, d):
        return self.go(lambda: (self.at(far, r0, n), self.at(far, r0, n), self.gs.at[i], self.gr.at[i]), d)

    def spread(self):
        self.g1, self.g2, self.g3 = {}, {}, {}
        for color, (r0, n) in enumerate(CUTS[self.pr]):
            self.p3[color].wait_recv()
            self.at('', r0, n)[...] = self.mine(self.e[3, color])[pl.ds(r0, n), :] + self.r3[pl.ds(r0, n), :]
            for k, (col, q0, qn, ab) in enumerate(self.parts()):
                if col == color:
                    self.g1[k] = self.hand('', q0, qn, k, ab[0])
                    self.g2[k] = self.hand('', q0, qn, 4 + k, ab[1])
        for k, (col, r0, n, ab) in enumerate(self.parts()):
            self.sibling('', r0, n, k)

    def forward(self):
        for k, (col, r0, n, ab) in enumerate(self.parts()):
            self.g1[k].wait_recv()
            self.g3[k] = self.hand(ab[0], r0, n, 8 + k, ab[1])
            self.sibling(ab[0], r0, n, 4 + k)

    def collect(self):
        for k, (col, r0, n, ab) in enumerate(self.parts()):
            self.g2[k].wait_recv()
            self.sibling(ab[1], r0, n, 8 + k)
        for k, (col, r0, n, ab) in enumerate(self.parts()):
            self.g3[k].wait_recv()
            self.sibling('xy', r0, n, 12 + k)

    def finish(self):
        for cp in self.sib:
            cp.wait()
        for cp in self.sends:
            cp.wait_send()


def reduce_kernel(g_h, dx_in, u_h, dmid_h, ctx_h, dqkv_h, out1, out2, dx, acc, full, ub, qb, cb, mb, ra, r1, r2, r3, rb, s1, s2, s3, bsem,
                  ds1, dr1, ls1, ps1, pr1, gs1, gr1, cs1, cr1, ds2, dr2, ls2, ps2, pr2, gs2, gr2, cs2, cr2, xs_, xr_):
    mi = lax.axis_index('model')
    di = lax.axis_index('data')
    core, x, y = di % 2, (di // 2) % 2, di // 4
    me = {'x': x, 'y': y, 'z': mi}
    dev = {'x': {'model': mi, 'data': di + 2 - 4 * x}, 'y': {'model': mi, 'data': di + 4 - 8 * y},
           'z': {'model': 1 - mi, 'data': di}, 'c': {'model': mi, 'data': di + 1 - 2 * core}}

    def rdma(ends, d):
        return Later(lambda: pltpu.make_async_remote_copy(*ends(), device_id=dev[d], device_id_type=MESH_ID))

    barrier = pltpu.get_barrier_semaphore()
    for d in 'xyzc':
        pl.semaphore_signal(barrier, inc=1, device_id=dev[d], device_id_type=MESH_ID)
    pl.semaphore_wait(barrier, 4)

    def g_at(e, c):
        return g_h.at[e // 4, (e % 4) * 2 + c]

    mlp = Summed(PR1, lambda e: acc.at[e], lambda e: g_at(e, 1 - core), lambda e: g_at(e, core), out1, ra, r1, r2, r3,
                 (ds1, dr1, ls1, ps1, pr1, gs1, gr1, cs1, cr1), me, core, rdma)
    att = Summed(PR2, lambda e: full.at[e * 2 + core], lambda e: full.at[e * 2 + 1 - core], None, out2, rb, s1, s2, s3,
                 (ds2, dr2, ls2, ps2, pr2, gs2, gr2, cs2, cr2), me, core, rdma)

    def fetch(i, slot):
        two = pl.ds(2 * i, 2)
        return [pltpu.make_async_copy(u_h.at[two], ub.at[slot], bsem.at[slot, 0]),
                pltpu.make_async_copy(dqkv_h.at[two], qb.at[slot], bsem.at[slot, 1])]

    def fetch_o(i, slot):
        two = pl.ds(2 * i, 2)
        return [pltpu.make_async_copy(ctx_h.at[two], cb.at[slot], bsem.at[3 + slot, 0]),
                pltpu.make_async_copy(dmid_h.at[two], mb.at[slot], bsem.at[3 + slot, 1])]

    def begin(cs):
        for c in cs:
            c.start()

    def end(cs):
        for c in cs:
            c.wait()

    mlp.start()
    for i in range(2):
        begin(fetch(i, i))
    for i in range(2):
        begin(fetch_o(i, i))
    full[...] = jnp.zeros_like(full)

    def loop(fetch_fn, products, hooks):
        def body(i, carry):
            slot = i % 3
            end(fetch_fn(i, slot))

            @pl.when(i < NB - 2)
            def _():
                begin(fetch_fn(i + 2, (i + 2) % 3))

            products(slot)
            for at, hook in hooks.items():
                pl.when(i == at)(hook)
            return carry
        lax.fori_loop(0, NB, body, 0)

    def qkv_products(slot):
        for j in range(6):
            p = None
            for k in range(2):
                d = dot_nt(ub[slot, k], qb[slot, k, pl.ds(256 * j, 256), :])
                p = d if p is None else p + d
            t = (j // 3) * 8 + 2 * (j % 3)
            full[t] += p[:256]
            full[t + 1] += p[256:]

    def o_products(slot):
        for z in range(2):
            for c in range(2):
                p = None
                for k in range(2):
                    d = dot_nt(cb[slot, k, pl.ds(256 * z, 256), :], mb[slot, k, pl.ds(256 * c, 256), :])
                    p = d if p is None else p + d
                full[z * 8 + 6 + c] += p

    nseq = dx.shape[0] // 2
    mine_x, theirs_x = dx.at[mi * nseq + nseq - 1], dx.at[(1 - mi) * nseq + nseq - 1]
    dx_out = rdma(lambda: (mine_x, mine_x, xs_.at[0], xr_.at[0]), 'z')

    loop(fetch, qkv_products, {2: mlp.phase1, 4: mlp.fold_kept, 8: mlp.phase2})
    loop(fetch_o, o_products, {6: mlp.phase3})
    att.start()
    dx_out.start()
    mlp.spread()
    att.phase1()
    att.fold_kept()
    mlp.forward()
    att.phase2()
    mlp.collect()
    att.phase3()
    att.spread()
    att.forward()
    att.collect()
    mlp.finish()
    att.finish()
    dx_out.wait_send()
    rdma(lambda: (theirs_x, theirs_x, xs_.at[0], xr_.at[0]), 'z').wait_recv()


def run_reduce(grad, dx, u, dmid, ctx, dqkv):
    V = pltpu.VMEM
    S = pltpu.SemaphoreType.DMA
    anyspec = pl.BlockSpec(memory_space=pl.ANY)
    sems = [S((24,)), S((24,)), S((24,)), S((21,)), S((21,)), S((12,)), S((12,)), S((16,)), S((16,))]
    return pl.pallas_call(
        reduce_kernel,
        in_specs=[anyspec] * 6,
        out_specs=[pl.BlockSpec(memory_space=pltpu.VMEM)] * 2 + [anyspec],
        out_shape=[jax.ShapeDtypeStruct((8, PR1, GL), F32), jax.ShapeDtypeStruct((8, PR2, GL), F32), jax.ShapeDtypeStruct(dx.shape, dx.dtype)],
        scratch_shapes=[V((8, PR1, GL), F32), V((16, PR2, GL), F32),
                        V((3, 2, D, T), BF16), V((3, 2, 1536, T), BF16), V((3, 2, D, T), BF16), V((3, 2, D, T), BF16),
                        V((8, PR1, GL), F32), V((4, PR1, GL), F32), V((2, PR1, GL), F32), V((PR1, GL), F32),
                        V((8, PR2, GL), F32), V((4, PR2, GL), F32), V((2, PR2, GL), F32), V((PR2, GL), F32), S((6, 2))]
                       + sems + sems + [S((1,)), S((1,))],
        input_output_aliases={1: 2},
        compiler_params=pltpu.CompilerParams(vmem_limit_bytes=47_000_000, collective_id=1, has_side_effects=True),
    )(grad, dx, u, dmid, ctx, dqkv)


def place_kernel(a, b, o_q, o_k, o_v, o_o, o_1, o_2, sem):
    cps = []

    def move(src, dst):
        cps.append(pltpu.make_async_copy(src, dst, sem.at[len(cps)]))
        cps[-1].start()

    for k in range(4):
        move(a.at[k], o_1.at[:, pl.ds(256 * k, 256)])
        move(a.at[4 + k], o_2.at[pl.ds(512 * (k % 2), 512), pl.ds(256 * (k // 2), 256)])
    for j, o in enumerate((o_q, o_k, o_v)):
        for i in range(2):
            move(b.at[2 * j + i], o.at[pl.ds(256 * i, 256), :])
    for k in range(2):
        move(b.at[6 + k], o_o.at[:, pl.ds(256 * k, 256)])
    for c in cps:
        c.wait()


def run_place(a, b):
    shapes = [(512, 256)] * 3 + [(256, 512), (512, 1024), (1024, 512)]
    return pl.pallas_call(
        place_kernel,
        in_specs=[pl.BlockSpec(memory_space=pltpu.VMEM)] * 2,
        out_specs=[pl.BlockSpec(memory_space=pltpu.HBM)] * 6,
        out_shape=[jax.ShapeDtypeStruct(s, F32) for s in shapes],
        scratch_shapes=[pltpu.SemaphoreType.DMA((16,))],
        compiler_params=pltpu.CompilerParams(vmem_limit_bytes=2_000_000),
    )(a, b)


def solution(mesh):
    spec_col, spec_row, spec_act, spec_rep = P(None, 'model'), P('model', None), P('data', None, None), P(None, None)

    def device_step(x_in, cot_out, step_emb, w_q, w_k, w_v, w_o, w_1, w_2):
        dx, grad, *rest = run_kernel(x_in, cot_out, step_emb, (w_q, w_k, w_v, w_o, w_1, w_2), x_in.shape[0] // 2)
        a, b, dx = run_reduce(grad, dx, *rest)
        return (*run_place(a, b), dx)

    return jax.shard_map(device_step, mesh=mesh,
                         in_specs=(spec_act, spec_act, spec_rep, spec_col, spec_col, spec_col, spec_row, spec_col, spec_row),
                         out_specs=(spec_col, spec_col, spec_col, spec_row, spec_col, spec_row, spec_act),
                         check_vma=False)
```

```python
import functools

import jax
import jax.numpy as jnp
from jax import lax
from jax.experimental import pallas as pl
from jax.experimental.pallas import tpu as pltpu
from jax.sharding import PartitionSpec as P

F32, BF16 = jnp.float32, jnp.bfloat16
T, D, FF, H, E, L = 512, 512, 2048, 8, 64, 4
EPS = 1e-6
CEXP = E ** -0.5 * 1.4426950408889634
SCALE = E ** -0.5
GK0 = 0.7978845608028654
GK1 = 0.044715
R = 32
LN = 128


def dot_nn(a, b):
    return lax.dot_general(a, b, (((1,), (0,)), ((), ())), preferred_element_type=F32)


def dot_nt(a, b):
    return lax.dot_general(a, b, (((1,), (1,)), ((), ())), preferred_element_type=F32)


def rows(r, n=R):
    return pl.ds(r, n)


def wide(e):
    return jnp.concatenate([e] * (T // LN), axis=1)


def col_sum(tile_fn):
    accs = [None, None]
    for i, r in enumerate(range(0, D, R)):
        v = tile_fn(r)
        accs[i % 2] = v if accs[i % 2] is None else accs[i % 2] + v
    return jnp.sum(accs[0] + accs[1], axis=0, keepdims=True)


def rms_of(tile_fn):
    def sq(r):
        v = tile_fn(r)
        return v * v
    return lax.rsqrt(col_sum(sq) * (1.0 / D) + EPS)


def weave(*streams):
    total = max(len(s) for s in streams)
    done = [0] * len(streams)
    for t in range(total):
        for k, s in enumerate(streams):
            upto = -(-len(s) * (t + 1) // total)
            while done[k] < upto:
                s[done[k]]()
                done[k] += 1


def gelu_fwd(z):
    return z * jax.nn.sigmoid(z * (2 * GK0 + (2 * GK0 * GK1) * (z * z)))


def gelu_both(z):
    z2 = z * z
    s = jax.nn.sigmoid(z * (2 * GK0 + (2 * GK0 * GK1) * z2))
    g = z * s
    return g, s + (g * (1.0 - s)) * (2 * GK0 + (6 * GK0 * GK1) * z2)


def qrow(hd):
    return 768 * (hd // 4) + 64 * (hd % 4)


def pad_head(block, hh):
    zero = jnp.zeros_like(block)
    return jnp.concatenate([block, zero] if hh == 0 else [zero, block], axis=0)


def zip_pad(a, b):
    return [(a[i:i + 1], b[i:i + 1]) for i in range(max(len(a), len(b)))]


def max_cols(ref, cols):
    accs = [None] * 4
    for i, r in enumerate(range(0, T, 64)):
        v = ref[rows(r, 64), cols]
        accs[i % 4] = v if accs[i % 4] is None else jnp.maximum(accs[i % 4], v)
    m = jnp.maximum(jnp.maximum(accs[0], accs[1]), jnp.maximum(accs[2], accs[3]))
    return jnp.max(m, axis=0, keepdims=True)

GL, PR1, PR2 = 256, 512, 256


MESH_ID = pl.DeviceIdType.MESH
NW = 6


def other(i):
    return 1 - i


def kernel(nseq, x_ref, cot_ref, emb_ref, wq_h, wk_h, wv_h, wo_h, w1_h, w2_h,
           dx_h, grad_h, u_h, dmid_h, ctx_h, dqkv_h,
           wqkv, wo, w1, w2, wqkvt, wot, w1t, w2t, g1, g2,
           xs, qkv, ctx, ctxl, hs, zs, lse, rsc, us, ms, act, dz, dn, dmid2, dctx, dqkv2, tmp, sbuf, lcol, dcol, dxs,
           embv, ssem, sem, zsend, zrecv, gsend, grecv, xloc, xsend, xrecv):
    step = pl.program_id(0)
    mi = lax.axis_index('model')
    di = lax.axis_index('data')
    core = di % 2
    zdev = {'model': 1 - mi, 'data': di}
    cdev = {'model': mi, 'data': di + 1 - 2 * core}

    def place(k, m, r0, n):
        if k < 3:
            return wqkv.at[pl.ds(r0, n), pl.ds(768 * m + 256 * k, 256)]
        if k == 3:
            return wo.at[pl.ds(256 * m + r0, n), :]
        if k == 4:
            return w1.at[pl.ds(r0, n), pl.ds(1024 * m, 1024)]
        return w2.at[pl.ds(1024 * m + r0, n), :]

    xx, yy = (di // 2) % 2, di // 4
    dev = {'x': {'model': mi, 'data': di + 2 - 4 * xx}, 'y': {'model': mi, 'data': di + 4 - 8 * yy}, 'z': zdev, 'c': cdev}

    w_hbm = (wq_h, wk_h, wv_h, wo_h, w1_h, w2_h)
    w_rows = (512, 512, 512, 256, 512, 1024)
    groups = ((0, 1, 2), (3,), (4,), (5,))

    def region(g, far, color):
        k = groups[g][0]
        pr = w_rows[k] // 8
        py = 1 - yy if 'y' in far else yy
        px = 1 - xx if 'x' in far else xx
        r0, n = (py * 4 + px * 2 + core) * pr, pr
        if color is not None:
            r0, n = r0 + color * (pr // 2), pr // 2
        if g == 0:
            return wqkv.at[pl.ds(r0, n), pl.ds(768 * (1 - mi), 768)]
        return place(k, 1 - mi, r0, n)

    def turn(m_):
        for j in range(3):
            c = pl.ds(pl.multiple_of(768 * m_ + 256 * j, 256), 256)
            wqkvt[c, :] = wqkv[:, c].T
        c = pl.ds(pl.multiple_of(256 * m_, 256), 256)
        wot[:, c] = wo[c, :].T
        for j in range(2):
            c = pl.ds(pl.multiple_of(1024 * m_ + 512 * j, 512), 512)
            w1t[c, :] = w1[:, c].T
            w2t[:, c] = w2[c, :].T

    def load_weights():
        barrier = pltpu.get_barrier_semaphore()
        for d in 'xyzc':
            pl.semaphore_signal(barrier, inc=1, device_id=dev[d], device_id_type=MESH_ID)
        pl.semaphore_wait(barrier, 4)
        zc, local, plane, sib = {}, [], {}, []

        def hand(g, far, color, d, i):
            o = region(g, far, color)
            cp = pltpu.make_async_remote_copy(o, o, gsend.at[g, i], grecv.at[g, i], device_id=dev[d], device_id_type=MESH_ID)
            cp.start()
            return cp

        for k in range(NW):
            pr = w_rows[k] // 8
            zc[k] = pltpu.make_async_remote_copy(w_hbm[k].at[pl.ds(di * pr, pr), :], place(k, mi, di * pr, pr),
                                                 zsend.at[k], zrecv.at[k], device_id=zdev, device_id_type=MESH_ID)
            zc[k].start()
        for k in range(NW):
            local.append(pltpu.make_async_copy(w_hbm[k], place(k, mi, 0, w_rows[k]), sem.at[k]))
            local[-1].start()

        def own(g):
            for k in groups[g]:
                zc[k].wait_recv()
            for color, ab in enumerate(('xy', 'yx')):
                plane[g, color, 0] = hand(g, '', color, ab[0], 3 * color)
                plane[g, color, 1] = hand(g, '', color, ab[1], 3 * color + 1)
            sib.append(hand(g, '', None, 'c', 6))

        def forward(g):
            for color, ab in enumerate(('xy', 'yx')):
                plane[g, color, 0].wait_recv()
                plane[g, color, 2] = hand(g, ab[0], color, ab[1], 3 * color + 2)
                sib.append(hand(g, ab[0], color, 'c', 7 + 3 * color))

        def finish(g):
            for color, ab in enumerate(('xy', 'yx')):
                plane[g, color, 1].wait_recv()
                sib.append(hand(g, ab[1], color, 'c', 8 + 3 * color))
            for color in range(2):
                plane[g, color, 2].wait_recv()
                sib.append(hand(g, 'xy', color, 'c', 9 + 3 * color))

        for cp in local:
            cp.wait()
        turn(mi)
        for l_ in range(L):
            embv[l_] = jnp.broadcast_to(emb_ref[l_:l_ + 1, :].astype(F32), (LN, D)).T
        own(0)
        own(1)
        own(2)
        forward(0)
        forward(1)
        own(3)
        forward(2)
        finish(0)
        finish(1)
        forward(3)
        finish(2)
        finish(3)
        for k in range(NW):
            zc[k].wait_send()
        for cp in plane.values():
            cp.wait_send()
        for cp in sib:
            cp.wait()

    @pl.when(step == 0)
    def _():
        load_weights()
        turn(1 - mi)
        g1[...] = jnp.zeros_like(g1)
        g2[...] = jnp.zeros_like(g2)

    def stash(k, names, at=0):
        pairs = dict(ctx=(ctx.at[k % L], ctx_h), u=(us.at[k % L], u_h), dmid=(dmid2.at[at], dmid_h), dqkv=(dqkv2.at[at], dqkv_h))
        return [pltpu.make_async_copy(pairs[n][0], pairs[n][1].at[k], ssem.at[at, list(pairs).index(n)]) for n in names]

    def start_all(cs):
        for c in cs:
            c.start()

    def wait_all(cs):
        for c in cs:
            c.wait()

    @pl.when(step == 0)
    def _():
        start_all(stash(L - 1, ('dmid', 'dqkv'), 0))
        start_all(stash(L - 2, ('dmid', 'dqkv'), 1))

    xs[0] = x_ref[0].T
    half = [pl.ds(0, 256), pl.ds(256, 256)]

    def s_tile(l, cols=slice(None)):
        w = 4 if cols == slice(None) else 2
        return lambda r: xs[l, rows(r), cols].astype(F32) + jnp.concatenate([embv[l, rows(r), :]] * w, axis=1)

    def norm_into(dst, tile_fn, l, k, fresh, cols=slice(None)):
        box = {}

        def stat():
            if fresh:
                box['r'] = rms_of(tile_fn)
                rsc[l, pl.ds(k, 1), cols] = box['r']
            else:
                box['r'] = rsc[l, pl.ds(k, 1), cols]

        def put(r):
            dst[rows(r), cols] = (tile_fn(r) * box['r']).astype(BF16)

        return [stat] + [functools.partial(put, r) for r in range(0, D, R)]

    def pull_into(dst, base, tile_of, dy, l, k):
        out = []
        for cols in half:
            tile_fn = tile_of(l, cols)
            box = {}

            def stat(cols=cols, tile_fn=tile_fn, box=box):
                a = col_sum(lambda r: dy[rows(r), cols].astype(F32) * tile_fn(r)) * (1.0 / D)
                rr = rsc[l, pl.ds(k, 1), cols]
                box['r'] = rr
                box['a'] = rr * rr * rr * a

            def put(r, cols=cols, tile_fn=tile_fn, box=box):
                g = dy[rows(r), cols].astype(F32)
                dst[rows(r), cols] = (base[rows(r), cols].astype(F32) + (box['r'] * g - tile_fn(r) * box['a'])).astype(BF16)

            out += [stat] + [functools.partial(put, r) for r in range(0, D, R)]
        return out

    def run(stream):
        for f in stream:
            f()

    def h_tile(l, cols=slice(None)):
        return lambda r: hs[l, rows(r), cols].astype(F32)

    def fwd(l, carry):
        for c in range(2):
            run(norm_into(us.at[l], s_tile(l, half[c]), l, 0, True, half[c]))
        for j in range(3):
            qkv[l, pl.ds(512 * j, 512), :] = dot_nn(wqkvt[pl.ds(512 * j, 512), :], us[l]).astype(BF16)

        kps, mxs = {}, {}
        inv = {}

        def stage_a(hd):
            p, hh = divmod(hd, 2)

            def first():
                if hh == 0:
                    kps[p] = qkv[l, pl.ds(qrow(hd) + 256, 128), :].T

            def part(c):
                qp = pad_head(qkv[l, pl.ds(qrow(hd), 64), half[c]], hh)
                st = dot_nn(kps[p], qp)
                sbuf[hd % 2, :, half[c]] = st
                mxs[hd, c] = jnp.max(st.reshape(64, 8, 256), axis=0)

            return [first, lambda: part(0), lambda: part(1)]

        def stage_b(hd):
            sref, eref = sbuf.at[hd % 2], act.at[pl.ds(512 * (hd % 2), 512), :]

            def group(g):
                cols = half[g]
                mx = jnp.max(mxs[hd, g], axis=0, keepdims=True)
                accs = [None, None]
                for i, r in enumerate(range(0, T, 16)):
                    e = jnp.exp2((sref[rows(r, 16), cols] - mx) * CEXP)
                    accs[i % 2] = e if accs[i % 2] is None else accs[i % 2] + e
                    eref[rows(r, 16), cols] = e.astype(BF16)
                sm = jnp.sum(accs[0] + accs[1], axis=0, keepdims=True)
                lse[l, pl.ds(hd, 1), cols] = mx + jnp.log2(sm) * (1.0 / CEXP)
                inv[hd, g] = 1.0 / sm

            return [functools.partial(group, g) for g in range(2)]

        def stage_c(hd):
            def part(c):
                cn = dot_nn(qkv[l, pl.ds(qrow(hd) + 512, 64), :], act[pl.ds(512 * (hd % 2), 512), half[c]])
                cn = cn * inv[hd, c]
                hi = cn.astype(BF16)
                ctx[l, pl.ds(64 * hd, 64), half[c]] = hi
                ctxl[l, pl.ds(64 * hd, 64), half[c]] = (cn - hi.astype(F32)).astype(BF16)

            return [lambda: part(0), lambda: part(1)]

        run(stage_a(0))
        for hd in range(H + 1):
            mx = []
            for x_, y_ in zip_pad(stage_a(hd + 1) if hd + 1 < H else [], stage_c(hd - 1) if hd >= 1 else []):
                mx += x_ + y_
            va = stage_b(hd) if hd < H else []
            weave(mx, va)

        for c in range(2):
            o = dot_nn(wot[...], ctx[l, :, half[c]])
            for r in range(0, D, R):
                sx = xs[l, rows(r), half[c]].astype(F32) + jnp.concatenate([embv[l, rows(r), :]] * 2, axis=1)
                hs[l, rows(r), half[c]] = (sx + o[r:r + R]).astype(BF16)
        for c in range(2):
            run(norm_into(ms.at[l], h_tile(l, half[c]), l, 1, True, half[c]))

        def z_dot(j):
            def f(c):
                js = pl.ds(512 * j, 512)
                zs[l, js, half[c]] = dot_nn(w1t[js, :], ms[l, :, half[c]]).astype(BF16)
            return [lambda: f(0), lambda: f(1)]

        def gelu_stream(j):
            def f(r, c):
                act[rows(r, 64), half[c]] = gelu_fwd(zs[l, rows(r, 64), half[c]].astype(F32)).astype(BF16)
            return [functools.partial(f, r, c) for r in range(512 * j, 512 * j + 512, 64) for c in range(2)]

        @pl.when(l < L - 1)
        def _():
            run(z_dot(0))
            for j in range(4):
                weave(z_dot(j + 1) if j < 3 else [], gelu_stream(j))
            for c in range(2):
                o = dot_nn(w2t[...], act[:, half[c]])
                for r in range(0, D, R):
                    xs[l + 1, rows(r), half[c]] = (hs[l, rows(r), half[c]].astype(F32) + o[r:r + R]).astype(BF16)

        @pl.when(l == L - 1)
        def _():
            for j in range(4):
                run(z_dot(j))
                dn[:, pl.ds(128 * j, 128)] = cot_ref[0, pl.ds(128 * j, 128), :].T
        return carry

    lax.fori_loop(0, L, fwd, 0)


    def bwd(i, carry):
        l = L - 1 - i
        k = step * L + l
        dmid, dqkv = dmid2.at[i % 2], dqkv2.at[i % 2]
        wait_all(stash(k, ('dmid', 'dqkv'), i % 2))
        start_all(stash(k, ('ctx', 'u')))

        def dg_dot(j):
            def f(c):
                js = pl.ds(512 * j, 512)
                dz[js, half[c]] = dot_nn(w2[js, :], dn[:, half[c]]).astype(BF16)
            return [lambda: f(0), lambda: f(1)]

        def gelu_stream(j):
            def f(r, c):
                g, gp = gelu_both(zs[l, rows(r, 64), half[c]].astype(F32))
                act[rows(r, 64), half[c]] = g.astype(BF16)
                dz[rows(r, 64), half[c]] = (dz[rows(r, 64), half[c]].astype(F32) * gp).astype(BF16)
            return [functools.partial(f, r, c) for r in range(512 * j, 512 * j + 512, 64) for c in range(2)]

        def wgrad(j):
            js = pl.ds(512 * j, 512)

            def a(c):
                g2[js, half[c]] += dot_nt(act[js, :], dn[half[c], :])

            def b(c):
                jc = pl.ds(512 * j + 256 * c, 256)
                g1[:, jc] += dot_nt(ms[l], dz[jc, :])
            return [lambda: a(0), lambda: a(1), lambda: b(0), lambda: b(1)]

        run(dg_dot(0))
        def dm_part(k0, k1, last):
            def f(c):
                p = dot_nn(w1[:, 512 * k0:512 * k1], dz[pl.ds(512 * k0, 512 * (k1 - k0)), half[c]])
                if k0 > 0:
                    p = sbuf[0, :, half[c]] + p
                if last:
                    tmp[:, half[c]] = p.astype(BF16)
                else:
                    sbuf[0, :, half[c]] = p
            return [lambda: f(0), lambda: f(1)]

        weave(dg_dot(1) + dg_dot(2) + dg_dot(3), gelu_stream(0))
        weave(wgrad(0), gelu_stream(1))
        weave(wgrad(1) + dm_part(0, 2, False), gelu_stream(2))
        weave(wgrad(2), gelu_stream(3))
        run(dm_part(2, 4, True))
        weave(wgrad(3), pull_into(dmid, dn, h_tile, tmp, l, 1))
        for c in range(2):
            dctx[:, half[c]] = dot_nn(wo[...], dmid[:, half[c]]).astype(BF16)

        qps, dcs = {}, {}

        def column(row):
            return jnp.broadcast_to(row, (LN, T)).T

        def stage_a(hd):
            p, hh = divmod(hd, 2)
            hsl = pl.ds(64 * hd, 64)

            def first():
                if hh == 0:
                    qps[p] = qkv[l, pl.ds(qrow(hd), 128), :].T
                    dcs[p] = dctx[pl.ds(64 * hd, 128), :].T
                c = ctx[l, hsl, :].astype(F32) + ctxl[l, hsl, :].astype(F32)
                dcol[hd % 2] = column(jnp.sum(dctx[hsl, :].astype(F32) * c, axis=0, keepdims=True))
                lcol[hd % 2] = column(lse[l, pl.ds(hd, 1), :])

            def s_part(c):
                kp = pad_head(qkv[l, pl.ds(qrow(hd) + 256, 64), half[c]], hh)
                sbuf[hd % 2, :, half[c]] = dot_nn(qps[p], kp)

            def p_part(c):
                vp = pad_head(qkv[l, pl.ds(qrow(hd) + 512, 64), half[c]], hh)
                dz[pl.ds(512 * (hd % 2), 512), half[c]] = dot_nn(dcs[p], vp).astype(BF16)

            return [first] + [functools.partial(f, c) for f in (s_part, p_part) for c in range(2)]

        def merge(xs_, ys_):
            out = []
            for i in range(max(len(xs_), len(ys_))):
                out += xs_[i:i + 1] + ys_[i:i + 1]
            return out

        def stage_b(hd):
            sl = 512 * (hd % 2)

            def group(g, r0):
                cols = half[g]
                for r in range(r0, r0 + 64, 64):
                    lc = lcol[hd % 2, rows(r, 64), :]
                    dc = dcol[hd % 2, rows(r, 64), :]
                    pr = jnp.exp2((sbuf[hd % 2, rows(r, 64), cols] - jnp.concatenate([lc, lc], axis=1)) * CEXP)
                    act[rows(sl + r, 64), cols] = pr.astype(BF16)
                    dp = dz[rows(sl + r, 64), cols].astype(F32)
                    act[rows(1024 + sl + r, 64), cols] = (pr * (dp - jnp.concatenate([dc, dc], axis=1))).astype(BF16)

            return [functools.partial(group, g, r0) for r0 in range(0, T, 64) for g in range(2)]

        def stage_c(hd):
            sl = 512 * (hd % 2)
            pb = act.at[pl.ds(sl, 512), :]
            db = act.at[pl.ds(1024 + sl, 512), :]
            hsl = pl.ds(64 * hd, 64)

            def f_v(c):
                dqkv[pl.ds(qrow(hd) + 512, 64), half[c]] = dot_nn(dctx[hsl, :], pb[:, half[c]]).astype(BF16)

            def f_k(c):
                dk = dot_nn(qkv[l, pl.ds(qrow(hd), 64), :], db[:, half[c]]) * SCALE
                dqkv[pl.ds(qrow(hd) + 256, 64), half[c]] = dk.astype(BF16)

            def f_q(c):
                dq = dot_nt(qkv[l, pl.ds(qrow(hd) + 256, 64), :], db[half[c], :]) * SCALE
                dqkv[pl.ds(qrow(hd), 64), half[c]] = dq.astype(BF16)

            return [functools.partial(f, c) for f in (f_v, f_k, f_q) for c in range(2)]

        run(stage_a(0))
        for hd in range(H + 1):
            ma = stage_a(hd + 1) if hd + 1 < H else []
            mc = stage_c(hd - 1) if hd >= 1 else []
            va = stage_b(hd) if hd < H else []
            weave(merge(mc, ma), va)

        for c in range(2):
            tmp[:, half[c]] = dot_nn(wqkv[...], dqkv[:, half[c]]).astype(BF16)
        weave([], pull_into(dn, dmid, s_tile, tmp, l, 0))
        wait_all(stash(k, ('ctx', 'u')))
        start_all(stash(k, ('dmid', 'dqkv'), i % 2))
        return carry

    lax.fori_loop(0, L, bwd, 0)
    slot = step % 2

    def dx_copies(s, at):
        here = dx_h.at[mi * nseq + s]
        loc = pltpu.make_async_copy(dxs.at[at], here, xloc.at[at])
        rem = pltpu.make_async_remote_copy(dxs.at[at], here, xsend.at[at], xrecv.at[s], device_id=zdev, device_id_type=MESH_ID)
        return loc, rem

    def dx_drain(s, at):
        loc, rem = dx_copies(s, at)
        loc.wait()
        rem.wait_send()

    @pl.when(step >= 2)
    def _():
        dx_drain(step - 2, slot)

    dxs[slot] = dn[...].T
    dx_copies(step, slot)[0].start()

    @pl.when(step < nseq - 1)
    def _():
        dx_copies(step, slot)[1].start()

    @pl.when(step == nseq - 1)
    def _():
        for at in range(2):
            wait_all(stash(0, ('dmid', 'dqkv'), at))
        cps = []
        for m_ in range(2):
            for k in range(4):
                cps.append((g1.at[:, pl.ds(1024 * m_ + 256 * k, 256)], grad_h.at[m_, k]))
                cps.append((g2.at[pl.ds(1024 * m_ + 512 * (k % 2), 512), pl.ds(256 * (k // 2), 256)], grad_h.at[m_, 4 + k]))
        cps = [pltpu.make_async_copy(s, d, sem.at[i]) for i, (s, d) in enumerate(cps)]
        for c in cps:
            c.start()
        dx_drain(nseq - 2, (nseq - 2) % 2)
        dx_copies(nseq - 1, (nseq - 1) % 2)[0].wait()
        for s in range(nseq - 1):
            theirs = dx_h.at[(1 - mi) * nseq + s]
            pltpu.make_async_remote_copy(dxs.at[s % 2], theirs, xsend.at[s % 2], xrecv.at[s],
                                         device_id=zdev, device_id_type=MESH_ID).wait_recv()
        for c in cps:
            c.wait()


def run_kernel(x, cot, emb, ws, nseq):
    blk = pl.BlockSpec((1, T, D), lambda i: (lax.axis_index('model') * nseq + i, 0, 0))
    anyspec = pl.BlockSpec(memory_space=pl.ANY)
    V = pltpu.VMEM
    S = pltpu.SemaphoreType.DMA
    return pl.pallas_call(
        functools.partial(kernel, nseq),
        grid=(nseq,),
        in_specs=[blk, blk, pl.BlockSpec(memory_space=pltpu.VMEM)] + [anyspec] * NW,
        out_specs=[anyspec] * 6,
        out_shape=[jax.ShapeDtypeStruct((2 * nseq, T, D), BF16), jax.ShapeDtypeStruct((2, 8, PR1, GL), F32)]
                  + [jax.ShapeDtypeStruct((nseq * L, n, T), BF16) for n in (D, D, D, 1536)],
        scratch_shapes=[V((D, 1536), BF16), V((D, D), BF16), V((D, FF), BF16), V((FF, D), BF16),
                        V((1536, D), BF16), V((D, D), BF16), V((FF, D), BF16), V((D, FF), BF16),
                        V((D, FF), F32), V((FF, D), F32),
                        V((L, D, T), BF16), V((L, 1536, T), BF16), V((L, D, T), BF16), V((L, D, T), BF16), V((L, D, T), BF16),
                        V((L, FF, T), BF16), V((L, H, T), F32), V((L, 2, T), F32), V((L, D, T), BF16), V((L, D, T), BF16), V((FF, T), BF16),
                        V((FF, T), BF16), V((D, T), BF16), V((2, D, T), BF16), V((D, T), BF16), V((2, 1536, T), BF16), V((D, T), BF16),
                        V((2, T, T), F32), V((2, T, LN), F32), V((2, T, LN), F32), V((2, T, D), BF16),
                        V((L, D, LN), F32), S((2, 4)), S((16,)), S((NW,)), S((NW,)), S((4, 13)), S((4, 13)), S((2,)), S((2,)), S((nseq,))],
        compiler_params=pltpu.CompilerParams(dimension_semantics=("arbitrary",), vmem_limit_bytes=67_000_000, collective_id=0, has_side_effects=True),
    )(x, cot, emb, *ws)


ORDERS = ('xyz', 'yzx', 'zxy')
SPREAD = ('xy', 'yx', None)
CUTS = {PR1: ((0, 176), (176, 168), (344, 168)), PR2: ((0, 88), (88, 88), (176, 80))}
NB = 12


class Later:
    def __init__(self, make):
        self.make = make

    def start(self):
        self.make().start()

    def wait(self):
        self.make().wait()

    def wait_recv(self):
        self.make().wait_recv()

    def wait_send(self):
        self.make().wait_send()


class Summed:
    def __init__(self, pr, mine, other, load, out, rd, r1, r2, r3, sems, me, core, rdma):
        self.pr, self.mine, self.other, self.load, self.out = pr, mine, other, load, out
        self.rd, self.r1, self.r2, self.r3, self.me, self.core, self.rdma = rd, r1, r2, r3, me, core, rdma
        self.ds, self.dr, self.ls, self.ps, self.prv, self.gs, self.gr, self.cs, self.cr = sems
        self.sends, self.sib = [], []

    def piece(self, far):
        pos = {ax: (1 - v if ax in far else v) for ax, v in self.me.items()}
        return (pos['z'] * 2 + pos['y']) * 2 + pos['x']

    def kept(self, color):
        a, b, c = ORDERS[color]
        return [b + c, b, c, '']

    def go(self, ends, d):
        cp = self.rdma(ends, d)
        cp.start()
        self.sends.append(cp)
        return cp

    def rows(self, color):
        return pl.ds(*CUTS[self.pr][color])

    def add(self, dst, src, color):
        r = self.rows(color)
        dst[r, :] += src[r, :]

    def start(self):
        self.d, self.l = {}, {}
        i = 0
        for first in (True, False):
            for j in range(4):
                for color in range(3):
                    k = self.kept(color)[j]
                    e = self.piece(ORDERS[color][0] + k if first else k)
                    r = self.rows(color)
                    self.d[first, j, color] = (e, self.go(
                        lambda e=e, r=r, i=i: (self.other(e).at[r, :], self.rd.at[e, r, :], self.ds.at[i], self.dr.at[i]), 'c'))
                    if self.load is not None:
                        cp = Later(lambda e=e, r=r, i=i: pltpu.make_async_copy(self.load(e).at[r, :], self.mine(e).at[r, :], self.ls.at[i]))
                        cp.start()
                        self.l[first, j, color] = cp
                    i += 1

    def fold(self, first, j, color):
        e, cp = self.d[first, j, color]
        cp.wait_recv()
        if self.load is not None:
            self.l[first, j, color].wait()
        self.add(self.mine(e), self.rd.at[e], color)
        return e

    def phase1(self):
        self.p1, self.p2, self.p3 = {}, {}, {}
        for j in range(4):
            for color in range(3):
                e, r, i = self.fold(True, j, color), self.rows(color), 3 * j + color
                self.p1[j, color] = self.go(
                    lambda e=e, r=r, i=i, j=j: (self.mine(e).at[r, :], self.r1.at[j, r, :], self.ps.at[i], self.prv.at[i]), ORDERS[color][0])

    def fold_kept(self):
        self.e = {(j, color): self.fold(False, j, color) for j in range(4) for color in range(3)}

    def take1(self, j, color):
        self.p1[j, color].wait_recv()
        e = self.e[j, color]
        self.add(self.mine(e), self.r1.at[j], color)
        return e

    def phase2(self):
        for j in range(2):
            for color in range(3):
                e, r, i = self.take1(j, color), self.rows(color), 12 + 3 * j + color
                self.p2[j, color] = self.go(
                    lambda e=e, r=r, i=i, j=j: (self.mine(e).at[r, :], self.r2.at[j, r, :], self.ps.at[i], self.prv.at[i]), ORDERS[color][1])

    def phase3(self):
        for color in range(3):
            e, r, i = self.take1(2, color), self.rows(color), 18 + color
            self.p2[0, color].wait_recv()
            self.add(self.mine(e), self.r2.at[0], color)
            self.p3[color] = self.go(
                lambda e=e, r=r, i=i: (self.mine(e).at[r, :], self.r3.at[r, :], self.ps.at[i], self.prv.at[i]), ORDERS[color][2])
        for color in range(3):
            e = self.take1(3, color)
            self.p2[1, color].wait_recv()
            self.add(self.mine(e), self.r2.at[1], color)

    def at(self, far, r0, n):
        y = 1 - self.me['y'] if 'y' in far else self.me['y']
        x = 1 - self.me['x'] if 'x' in far else self.me['x']
        return self.out.at[(y * 2 + x) * 2 + self.core, pl.ds(r0, n), :]

    def parts(self):
        out = []
        for color, (r0, n) in enumerate(CUTS[self.pr]):
            if SPREAD[color]:
                out.append((color, r0, n, SPREAD[color]))
            else:
                h = n // 16 * 8
                out += [(color, r0, h, 'xy'), (color, r0 + h, n - h, 'yx')]
        return out

    def sibling(self, far, r0, n, i):
        cp = self.rdma(lambda: (self.at(far, r0, n), self.at(far, r0, n), self.cs.at[i], self.cr.at[i]), 'c')
        cp.start()
        self.sib.append(cp)

    def hand(self, far, r0, n, i, d):
        return self.go(lambda: (self.at(far, r0, n), self.at(far, r0, n), self.gs.at[i], self.gr.at[i]), d)

    def spread(self):
        self.g1, self.g2, self.g3 = {}, {}, {}
        for color, (r0, n) in enumerate(CUTS[self.pr]):
            self.p3[color].wait_recv()
            self.at('', r0, n)[...] = self.mine(self.e[3, color])[pl.ds(r0, n), :] + self.r3[pl.ds(r0, n), :]
            for k, (col, q0, qn, ab) in enumerate(self.parts()):
                if col == color:
                    self.g1[k] = self.hand('', q0, qn, k, ab[0])
                    self.g2[k] = self.hand('', q0, qn, 4 + k, ab[1])
        for k, (col, r0, n, ab) in enumerate(self.parts()):
            self.sibling('', r0, n, k)

    def forward(self):
        for k, (col, r0, n, ab) in enumerate(self.parts()):
            self.g1[k].wait_recv()
            self.g3[k] = self.hand(ab[0], r0, n, 8 + k, ab[1])
            self.sibling(ab[0], r0, n, 4 + k)

    def collect(self):
        for k, (col, r0, n, ab) in enumerate(self.parts()):
            self.g2[k].wait_recv()
            self.sibling(ab[1], r0, n, 8 + k)
        for k, (col, r0, n, ab) in enumerate(self.parts()):
            self.g3[k].wait_recv()
            self.sibling('xy', r0, n, 12 + k)

    def finish(self):
        for cp in self.sib:
            cp.wait()
        for cp in self.sends:
            cp.wait_send()


def reduce_kernel(g_h, dx_in, u_h, dmid_h, ctx_h, dqkv_h, out1, out2, dx, acc, full, ub, qb, cb, mb, ra, r1, r2, r3, rb, s1, s2, s3, bsem,
                  ds1, dr1, ls1, ps1, pr1, gs1, gr1, cs1, cr1, ds2, dr2, ls2, ps2, pr2, gs2, gr2, cs2, cr2, xs_, xr_):
    mi = lax.axis_index('model')
    di = lax.axis_index('data')
    core, x, y = di % 2, (di // 2) % 2, di // 4
    me = {'x': x, 'y': y, 'z': mi}
    dev = {'x': {'model': mi, 'data': di + 2 - 4 * x}, 'y': {'model': mi, 'data': di + 4 - 8 * y},
           'z': {'model': 1 - mi, 'data': di}, 'c': {'model': mi, 'data': di + 1 - 2 * core}}

    def rdma(ends, d):
        return Later(lambda: pltpu.make_async_remote_copy(*ends(), device_id=dev[d], device_id_type=MESH_ID))

    barrier = pltpu.get_barrier_semaphore()
    for d in 'xyzc':
        pl.semaphore_signal(barrier, inc=1, device_id=dev[d], device_id_type=MESH_ID)
    pl.semaphore_wait(barrier, 4)

    def g_at(e, c):
        return g_h.at[e // 4, (e % 4) * 2 + c]

    mlp = Summed(PR1, lambda e: acc.at[e], lambda e: g_at(e, 1 - core), lambda e: g_at(e, core), out1, ra, r1, r2, r3,
                 (ds1, dr1, ls1, ps1, pr1, gs1, gr1, cs1, cr1), me, core, rdma)
    att = Summed(PR2, lambda e: full.at[e * 2 + core], lambda e: full.at[e * 2 + 1 - core], None, out2, rb, s1, s2, s3,
                 (ds2, dr2, ls2, ps2, pr2, gs2, gr2, cs2, cr2), me, core, rdma)

    def fetch(i, slot):
        two = pl.ds(2 * i, 2)
        return [pltpu.make_async_copy(u_h.at[two], ub.at[slot], bsem.at[slot, 0]),
                pltpu.make_async_copy(dqkv_h.at[two], qb.at[slot], bsem.at[slot, 1])]

    def fetch_o(i, slot):
        two = pl.ds(2 * i, 2)
        return [pltpu.make_async_copy(ctx_h.at[two], cb.at[slot], bsem.at[3 + slot, 0]),
                pltpu.make_async_copy(dmid_h.at[two], mb.at[slot], bsem.at[3 + slot, 1])]

    def begin(cs):
        for c in cs:
            c.start()

    def end(cs):
        for c in cs:
            c.wait()

    mlp.start()
    for i in range(2):
        begin(fetch(i, i))
    for i in range(2):
        begin(fetch_o(i, i))
    full[...] = jnp.zeros_like(full)

    def loop(fetch_fn, products, hooks):
        def body(i, carry):
            slot = i % 3
            end(fetch_fn(i, slot))

            @pl.when(i < NB - 2)
            def _():
                begin(fetch_fn(i + 2, (i + 2) % 3))

            products(slot)
            for at, hook in hooks.items():
                pl.when(i == at)(hook)
            return carry
        lax.fori_loop(0, NB, body, 0)

    def qkv_products(slot):
        for j in range(6):
            p = None
            for k in range(2):
                d = dot_nt(ub[slot, k], qb[slot, k, pl.ds(256 * j, 256), :])
                p = d if p is None else p + d
            t = (j // 3) * 8 + 2 * (j % 3)
            full[t] += p[:256]
            full[t + 1] += p[256:]

    def o_products(slot):
        for z in range(2):
            for c in range(2):
                p = None
                for k in range(2):
                    d = dot_nt(cb[slot, k, pl.ds(256 * z, 256), :], mb[slot, k, pl.ds(256 * c, 256), :])
                    p = d if p is None else p + d
                full[z * 8 + 6 + c] += p

    nseq = dx.shape[0] // 2
    mine_x, theirs_x = dx.at[mi * nseq + nseq - 1], dx.at[(1 - mi) * nseq + nseq - 1]
    dx_out = rdma(lambda: (mine_x, mine_x, xs_.at[0], xr_.at[0]), 'z')

    loop(fetch, qkv_products, {2: mlp.phase1, 4: mlp.fold_kept, 8: mlp.phase2})
    loop(fetch_o, o_products, {6: mlp.phase3})
    att.start()
    dx_out.start()
    mlp.spread()
    att.phase1()
    att.fold_kept()
    mlp.forward()
    att.phase2()
    mlp.collect()
    att.phase3()
    att.spread()
    att.forward()
    att.collect()
    mlp.finish()
    att.finish()
    dx_out.wait_send()
    rdma(lambda: (theirs_x, theirs_x, xs_.at[0], xr_.at[0]), 'z').wait_recv()


def run_reduce(grad, dx, u, dmid, ctx, dqkv):
    V = pltpu.VMEM
    S = pltpu.SemaphoreType.DMA
    anyspec = pl.BlockSpec(memory_space=pl.ANY)
    sems = [S((24,)), S((24,)), S((24,)), S((21,)), S((21,)), S((12,)), S((12,)), S((16,)), S((16,))]
    return pl.pallas_call(
        reduce_kernel,
        in_specs=[anyspec] * 6,
        out_specs=[pl.BlockSpec(memory_space=pltpu.VMEM)] * 2 + [anyspec],
        out_shape=[jax.ShapeDtypeStruct((8, PR1, GL), F32), jax.ShapeDtypeStruct((8, PR2, GL), F32), jax.ShapeDtypeStruct(dx.shape, dx.dtype)],
        scratch_shapes=[V((8, PR1, GL), F32), V((16, PR2, GL), F32),
                        V((3, 2, D, T), BF16), V((3, 2, 1536, T), BF16), V((3, 2, D, T), BF16), V((3, 2, D, T), BF16),
                        V((8, PR1, GL), F32), V((4, PR1, GL), F32), V((2, PR1, GL), F32), V((PR1, GL), F32),
                        V((8, PR2, GL), F32), V((4, PR2, GL), F32), V((2, PR2, GL), F32), V((PR2, GL), F32), S((6, 2))]
                       + sems + sems + [S((1,)), S((1,))],
        input_output_aliases={1: 2},
        compiler_params=pltpu.CompilerParams(vmem_limit_bytes=47_000_000, collective_id=1, has_side_effects=True),
    )(grad, dx, u, dmid, ctx, dqkv)


def place_kernel(a, b, o_q, o_k, o_v, o_o, o_1, o_2, sem):
    cps = []

    def move(src, dst):
        cps.append(pltpu.make_async_copy(src, dst, sem.at[len(cps)]))
        cps[-1].start()

    for k in range(4):
        move(a.at[k], o_1.at[:, pl.ds(256 * k, 256)])
        move(a.at[4 + k], o_2.at[pl.ds(512 * (k % 2), 512), pl.ds(256 * (k // 2), 256)])
    for j, o in enumerate((o_q, o_k, o_v)):
        for i in range(2):
            move(b.at[2 * j + i], o.at[pl.ds(256 * i, 256), :])
    for k in range(2):
        move(b.at[6 + k], o_o.at[:, pl.ds(256 * k, 256)])
    for c in cps:
        c.wait()


def run_place(a, b):
    shapes = [(512, 256)] * 3 + [(256, 512), (512, 1024), (1024, 512)]
    return pl.pallas_call(
        place_kernel,
        in_specs=[pl.BlockSpec(memory_space=pltpu.VMEM)] * 2,
        out_specs=[pl.BlockSpec(memory_space=pltpu.HBM)] * 6,
        out_shape=[jax.ShapeDtypeStruct(s, F32) for s in shapes],
        scratch_shapes=[pltpu.SemaphoreType.DMA((16,))],
        compiler_params=pltpu.CompilerParams(vmem_limit_bytes=2_000_000),
    )(a, b)


def solution(mesh):
    spec_col, spec_row, spec_act, spec_rep = P(None, 'model'), P('model', None), P('data', None, None), P(None, None)

    def device_step(x_in, cot_out, step_emb, w_q, w_k, w_v, w_o, w_1, w_2):
        dx, grad, *rest = run_kernel(x_in, cot_out, step_emb, (w_q, w_k, w_v, w_o, w_1, w_2), x_in.shape[0] // 2)
        a, b, dx = run_reduce(grad, dx, *rest)
        return (*run_place(a, b), dx)

    return jax.shard_map(device_step, mesh=mesh,
                         in_specs=(spec_act, spec_act, spec_rep, spec_col, spec_col, spec_col, spec_row, spec_col, spec_row),
                         out_specs=(spec_col, spec_col, spec_col, spec_row, spec_col, spec_row, spec_act),
                         check_vma=False)
```
